32 devices in a mesh: head: 2 (over x), blk: 16 (over z, y, core).
Axes of the slice: x: 2, y: 2, z: 4, core: 2. Of those that a mesh axis runs over, the one named last changes fastest.
Arguments:
- hidden: bfloat16 [2, 2048, 1024], P(None, ('head', 'blk')), may hold values from -3 to 3
- pos_ids: int32 [2, 2048], P(None, ('head', 'blk')), may hold values from 0 to 8191
- type_ids: int32 [2, 2048], P(None, ('head', 'blk')), may hold values from 0 to 1, as said below
- cotangent: bfloat16 [2, 2048, 1024], P(None, ('head', 'blk')), may hold values from -6 to 6
- pos_table: bfloat16 [8192, 1024], P('blk'), may hold values from -4 to 4
- type_table: bfloat16 [2, 1024], P(None, 'blk'), may hold values from -4 to 4
- query_key_value_weight: bfloat16 [1024, 3072], P('blk'), may hold values from -0.1875 to 0.1875
- attention_output_weight: bfloat16 [1024, 1024], P('blk'), may hold values from -6 to 6
- up_projection_weight: bfloat16 [1024, 4096], P('blk'), may hold values from -0.1875 to 0.1875
- down_projection_weight: bfloat16 [4096, 1024], P('blk'), may hold values from -0.09375 to 0.09375
- up_projection_bias: bfloat16 [4096], P('blk'), may hold values from -4 to 4
- norm_gains: bfloat16 [2, 1024], P(None, 'blk'), may hold values from 0.5 to 1.5
- biases: bfloat16 [6, 1024], P(None, 'blk'), may hold values from -4 to 4
Outputs:
- layer_out: bfloat16 [2, 2048, 1024], P(None, ('head', 'blk'))
- grad_hidden: float32 [2, 2048, 1024], P(None, ('head', 'blk'))
- grad_pos_table: float32 [8192, 1024], P('blk')
- grad_type_table: float32 [2, 1024], P(None, 'blk')
- grad_qkv_weight: float32 [1024, 3072], P('blk')
- grad_out_weight: float32 [1024, 1024], P('blk')
- grad_up_weight: float32 [1024, 4096], P('blk')
- grad_down_weight: float32 [4096, 1024], P('blk')
- grad_up_bias: float32 [4096], P('blk')
- grad_norm_gains: float32 [2, 1024], P(None, 'blk')
- grad_biases: float32 [6, 1024], P(None, 'blk')
The draws below stay inside these ranges and needn't reach their ends.
Inputs may be any that keep to these rules, and one draw needn't show every extreme that they name: `type_ids`: in each sequence the ids are 0 up to some token and 1 from it on, both present.
All inputs are finite; a program needn't handle non-finite values.
Results may differ from the reference program's by a relative error of at most 0.03.
Values may be sent and summed in bfloat16 or wider, within the bound.
A program may use at most 256 MiB of HBM per device.

```python
import math
import jax
import jax.numpy as jnp
from jax import lax

D = 1024
HEADS = 16
FF = 4096
MAXPOS = 8192
SEQS = 2
LEN = 2048


def draw_hidden(key, part):
    first_key = jax.random.fold_in(jax.random.fold_in(key, 11), 0)
    base = jnp.clip(jax.random.normal(first_key, (SEQS, LEN, D), jnp.float32), -3.0, 3.0)
    return base.astype(jnp.bfloat16)


def draw_pos_ids(key, part):
    drawn = jax.random.randint(jax.random.fold_in(key, 23), (SEQS, LEN), 0, MAXPOS).astype(jnp.int32)
    row_index = jnp.arange(SEQS, dtype=jnp.int32)[:, None]
    along = jnp.arange(LEN, dtype=jnp.int32)[None, :]
    drawn = jnp.where((row_index == 0) & (along == 0), MAXPOS - 1, drawn)
    drawn = jnp.where((row_index == 0) & (along == 1), 0, drawn)
    return drawn.astype(jnp.int32)


def draw_type_ids(key, part):
    split_at = jax.random.randint(jax.random.fold_in(key, 37), (SEQS, 1), 1, LEN).astype(jnp.int32)
    along = jnp.arange(LEN, dtype=jnp.int32)[None, :]
    return (along >= split_at).astype(jnp.int32)


def level_of(own_key, shape, shards, least, high):
    def one(dim, parts):
        heights = jax.random.uniform(jax.random.fold_in(jax.random.fold_in(own_key, 6), dim), (parts,), jnp.float32, least / len(shards), high / len(shards))
        return jnp.repeat(jnp.exp(heights), shape[dim] // parts).reshape((-1,) + (1,) * (len(shape) - dim - 1))

    factor_of = one(*shards[0])
    for cut in shards[1:]:
        factor_of = factor_of * one(*cut)
    return factor_of


def noise(rng, shape, scale, limit, shards=(), kind=jnp.bfloat16):
    loudness = level_of(rng, shape, shards, -0.22, 0.18) if shards else 1.0
    array = jax.random.normal(rng, shape, jnp.float32) * scale * loudness
    return jnp.minimum(jnp.maximum(array, -limit), limit).astype(kind)


def setup_inputs(seed: int = 0) -> dict:
    streams_of = jax.random.split(jax.random.key(seed), 14)
    hidden = draw_hidden(jax.random.fold_in(streams_of[13], 71), 0)
    pos_ids = draw_pos_ids(jax.random.fold_in(streams_of[13], 71), 0)
    type_ids = draw_type_ids(jax.random.fold_in(streams_of[13], 71), 0)
    cotangent = noise(streams_of[3], (SEQS, LEN, D), 1.0, 6.0, ((1, 32),))
    pos_table = noise(streams_of[4], (MAXPOS, D), 0.5, 4.0, ((0, 16),))
    type_table = noise(streams_of[5], (2, D), 0.5, 4.0, ((1, 16),))
    query_key_value_weight = noise(streams_of[6], (D, 3 * D), D ** -0.5, 0.1875, ((0, 16),))
    attention_output_weight = noise(streams_of[7], (D, D), ((LEN ** 0.5) * ((3 * D) ** -0.5)), 6.0, ((0, 16),))
    up_projection_weight = noise(streams_of[8], (D, FF), D ** -0.5, 0.1875, ((0, 16),))
    down_projection_weight = noise(streams_of[9], (FF, D), FF ** -0.5, 0.09375, ((0, 16),))
    up_projection_bias = noise(streams_of[10], (FF,), 0.5, 4.0, ((0, 16),))
    norm_gains = jnp.clip(1.0 + 0.1 * jax.random.normal(streams_of[11], (2, D), jnp.float32), 0.5, 1.5).astype(jnp.bfloat16)
    biases = noise(streams_of[12], (6, D), 0.5, 4.0, ((1, 16),))
    return {"hidden": hidden, "pos_ids": pos_ids, "type_ids": type_ids, "cotangent": cotangent, "pos_table": pos_table, "type_table": type_table, "query_key_value_weight": query_key_value_weight, "attention_output_weight": attention_output_weight, "up_projection_weight": up_projection_weight, "down_projection_weight": down_projection_weight, "up_projection_bias": up_projection_bias, "norm_gains": norm_gains, "biases": biases}


@jax.custom_vjp
def low_precision(v):
    return lax.optimization_barrier(v.astype(jnp.bfloat16)).astype(jnp.float32)

@jax.custom_vjp
def low_precision_backward(v):
    return v

def low_keep(v):
    return (low_precision(v), None)

def low_pass(kept, grad):
    return (grad,)

def back_keep(v):
    return (v, None)

def back_low(kept, grad):
    return (low_precision(grad),)
low_precision.defvjp(low_keep, low_pass)
low_precision_backward.defvjp(back_keep, back_low)

def round_both(values_in):
    return low_precision(low_precision_backward(values_in))

def norm_layer(values_in, gain_row, offset_row):
    average = lax.optimization_barrier(jnp.mean(values_in, axis=-1, keepdims=True))
    centred = values_in - average
    variance = lax.optimization_barrier(jnp.mean(centred * centred, axis=-1, keepdims=True))
    return centred * lax.rsqrt(variance + 1e-12) * gain_row + offset_row

def attend(query_seq, key_seq, value_seq):
    length, head_count, head_size = query_seq.shape
    block_size = math.gcd(length, 512)
    score_scale = 1.0 / math.sqrt(head_size)

    def one_block(query_block):
        scores = jnp.einsum('qhe,khe->hqk', query_block, key_seq, precision=lax.Precision.HIGHEST) * score_scale
        weights = low_precision(jax.nn.softmax(low_precision_backward(scores), axis=-1))
        return jnp.einsum('hqk,khe->qhe', weights, value_seq, precision=lax.Precision.HIGHEST)
    blocks = query_seq.reshape(length // block_size, block_size, head_count, head_size)
    return lax.map(jax.checkpoint(one_block), blocks).reshape(length, head_count, head_size)

def forward(hidden, pos_table, type_table, query_key_value_weight, attention_output_weight, up_projection_weight, down_projection_weight, up_projection_bias, norm_gains, biases, pos_ids, type_ids):
    highest_precision = lax.Precision.HIGHEST
    seq_count, length, model_width = hidden.shape
    head_size = model_width // HEADS
    embedded_tokens = hidden + pos_table[pos_ids] + type_table[type_ids]
    projected_rows = jnp.einsum('yab,bq->yaq', low_precision(embedded_tokens), query_key_value_weight, precision=highest_precision)
    queries = round_both(projected_rows[..., :model_width] + biases[0])
    keys_whole = round_both(projected_rows[..., model_width:2 * model_width])
    values_whole = round_both(projected_rows[..., 2 * model_width:] + biases[1])
    head_shape = (seq_count, length, HEADS, head_size)
    attention_result = jax.vmap(attend)(queries.reshape(head_shape), keys_whole.reshape(head_shape), values_whole.reshape(head_shape))
    attention_result = round_both(attention_result.reshape(seq_count, length, model_width))
    residual_branch = low_precision_backward(jnp.einsum('zjr,rn->zjn', attention_result, attention_output_weight, precision=highest_precision) + biases[2])
    first_layer_norm = norm_layer(embedded_tokens + residual_branch, norm_gains[0], biases[3])
    inner_product_sum = low_precision_backward(jnp.einsum('yab,bq->yaq', low_precision(first_layer_norm), up_projection_weight, precision=highest_precision) + up_projection_bias)
    gelu_activations = low_precision(jax.nn.gelu(inner_product_sum, approximate=False))
    second_layer_norm = low_precision_backward(jnp.einsum('ixp,po->ixo', gelu_activations, down_projection_weight, precision=highest_precision) + biases[4])
    return norm_layer(first_layer_norm + second_layer_norm, norm_gains[1], biases[5])

def reference(hidden, pos_ids, type_ids, cotangent, pos_table, type_table, query_key_value_weight, attention_output_weight, up_projection_weight, down_projection_weight, up_projection_bias, norm_gains, biases):
    floats = [hidden.astype(jnp.float32), pos_table.astype(jnp.float32), type_table.astype(jnp.float32), query_key_value_weight.astype(jnp.float32), attention_output_weight.astype(jnp.float32), up_projection_weight.astype(jnp.float32), down_projection_weight.astype(jnp.float32), up_projection_bias.astype(jnp.float32), norm_gains.astype(jnp.float32), biases.astype(jnp.float32)]

    def apply_layer(*params):
        return forward(*params, pos_ids, type_ids)
    output, pullback = jax.vjp(apply_layer, *floats)
    grads = pullback(cotangent.astype(jnp.float32))
    return (output.astype(jnp.bfloat16), grads[0], grads[1], grads[2], grads[3], grads[4], grads[5], grads[6], grads[7], grads[8], grads[9])
```

```python
import functools
import math

import jax
import jax.numpy as jnp
from jax import lax
from jax.experimental import pallas as pl
from jax.experimental.pallas import tpu as pltpu
from jax.sharding import PartitionSpec as P

HEADS = 16
MESH = pl.DeviceIdType.MESH
F32 = jnp.float32
BF16 = jnp.bfloat16
VSPEC = pl.BlockSpec(memory_space=pltpu.VMEM)


def place():
    h = lax.axis_index("head")
    b = lax.axis_index("blk")
    return h, b // 4, (b // 2) % 2, b % 2


def blk(o, y, c):
    return (o * 2 + y) * 2 + c


def remote(src, dst, sems, index, device):
    return pltpu.make_async_remote_copy(
        src_ref=src,
        dst_ref=dst,
        send_sem=sems.at[0, index],
        recv_sem=sems.at[1, index],
        device_id=device,
        device_id_type=MESH,
    )


def greet(devices):
    barrier = pltpu.get_barrier_semaphore()
    for device in devices:
        pl.semaphore_signal(barrier, inc=1, device_id=device, device_id_type=MESH)
    pl.semaphore_wait(barrier, len(devices))


def comm_call(kernel, name, outs, ins, scratch, copies, cid, limit=None):
    return pl.pallas_call(
        kernel,
        name=name,
        out_shape=[jax.ShapeDtypeStruct(s, d) for s, d in outs],
        in_specs=[VSPEC] * len(ins),
        out_specs=[VSPEC] * len(outs),
        scratch_shapes=[pltpu.VMEM(s, d) for s, d in scratch]
        + [pltpu.SemaphoreType.DMA((2, copies))],
        compiler_params=pltpu.CompilerParams(
            collective_id=cid, has_side_effects=True, vmem_limit_bytes=limit
        ),
    )(*ins)


def plane_gather_kernel(x_ref, out_ref, sems):
    h, o, y, c = place()
    dev_x, dev_y, dev_c = (1 - h, blk(o, y, c)), (h, blk(o, 1 - y, c)), (h, blk(o, y, 1 - c))
    mine = h * 4 + y * 2 + c
    of_x = (1 - h) * 4 + y * 2 + c
    of_y = h * 4 + (1 - y) * 2 + c
    of_d = (1 - h) * 4 + (1 - y) * 2 + c
    greet((dev_x, dev_y, dev_c))
    sent = []

    def go(src, slot, index, device, half=None):
        if half is None:
            copy = remote(src, out_ref.at[:, slot], sems, index, device)
        else:
            copy = remote(src, out_ref.at[half, slot], sems, index, device)
        copy.start()
        sent.append(copy)

    def arrived(slot, index, device, half=None):
        ref = out_ref.at[:, slot] if half is None else out_ref.at[half, slot]
        remote(ref, ref, sems, index, device).wait_recv()

    go(x_ref, mine, 0, dev_x)
    go(x_ref, mine, 1, dev_y)
    go(x_ref, mine, 2, dev_c)
    out_ref[:, pl.ds(mine, 1)] = x_ref[...][:, None]
    arrived(of_x, 0, dev_x)
    go(out_ref.at[0, of_x], of_x, 3, dev_y, 0)
    go(out_ref.at[:, of_x], of_x, 4, dev_c)
    arrived(of_y, 1, dev_y)
    go(out_ref.at[1, of_y], of_y, 5, dev_x, 1)
    go(out_ref.at[:, of_y], of_y, 6, dev_c)
    arrived(of_d, 3, dev_y, 0)
    go(out_ref.at[0, of_d], of_d, 7, dev_c, 0)
    arrived(of_d, 5, dev_x, 1)
    go(out_ref.at[1, of_d], of_d, 8, dev_c, 1)
    flip = 1 - 2 * c
    arrived(mine + flip, 2, dev_c)
    arrived(of_x + flip, 4, dev_c)
    arrived(of_y + flip, 6, dev_c)
    arrived(of_d + flip, 7, dev_c, 0)
    arrived(of_d + flip, 8, dev_c, 1)
    for copy in sent:
        copy.wait_send()


def plane_gather(x, cid):
    two, rows, width = x.shape
    (out,) = comm_call(
        plane_gather_kernel, "plane_gather", [((2, 8, rows, width), x.dtype)], [x], [], 9, cid
    )
    return out


def plane_scatter_kernel(x_ref, out_ref, near, part, from_x, from_y, diag, sems):
    h, o, y, c = place()
    dev_x, dev_y, dev_c = (1 - h, blk(o, y, c)), (h, blk(o, 1 - y, c)), (h, blk(o, y, 1 - c))
    mine = h * 4 + y * 2 + c
    of_x = (1 - h) * 4 + y * 2 + c
    of_y = h * 4 + (1 - y) * 2 + c
    of_d = (1 - h) * 4 + (1 - y) * 2 + c
    flip = 1 - 2 * c
    greet((dev_x, dev_y, dev_c))
    sent = []

    def go(src, dst, index, device):
        copy = remote(src, dst, sems, index, device)
        copy.start()
        sent.append(copy)

    def arrived(dst, index, device):
        remote(dst, dst, sems, index, device).wait_recv()

    for k, slot in enumerate((of_d, of_x, of_y, mine)):
        go(x_ref.at[:, slot + flip], near.at[k], k, dev_c)

    def add(k, slot, half):
        return x_ref[half, slot].astype(F32) + near[k, half].astype(F32)

    arrived(near.at[0], 0, dev_c)
    part[0, 0] = add(0, of_d, 0).astype(BF16)
    go(part.at[0, 0], diag.at[0], 4, dev_x)
    part[0, 1] = add(0, of_d, 1).astype(BF16)
    go(part.at[0, 1], diag.at[1], 5, dev_y)
    arrived(near.at[1], 1, dev_c)
    part[1, 0] = add(1, of_x, 0).astype(BF16)
    go(part.at[1, 0], from_x.at[0], 6, dev_x)
    arrived(near.at[2], 2, dev_c)
    part[2, 1] = add(2, of_y, 1).astype(BF16)
    go(part.at[2, 1], from_y.at[1], 7, dev_y)
    arrived(diag.at[1], 5, dev_y)
    part[1, 1] = (add(1, of_x, 1) + diag[1].astype(F32)).astype(BF16)
    go(part.at[1, 1], from_x.at[1], 8, dev_x)
    arrived(diag.at[0], 4, dev_x)
    part[2, 0] = (add(2, of_y, 0) + diag[0].astype(F32)).astype(BF16)
    go(part.at[2, 0], from_y.at[0], 9, dev_y)
    arrived(near.at[3], 3, dev_c)
    arrived(from_x.at[0], 6, dev_x)
    arrived(from_y.at[1], 7, dev_y)
    arrived(from_x.at[1], 8, dev_x)
    arrived(from_y.at[0], 9, dev_y)
    for half in range(2):
        out_ref[half] = (
            add(3, mine, half) + from_x[half].astype(F32) + from_y[half].astype(F32)
        )
    for copy in sent:
        copy.wait_send()


def plane_scatter(x, cid):
    two, eight, rows, width = x.shape
    (out,) = comm_call(
        plane_scatter_kernel,
        "plane_scatter",
        [((2, rows, width), F32)],
        [x],
        [
            ((4, 2, rows, width), BF16),
            ((3, 2, rows, width), BF16),
            ((2, rows, width), BF16),
            ((2, rows, width), BF16),
            ((2, rows, width), BF16),
        ],
        10,
        cid,
    )
    return out


def small_gather_kernel(n, x_ref, out_ref, sems):
    h = lax.axis_index("head")
    b = lax.axis_index("blk")
    greet([(h, (b + k) % n) for k in range(1, n)])
    copies = []
    for k in range(1, n):
        copy = remote(x_ref, out_ref.at[b], sems, k, (h, (b + k) % n))
        copy.start()
        copies.append(copy)
    out_ref[pl.ds(b, 1)] = x_ref[...][None]
    for copy in copies:
        copy.wait()


def small_gather(x, n, cid):
    (out,) = comm_call(
        functools.partial(small_gather_kernel, n),
        "small_gather",
        [((n,) + x.shape, x.dtype)],
        [x],
        [],
        n,
        cid,
    )
    return out


def small_scatter_kernel(n, x_ref, out_ref, held, sems):
    h = lax.axis_index("head")
    b = lax.axis_index("blk")
    others = [(h, (b + k) % n) for k in range(1, n)] + [(1 - h, (b + k) % n) for k in range(n)]
    greet(others)
    copies = []
    for k, (to_h, to_b) in enumerate(others):
        copy = remote(x_ref.at[to_b], held.at[k], sems, k, (to_h, to_b))
        copy.start()
        copies.append(copy)
    for copy in copies:
        copy.wait()
    out_ref[...] = x_ref[b] + jnp.sum(held[...], axis=0)


def small_scatter(x, n, cid):
    (out,) = comm_call(
        functools.partial(small_scatter_kernel, n),
        "small_scatter",
        [(x.shape[1:], F32)],
        [x],
        [((2 * n - 1,) + x.shape[1:], F32)],
        2 * n - 1,
        cid,
    )
    return out


def weight_kernel(wu_ref, wd_ref, wo_ref, ou_ref, od_ref, oo_ref, usem, dsem, osem):
    h = lax.axis_index("head")
    b = lax.axis_index("blk")
    o, g = b // 4, b % 4
    greet([(h, (b + k) % 16) for k in range(1, 16)])
    sent = []
    for k in range(1, 16):
        to = (b + k) % 16
        copy = remote(wu_ref.at[to % 4], ou_ref.at[b], usem, k, (h, to))
        copy.start()
        sent.append(copy)
    has = o // 2 == h
    for k in range(1, 4):
        to = (h, ((o + k) % 4) * 4 + g)

        @pl.when(has)
        def _():
            remote(wo_ref, oo_ref.at[o % 2], osem, k, to).start()

        copy = remote(wd_ref, od_ref.at[o], dsem, k, to)
        copy.start()
        sent.append(copy)
    ou_ref[pl.ds(b, 1)] = wu_ref[pl.ds(g, 1)]
    od_ref[pl.ds(o, 1)] = wd_ref[...][None]

    @pl.when(has)
    def _():
        oo_ref[pl.ds(o % 2, 1)] = wo_ref[...][None]

    for copy in sent:
        copy.wait()
    for k in range(1, 4):
        source = (o + 4 - k) % 4

        @pl.when(has)
        def _():
            remote(wo_ref, oo_ref.at[o % 2], osem, k, (h, b)).wait_send()

        @pl.when(source // 2 == h)
        def _():
            remote(wo_ref, oo_ref.at[source % 2], osem, k, (h, b)).wait_recv()


def weight_exchange(wu, wd, wo, cid):
    return pl.pallas_call(
        weight_kernel,
        name="weight_exchange",
        out_shape=[
            jax.ShapeDtypeStruct((16,) + wu.shape[1:], BF16),
            jax.ShapeDtypeStruct((4,) + wd.shape, BF16),
            jax.ShapeDtypeStruct((2,) + wo.shape, BF16),
        ],
        in_specs=[VSPEC] * 3,
        out_specs=[VSPEC] * 3,
        scratch_shapes=[
            pltpu.SemaphoreType.DMA((2, 16)),
            pltpu.SemaphoreType.DMA((2, 4)),
            pltpu.SemaphoreType.DMA((2, 4)),
        ],
        compiler_params=pltpu.CompilerParams(collective_id=cid, has_side_effects=True),
    )(wu, wd, wo)


def rows_kernel(x_ref, out_ref, near, part, from_y, part_z, from_z, csem, ysem, zsem):
    h, o, y, c = place()
    dev_y, dev_c = (h, blk(o, 1 - y, c)), (h, blk(o, y, 1 - c))
    others = [(o + k) % 4 for k in range(1, 4)]
    greet([dev_y, dev_c] + [(h, blk(z, y, c)) for z in others])
    order = others + [o]
    sent = []
    for j, z in enumerate(order):
        for i, yy in enumerate((1 - y, y)):
            copy = remote(x_ref.at[z, yy, 1 - c], near.at[i, j], csem, i * 4 + j, dev_c)
            copy.start()
            sent.append(copy)
    for j, z in enumerate(order):
        remote(near.at[0, j], near.at[0, j], csem, j, dev_c).wait_recv()
        part[j] = (x_ref[z, 1 - y, c].astype(F32) + near[0, j].astype(F32)).astype(BF16)
        copy = remote(part.at[j], from_y.at[j], ysem, j, dev_y)
        copy.start()
        sent.append(copy)
    for j, z in enumerate(order):
        remote(near.at[1, j], near.at[1, j], csem, 4 + j, dev_c).wait_recv()
        remote(from_y.at[j], from_y.at[j], ysem, j, dev_y).wait_recv()
        total = x_ref[z, y, c].astype(F32) + near[1, j].astype(F32) + from_y[j].astype(F32)
        part_z[j] = total.astype(BF16)
        if j < 3:
            copy = remote(part_z.at[j], from_z.at[j], zsem, j, (h, blk(z, y, c)))
            copy.start()
            sent.append(copy)
    for j in range(3):
        remote(from_z.at[j], from_z.at[j], zsem, j, (h, blk(o, y, c))).wait_recv()
    out_ref[...] = part_z[3].astype(F32) + jnp.sum(from_z[...].astype(F32), axis=0)
    for copy in sent:
        copy.wait_send()


def rows_scatter(x, cid):
    rows, width = x.shape[3:]
    block = (rows, width)
    return pl.pallas_call(
        rows_kernel,
        name="rows_scatter",
        out_shape=jax.ShapeDtypeStruct(block, F32),
        in_specs=[VSPEC],
        out_specs=VSPEC,
        scratch_shapes=[
            pltpu.VMEM((2, 4) + block, BF16),
            pltpu.VMEM((4,) + block, BF16),
            pltpu.VMEM((4,) + block, BF16),
            pltpu.VMEM((4,) + block, BF16),
            pltpu.VMEM((3,) + block, BF16),
            pltpu.SemaphoreType.DMA((2, 8)),
            pltpu.SemaphoreType.DMA((2, 4)),
            pltpu.SemaphoreType.DMA((2, 3)),
        ],
        compiler_params=pltpu.CompilerParams(
            collective_id=cid, has_side_effects=True, vmem_limit_bytes=48 << 20
        ),
    )(x)


def blk_gather_kernel(x_ref, out_ref, zsem, ysem, csem):
    h, o, y, c = place()
    dev_y, dev_c = (h, blk(o, 1 - y, c)), (h, blk(o, y, 1 - c))
    others = [(o + k) % 4 for k in range(1, 4)]
    greet([dev_y, dev_c] + [(h, blk(z, y, c)) for z in others])
    sent = []

    def go(src, z, yy, sem, index, device):
        copy = remote(src, out_ref.at[z, yy, c], sem, index, device)
        copy.start()
        sent.append(copy)

    def arrived(z, yy, cc, sem, index):
        ref = out_ref.at[z, yy, cc]
        remote(ref, ref, sem, index, dev_c).wait_recv()

    for j, z in enumerate(others):
        go(x_ref, o, y, zsem, j, (h, blk(z, y, c)))
    go(x_ref, o, y, ysem, 0, dev_y)
    go(x_ref, o, y, csem, 0, dev_c)
    out_ref[o, y, c] = x_ref[...]
    froms = [(o + 4 - k) % 4 for k in range(1, 4)]
    for j, z in enumerate(froms):
        arrived(z, y, c, zsem, j)
        go(out_ref.at[z, y, c], z, y, ysem, 1 + j, dev_y)
        go(out_ref.at[z, y, c], z, y, csem, 1 + j, dev_c)
    for j, z in enumerate([o] + froms):
        arrived(z, 1 - y, c, ysem, j)
        go(out_ref.at[z, 1 - y, c], z, 1 - y, csem, 4 + j, dev_c)
    for j, z in enumerate([o] + froms):
        arrived(z, y, 1 - c, csem, j)
        arrived(z, 1 - y, 1 - c, csem, 4 + j)
    for copy in sent:
        copy.wait_send()


def blk_gather(x, cid):
    return pl.pallas_call(
        blk_gather_kernel,
        name="blk_gather",
        out_shape=jax.ShapeDtypeStruct((4, 2, 2) + x.shape, x.dtype),
        in_specs=[VSPEC],
        out_specs=VSPEC,
        scratch_shapes=[
            pltpu.SemaphoreType.DMA((2, 3)),
            pltpu.SemaphoreType.DMA((2, 4)),
            pltpu.SemaphoreType.DMA((2, 8)),
        ],
        compiler_params=pltpu.CompilerParams(collective_id=cid, has_side_effects=True),
    )(x)


def to_pairs_kernel(rows, cols, x_ref, out_ref, sems):
    h = lax.axis_index("head")
    b = lax.axis_index("blk")
    o, g = b // 4, b % 4
    greet([(h, ((o + k) % 4) * 4 + g) for k in range(1, 4)])

    def block(z):
        s, j = z // 2, z % 2
        return x_ref.at[pl.ds(j * rows, rows), pl.ds(s * cols, cols)]

    copies = []
    for k in range(1, 4):
        to = (o + k) % 4
        copy = remote(block(to), out_ref.at[:, pl.ds(o * cols, cols)], sems, k, (h, to * 4 + g))
        copy.start()
        copies.append(copy)
    out_ref[:, pl.ds(o * cols, cols)] = block(o)[...]
    for copy in copies:
        copy.wait()


def to_pairs(x, cid):
    rows, cols = x.shape[0] // 2, x.shape[1] // 2
    (out,) = comm_call(
        functools.partial(to_pairs_kernel, rows, cols),
        "to_pairs",
        [((rows, 4 * cols), x.dtype)],
        [x],
        [],
        4,
        cid,
    )
    return out


def from_pairs_kernel(rows, cols, x_ref, out_ref, sems):
    h = lax.axis_index("head")
    b = lax.axis_index("blk")
    o, g = b // 4, b % 4
    greet([(h, ((o + k) % 4) * 4 + g) for k in range(1, 4)])
    s, j = o // 2, o % 2

    def spot():
        return out_ref.at[pl.ds(j * rows, rows), pl.ds(s * cols, cols)]

    copies = []
    for k in range(1, 4):
        to = (o + k) % 4
        copy = remote(x_ref.at[:, pl.ds(to * cols, cols)], spot(), sems, k, (h, to * 4 + g))
        copy.start()
        copies.append(copy)
    out_ref[pl.ds(j * rows, rows), pl.ds(s * cols, cols)] = x_ref[:, pl.ds(o * cols, cols)]
    for copy in copies:
        copy.wait()


def from_pairs(x, cid):
    rows, cols = x.shape[0], x.shape[1] // 4
    (out,) = comm_call(
        functools.partial(from_pairs_kernel, rows, cols),
        "from_pairs",
        [((2 * rows, 2 * cols), x.dtype)],
        [x],
        [],
        4,
        cid,
    )
    return out


def grad_kernel(
    gu_ref, gd_ref, go_ref, ou_ref, od_ref, oo_ref, ru, rd, ro, su, zsem, dsem, osem, usem, xsem
):
    h, o, y, c = place()
    g = y * 2 + c
    t = h * 4 + g
    plane = [((t + k) % 8 // 4, o * 4 + (t + k) % 4) for k in range(1, 8)]
    others = [(o + k) % 4 for k in range(1, 4)]
    greet(plane + [(h, z * 4 + g) for z in others])
    dev_x = (1 - h, o * 4 + g)
    has = o // 2 == h
    sent = []
    for k, z in enumerate(others):
        for src, dst, sem in ((gu_ref, ru, zsem), (gd_ref, rd, dsem)):
            copy = remote(src.at[z], dst.at[k], sem, k, (h, z * 4 + g))
            copy.start()
            sent.append(copy)

        @pl.when(z // 2 == h)
        def _():
            remote(go_ref.at[z % 2], ro.at[k], osem, k, (h, z * 4 + g)).start()

    for k in range(3):
        remote(ru.at[k], ru.at[k], zsem, k, dev_x).wait_recv()
    su[...] = (gu_ref[o].astype(F32) + jnp.sum(ru[...].astype(F32), axis=0)).astype(BF16)
    for k, (to_h, to_b) in enumerate(plane):
        copy = remote(su.at[to_b % 4], ou_ref.at[t], usem, k, (to_h, to_b))
        copy.start()
        sent.append(copy)
    ou_ref[pl.ds(t, 1)] = su[pl.ds(g, 1)]
    for k in range(3):
        remote(rd.at[k], rd.at[k], dsem, k, dev_x).wait_recv()
    od_ref[h] = (gd_ref[o].astype(F32) + jnp.sum(rd[...].astype(F32), axis=0)).astype(BF16)
    copy = remote(od_ref.at[h], od_ref.at[h], xsem, 0, dev_x)
    copy.start()
    sent.append(copy)

    @pl.when(has)
    def _():
        for k in range(3):
            remote(ro.at[k], ro.at[k], osem, k, dev_x).wait_recv()
        oo_ref[...] = (go_ref[o % 2].astype(F32) + jnp.sum(ro[...].astype(F32), axis=0)).astype(
            BF16
        )
        remote(oo_ref, oo_ref, xsem, 1, dev_x).start()
        remote(oo_ref, oo_ref, xsem, 1, dev_x).wait_send()

    @pl.when(jnp.logical_not(has))
    def _():
        remote(oo_ref, oo_ref, xsem, 1, dev_x).wait_recv()

    for k, z in enumerate(others):

        @pl.when(z // 2 == h)
        def _():
            remote(go_ref.at[z % 2], ro.at[k], osem, k, dev_x).wait_send()

    for k in range(7):
        source = (t + 7 - k) % 8
        remote(su.at[0], ou_ref.at[source], usem, k, dev_x).wait_recv()
    remote(od_ref.at[1 - h], od_ref.at[1 - h], xsem, 0, dev_x).wait_recv()
    for copy in sent:
        copy.wait_send()


def grad_exchange(gu, gd, go, cid):
    ublock, dblock, oblock = gu.shape[1:], gd.shape[1:], go.shape[1:]
    return pl.pallas_call(
        grad_kernel,
        name="grad_exchange",
        out_shape=[
            jax.ShapeDtypeStruct((8,) + ublock[1:], BF16),
            jax.ShapeDtypeStruct((2,) + dblock, BF16),
            jax.ShapeDtypeStruct(oblock, BF16),
        ],
        in_specs=[VSPEC] * 3,
        out_specs=[VSPEC] * 3,
        scratch_shapes=[
            pltpu.VMEM((3,) + ublock, BF16),
            pltpu.VMEM((3,) + dblock, BF16),
            pltpu.VMEM((3,) + oblock, BF16),
            pltpu.VMEM(ublock, BF16),
            pltpu.SemaphoreType.DMA((2, 3)),
            pltpu.SemaphoreType.DMA((2, 3)),
            pltpu.SemaphoreType.DMA((2, 3)),
            pltpu.SemaphoreType.DMA((2, 7)),
            pltpu.SemaphoreType.DMA((2, 2)),
        ],
        compiler_params=pltpu.CompilerParams(collective_id=cid, has_side_effects=True),
    )(gu, gd, go)


def pair_sum_kernel(x_ref, out_ref, held, sems):
    h = lax.axis_index("head")
    b = lax.axis_index("blk")
    dev_x = (1 - h, b)
    greet([dev_x])
    pieces = x_ref.shape[0]
    copies = [remote(x_ref.at[k], held.at[k], sems, k, dev_x) for k in range(pieces)]
    for copy in copies:
        copy.start()
    for k, copy in enumerate(copies):
        copy.wait()
        out_ref[k] = x_ref[k].astype(F32) + held[k].astype(F32)


def pair_sum(x, cid):
    (out,) = comm_call(
        pair_sum_kernel, "pair_sum", [(x.shape, F32)], [x], [(x.shape, BF16)], x.shape[0], cid
    )
    return out


def attend_kernel(scale, x_ref, o_ref, low_ref, lse_ref, keys):
    e = o_ref.shape[0]
    step = pl.program_id(0)
    cols = o_ref.shape[1]

    @pl.when(step == 0)
    def _():
        keys[...] = x_ref[e : 2 * e].astype(F32).T.astype(BF16)

    q = (x_ref[0:e, pl.ds(pl.multiple_of(step * cols, cols), cols)].astype(F32) * scale).astype(
        BF16
    )
    s = jnp.dot(keys[...], q, preferred_element_type=F32)
    peak = jnp.max(s, axis=0, keepdims=True)
    p = jnp.exp(s - peak)
    total = jnp.sum(p, axis=0, keepdims=True)
    o = jnp.dot(x_ref[2 * e : 3 * e], p.astype(BF16), preferred_element_type=F32) / total
    o_ref[...] = o
    low_ref[...] = o.astype(BF16)
    lse_ref[...] = peak + jnp.log(total)


def attend(x, scale, cols=256):
    rows, length = x.shape
    e = rows // 3
    return pl.pallas_call(
        functools.partial(attend_kernel, scale),
        name="attend",
        grid=(length // cols,),
        out_shape=[
            jax.ShapeDtypeStruct((e, length), F32),
            jax.ShapeDtypeStruct((e, length), BF16),
            jax.ShapeDtypeStruct((1, length), F32),
        ],
        in_specs=[pl.BlockSpec((rows, length), lambda i: (0, 0))],
        out_specs=[
            pl.BlockSpec((e, cols), lambda i: (0, i)),
            pl.BlockSpec((e, cols), lambda i: (0, i)),
            pl.BlockSpec((1, cols), lambda i: (0, i)),
        ],
        scratch_shapes=[pltpu.VMEM((length, e), BF16)],
        compiler_params=pltpu.CompilerParams(vmem_limit_bytes=48 << 20),
    )(x)


def attend_back_kernel(scale, x_ref, g_ref, o_ref, lse_ref, out_ref, keys, values, dk, dv):
    e = o_ref.shape[0]
    step = pl.program_id(0)
    cols = o_ref.shape[1]

    @pl.when(step == 0)
    def _():
        keys[...] = x_ref[e : 2 * e].astype(F32).T.astype(BF16)
        values[...] = x_ref[2 * e : 3 * e].astype(F32).T.astype(BF16)
        dk[...] = jnp.zeros_like(dk)
        dv[...] = jnp.zeros_like(dv)

    here = pl.ds(pl.multiple_of(step * cols, cols), cols)
    q32 = x_ref[0:e, here].astype(F32) * scale
    q = q32.astype(BF16)
    g32 = g_ref[...].astype(F32)
    delta = jnp.sum(g32 * o_ref[...], axis=0, keepdims=True)
    s = jnp.dot(keys[...], q, preferred_element_type=F32)
    p = jnp.exp(s - lse_ref[...])
    dv[...] += jnp.dot(p.astype(BF16), g32.T.astype(BF16), preferred_element_type=F32)
    dp = jnp.dot(values[...], g_ref[...], preferred_element_type=F32)
    ds = (p * (dp - delta)).astype(BF16)
    dk[...] += jnp.dot(ds, q32.T.astype(BF16), preferred_element_type=F32)
    dq = jnp.dot(x_ref[e : 2 * e], ds, preferred_element_type=F32) * scale
    out_ref[0:e, here] = dq.astype(BF16)

    @pl.when(step == pl.num_programs(0) - 1)
    def _():
        out_ref[e : 2 * e] = dk[...].T.astype(BF16)
        out_ref[2 * e : 3 * e] = dv[...].T.astype(BF16)


def attend_back(x, g, o, lse, scale, cols=256):
    rows, length = x.shape
    e = rows // 3
    return pl.pallas_call(
        functools.partial(attend_back_kernel, scale),
        name="attend_back",
        grid=(length // cols,),
        out_shape=jax.ShapeDtypeStruct((rows, length), BF16),
        in_specs=[
            pl.BlockSpec((rows, length), lambda i: (0, 0)),
            pl.BlockSpec((e, cols), lambda i: (0, i)),
            pl.BlockSpec((e, cols), lambda i: (0, i)),
            pl.BlockSpec((1, cols), lambda i: (0, i)),
        ],
        out_specs=pl.BlockSpec((rows, length), lambda i: (0, 0)),
        scratch_shapes=[
            pltpu.VMEM((length, e), BF16),
            pltpu.VMEM((length, e), BF16),
            pltpu.VMEM((length, e), F32),
            pltpu.VMEM((length, e), F32),
        ],
        compiler_params=pltpu.CompilerParams(vmem_limit_bytes=48 << 20),
    )(x, g, o, lse)


def norm_layer(values_in, gain_row, offset_row):
    average = jnp.mean(values_in, axis=-1, keepdims=True)
    centred = values_in - average
    variance = jnp.mean(centred * centred, axis=-1, keepdims=True)
    return centred * lax.rsqrt(variance + 1e-12) * gain_row + offset_row


def gelu_exact(inner_product_sum):
    return jax.nn.gelu(inner_product_sum, approximate=False)


def widest_block(length, limit):
    return max(
        (candidate for candidate in range(1, min(length, limit) + 1) if length % candidate == 0)
    )


def block_scores(query_heads, key_block, score_scale):
    return (
        jnp.einsum("sqhe,skhe->shqk", query_heads, key_block, preferred_element_type=jnp.float32)
        * score_scale
    )


def key_side(query_block, grad_block, lse_block, delta_block, key_heads, value_heads, score_scale):
    scores = block_scores(query_block, key_heads, score_scale)
    weights = jnp.exp(scores - lse_block[..., None])
    more_values = jnp.einsum(
        "shqk,sqhe->shke",
        weights.astype(jnp.bfloat16),
        grad_block,
        preferred_element_type=jnp.float32,
    )
    grad_weights = jnp.einsum(
        "sqhe,skhe->shqk", grad_block, value_heads, preferred_element_type=jnp.float32
    )
    grad_scores = weights * (grad_weights - delta_block[..., None])
    more_keys = jnp.einsum(
        "shqk,sqhe->shke",
        grad_scores.astype(jnp.bfloat16),
        query_block,
        preferred_element_type=jnp.float32,
    )
    return (more_keys, more_values)


def forward_fold(query_heads, score_scale, head_count, head_size):

    def fold_keys(running, portion, offset):
        key_piece, value_piece = portion
        seq_count, length = (key_piece.shape[0], key_piece.shape[1])
        block_size = widest_block(length, 512)

        def one_step(block_index, carried):
            row_peak, row_total, weighted = carried
            row_start = block_index * block_size
            key_block = lax.dynamic_slice_in_dim(key_piece, row_start, block_size, 1).reshape(
                seq_count, block_size, head_count, head_size
            )
            value_block = lax.dynamic_slice_in_dim(value_piece, row_start, block_size, 1).reshape(
                seq_count, block_size, head_count, head_size
            )
            scores = block_scores(query_heads, key_block, score_scale)
            new_peak = jnp.maximum(row_peak, jnp.max(scores, axis=-1))
            shrink = jnp.exp(row_peak - new_peak)
            weights = jnp.exp(scores - new_peak[..., None])
            row_total = row_total * shrink + jnp.sum(weights, axis=-1)
            weighted = weighted * shrink[..., None] + jnp.einsum(
                "shqk,skhe->shqe",
                weights.astype(jnp.bfloat16),
                value_block,
                preferred_element_type=jnp.float32,
            )
            return (new_peak, row_total, weighted)

        return lax.fori_loop(0, length // block_size, one_step, running)

    return fold_keys


def query_fold(query_heads, grad_heads, log_totals, delta_rows, score_scale, head_count, head_size):

    def fold_keys(running, portion, offset):
        key_piece, value_piece = portion
        seq_count, length = (key_piece.shape[0], key_piece.shape[1])
        block_size = widest_block(length, 512)

        def one_step(block_index, weighted):
            row_start = block_index * block_size
            key_block = lax.dynamic_slice_in_dim(key_piece, row_start, block_size, 1).reshape(
                seq_count, block_size, head_count, head_size
            )
            value_block = lax.dynamic_slice_in_dim(value_piece, row_start, block_size, 1).reshape(
                seq_count, block_size, head_count, head_size
            )
            scores = block_scores(query_heads, key_block, score_scale)
            weights = jnp.exp(scores - log_totals[..., None])
            grad_weights = jnp.einsum(
                "sqhe,skhe->shqk", grad_heads, value_block, preferred_element_type=jnp.float32
            )
            grad_scores = weights * (grad_weights - delta_rows[..., None])
            return weighted + jnp.einsum(
                "shqk,skhe->shqe",
                grad_scores.astype(jnp.bfloat16),
                key_block,
                preferred_element_type=jnp.float32,
            )

        return lax.fori_loop(0, length // block_size, one_step, running)

    return fold_keys


def key_fold(key_heads, value_heads, score_scale, head_count, head_size):

    def fold_queries(running, portion, offset):
        query_piece, grad_piece, lse_piece, delta_piece = portion
        seq_count, length = (query_piece.shape[0], query_piece.shape[1])
        block_size = widest_block(length, 512)

        def one_step(block_index, carried):
            grad_keys, grad_values = carried
            row_start = block_index * block_size
            query_block = lax.dynamic_slice_in_dim(query_piece, row_start, block_size, 1).reshape(
                seq_count, block_size, head_count, head_size
            )
            grad_block = lax.dynamic_slice_in_dim(grad_piece, row_start, block_size, 1).reshape(
                seq_count, block_size, head_count, head_size
            )
            lse_block = lax.dynamic_slice_in_dim(lse_piece, row_start, block_size, 1).transpose(
                0, 2, 1
            )
            delta_block = lax.dynamic_slice_in_dim(delta_piece, row_start, block_size, 1).transpose(
                0, 2, 1
            )
            more_keys, more_values = key_side(
                query_block, grad_block, lse_block, delta_block, key_heads, value_heads, score_scale
            )
            return (grad_keys + more_keys, grad_values + more_values)

        return lax.fori_loop(0, length // block_size, one_step, running)

    return fold_queries


def layer_in_blocks(
    hidden,
    pos_ids,
    type_ids,
    cotangent,
    pos_table,
    type_table,
    query_key_value_weight,
    attention_output_weight,
    up_projection_weight,
    down_projection_weight,
    up_projection_bias,
    norm_gains,
    biases,
):
    seq_count, seg_tokens, model_width = hidden.shape
    row_count = seq_count * seg_tokens
    head_count = HEADS // lax.axis_size("head")
    head_size = model_width // HEADS
    local_width = head_count * head_size
    query_rows = lax.axis_size("head") * seg_tokens
    score_scale = 1.0 / math.sqrt(head_size)

    def fetch_weights():
        return (
            lax.all_gather(query_key_value_weight, "blk", axis=0, tiled=True),
            lax.all_gather(attention_output_weight, "blk", axis=0, tiled=True),
            lax.all_gather(up_projection_weight, "blk", axis=0, tiled=True),
            lax.all_gather(down_projection_weight, "blk", axis=0, tiled=True),
            lax.all_gather(up_projection_bias, "blk", axis=0, tiled=True),
            lax.all_gather(norm_gains, "blk", axis=1, tiled=True),
            lax.all_gather(biases, "blk", axis=1, tiled=True),
            lax.all_gather(type_table, "blk", axis=1, tiled=True),
        )

    qkv_full, out_full, up_full, down_full, up_bias_full, gain_full, bias_full, type_full = (
        fetch_weights()
    )
    bias_float = bias_full.astype(jnp.float32)
    gain_float = gain_full.astype(jnp.float32)
    flat_pos = pos_ids.reshape(row_count)
    portion = lax.all_gather(pos_table, "blk", axis=0, tiled=True)
    local_slots = flat_pos
    onehot = (
        local_slots[:, None] == jnp.arange(portion.shape[0], dtype=jnp.int32)[None, :]
    ).astype(jnp.bfloat16)
    positions = jnp.dot(onehot, portion, preferred_element_type=jnp.float32)
    is_second = type_ids.reshape(row_count, 1) == 1
    typed_rows = jnp.where(
        is_second, type_full[1].astype(jnp.float32), type_full[0].astype(jnp.float32)
    )
    embedded_tokens = (
        hidden.reshape(row_count, model_width).astype(jnp.float32) + positions + typed_rows
    )
    embedded_low = embedded_tokens.astype(jnp.bfloat16)
    projected_rows = jnp.dot(embedded_low, qkv_full, preferred_element_type=jnp.float32)
    token_shape = (seq_count, seg_tokens, model_width)
    queries = (
        (projected_rows[:, :model_width] + bias_float[0]).astype(jnp.bfloat16).reshape(token_shape)
    )
    keys_token = (
        projected_rows[:, model_width : 2 * model_width].astype(jnp.bfloat16).reshape(token_shape)
    )
    values_token = (
        (projected_rows[:, 2 * model_width :] + bias_float[1])
        .astype(jnp.bfloat16)
        .reshape(token_shape)
    )
    query_local, key_local, value_local = (
        lax.all_to_all(queries, "head", split_axis=2, concat_axis=1, tiled=True),
        lax.all_to_all(keys_token, "head", split_axis=2, concat_axis=1, tiled=True),
        lax.all_to_all(values_token, "head", split_axis=2, concat_axis=1, tiled=True),
    )
    head_shape = (seq_count, query_rows, head_count, head_size)
    query_heads = query_local.reshape(head_shape)
    key_heads = key_local.reshape(head_shape)
    value_heads = value_local.reshape(head_shape)
    start_peak = jnp.full((seq_count, head_count, query_rows), -jnp.inf, jnp.float32)
    start_total = jnp.zeros((seq_count, head_count, query_rows), jnp.float32)
    zero_heads = jnp.zeros((seq_count, head_count, query_rows, head_size), jnp.float32)
    fold_keys = forward_fold(query_heads, score_scale, head_count, head_size)
    row_peak, row_total, weighted = fold_keys(
        (start_peak, start_total, zero_heads),
        (
            lax.all_gather(key_local, "blk", axis=1, tiled=True),
            lax.all_gather(value_local, "blk", axis=1, tiled=True),
        ),
        jnp.int32(0),
    )
    log_totals = row_peak + jnp.log(row_total)
    attention_result = weighted / row_total[..., None]
    attended_low = (
        attention_result.transpose(0, 2, 1, 3)
        .reshape(seq_count, query_rows, local_width)
        .astype(jnp.bfloat16)
    )
    attended_token = lax.all_to_all(
        attended_low, "head", split_axis=1, concat_axis=2, tiled=True
    ).reshape(row_count, model_width)
    residual_branch = (
        jnp.dot(attended_token, out_full, preferred_element_type=jnp.float32) + bias_float[2]
    )
    first_layer_norm, first_pull = jax.vjp(
        norm_layer, embedded_tokens + residual_branch, gain_float[0], bias_float[3]
    )
    first_low = first_layer_norm.astype(jnp.bfloat16)
    inner_product_sum = jnp.dot(
        first_low, up_full, preferred_element_type=jnp.float32
    ) + up_bias_full.astype(jnp.float32)
    gelu_activations, gelu_pull = jax.vjp(gelu_exact, inner_product_sum)
    activated_low = gelu_activations.astype(jnp.bfloat16)
    second_layer_norm = (
        jnp.dot(activated_low, down_full, preferred_element_type=jnp.float32) + bias_float[4]
    )
    final_norm, final_pull = jax.vjp(
        norm_layer, first_layer_norm + second_layer_norm, gain_float[1], bias_float[5]
    )
    layer_out = final_norm.astype(jnp.bfloat16).reshape(token_shape)
    qkv_full, out_full, up_full, down_full, up_bias_full, gain_full, bias_full, type_full = (
        fetch_weights()
    )
    grad_final, grad_gain_two, grad_shift_two = final_pull(
        cotangent.reshape(row_count, model_width).astype(jnp.float32)
    )
    grad_second = grad_final.astype(jnp.bfloat16)
    grad_down = jnp.einsum(
        "rf,rd->fd", activated_low, grad_second, preferred_element_type=jnp.float32
    )
    grad_bias_second = jnp.sum(grad_second.astype(jnp.float32), axis=0)
    (grad_inner,) = gelu_pull(
        jnp.einsum("rd,fd->rf", grad_second, down_full, preferred_element_type=jnp.float32)
    )
    grad_inner_low = grad_inner.astype(jnp.bfloat16)
    grad_up = jnp.einsum("rd,rf->df", first_low, grad_inner_low, preferred_element_type=jnp.float32)
    grad_up_bias = jnp.sum(grad_inner_low.astype(jnp.float32), axis=0)
    grad_first = grad_final + jnp.einsum(
        "rf,df->rd", grad_inner_low, up_full, preferred_element_type=jnp.float32
    )
    grad_resid, grad_gain_one, grad_shift_one = first_pull(grad_first)
    grad_branch = grad_resid.astype(jnp.bfloat16)
    grad_out = jnp.einsum(
        "re,rd->ed", attended_token, grad_branch, preferred_element_type=jnp.float32
    )
    grad_bias_branch = jnp.sum(grad_branch.astype(jnp.float32), axis=0)
    grad_attended = (
        jnp.einsum("rd,ed->re", grad_branch, out_full, preferred_element_type=jnp.float32)
        .astype(jnp.bfloat16)
        .reshape(token_shape)
    )
    grad_local = lax.all_to_all(grad_attended, "head", split_axis=2, concat_axis=1, tiled=True)
    grad_heads = grad_local.reshape(head_shape)
    delta_rows = jnp.sum(
        grad_heads.astype(jnp.float32).transpose(0, 2, 1, 3) * attention_result, axis=-1
    )
    fold_queries = query_fold(
        query_heads, grad_heads, log_totals, delta_rows, score_scale, head_count, head_size
    )
    grad_query_sum = fold_queries(
        zero_heads,
        (
            lax.all_gather(key_local, "blk", axis=1, tiled=True),
            lax.all_gather(value_local, "blk", axis=1, tiled=True),
        ),
        jnp.int32(0),
    )
    fold_side = key_fold(key_heads, value_heads, score_scale, head_count, head_size)
    grad_key_sum, grad_value_sum = fold_side(
        (zero_heads, zero_heads),
        (
            lax.all_gather(query_local.astype(jnp.float32), "blk", axis=1, tiled=True).astype(
                jnp.bfloat16
            ),
            lax.all_gather(grad_local.astype(jnp.float32), "blk", axis=1, tiled=True).astype(
                jnp.bfloat16
            ),
            lax.all_gather(log_totals.transpose(0, 2, 1), "blk", axis=1, tiled=True),
            lax.all_gather(delta_rows.transpose(0, 2, 1), "blk", axis=1, tiled=True),
        ),
        jnp.int32(0),
    )
    grad_keys_local = (
        (grad_key_sum * score_scale)
        .transpose(0, 2, 1, 3)
        .reshape(seq_count, query_rows, local_width)
        .astype(jnp.bfloat16)
    )
    grad_values_local = (
        grad_value_sum.transpose(0, 2, 1, 3)
        .reshape(seq_count, query_rows, local_width)
        .astype(jnp.bfloat16)
    )
    grad_query_local = (
        (grad_query_sum * score_scale)
        .transpose(0, 2, 1, 3)
        .reshape(seq_count, query_rows, local_width)
        .astype(jnp.bfloat16)
    )
    grad_query_token, grad_key_token, grad_value_token = (
        lax.all_to_all(grad_query_local, "head", split_axis=1, concat_axis=2, tiled=True),
        lax.all_to_all(grad_keys_local, "head", split_axis=1, concat_axis=2, tiled=True),
        lax.all_to_all(grad_values_local, "head", split_axis=1, concat_axis=2, tiled=True),
    )
    grad_qkv = jnp.concatenate(
        [grad_query_token, grad_key_token, grad_value_token], axis=-1
    ).reshape(row_count, 3 * model_width)
    grad_qkv_full = jnp.einsum(
        "rd,rf->df", embedded_low, grad_qkv, preferred_element_type=jnp.float32
    )
    grad_bias_query = jnp.sum(
        grad_query_token.astype(jnp.float32).reshape(row_count, model_width), axis=0
    )
    grad_bias_value = jnp.sum(
        grad_value_token.astype(jnp.float32).reshape(row_count, model_width), axis=0
    )
    grad_embedded = grad_resid + jnp.einsum(
        "rf,df->rd", grad_qkv, qkv_full, preferred_element_type=jnp.float32
    )
    second_mask = is_second.astype(jnp.float32)
    grad_type_one = jnp.sum(grad_embedded * second_mask, axis=0)
    grad_type_zero = jnp.sum(grad_embedded * (1.0 - second_mask), axis=0)
    length = lax.axis_size("blk") * pos_table.shape[0]
    local_slots = flat_pos
    inside = (local_slots >= 0) & (local_slots < length)
    slot_index = jnp.where(inside, local_slots, length)
    buffer = jnp.zeros((length + 1, model_width), jnp.float32).at[slot_index].add(grad_embedded)
    grad_positions = lax.psum_scatter(buffer[:length], "blk", scatter_dimension=0, tiled=True)
    gain_stack = jnp.stack([grad_gain_one, grad_gain_two])
    bias_stack = jnp.stack(
        [
            grad_bias_query,
            grad_bias_value,
            grad_bias_branch,
            grad_shift_one,
            grad_bias_second,
            grad_shift_two,
        ]
    )
    type_stack = jnp.stack([grad_type_zero, grad_type_one])
    (
        shard_qkv,
        shard_out,
        shard_up,
        shard_down,
        shard_up_bias,
        shard_gains,
        shard_biases,
        shard_types,
    ) = (
        lax.psum_scatter(grad_qkv_full, "blk", scatter_dimension=0, tiled=True),
        lax.psum_scatter(grad_out, "blk", scatter_dimension=0, tiled=True),
        lax.psum_scatter(grad_up, "blk", scatter_dimension=0, tiled=True),
        lax.psum_scatter(grad_down, "blk", scatter_dimension=0, tiled=True),
        lax.psum_scatter(grad_up_bias, "blk", scatter_dimension=0, tiled=True),
        lax.psum_scatter(gain_stack, "blk", scatter_dimension=1, tiled=True),
        lax.psum_scatter(bias_stack, "blk", scatter_dimension=1, tiled=True),
        lax.psum_scatter(type_stack, "blk", scatter_dimension=1, tiled=True),
    )
    (
        total_qkv,
        total_out,
        total_up,
        total_down,
        total_up_bias,
        total_gains,
        total_biases,
        total_types,
        total_positions,
    ) = lax.psum(
        (
            shard_qkv,
            shard_out,
            shard_up,
            shard_down,
            shard_up_bias,
            shard_gains,
            shard_biases,
            shard_types,
            grad_positions,
        ),
        "head",
    )
    grad_hidden = grad_embedded.reshape(token_shape)
    return (
        layer_out,
        grad_hidden,
        total_positions,
        total_types,
        total_qkv,
        total_out,
        total_up,
        total_down,
        total_up_bias,
        total_gains,
        total_biases,
    )


def layer_in_planes(
    hidden,
    pos_ids,
    type_ids,
    cotangent,
    pos_table,
    type_table,
    query_key_value_weight,
    attention_output_weight,
    up_projection_weight,
    down_projection_weight,
    up_projection_bias,
    norm_gains,
    biases,
):
    seqs, seg, width = hidden.shape
    blks = lax.axis_size("blk")
    h = lax.axis_index("head")
    b = lax.axis_index("blk")
    o, g = b // 4, b % 4
    rows = seqs * seg
    e = width // HEADS
    ff = up_projection_weight.shape[1]
    scale = 1.0 / math.sqrt(e)
    slots = pos_table.shape[0]
    fcols = ff // blks // 2
    plane_rows = 8 * rows

    small = jnp.concatenate(
        [
            biases.astype(F32),
            norm_gains.astype(F32),
            type_table.astype(F32),
            up_projection_bias.astype(F32).reshape(4, e),
        ]
    ).reshape(7, 2 * e)
    packed = jnp.concatenate([small, pos_ids.astype(F32).reshape(1, rows)])
    everyone = small_gather(packed, blks, 0)
    params = everyone[:, :7].reshape(blks, 14, e).transpose(1, 0, 2)
    vectors = params[:10].reshape(10, width)
    bias_float, gain_float, type_float = vectors[:6], vectors[6:8], vectors[8:10]
    up_bias = lax.dynamic_slice_in_dim(
        params[10:].transpose(1, 0, 2).reshape(4, 4, 2, fcols), h, 1, 2
    )
    up_bias = lax.dynamic_slice_in_dim(up_bias, g, 1, 1).reshape(1, 4 * fcols)
    all_ids = everyone[:, 7].astype(jnp.int32)

    qkv_cut = query_key_value_weight.reshape(e, 3, 2, 2, 4, e)
    qkv_cut = lax.dynamic_slice_in_dim(qkv_cut, h, 1, 2).reshape(e, 3, 2, 4, e)
    qkv_cut = qkv_cut.transpose(3, 0, 2, 1, 4).reshape(4, e, 6 * e)
    up_cut = up_projection_weight.reshape(e, 4, 4, 2, fcols)
    up_cut = lax.dynamic_slice_in_dim(up_cut, h, 1, 3).reshape(e, 4, 4, fcols)
    up_cut = up_cut.transpose(2, 0, 1, 3).reshape(4, e, 4 * fcols)
    down_cut = lax.dynamic_slice_in_dim(down_projection_weight, h * fcols, fcols, 0)
    wide, down_all, out_all = weight_exchange(
        jnp.concatenate([qkv_cut, up_cut], axis=2), down_cut, attention_output_weight, 1
    )
    qkv_own = wide[:, :, : 6 * e].reshape(width, 6 * e)
    up_own = wide[:, :, 6 * e :].reshape(width, 4 * fcols)
    down_own = down_all.reshape(4 * fcols, width)
    out_own = out_all.reshape(2 * e, width)

    local_ids = all_ids.reshape(blks * rows, 1) - b * slots
    onehot = (local_ids == lax.broadcasted_iota(jnp.int32, (1, slots), 1)).astype(BF16)
    found = jnp.dot(onehot, pos_table, preferred_element_type=F32).astype(BF16)
    positions = rows_scatter(found.reshape(4, 2, 2, rows, width), 2)
    is_second = type_ids.reshape(rows, 1) == 1
    typed = jnp.where(is_second, type_float[1], type_float[0])
    embedded = hidden.reshape(rows, width).astype(F32) + positions + typed
    token_shape = (seqs, seg, width)

    plane_low = plane_gather(embedded.astype(BF16).reshape(token_shape), 3).reshape(
        plane_rows, width
    )
    bias_heads = bias_float.reshape(6, 2, 2, 4, e)
    bias_heads = lax.dynamic_slice_in_dim(bias_heads, h, 1, 1)
    bias_heads = lax.dynamic_slice_in_dim(bias_heads, g, 1, 3).reshape(6, 2, e)
    qkv_bias = jnp.stack(
        [bias_heads[0], jnp.zeros_like(bias_heads[0]), bias_heads[1]], axis=1
    ).reshape(6 * e, 1)
    projected = (
        jnp.einsum("kf,rk->fr", qkv_own, plane_low, preferred_element_type=F32) + qkv_bias
    ).astype(BF16)
    pair_qkv = to_pairs(projected, 4)
    pair_out, pair_low, lse = attend(pair_qkv, scale)
    attended = from_pairs(pair_low, 5)
    branch = jnp.einsum("fr,fd->rd", attended, out_own, preferred_element_type=F32).astype(BF16)
    branch = plane_scatter(branch.reshape(seqs, 8, seg, width), 6).reshape(rows, width)
    first, first_pull = jax.vjp(
        norm_layer, embedded + (branch + bias_float[2]), gain_float[0], bias_float[3]
    )

    first_low = plane_gather(first.astype(BF16).reshape(token_shape), 3).reshape(plane_rows, width)
    inner = jnp.dot(first_low, up_own, preferred_element_type=F32) + up_bias
    activated, gelu_pull = jax.vjp(gelu_exact, inner)
    activated_low = activated.astype(BF16)
    second = jnp.dot(activated_low, down_own, preferred_element_type=F32).astype(BF16)
    second = plane_scatter(second.reshape(seqs, 8, seg, width), 6).reshape(rows, width)
    final, final_pull = jax.vjp(
        norm_layer, first + (second + bias_float[4]), gain_float[1], bias_float[5]
    )
    layer_out = final.astype(BF16).reshape(token_shape)

    grad_final, grad_gain_two, grad_shift_two = final_pull(
        cotangent.reshape(rows, width).astype(F32)
    )
    grad_low = grad_final.astype(BF16)
    grad_bias_second = jnp.sum(grad_low.astype(F32), axis=0)
    plane_grad = plane_gather(grad_low.reshape(token_shape), 3).reshape(plane_rows, width)
    grad_down = jnp.einsum(
        "rf,rd->fd", activated_low, plane_grad, preferred_element_type=F32
    ).astype(BF16)
    (grad_inner,) = gelu_pull(
        jnp.einsum("rd,fd->rf", plane_grad, down_own, preferred_element_type=F32)
    )
    grad_inner_low = grad_inner.astype(BF16)
    grad_up = jnp.einsum(
        "rd,rf->df", first_low, grad_inner_low, preferred_element_type=F32
    ).astype(BF16)
    grad_up_bias = jnp.sum(grad_inner_low.astype(F32), axis=0)
    grad_first = jnp.einsum(
        "rf,df->rd", grad_inner_low, up_own, preferred_element_type=F32
    ).astype(BF16)
    grad_first = plane_scatter(grad_first.reshape(seqs, 8, seg, width), 6).reshape(rows, width)
    grad_resid, grad_gain_one, grad_shift_one = first_pull(grad_final + grad_first)
    branch_low = grad_resid.astype(BF16)
    grad_bias_branch = jnp.sum(branch_low.astype(F32), axis=0)
    plane_branch = plane_gather(branch_low.reshape(token_shape), 3).reshape(plane_rows, width)
    grad_out = jnp.einsum(
        "fr,rd->fd", attended, plane_branch, preferred_element_type=F32
    ).astype(BF16)
    grad_attended = jnp.einsum(
        "fd,rd->fr", out_own, plane_branch, preferred_element_type=F32
    ).astype(BF16)
    pair_grad = to_pairs(grad_attended, 7)
    pair_dqkv = attend_back(pair_qkv, pair_grad, pair_out, lse, scale)
    grad_qkv = from_pairs(pair_dqkv, 8)
    grad_qkv_weight = jnp.einsum(
        "rk,fr->kf", plane_low, grad_qkv, preferred_element_type=F32
    ).astype(BF16)
    head_sums = jnp.sum(grad_qkv.astype(F32), axis=1).reshape(2, 3, e)
    back = jnp.einsum("fr,kf->rk", grad_qkv, qkv_own, preferred_element_type=F32).astype(BF16)
    back = plane_scatter(back.reshape(seqs, 8, seg, width), 6).reshape(rows, width)
    grad_embedded = grad_resid + back
    grad_hidden = grad_embedded.reshape(token_shape)

    all_grads = blk_gather(grad_embedded.astype(BF16), 9).reshape(blks * rows, width)
    flat_ids = all_ids.reshape(1, blks * rows) - b * slots
    pick = (flat_ids == lax.broadcasted_iota(jnp.int32, (slots, 1), 0)).astype(BF16)
    pos_part = jnp.dot(pick, all_grads, preferred_element_type=F32).astype(BF16)
    total_pos = pair_sum(pos_part.reshape(8, slots // 8, width), 10).reshape(slots, width)

    got_wide, got_down, got_out = grad_exchange(
        jnp.concatenate([grad_qkv_weight, grad_up], axis=1).reshape(4, 4, e, 6 * e + 4 * fcols),
        grad_down.reshape(4, fcols, width),
        grad_out.reshape(2, e, width),
        11,
    )
    total_qkv = (
        got_wide[:, :, : 6 * e]
        .reshape(2, 4, e, 2, 3, e)
        .transpose(2, 4, 0, 3, 1, 5)
        .reshape(e, 3 * width)
        .astype(F32)
    )
    total_up = (
        got_wide[:, :, 6 * e :]
        .reshape(2, 4, e, 4, fcols)
        .transpose(2, 3, 1, 0, 4)
        .reshape(e, ff)
        .astype(F32)
    )
    total_down = got_down.reshape(2 * fcols, width).astype(F32)
    total_out = got_out.astype(F32)

    second_mask = is_second.astype(F32)
    type_one = jnp.sum(grad_embedded * second_mask, axis=0)
    type_zero = jnp.sum(grad_embedded * (1.0 - second_mask), axis=0)

    def spread(part):
        whole = jnp.zeros((1, 2, 4, e), F32)
        whole = lax.dynamic_update_slice(
            jnp.zeros((2, 2, 4, e), F32), part.reshape(1, 2, 1, e), (h, 0, g, 0)
        )
        return whole.reshape(width)

    stacked = jnp.stack(
        [
            spread(head_sums[:, 0]),
            spread(head_sums[:, 2]),
            grad_bias_branch,
            grad_shift_one,
            grad_bias_second,
            grad_shift_two,
            grad_gain_one,
            grad_gain_two,
            type_zero,
            type_one,
        ]
    )
    up_spread = lax.dynamic_update_slice(
        jnp.zeros((4, 4, 2, fcols), F32), grad_up_bias.reshape(4, 1, 1, fcols), (0, g, h, 0)
    ).reshape(blks, 4, e)
    vector_pack = jnp.concatenate(
        [stacked.reshape(10, blks, e).transpose(1, 0, 2), up_spread], axis=1
    ).reshape(blks, 7, 2 * e)
    vector_pack = jnp.pad(vector_pack, ((0, 0), (0, 1), (0, 0)))
    totals = small_scatter(vector_pack, blks, 12)[:7].reshape(14, e)
    return (
        layer_out,
        grad_hidden,
        total_pos,
        totals[8:10],
        total_qkv,
        total_out,
        total_up,
        total_down,
        totals[10:14].reshape(4 * e),
        totals[6:8],
        totals[:6],
    )


def planes_fit(hidden, head_axis, blk_axis):
    seqs, seg, width = hidden.shape
    return head_axis == 2 and blk_axis == HEADS and seqs == 2 and seqs * seg == 2 * width // HEADS


def on_device(hidden, *rest):
    if planes_fit(hidden, lax.axis_size("head"), lax.axis_size("blk")):
        return layer_in_planes(hidden, *rest)
    return layer_in_blocks(hidden, *rest)


def solution(mesh):
    in_specs = (
        P(None, ("head", "blk"), None),
        P(None, ("head", "blk")),
        P(None, ("head", "blk")),
        P(None, ("head", "blk"), None),
        P("blk", None),
        P(None, "blk"),
        P("blk", None),
        P("blk", None),
        P("blk", None),
        P("blk", None),
        P("blk"),
        P(None, "blk"),
        P(None, "blk"),
    )
    out_specs = (
        P(None, ("head", "blk"), None),
        P(None, ("head", "blk"), None),
        P("blk", None),
        P(None, "blk"),
        P("blk", None),
        P("blk", None),
        P("blk", None),
        P("blk", None),
        P("blk"),
        P(None, "blk"),
        P(None, "blk"),
    )
    return jax.shard_map(
        on_device, mesh=mesh, in_specs=in_specs, out_specs=out_specs, check_vma=False
    )
```

```python
import functools
import math

import jax
import jax.numpy as jnp
from jax import lax
from jax.experimental import pallas as pl
from jax.experimental.pallas import tpu as pltpu
from jax.sharding import PartitionSpec as P

HEADS = 16
MESH = pl.DeviceIdType.MESH
F32 = jnp.float32
BF16 = jnp.bfloat16
VSPEC = pl.BlockSpec(memory_space=pltpu.VMEM)


def place():
    h = lax.axis_index("head")
    b = lax.axis_index("blk")
    return h, b // 4, (b // 2) % 2, b % 2


def blk(o, y, c):
    return (o * 2 + y) * 2 + c


def peer(dx, dz, dy, dc):
    h, o, y, c = place()
    flip = lambda v, d: 1 - v if d else v
    return flip(h, dx), blk((o + dz) % 4 if dz else o, flip(y, dy), flip(c, dc))


def remote(src, dst, sems, index, device):
    return pltpu.make_async_remote_copy(
        src_ref=src,
        dst_ref=dst,
        send_sem=sems.at[0, index],
        recv_sem=sems.at[1, index],
        device_id=device,
        device_id_type=MESH,
    )


def landed(ref, sems, index):
    remote(ref, ref, sems, index, peer(1, 0, 0, 0)).wait_recv()


def sems(count):
    return pltpu.SemaphoreType.DMA((2, count))


NEAR_X, NEAR_Y, NEAR_C = (1, 0, 0, 0), (0, 0, 1, 0), (0, 0, 0, 1)
COLUMN = ((0, 1, 0, 0), (0, 2, 0, 0), (0, 3, 0, 0))
PLANE = tuple(
    (dx, 0, dy, dc) for dx in range(2) for dy in range(2) for dc in range(2) if dx or dy or dc
)


class Part:
    def __init__(self, run, ins, outs, scratch, peers):
        self.run, self.ins, self.outs, self.scratch, self.peers = run, ins, outs, scratch, peers


def fused(name, cid, parts, limit=None):
    peers = sorted({p for part in parts for p in part.peers})
    ins = [x for part in parts for x in part.ins]
    outs = [s for part in parts for s in part.outs]
    scratch = [s for part in parts for s in part.scratch]

    def kernel(*refs):
        in_refs, out_refs = refs[: len(ins)], refs[len(ins) : len(ins) + len(outs)]
        own = refs[len(ins) + len(outs) :]
        gens = []
        i = j = k = 0
        for part in parts:
            gens.append(
                part.run(
                    in_refs[i : i + len(part.ins)],
                    out_refs[j : j + len(part.outs)],
                    own[k : k + len(part.scratch)],
                )
            )
            i, j, k = i + len(part.ins), j + len(part.outs), k + len(part.scratch)
        barrier = pltpu.get_barrier_semaphore()
        for p in peers:
            pl.semaphore_signal(barrier, inc=1, device_id=peer(*p), device_id_type=MESH)
        pl.semaphore_wait(barrier, len(peers))
        for gen in gens:
            next(gen)
        for gen in gens:
            for _ in gen:
                pass

    got = pl.pallas_call(
        kernel,
        name=name,
        out_shape=[jax.ShapeDtypeStruct(s, d) for s, d in outs],
        in_specs=[VSPEC] * len(ins),
        out_specs=[VSPEC] * len(outs),
        scratch_shapes=scratch,
        compiler_params=pltpu.CompilerParams(
            collective_id=cid, has_side_effects=True, vmem_limit_bytes=limit
        ),
    )(*ins)
    result = []
    for part in parts:
        result.append(got[: len(part.outs)])
        got = got[len(part.outs) :]
    return result


def plane_gather(x):
    two, r, n = x.shape

    def run(ins, outs, own):
        (x_ref,), (out_ref,), (sem,) = ins, outs, own
        h, o, y, c = place()
        dev_x, dev_y, dev_c = peer(*NEAR_X), peer(*NEAR_Y), peer(*NEAR_C)
        mine = h * 4 + y * 2 + c
        of_x = (1 - h) * 4 + y * 2 + c
        of_y = h * 4 + (1 - y) * 2 + c
        of_d = (1 - h) * 4 + (1 - y) * 2 + c
        sent = []

        def go(src, slot, index, device, half):
            copy = remote(src.at[half], out_ref.at[half, slot], sem, index, device)
            copy.start()
            sent.append(copy)

        go(x_ref, mine, 0, dev_x, 0)
        go(x_ref, mine, 1, dev_y, 1)
        go(x_ref, mine, 2, dev_x, 1)
        go(x_ref, mine, 3, dev_y, 0)
        go(x_ref, mine, 4, dev_c, 0)
        go(x_ref, mine, 5, dev_c, 1)
        yield
        out_ref[:, pl.ds(mine, 1)] = x_ref[...][:, None]

        def relay(slot, half, index, device, onward, to_core):
            landed(out_ref.at[half, slot], sem, index)
            if onward is not None:
                go(out_ref.at[:, slot], slot, onward, device, half)
            go(out_ref.at[:, slot], slot, to_core, dev_c, half)

        relay(of_x, 0, 0, dev_y, 6, 8)
        relay(of_y, 1, 1, dev_x, 7, 9)
        relay(of_x, 1, 2, None, None, 10)
        relay(of_y, 0, 3, None, None, 11)
        relay(of_d, 0, 6, None, None, 12)
        relay(of_d, 1, 7, None, None, 13)
        flip = 1 - 2 * c
        for slot, half, index in (
            (mine, 0, 4),
            (mine, 1, 5),
            (of_x, 0, 8),
            (of_y, 1, 9),
            (of_x, 1, 10),
            (of_y, 0, 11),
            (of_d, 0, 12),
            (of_d, 1, 13),
        ):
            landed(out_ref.at[half, slot + flip], sem, index)
        for copy in sent:
            copy.wait_send()

    return Part(run, [x], [((2, 8, r, n), x.dtype)], [sems(14)], [NEAR_X, NEAR_Y, NEAR_C])


def plane_scatter(x):
    two, eight, r, n = x.shape

    def run(ins, outs, own):
        (x_ref,), (out_ref,), (near, part, from_x, from_y, diag, sem) = ins, outs, own
        h, o, y, c = place()
        dev_x, dev_y, dev_c = peer(*NEAR_X), peer(*NEAR_Y), peer(*NEAR_C)
        mine = h * 4 + y * 2 + c
        of_x = (1 - h) * 4 + y * 2 + c
        of_y = h * 4 + (1 - y) * 2 + c
        of_d = (1 - h) * 4 + (1 - y) * 2 + c
        flip = 1 - 2 * c
        sent = []

        def go(src, dst, index, device):
            copy = remote(src, dst, sem, index, device)
            copy.start()
            sent.append(copy)

        order = (of_d, of_x, of_y, mine)
        for half in range(2):
            go(x_ref.at[half, of_d + flip], near.at[0, half], half, dev_c)
        go(x_ref.at[0, of_x + flip], near.at[1, 0], 2, dev_c)
        go(x_ref.at[1, of_y + flip], near.at[2, 1], 5, dev_c)
        go(x_ref.at[1, of_x + flip], near.at[1, 1], 3, dev_c)
        go(x_ref.at[0, of_y + flip], near.at[2, 0], 4, dev_c)
        for half in range(2):
            go(x_ref.at[half, mine + flip], near.at[3, half], 6 + half, dev_c)
        yield

        def add(k, half):
            landed(near.at[k, half], sem, 2 * k + half)
            return x_ref[half, order[k]].astype(F32) + near[k, half].astype(F32)

        part[0, 0] = add(0, 0).astype(BF16)
        go(part.at[0, 0], diag.at[0], 8, dev_x)
        part[0, 1] = add(0, 1).astype(BF16)
        go(part.at[0, 1], diag.at[1], 9, dev_y)
        part[1, 0] = add(1, 0).astype(BF16)
        go(part.at[1, 0], from_x.at[0], 10, dev_x)
        part[2, 1] = add(2, 1).astype(BF16)
        go(part.at[2, 1], from_y.at[1], 11, dev_y)
        kept_x = add(1, 1)
        landed(diag.at[1], sem, 9)
        part[1, 1] = (kept_x + diag[1].astype(F32)).astype(BF16)
        go(part.at[1, 1], from_x.at[1], 12, dev_x)
        kept_y = add(2, 0)
        landed(diag.at[0], sem, 8)
        part[2, 0] = (kept_y + diag[0].astype(F32)).astype(BF16)
        go(part.at[2, 0], from_y.at[0], 13, dev_y)
        for half in range(2):
            out_ref[half] = add(3, half)
        for half, ix, iy in ((0, 10, 13), (1, 12, 11)):
            landed(from_x.at[half], sem, ix)
            landed(from_y.at[half], sem, iy)
            out_ref[half] += from_x[half].astype(F32) + from_y[half].astype(F32)
        for copy in sent:
            copy.wait_send()

    return Part(
        run,
        [x],
        [((2, r, n), F32)],
        [
            pltpu.VMEM((4, 2, r, n), BF16),
            pltpu.VMEM((3, 2, r, n), BF16),
            pltpu.VMEM((2, r, n), BF16),
            pltpu.VMEM((2, r, n), BF16),
            pltpu.VMEM((2, r, n), BF16),
            sems(14),
        ],
        [NEAR_X, NEAR_Y, NEAR_C],
    )


def exchange(x, peers, out_lead, source, target):
    peers = list(peers)

    def coords(p):
        h, o, y, c = place()
        flip = lambda v, d: 1 - v if d else v
        return flip(h, p[0]), (o + p[1]) % 4 if p[1] else o, flip(y, p[2]), flip(c, p[3])

    def run(ins, outs, own):
        (x_ref,), (out_ref,), (sem,) = ins, outs, own
        me = place()
        copies = []
        for k, p in enumerate(peers):
            copy = remote(
                source(x_ref, coords(p)), target(out_ref, me), sem, k, peer(*p)
            )
            copy.start()
            copies.append(copy)
        yield
        target(out_ref, me)[...] = source(x_ref, me)[...]
        for copy in copies:
            copy.wait()

    return Part(run, [x], [(out_lead, x.dtype)], [sems(len(peers))], peers)


def line_gather(x):
    return exchange(x, COLUMN, (4,) + x.shape, lambda r, d: r, lambda r, s: r.at[s[1]])


def blk_exchange(x):
    return exchange(
        x,
        [(0, 0, 1, 0), (0, 0, 0, 1), (0, 0, 1, 1)],
        x.shape,
        lambda r, d: r.at[d[2] * 2 + d[3]],
        lambda r, s: r.at[s[2] * 2 + s[3]],
    )


def small_gather(x):
    peers = [
        (0, dz, dy, dc) for dz in range(4) for dy in range(2) for dc in range(2) if dz or dy or dc
    ]
    return exchange(x, peers, (16,) + x.shape, lambda r, d: r, lambda r, s: r.at[blk(*s[1:])])


def pair_copy(x):
    return exchange(x, [NEAR_X], (2,) + x.shape, lambda r, d: r, lambda r, s: r.at[s[0]])


def line_sum(x):
    block = x.shape[1:]

    def run(ins, outs, own):
        (x_ref,), (out_ref,), (held, sem) = ins, outs, own
        o = place()[1]
        copies = []
        for k, p in enumerate(COLUMN):
            copy = remote(x_ref.at[(o + k + 1) % 4], held.at[k], sem, k, peer(*p))
            copy.start()
            copies.append(copy)
        yield
        for copy in copies:
            copy.wait()
        total = x_ref[o].astype(F32)
        for k in range(3):
            total += held[k].astype(F32)
        out_ref[...] = total.astype(BF16)

    return Part(
        run, [x], [(block, BF16)], [pltpu.VMEM((3,) + block, BF16), sems(3)], COLUMN
    )


def plane_spread(x, width, spots):
    four, r, n = x.shape
    lanes = 128
    pieces = n // lanes

    def run(ins, outs, own):
        (x_ref,), (out_ref,), (sem,) = ins, outs, own
        h, o, y, c = place()
        t = h * 4 + y * 2 + c
        columns = [
            out_ref.at[:, pl.ds(pl.multiple_of(lane * lanes, lanes), lanes)] for lane in spots(t)
        ]
        copies = []
        for k, p in enumerate(PLANE):
            to = (1 - y if p[2] else y) * 2 + (1 - c if p[3] else c)
            for i in range(pieces):
                src = x_ref.at[to, :, pl.ds(i * lanes, lanes)]
                copy = remote(src, columns[i], sem, k * pieces + i, peer(*p))
                copy.start()
                copies.append(copy)
        yield
        for i in range(pieces):
            columns[i][...] = x_ref[y * 2 + c, :, i * lanes : (i + 1) * lanes]
        for copy in copies:
            copy.wait()

    return Part(run, [x], [((r, width), x.dtype)], [sems(7 * pieces)], PLANE)


def place_copy(src, dst, send_sem, recv_sem, device):
    return pltpu.make_async_remote_copy(
        src_ref=src,
        dst_ref=dst,
        send_sem=send_sem,
        recv_sem=recv_sem,
        device_id=device,
        device_id_type=MESH,
    )


BLK = tuple(
    (0, dz, dy, dc) for dz in range(4) for dy in range(2) for dc in range(2) if dz or dy or dc
)


def out_weights(w):
    r, n = w.shape

    def run(ins, outs, own):
        (w_ref,), (out_ref,), (send, recv) = ins, outs, own
        h, o, y, c = place()
        has = o // 2 == h
        serves = (o % 2 == y) & (y == c)

        def each(act):
            for k in range(4):
                device = (h, blk((o + k) % 4, o % 2, y))
                copy = place_copy(w_ref, out_ref.at[c], send.at[k], recv.at[c], device)

                @pl.when(has if k else has & jnp.logical_not(serves))
                def _():
                    act(copy)

        each(lambda copy: copy.start())
        yield

        @pl.when(has & serves)
        def _():
            out_ref[pl.ds(c, 1)] = w_ref[...][None]

        each(lambda copy: copy.wait_send())
        for core in range(2):
            from_self = (o == 2 * h + y) & (y == c) & (c == core)
            ref = out_ref.at[core]

            @pl.when(jnp.logical_not(from_self))
            def _():
                place_copy(ref, ref, send.at[0], recv.at[core], (h, blk(o, y, c))).wait_recv()

    scratch = [pltpu.SemaphoreType.DMA((4,)), pltpu.SemaphoreType.DMA((2,))]
    return Part(run, [w], [((2, r, n), BF16)], scratch, BLK)


def out_grads(x):
    two, r, n = x.shape

    def run(ins, outs, own):
        (x_ref,), (out_ref,), (held, send, recv) = ins, outs, own
        h, o, y, c = place()
        has = o // 2 == h

        def each(act):
            for j in range(2):
                device = (h, blk(2 * h + y, c, j))
                copy = place_copy(x_ref.at[j], held.at[o], send.at[j], recv.at[o], device)

                @pl.when(jnp.logical_not((o == 2 * h + y) & (y == c) & (c == j)))
                def _():
                    act(copy)

        each(lambda copy: copy.start())
        yield
        out_ref[...] = jnp.zeros_like(out_ref)
        for z in range(4):
            mine = (z == o) & (o % 2 == y) & (y == c)

            @pl.when(has & mine)
            def _():
                out_ref[...] += x_ref[c].astype(F32)

            @pl.when(has & jnp.logical_not(mine))
            def _():
                ref = held.at[z]
                place_copy(ref, ref, send.at[0], recv.at[z], (h, blk(o, y, c))).wait_recv()
                out_ref[...] += held[z].astype(F32)

        each(lambda copy: copy.wait_send())

    scratch = [
        pltpu.VMEM((4, r, n), BF16),
        pltpu.SemaphoreType.DMA((2,)),
        pltpu.SemaphoreType.DMA((4,)),
    ]
    return Part(run, [x], [((r, n), F32)], scratch, BLK)


def mirrored():
    o = place()[1]
    far = o // 2
    seen = lambda v: v * (1 - 2 * far) + 3 * far
    return seen(o), seen


def rows_scatter(x):
    r, n = x.shape[3:]

    def run(ins, outs, own):
        (x_ref,), (out_ref,), (near, part, from_y, term, ends, mids, last, csem, ysem, zsem) = (
            ins,
            outs,
            own,
        )
        h, o, y, c = place()
        at, seen = mirrored()
        dev_y, dev_c = peer(*NEAR_Y), peer(*NEAR_C)
        order = [seen(3), seen(2), seen(1 - at), o]
        end, inner, other = (h, blk(seen(0), y, c)), (h, blk(seen(1), y, c)), (h, blk(seen(2), y, c))
        sent = []
        for i, yy in enumerate((1 - y, y)):
            for j, z in enumerate(order):
                copy = remote(x_ref.at[z, yy, 1 - c], near.at[i, j], csem, i * 4 + j, dev_c)
                copy.start()
                sent.append(copy)
        yield
        for j, z in enumerate(order):
            landed(near.at[0, j], csem, j)
            part[j] = x_ref[z, 1 - y, c] + near[0, j]
            copy = remote(part.at[j], from_y.at[j], ysem, j, dev_y)
            copy.start()
            sent.append(copy)
        for j, z in enumerate(order):
            landed(near.at[1, j], csem, 4 + j)
            landed(from_y.at[j], ysem, j)
            term[j] = x_ref[z, y, c] + near[1, j] + from_y[j]
            if j < 3:

                @pl.when(at == 0)
                def _():
                    remote(term.at[j], ends.at[j], zsem, j, inner).start()

            if j < 2:

                @pl.when(at == 1)
                def _():
                    landed(ends.at[j], zsem, j)
                    term[j] += ends[j]
                    remote(term.at[j], mids.at[j], zsem, 3 + j, other).start()

        @pl.when(at == 1)
        def _():
            landed(mids.at[0], zsem, 3)
            term[2] += mids[0]
            remote(term.at[2], last, zsem, 5, end).start()
            landed(ends.at[2], zsem, 2)
            landed(mids.at[1], zsem, 4)
            out_ref[...] = (term[3] + ends[2] + mids[1]).astype(F32)
            for j in range(2):
                remote(term.at[j], mids.at[j], zsem, 3 + j, other).wait_send()
            remote(term.at[2], last, zsem, 5, end).wait_send()

        @pl.when(at == 0)
        def _():
            landed(last, zsem, 5)
            out_ref[...] = (term[3] + last[...]).astype(F32)
            for j in range(3):
                remote(term.at[j], ends.at[j], zsem, j, inner).wait_send()

        for copy in sent:
            copy.wait_send()

    block = (r, n)
    scratch = [
        pltpu.VMEM((2, 4) + block, BF16),
        pltpu.VMEM((4,) + block, BF16),
        pltpu.VMEM((4,) + block, BF16),
        pltpu.VMEM((4,) + block, BF16),
        pltpu.VMEM((3,) + block, BF16),
        pltpu.VMEM((2,) + block, BF16),
        pltpu.VMEM(block, BF16),
        sems(8),
        sems(4),
        sems(6),
    ]
    return Part(run, [x], [(block, F32)], scratch, (NEAR_Y, NEAR_C) + COLUMN)


def blk_gather(x):
    r, n = x.shape

    def run(ins, outs, own):
        (x_ref,), (out_ref,), (zsem, ysem, csem) = ins, outs, own
        h, o, y, c = place()
        at, seen = mirrored()
        dev_y, dev_c = peer(*NEAR_Y), peer(*NEAR_C)
        end, inner, other = (h, blk(seen(0), y, c)), (h, blk(seen(1), y, c)), (h, blk(seen(2), y, c))
        sent = []

        def spot(z, yy=y, cc=c):
            return out_ref.at[z, yy, cc]

        def go(src, z, yy, sem, index, device):
            copy = remote(src, spot(z, yy), sem, index, device)
            copy.start()
            sent.append(copy)

        def line(src, z, index, device):
            return remote(src, spot(z), zsem, index, device)

        @pl.when(at == 0)
        def _():
            line(x_ref, o, 0, inner).start()

        @pl.when(at == 1)
        def _():
            line(x_ref, o, 1, end).start()
            line(x_ref, o, 2, other).start()

        go(x_ref, o, y, ysem, 0, dev_y)
        go(x_ref, o, y, csem, 0, dev_c)
        yield
        out_ref[o, y, c] = x_ref[...]

        def onward(j, z):
            go(spot(z), z, y, ysem, j, dev_y)
            go(spot(z), z, y, csem, j, dev_c)

        first = seen(1 - at)

        @pl.when(at == 0)
        def _():
            landed(spot(seen(1)), zsem, 1)

        @pl.when(at == 1)
        def _():
            landed(spot(seen(0)), zsem, 0)
            line(spot(seen(0)), seen(0), 3, other).start()

        onward(1, first)

        @pl.when(at == 0)
        def _():
            landed(spot(seen(2)), zsem, 4)

        @pl.when(at == 1)
        def _():
            landed(spot(seen(2)), zsem, 2)
            line(spot(seen(2)), seen(2), 4, end).start()

        onward(2, seen(2))

        @pl.when(at == 0)
        def _():
            landed(spot(seen(3)), zsem, 5)

        @pl.when(at == 1)
        def _():
            landed(spot(seen(3)), zsem, 3)
            line(spot(seen(3)), seen(3), 5, end).start()

        onward(3, seen(3))
        for j, z in enumerate((o, first, seen(2), seen(3))):
            landed(spot(z, 1 - y), ysem, j)
            go(spot(z, 1 - y), z, 1 - y, csem, 4 + j, dev_c)
        for j, z in enumerate((o, first, seen(2), seen(3))):
            landed(spot(z, y, 1 - c), csem, j)
            landed(spot(z, 1 - y, 1 - c), csem, 4 + j)

        @pl.when(at == 0)
        def _():
            line(x_ref, o, 0, inner).wait_send()

        @pl.when(at == 1)
        def _():
            line(x_ref, o, 1, end).wait_send()
            line(x_ref, o, 2, other).wait_send()
            line(spot(seen(0)), seen(0), 3, other).wait_send()
            line(spot(seen(2)), seen(2), 4, end).wait_send()
            line(spot(seen(3)), seen(3), 5, end).wait_send()

        for copy in sent:
            copy.wait_send()

    return Part(
        run,
        [x],
        [((4, 2, 2, r, n), x.dtype)],
        [sems(6), sems(4), sems(8)],
        (NEAR_Y, NEAR_C) + COLUMN,
    )


def pair_sum(x):
    n = x.shape[0]

    def run(ins, outs, own):
        (x_ref,), (out_ref,), (held, sem) = ins, outs, own
        copies = [remote(x_ref.at[k], held.at[k], sem, k, peer(*NEAR_X)) for k in range(n)]
        for copy in copies:
            copy.start()
        yield
        for k, copy in enumerate(copies):
            copy.wait()
            out_ref[k] = x_ref[k].astype(F32) + held[k].astype(F32)

    return Part(
        run, [x], [(x.shape, F32)], [pltpu.VMEM(x.shape, x.dtype), sems(n)], [NEAR_X]
    )


def small_scatter(x):
    peers = [
        (dx, dz, dy, dc)
        for dx in range(2)
        for dz in range(4)
        for dy in range(2)
        for dc in range(2)
        if dx or dz or dy or dc
    ]
    block = x.shape[1:]

    def run(ins, outs, own):
        (x_ref,), (out_ref,), (held, sem) = ins, outs, own
        h, o, y, c = place()
        copies = []
        for k, p in enumerate(peers):
            to = peer(*p)
            copy = remote(x_ref.at[to[1]], held.at[k], sem, k, to)
            copy.start()
            copies.append(copy)
        yield
        for copy in copies:
            copy.wait()
        out_ref[...] = x_ref[blk(o, y, c)] + jnp.sum(held[...], axis=0)

    return Part(
        run, [x], [(block, F32)], [pltpu.VMEM((31,) + block, F32), sems(31)], peers
    )


def attend(x, scale, cols=256):
    three, two, e, wide = x.shape
    n = wide // 2
    length = 4 * n

    def run(ins, outs, own):
        (x_ref,), (back_ref, held, o_ref, lse_ref), (keys, low, isem, osem) = ins, outs, own
        o = place()[1]
        copies = []
        for k, p in enumerate(COLUMN):
            z = (o + k + 1) % 4
            copy = remote(
                x_ref.at[:, z % 2, :, pl.ds(pl.multiple_of((z // 2) * n, n), n)],
                held.at[:, :, pl.ds(pl.multiple_of(o * n, n), n)],
                isem,
                k,
                peer(*p),
            )
            copy.start()
            copies.append(copy)
        yield
        mine = pl.ds(pl.multiple_of((o // 2) * n, n), n)
        held[:, :, pl.ds(pl.multiple_of(o * n, n), n)] = x_ref[:, o % 2, :, mine]
        for copy in copies:
            copy.wait()
        keys[...] = held[1].astype(F32).T.astype(BF16)

        def back(i, z):
            return remote(
                low.at[:, pl.ds(pl.multiple_of(z * n, n), n)],
                back_ref.at[o % 2, :, mine],
                osem,
                i,
                (place()[0], z * 4 + lax.axis_index("blk") % 4),
            )

        @pl.loop(0, 4 * (n // cols))
        def _(step):
            i = step // (n // cols)
            z = (o + 1 + i) % 4
            at = pl.ds(pl.multiple_of(z * n + step % (n // cols) * cols, cols), cols)
            q = (held[0, :, at].astype(F32) * scale).astype(BF16)
            s = jnp.dot(keys[...], q, preferred_element_type=F32)
            peak = jnp.max(s, axis=0, keepdims=True)
            p = jnp.exp(s - peak)
            total = jnp.sum(p, axis=0, keepdims=True)
            out = jnp.dot(held[2], p.astype(BF16), preferred_element_type=F32) / total
            o_ref[:, at] = out
            low[:, at] = out.astype(BF16)
            lse_ref[:, at] = peak + jnp.log(total)

            @pl.when((step % (n // cols) == n // cols - 1) & (i < 3))
            def _():
                back(i, z).start()

        back_ref[o % 2, :, mine] = low[:, pl.ds(pl.multiple_of(o * n, n), n)]
        for i in range(3):
            back(i, (o + 1 + i) % 4).wait_send()
            z = (o + 3 - i) % 4
            ref = back_ref.at[z % 2, :, pl.ds(pl.multiple_of((z // 2) * n, n), n)]
            landed(ref, osem, i)

    return Part(
        run,
        [x],
        [
            ((two, e, wide), BF16),
            ((three, e, length), BF16),
            ((e, length), F32),
            ((1, length), F32),
        ],
        [pltpu.VMEM((length, e), BF16), pltpu.VMEM((e, length), BF16), sems(3), sems(3)],
        COLUMN,
    )


def attend_back(g, held, out, lse, scale, rows=256):
    three, e, length = held.shape
    n = length // 4

    def run(ins, outs, own):
        (g_ref, held_ref, o_ref, lse_ref), (back_ref,) = ins, outs
        gs, qs, q_rows, g_rows, dq, delta, low, isem, ksem, qsem = own
        o = place()[1]
        copies = []
        for k, p in enumerate(COLUMN):
            z = (o + k + 1) % 4
            copy = remote(
                g_ref.at[z % 2, :, pl.ds(pl.multiple_of((z // 2) * n, n), n)],
                gs.at[:, pl.ds(pl.multiple_of(o * n, n), n)],
                isem,
                k,
                peer(*p),
            )
            copy.start()
            copies.append(copy)
        yield
        mine = pl.ds(pl.multiple_of((o // 2) * n, n), n)
        gs[:, pl.ds(pl.multiple_of(o * n, n), n)] = g_ref[o % 2, :, mine]
        q32 = held_ref[0].astype(F32) * scale
        qs[...] = q32.astype(BF16)
        q_rows[...] = q32.T.astype(BF16)
        dq[...] = jnp.zeros_like(dq)
        for copy in copies:
            copy.wait()
        g32 = gs[...].astype(F32)
        g_rows[...] = g32.T.astype(BF16)
        delta[...] = jnp.sum(g32 * o_ref[...], axis=0, keepdims=True)

        def back(part, sem, i, z):
            return remote(
                low.at[part, :, pl.ds(pl.multiple_of(z * n, n), n)],
                back_ref.at[part, o % 2, :, mine],
                sem,
                i,
                (place()[0], z * 4 + lax.axis_index("blk") % 4),
            )

        late = pl.ds(1, 2)
        steps = n // rows

        @pl.loop(0, 4 * steps)
        def _(step):
            i = step // steps
            z = (o + 1 + i) % 4
            at = pl.ds(pl.multiple_of(z * n + step % steps * rows, rows), rows)
            k_cols = held_ref[1, :, at]
            k_rows = k_cols.astype(F32).T.astype(BF16)
            v_rows = held_ref[2, :, at].astype(F32).T.astype(BF16)
            s = jnp.dot(k_rows, qs[...], preferred_element_type=F32)
            p = jnp.exp(s - lse_ref[...])
            dv = jnp.dot(p.astype(BF16), g_rows[...], preferred_element_type=F32)
            dp = jnp.dot(v_rows, gs[...], preferred_element_type=F32)
            ds = (p * (dp - delta[...])).astype(BF16)
            dk = jnp.dot(ds, q_rows[...], preferred_element_type=F32)
            dq[...] += jnp.dot(k_cols, ds, preferred_element_type=F32)
            low[1, :, at] = dk.T.astype(BF16)
            low[2, :, at] = dv.T.astype(BF16)

            @pl.when((step % steps == steps - 1) & (i < 3))
            def _():
                back(late, ksem, i, z).start()

        low[0] = (dq[...] * scale).astype(BF16)
        for i in range(3):
            back(pl.ds(0, 1), qsem, i, (o + 1 + i) % 4).start()
        back_ref[:, o % 2, :, mine] = low[:, :, pl.ds(pl.multiple_of(o * n, n), n)]
        for i in range(3):
            back(late, ksem, i, (o + 1 + i) % 4).wait_send()
            back(pl.ds(0, 1), qsem, i, (o + 1 + i) % 4).wait_send()
            z = (o + 3 - i) % 4
            there = pl.ds(pl.multiple_of((z // 2) * n, n), n)
            landed(back_ref.at[late, z % 2, :, there], ksem, i)
            landed(back_ref.at[pl.ds(0, 1), z % 2, :, there], qsem, i)

    return Part(
        run,
        [g, held, out, lse],
        [((three,) + g.shape, BF16)],
        [
            pltpu.VMEM((e, length), BF16),
            pltpu.VMEM((e, length), BF16),
            pltpu.VMEM((length, e), BF16),
            pltpu.VMEM((length, e), BF16),
            pltpu.VMEM((e, length), F32),
            pltpu.VMEM((1, length), F32),
            pltpu.VMEM((three, e, length), BF16),
            sems(3),
            sems(3),
            sems(3),
        ],
        COLUMN,
    )


def norm_layer(values_in, gain_row, offset_row):
    average = jnp.mean(values_in, axis=-1, keepdims=True)
    centred = values_in - average
    variance = jnp.mean(centred * centred, axis=-1, keepdims=True)
    return centred * lax.rsqrt(variance + 1e-12) * gain_row + offset_row


def gelu_exact(inner_product_sum):
    return jax.nn.gelu(inner_product_sum, approximate=False)


def widest_block(length, limit):
    return max(
        (candidate for candidate in range(1, min(length, limit) + 1) if length % candidate == 0)
    )


def block_scores(query_heads, key_block, score_scale):
    return (
        jnp.einsum("sqhe,skhe->shqk", query_heads, key_block, preferred_element_type=jnp.float32)
        * score_scale
    )


def key_side(query_block, grad_block, lse_block, delta_block, key_heads, value_heads, score_scale):
    scores = block_scores(query_block, key_heads, score_scale)
    weights = jnp.exp(scores - lse_block[..., None])
    more_values = jnp.einsum(
        "shqk,sqhe->shke",
        weights.astype(jnp.bfloat16),
        grad_block,
        preferred_element_type=jnp.float32,
    )
    grad_weights = jnp.einsum(
        "sqhe,skhe->shqk", grad_block, value_heads, preferred_element_type=jnp.float32
    )
    grad_scores = weights * (grad_weights - delta_block[..., None])
    more_keys = jnp.einsum(
        "shqk,sqhe->shke",
        grad_scores.astype(jnp.bfloat16),
        query_block,
        preferred_element_type=jnp.float32,
    )
    return (more_keys, more_values)


def forward_fold(query_heads, score_scale, head_count, head_size):

    def fold_keys(running, portion, offset):
        key_piece, value_piece = portion
        seq_count, length = (key_piece.shape[0], key_piece.shape[1])
        block_size = widest_block(length, 512)

        def one_step(block_index, carried):
            row_peak, row_total, weighted = carried
            row_start = block_index * block_size
            key_block = lax.dynamic_slice_in_dim(key_piece, row_start, block_size, 1).reshape(
                seq_count, block_size, head_count, head_size
            )
            value_block = lax.dynamic_slice_in_dim(value_piece, row_start, block_size, 1).reshape(
                seq_count, block_size, head_count, head_size
            )
            scores = block_scores(query_heads, key_block, score_scale)
            new_peak = jnp.maximum(row_peak, jnp.max(scores, axis=-1))
            shrink = jnp.exp(row_peak - new_peak)
            weights = jnp.exp(scores - new_peak[..., None])
            row_total = row_total * shrink + jnp.sum(weights, axis=-1)
            weighted = weighted * shrink[..., None] + jnp.einsum(
                "shqk,skhe->shqe",
                weights.astype(jnp.bfloat16),
                value_block,
                preferred_element_type=jnp.float32,
            )
            return (new_peak, row_total, weighted)

        return lax.fori_loop(0, length // block_size, one_step, running)

    return fold_keys


def query_fold(query_heads, grad_heads, log_totals, delta_rows, score_scale, head_count, head_size):

    def fold_keys(running, portion, offset):
        key_piece, value_piece = portion
        seq_count, length = (key_piece.shape[0], key_piece.shape[1])
        block_size = widest_block(length, 512)

        def one_step(block_index, weighted):
            row_start = block_index * block_size
            key_block = lax.dynamic_slice_in_dim(key_piece, row_start, block_size, 1).reshape(
                seq_count, block_size, head_count, head_size
            )
            value_block = lax.dynamic_slice_in_dim(value_piece, row_start, block_size, 1).reshape(
                seq_count, block_size, head_count, head_size
            )
            scores = block_scores(query_heads, key_block, score_scale)
            weights = jnp.exp(scores - log_totals[..., None])
            grad_weights = jnp.einsum(
                "sqhe,skhe->shqk", grad_heads, value_block, preferred_element_type=jnp.float32
            )
            grad_scores = weights * (grad_weights - delta_rows[..., None])
            return weighted + jnp.einsum(
                "shqk,skhe->shqe",
                grad_scores.astype(jnp.bfloat16),
                key_block,
                preferred_element_type=jnp.float32,
            )

        return lax.fori_loop(0, length // block_size, one_step, running)

    return fold_keys


def key_fold(key_heads, value_heads, score_scale, head_count, head_size):

    def fold_queries(running, portion, offset):
        query_piece, grad_piece, lse_piece, delta_piece = portion
        seq_count, length = (query_piece.shape[0], query_piece.shape[1])
        block_size = widest_block(length, 512)

        def one_step(block_index, carried):
            grad_keys, grad_values = carried
            row_start = block_index * block_size
            query_block = lax.dynamic_slice_in_dim(query_piece, row_start, block_size, 1).reshape(
                seq_count, block_size, head_count, head_size
            )
            grad_block = lax.dynamic_slice_in_dim(grad_piece, row_start, block_size, 1).reshape(
                seq_count, block_size, head_count, head_size
            )
            lse_block = lax.dynamic_slice_in_dim(lse_piece, row_start, block_size, 1).transpose(
                0, 2, 1
            )
            delta_block = lax.dynamic_slice_in_dim(delta_piece, row_start, block_size, 1).transpose(
                0, 2, 1
            )
            more_keys, more_values = key_side(
                query_block, grad_block, lse_block, delta_block, key_heads, value_heads, score_scale
            )
            return (grad_keys + more_keys, grad_values + more_values)

        return lax.fori_loop(0, length // block_size, one_step, running)

    return fold_queries


def layer_in_blocks(
    hidden,
    pos_ids,
    type_ids,
    cotangent,
    pos_table,
    type_table,
    query_key_value_weight,
    attention_output_weight,
    up_projection_weight,
    down_projection_weight,
    up_projection_bias,
    norm_gains,
    biases,
):
    seq_count, seg_tokens, model_width = hidden.shape
    row_count = seq_count * seg_tokens
    head_count = HEADS // lax.axis_size("head")
    head_size = model_width // HEADS
    local_width = head_count * head_size
    query_rows = lax.axis_size("head") * seg_tokens
    score_scale = 1.0 / math.sqrt(head_size)

    def fetch_weights():
        return (
            lax.all_gather(query_key_value_weight, "blk", axis=0, tiled=True),
            lax.all_gather(attention_output_weight, "blk", axis=0, tiled=True),
            lax.all_gather(up_projection_weight, "blk", axis=0, tiled=True),
            lax.all_gather(down_projection_weight, "blk", axis=0, tiled=True),
            lax.all_gather(up_projection_bias, "blk", axis=0, tiled=True),
            lax.all_gather(norm_gains, "blk", axis=1, tiled=True),
            lax.all_gather(biases, "blk", axis=1, tiled=True),
            lax.all_gather(type_table, "blk", axis=1, tiled=True),
        )

    qkv_full, out_full, up_full, down_full, up_bias_full, gain_full, bias_full, type_full = (
        fetch_weights()
    )
    bias_float = bias_full.astype(jnp.float32)
    gain_float = gain_full.astype(jnp.float32)
    flat_pos = pos_ids.reshape(row_count)
    portion = lax.all_gather(pos_table, "blk", axis=0, tiled=True)
    local_slots = flat_pos
    onehot = (
        local_slots[:, None] == jnp.arange(portion.shape[0], dtype=jnp.int32)[None, :]
    ).astype(jnp.bfloat16)
    positions = jnp.dot(onehot, portion, preferred_element_type=jnp.float32)
    is_second = type_ids.reshape(row_count, 1) == 1
    typed_rows = jnp.where(
        is_second, type_full[1].astype(jnp.float32), type_full[0].astype(jnp.float32)
    )
    embedded_tokens = (
        hidden.reshape(row_count, model_width).astype(jnp.float32) + positions + typed_rows
    )
    embedded_low = embedded_tokens.astype(jnp.bfloat16)
    projected_rows = jnp.dot(embedded_low, qkv_full, preferred_element_type=jnp.float32)
    token_shape = (seq_count, seg_tokens, model_width)
    queries = (
        (projected_rows[:, :model_width] + bias_float[0]).astype(jnp.bfloat16).reshape(token_shape)
    )
    keys_token = (
        projected_rows[:, model_width : 2 * model_width].astype(jnp.bfloat16).reshape(token_shape)
    )
    values_token = (
        (projected_rows[:, 2 * model_width :] + bias_float[1])
        .astype(jnp.bfloat16)
        .reshape(token_shape)
    )
    query_local, key_local, value_local = (
        lax.all_to_all(queries, "head", split_axis=2, concat_axis=1, tiled=True),
        lax.all_to_all(keys_token, "head", split_axis=2, concat_axis=1, tiled=True),
        lax.all_to_all(values_token, "head", split_axis=2, concat_axis=1, tiled=True),
    )
    head_shape = (seq_count, query_rows, head_count, head_size)
    query_heads = query_local.reshape(head_shape)
    key_heads = key_local.reshape(head_shape)
    value_heads = value_local.reshape(head_shape)
    start_peak = jnp.full((seq_count, head_count, query_rows), -jnp.inf, jnp.float32)
    start_total = jnp.zeros((seq_count, head_count, query_rows), jnp.float32)
    zero_heads = jnp.zeros((seq_count, head_count, query_rows, head_size), jnp.float32)
    fold_keys = forward_fold(query_heads, score_scale, head_count, head_size)
    row_peak, row_total, weighted = fold_keys(
        (start_peak, start_total, zero_heads),
        (
            lax.all_gather(key_local, "blk", axis=1, tiled=True),
            lax.all_gather(value_local, "blk", axis=1, tiled=True),
        ),
        jnp.int32(0),
    )
    log_totals = row_peak + jnp.log(row_total)
    attention_result = weighted / row_total[..., None]
    attended_low = (
        attention_result.transpose(0, 2, 1, 3)
        .reshape(seq_count, query_rows, local_width)
        .astype(jnp.bfloat16)
    )
    attended_token = lax.all_to_all(
        attended_low, "head", split_axis=1, concat_axis=2, tiled=True
    ).reshape(row_count, model_width)
    residual_branch = (
        jnp.dot(attended_token, out_full, preferred_element_type=jnp.float32) + bias_float[2]
    )
    first_layer_norm, first_pull = jax.vjp(
        norm_layer, embedded_tokens + residual_branch, gain_float[0], bias_float[3]
    )
    first_low = first_layer_norm.astype(jnp.bfloat16)
    inner_product_sum = jnp.dot(
        first_low, up_full, preferred_element_type=jnp.float32
    ) + up_bias_full.astype(jnp.float32)
    gelu_activations, gelu_pull = jax.vjp(gelu_exact, inner_product_sum)
    activated_low = gelu_activations.astype(jnp.bfloat16)
    second_layer_norm = (
        jnp.dot(activated_low, down_full, preferred_element_type=jnp.float32) + bias_float[4]
    )
    final_norm, final_pull = jax.vjp(
        norm_layer, first_layer_norm + second_layer_norm, gain_float[1], bias_float[5]
    )
    layer_out = final_norm.astype(jnp.bfloat16).reshape(token_shape)
    qkv_full, out_full, up_full, down_full, up_bias_full, gain_full, bias_full, type_full = (
        fetch_weights()
    )
    grad_final, grad_gain_two, grad_shift_two = final_pull(
        cotangent.reshape(row_count, model_width).astype(jnp.float32)
    )
    grad_second = grad_final.astype(jnp.bfloat16)
    grad_down = jnp.einsum(
        "rf,rd->fd", activated_low, grad_second, preferred_element_type=jnp.float32
    )
    grad_bias_second = jnp.sum(grad_second.astype(jnp.float32), axis=0)
    (grad_inner,) = gelu_pull(
        jnp.einsum("rd,fd->rf", grad_second, down_full, preferred_element_type=jnp.float32)
    )
    grad_inner_low = grad_inner.astype(jnp.bfloat16)
    grad_up = jnp.einsum("rd,rf->df", first_low, grad_inner_low, preferred_element_type=jnp.float32)
    grad_up_bias = jnp.sum(grad_inner_low.astype(jnp.float32), axis=0)
    grad_first = grad_final + jnp.einsum(
        "rf,df->rd", grad_inner_low, up_full, preferred_element_type=jnp.float32
    )
    grad_resid, grad_gain_one, grad_shift_one = first_pull(grad_first)
    grad_branch = grad_resid.astype(jnp.bfloat16)
    grad_out = jnp.einsum(
        "re,rd->ed", attended_token, grad_branch, preferred_element_type=jnp.float32
    )
    grad_bias_branch = jnp.sum(grad_branch.astype(jnp.float32), axis=0)
    grad_attended = (
        jnp.einsum("rd,ed->re", grad_branch, out_full, preferred_element_type=jnp.float32)
        .astype(jnp.bfloat16)
        .reshape(token_shape)
    )
    grad_local = lax.all_to_all(grad_attended, "head", split_axis=2, concat_axis=1, tiled=True)
    grad_heads = grad_local.reshape(head_shape)
    delta_rows = jnp.sum(
        grad_heads.astype(jnp.float32).transpose(0, 2, 1, 3) * attention_result, axis=-1
    )
    fold_queries = query_fold(
        query_heads, grad_heads, log_totals, delta_rows, score_scale, head_count, head_size
    )
    grad_query_sum = fold_queries(
        zero_heads,
        (
            lax.all_gather(key_local, "blk", axis=1, tiled=True),
            lax.all_gather(value_local, "blk", axis=1, tiled=True),
        ),
        jnp.int32(0),
    )
    fold_side = key_fold(key_heads, value_heads, score_scale, head_count, head_size)
    grad_key_sum, grad_value_sum = fold_side(
        (zero_heads, zero_heads),
        (
            lax.all_gather(query_local.astype(jnp.float32), "blk", axis=1, tiled=True).astype(
                jnp.bfloat16
            ),
            lax.all_gather(grad_local.astype(jnp.float32), "blk", axis=1, tiled=True).astype(
                jnp.bfloat16
            ),
            lax.all_gather(log_totals.transpose(0, 2, 1), "blk", axis=1, tiled=True),
            lax.all_gather(delta_rows.transpose(0, 2, 1), "blk", axis=1, tiled=True),
        ),
        jnp.int32(0),
    )
    grad_keys_local = (
        (grad_key_sum * score_scale)
        .transpose(0, 2, 1, 3)
        .reshape(seq_count, query_rows, local_width)
        .astype(jnp.bfloat16)
    )
    grad_values_local = (
        grad_value_sum.transpose(0, 2, 1, 3)
        .reshape(seq_count, query_rows, local_width)
        .astype(jnp.bfloat16)
    )
    grad_query_local = (
        (grad_query_sum * score_scale)
        .transpose(0, 2, 1, 3)
        .reshape(seq_count, query_rows, local_width)
        .astype(jnp.bfloat16)
    )
    grad_query_token, grad_key_token, grad_value_token = (
        lax.all_to_all(grad_query_local, "head", split_axis=1, concat_axis=2, tiled=True),
        lax.all_to_all(grad_keys_local, "head", split_axis=1, concat_axis=2, tiled=True),
        lax.all_to_all(grad_values_local, "head", split_axis=1, concat_axis=2, tiled=True),
    )
    grad_qkv = jnp.concatenate(
        [grad_query_token, grad_key_token, grad_value_token], axis=-1
    ).reshape(row_count, 3 * model_width)
    grad_qkv_full = jnp.einsum(
        "rd,rf->df", embedded_low, grad_qkv, preferred_element_type=jnp.float32
    )
    grad_bias_query = jnp.sum(
        grad_query_token.astype(jnp.float32).reshape(row_count, model_width), axis=0
    )
    grad_bias_value = jnp.sum(
        grad_value_token.astype(jnp.float32).reshape(row_count, model_width), axis=0
    )
    grad_embedded = grad_resid + jnp.einsum(
        "rf,df->rd", grad_qkv, qkv_full, preferred_element_type=jnp.float32
    )
    second_mask = is_second.astype(jnp.float32)
    grad_type_one = jnp.sum(grad_embedded * second_mask, axis=0)
    grad_type_zero = jnp.sum(grad_embedded * (1.0 - second_mask), axis=0)
    length = lax.axis_size("blk") * pos_table.shape[0]
    local_slots = flat_pos
    inside = (local_slots >= 0) & (local_slots < length)
    slot_index = jnp.where(inside, local_slots, length)
    buffer = jnp.zeros((length + 1, model_width), jnp.float32).at[slot_index].add(grad_embedded)
    grad_positions = lax.psum_scatter(buffer[:length], "blk", scatter_dimension=0, tiled=True)
    gain_stack = jnp.stack([grad_gain_one, grad_gain_two])
    bias_stack = jnp.stack(
        [
            grad_bias_query,
            grad_bias_value,
            grad_bias_branch,
            grad_shift_one,
            grad_bias_second,
            grad_shift_two,
        ]
    )
    type_stack = jnp.stack([grad_type_zero, grad_type_one])
    (
        shard_qkv,
        shard_out,
        shard_up,
        shard_down,
        shard_up_bias,
        shard_gains,
        shard_biases,
        shard_types,
    ) = (
        lax.psum_scatter(grad_qkv_full, "blk", scatter_dimension=0, tiled=True),
        lax.psum_scatter(grad_out, "blk", scatter_dimension=0, tiled=True),
        lax.psum_scatter(grad_up, "blk", scatter_dimension=0, tiled=True),
        lax.psum_scatter(grad_down, "blk", scatter_dimension=0, tiled=True),
        lax.psum_scatter(grad_up_bias, "blk", scatter_dimension=0, tiled=True),
        lax.psum_scatter(gain_stack, "blk", scatter_dimension=1, tiled=True),
        lax.psum_scatter(bias_stack, "blk", scatter_dimension=1, tiled=True),
        lax.psum_scatter(type_stack, "blk", scatter_dimension=1, tiled=True),
    )
    (
        total_qkv,
        total_out,
        total_up,
        total_down,
        total_up_bias,
        total_gains,
        total_biases,
        total_types,
        total_positions,
    ) = lax.psum(
        (
            shard_qkv,
            shard_out,
            shard_up,
            shard_down,
            shard_up_bias,
            shard_gains,
            shard_biases,
            shard_types,
            grad_positions,
        ),
        "head",
    )
    grad_hidden = grad_embedded.reshape(token_shape)
    return (
        layer_out,
        grad_hidden,
        total_positions,
        total_types,
        total_qkv,
        total_out,
        total_up,
        total_down,
        total_up_bias,
        total_gains,
        total_biases,
    )


BIG = 56 << 20


def layer_in_planes(
    hidden,
    pos_ids,
    type_ids,
    cotangent,
    pos_table,
    type_table,
    query_key_value_weight,
    attention_output_weight,
    up_projection_weight,
    down_projection_weight,
    up_projection_bias,
    norm_gains,
    biases,
):
    seqs, seg, width = hidden.shape
    blks = lax.axis_size("blk")
    h = lax.axis_index("head")
    b = lax.axis_index("blk")
    o, g = b // 4, b % 4
    rows = seqs * seg
    e = width // HEADS
    ff = up_projection_weight.shape[1]
    scale = 1.0 / math.sqrt(e)
    slots = pos_table.shape[0]
    fcols = ff // blks // 2
    plane_rows = 8 * rows

    small = jnp.concatenate(
        [
            biases.astype(F32),
            norm_gains.astype(F32),
            type_table.astype(F32),
            up_projection_bias.astype(F32).reshape(4, e),
        ]
    ).reshape(7, 2 * e)
    packed = jnp.concatenate([small, pos_ids.astype(F32).reshape(1, rows)])
    qkv_cut = query_key_value_weight.reshape(e, 3, 2, 4, 2 * e)
    qkv_cut = lax.dynamic_slice_in_dim(qkv_cut, h, 1, 2).reshape(e, 3, 4, 2 * e)
    qkv_cut = qkv_cut.transpose(2, 0, 1, 3).reshape(4, e, 6 * e)
    up_cut = up_projection_weight.reshape(e, 4, 4, 2, fcols)
    up_cut = lax.dynamic_slice_in_dim(up_cut, h, 1, 3).reshape(e, 4, 4, fcols)
    up_cut = up_cut.transpose(2, 0, 1, 3).reshape(4, e, 4 * fcols)
    down_cut = lax.dynamic_slice_in_dim(down_projection_weight, h * fcols, fcols, 0)
    half_down, half_up = fcols // 2, 2 * fcols
    (everyone,), (out_all,), (qkv_cut,), (up_cut,) = fused(
        "opening",
        0,
        [
            small_gather(packed),
            out_weights(attention_output_weight),
            blk_exchange(qkv_cut),
            blk_exchange(up_cut),
        ],
    )
    out_own = out_all.reshape(2 * e, width)
    params = everyone[:, :7].reshape(blks, 14, e).transpose(1, 0, 2)
    vectors = params[:10].reshape(10, width)
    bias_float, gain_float, type_float = vectors[:6], vectors[6:8], vectors[8:10]
    up_bias = lax.dynamic_slice_in_dim(
        params[10:].transpose(1, 0, 2).reshape(4, 4, 2, fcols), h, 1, 2
    )
    up_bias = lax.dynamic_slice_in_dim(up_bias, g, 1, 1).reshape(1, 4 * fcols)
    all_ids = everyone[:, 7].astype(jnp.int32)

    local_ids = all_ids.reshape(blks * rows, 1) - b * slots
    onehot = (local_ids == lax.broadcasted_iota(jnp.int32, (1, slots), 1)).astype(BF16)
    found = jnp.dot(onehot, pos_table, preferred_element_type=F32).astype(BF16)
    (positions,), (qkv_all,) = fused(
        "rows", 1, [rows_scatter(found.reshape(4, 2, 2, rows, width)), line_gather(qkv_cut)], BIG
    )
    qkv_own = qkv_all.reshape(width, 6 * e)
    is_second = type_ids.reshape(rows, 1) == 1
    typed = jnp.where(is_second, type_float[1], type_float[0])
    embedded = hidden.reshape(rows, width).astype(F32) + positions + typed
    token_shape = (seqs, seg, width)

    (plane_low,), (up_first,) = fused(
        "gather_tokens",
        2,
        [
            plane_gather(embedded.astype(BF16).reshape(token_shape)),
            line_gather(up_cut[:, :, :half_up]),
        ],
    )
    plane_low = plane_low.reshape(plane_rows, width)
    bias_heads = bias_float.reshape(6, 8, 2 * e)
    bias_heads = lax.dynamic_slice_in_dim(bias_heads, h * 4 + g, 1, 1)[:, 0]
    qkv_bias = jnp.concatenate(
        [bias_heads[0], jnp.zeros_like(bias_heads[0]), bias_heads[1]]
    ).reshape(6 * e, 1)
    projected = (
        jnp.einsum("kf,rk->fr", qkv_own, plane_low, preferred_element_type=F32) + qkv_bias
    ).astype(BF16)
    (attended, pair_qkv, pair_out, lse), (down_first,) = fused(
        "attend",
        3,
        [
            attend(projected.reshape(3, 2, e, plane_rows), scale),
            line_gather(down_cut[:half_down]),
        ],
        BIG,
    )
    attended = attended.reshape(2 * e, plane_rows)
    branch = jnp.einsum("fr,fd->rd", attended, out_own, preferred_element_type=F32).astype(BF16)
    (branch,), (up_second,) = fused(
        "scatter_branch",
        4,
        [
            plane_scatter(branch.reshape(seqs, 8, seg, width)),
            line_gather(up_cut[:, :, half_up:]),
        ],
    )
    branch = branch.reshape(rows, width)
    first, first_pull = jax.vjp(
        norm_layer, embedded + (branch + bias_float[2]), gain_float[0], bias_float[3]
    )

    (first_low,), (down_second,) = fused(
        "gather_first",
        5,
        [
            plane_gather(first.astype(BF16).reshape(token_shape)),
            line_gather(down_cut[half_down:]),
        ],
    )
    first_low = first_low.reshape(plane_rows, width)
    up_own = jnp.concatenate([up_first, up_second], axis=3).reshape(width, 4 * fcols)
    down_own = jnp.concatenate([down_first, down_second], axis=1).reshape(4 * fcols, width)
    inner = jnp.dot(first_low, up_own, preferred_element_type=F32) + up_bias
    activated, gelu_pull = jax.vjp(gelu_exact, inner)
    activated_low = activated.astype(BF16)
    second = jnp.dot(activated_low, down_own, preferred_element_type=F32).astype(BF16)
    ((second,),) = fused("scatter_second", 6, [plane_scatter(second.reshape(seqs, 8, seg, width))])
    second = second.reshape(rows, width)
    final, final_pull = jax.vjp(
        norm_layer, first + (second + bias_float[4]), gain_float[1], bias_float[5]
    )
    layer_out = final.astype(BF16).reshape(token_shape)

    grad_final, grad_gain_two, grad_shift_two = final_pull(
        cotangent.reshape(rows, width).astype(F32)
    )
    grad_low = grad_final.astype(BF16)
    grad_bias_second = jnp.sum(grad_low.astype(F32), axis=0)
    ((plane_grad,),) = fused("gather_grad", 7, [plane_gather(grad_low.reshape(token_shape))])
    plane_grad = plane_grad.reshape(plane_rows, width)
    grad_down = jnp.einsum(
        "rf,rd->fd", activated_low, plane_grad, preferred_element_type=F32
    ).astype(BF16)
    (grad_inner,) = gelu_pull(
        jnp.einsum("rd,fd->rf", plane_grad, down_own, preferred_element_type=F32)
    )
    grad_inner_low = grad_inner.astype(BF16)
    grad_up = jnp.einsum(
        "rd,rf->df", first_low, grad_inner_low, preferred_element_type=F32
    ).astype(BF16)
    grad_up_bias = jnp.sum(grad_inner_low.astype(F32), axis=0)
    grad_first = jnp.einsum(
        "rf,df->rd", grad_inner_low, up_own, preferred_element_type=F32
    ).astype(BF16)
    grad_up = grad_up.reshape(4, 4, e, 4 * fcols)
    grad_down = grad_down.reshape(4, fcols, width)
    (grad_first,), (down_one,), (up_one,) = fused(
        "scatter_first",
        8,
        [
            plane_scatter(grad_first.reshape(seqs, 8, seg, width)),
            line_sum(grad_down[:, :half_down]),
            line_sum(grad_up[:, :, :, :half_up]),
        ],
    )
    grad_first = grad_first.reshape(rows, width)
    grad_resid, grad_gain_one, grad_shift_one = first_pull(grad_final + grad_first)
    branch_low = grad_resid.astype(BF16)
    grad_bias_branch = jnp.sum(branch_low.astype(F32), axis=0)
    (plane_branch,), (down_two,), (up_two,) = fused(
        "gather_branch",
        9,
        [
            plane_gather(branch_low.reshape(token_shape)),
            line_sum(grad_down[:, half_down:]),
            line_sum(grad_up[:, :, :, half_up:]),
        ],
    )
    plane_branch = plane_branch.reshape(plane_rows, width)
    grad_out = jnp.einsum(
        "fr,rd->fd", attended, plane_branch, preferred_element_type=F32
    ).astype(BF16)
    grad_attended = jnp.einsum(
        "fd,rd->fr", out_own, plane_branch, preferred_element_type=F32
    ).astype(BF16)
    (grad_qkv,), (out_total,), (got_up,), (got_down,) = fused(
        "attend_back",
        10,
        [
            attend_back(grad_attended.reshape(2, e, plane_rows), pair_qkv, pair_out, lse, scale),
            out_grads(grad_out.reshape(2, e, width)),
            plane_spread(
                jnp.concatenate([up_one, up_two], axis=2),
                ff,
                lambda t: [(i * 4 + t % 4) * 2 + t // 4 for i in range(4)],
            ),
            pair_copy(jnp.concatenate([down_one, down_two], axis=0)),
        ],
        BIG,
    )
    grad_qkv = grad_qkv.reshape(6 * e, plane_rows)
    grad_qkv_weight = jnp.einsum(
        "rk,fr->kf", plane_low, grad_qkv, preferred_element_type=F32
    ).astype(BF16)
    head_sums = jnp.sum(grad_qkv.astype(F32), axis=1).reshape(3, 2 * e)
    back = jnp.einsum("fr,kf->rk", grad_qkv, qkv_own, preferred_element_type=F32).astype(BF16)
    (back,), (qkv_total,), (got_out,) = fused(
        "scatter_back",
        11,
        [
            plane_scatter(back.reshape(seqs, 8, seg, width)),
            line_sum(grad_qkv_weight.reshape(4, 4, e, 6 * e)),
            pair_copy(out_total.astype(BF16)),
        ],
    )
    grad_embedded = grad_resid + back.reshape(rows, width)
    grad_hidden = grad_embedded.reshape(token_shape)

    second_mask = is_second.astype(F32)
    type_one = jnp.sum(grad_embedded * second_mask, axis=0)
    type_zero = jnp.sum(grad_embedded * (1.0 - second_mask), axis=0)

    def spread(part):
        whole = lax.dynamic_update_slice(
            jnp.zeros((8, 2 * e), F32), part.reshape(1, 2 * e), (h * 4 + g, 0)
        )
        return whole.reshape(width)

    stacked = jnp.stack(
        [
            spread(head_sums[0]),
            spread(head_sums[2]),
            grad_bias_branch,
            grad_shift_one,
            grad_bias_second,
            grad_shift_two,
            grad_gain_one,
            grad_gain_two,
            type_zero,
            type_one,
        ]
    )
    up_spread = lax.dynamic_update_slice(
        jnp.zeros((4, 4, 2, fcols), F32), grad_up_bias.reshape(4, 1, 1, fcols), (0, g, h, 0)
    ).reshape(blks, 4, e)
    vector_pack = jnp.concatenate(
        [stacked.reshape(10, blks, e).transpose(1, 0, 2), up_spread], axis=1
    ).reshape(blks, 7, 2 * e)
    vector_pack = jnp.pad(vector_pack, ((0, 0), (0, 1), (0, 0)))

    (all_grads,), (totals,), (got_qkv,) = fused(
        "closing",
        12,
        [
            blk_gather(grad_embedded.astype(BF16)),
            small_scatter(vector_pack),
            plane_spread(qkv_total, 3 * width, lambda t: [i * 8 + t for i in range(3)]),
        ],
    )
    totals = totals[:7].reshape(14, e)
    all_grads = all_grads.reshape(blks * rows, width)
    flat_ids = all_ids.reshape(1, blks * rows) - b * slots
    pick = (flat_ids == lax.broadcasted_iota(jnp.int32, (slots, 1), 0)).astype(BF16)
    pos_part = jnp.dot(pick, all_grads, preferred_element_type=F32).astype(BF16)
    ((total_pos,),) = fused("pos_sum", 13, [pair_sum(pos_part.reshape(8, slots // 8, width))])
    total_pos = total_pos.reshape(slots, width)
    total_qkv = got_qkv.astype(F32)
    total_up = got_up.astype(F32)
    total_down = got_down.reshape(2 * fcols, width).astype(F32)
    total_out = lax.dynamic_index_in_dim(got_out, o // 2, 0, False).astype(F32)
    return (
        layer_out,
        grad_hidden,
        total_pos,
        totals[8:10],
        total_qkv,
        total_out,
        total_up,
        total_down,
        totals[10:14].reshape(4 * e),
        totals[6:8],
        totals[:6],
    )


def planes_fit(hidden, head_axis, blk_axis):
    seqs, seg, width = hidden.shape
    return head_axis == 2 and blk_axis == HEADS and seqs == 2 and seqs * seg == 2 * width // HEADS


def on_device(hidden, *rest):
    if planes_fit(hidden, lax.axis_size("head"), lax.axis_size("blk")):
        return layer_in_planes(hidden, *rest)
    return layer_in_blocks(hidden, *rest)


def solution(mesh):
    in_specs = (
        P(None, ("head", "blk"), None),
        P(None, ("head", "blk")),
        P(None, ("head", "blk")),
        P(None, ("head", "blk"), None),
        P("blk", None),
        P(None, "blk"),
        P("blk", None),
        P("blk", None),
        P("blk", None),
        P("blk", None),
        P("blk"),
        P(None, "blk"),
        P(None, "blk"),
    )
    out_specs = (
        P(None, ("head", "blk"), None),
        P(None, ("head", "blk"), None),
        P("blk", None),
        P(None, "blk"),
        P("blk", None),
        P("blk", None),
        P("blk", None),
        P("blk", None),
        P("blk"),
        P(None, "blk"),
        P(None, "blk"),
    )
    return jax.shard_map(
        on_device, mesh=mesh, in_specs=in_specs, out_specs=out_specs, check_vma=False
    )
```

```python
import functools
import math

import jax
import jax.numpy as jnp
from jax import lax
from jax.experimental import pallas as pl
from jax.experimental.pallas import tpu as pltpu
from jax.sharding import PartitionSpec as P

HEADS = 16
MESH = pl.DeviceIdType.MESH
F32 = jnp.float32
BF16 = jnp.bfloat16
VSPEC = pl.BlockSpec(memory_space=pltpu.VMEM)


def place():
    h = lax.axis_index("head")
    b = lax.axis_index("blk")
    return h, b // 4, (b // 2) % 2, b % 2


def blk(o, y, c):
    return (o * 2 + y) * 2 + c


def peer(dx, dz, dy, dc):
    h, o, y, c = place()
    flip = lambda v, d: 1 - v if d else v
    return flip(h, dx), blk((o + dz) % 4 if dz else o, flip(y, dy), flip(c, dc))


def remote(src, dst, sems, index, device):
    return pltpu.make_async_remote_copy(
        src_ref=src,
        dst_ref=dst,
        send_sem=sems.at[0, index],
        recv_sem=sems.at[1, index],
        device_id=device,
        device_id_type=MESH,
    )


def landed(ref, sems, index):
    remote(ref, ref, sems, index, peer(1, 0, 0, 0)).wait_recv()


def sems(count):
    return pltpu.SemaphoreType.DMA((2, count))


NEAR_X, NEAR_Y, NEAR_C = (1, 0, 0, 0), (0, 0, 1, 0), (0, 0, 0, 1)
COLUMN = ((0, 1, 0, 0), (0, 2, 0, 0), (0, 3, 0, 0))
PLANE = tuple(
    (dx, 0, dy, dc) for dx in range(2) for dy in range(2) for dc in range(2) if dx or dy or dc
)


class Part:
    def __init__(self, run, ins, outs, scratch, peers):
        self.run, self.ins, self.outs, self.scratch, self.peers = run, ins, outs, scratch, peers
        self.turns = ()

    def on(self, *turns):
        self.turns = turns
        return self


def fused(name, cid, parts, limit=None):
    peers = sorted({p for part in parts for p in part.peers})
    ins = [x for part in parts for x in part.ins]
    outs = [s for part in parts for s in part.outs]
    scratch = [s for part in parts for s in part.scratch]

    def kernel(*refs):
        in_refs, out_refs = refs[: len(ins)], refs[len(ins) : len(ins) + len(outs)]
        own = refs[len(ins) + len(outs) :]
        gens = []
        i = j = k = 0
        for part in parts:
            gens.append(
                part.run(
                    in_refs[i : i + len(part.ins)],
                    out_refs[j : j + len(part.outs)],
                    own[k : k + len(part.scratch)],
                )
            )
            i, j, k = i + len(part.ins), j + len(part.outs), k + len(part.scratch)
        barrier = pltpu.get_barrier_semaphore()
        for p in peers:
            pl.semaphore_signal(barrier, inc=1, device_id=peer(*p), device_id_type=MESH)
        pl.semaphore_wait(barrier, len(peers))
        for gen in gens:
            next(gen)
        for turn, _ in enumerate(gens[0]):
            for part, gen in zip(parts, gens):
                if turn in part.turns:
                    next(gen)
        for gen in gens[1:]:
            for _ in gen:
                pass

    got = pl.pallas_call(
        kernel,
        name=name,
        out_shape=[jax.ShapeDtypeStruct(s, d) for s, d in outs],
        in_specs=[VSPEC] * len(ins),
        out_specs=[VSPEC] * len(outs),
        scratch_shapes=scratch,
        compiler_params=pltpu.CompilerParams(
            collective_id=cid, has_side_effects=True, vmem_limit_bytes=limit
        ),
    )(*ins)
    result = []
    for part in parts:
        result.append(got[: len(part.outs)])
        got = got[len(part.outs) :]
    return result


def plane_gather(x):
    two, r, n = x.shape

    def run(ins, outs, own):
        (x_ref,), (out_ref,), (sem,) = ins, outs, own
        h, o, y, c = place()
        dev_x, dev_y, dev_c = peer(*NEAR_X), peer(*NEAR_Y), peer(*NEAR_C)
        mine = h * 4 + y * 2 + c
        of_x = (1 - h) * 4 + y * 2 + c
        of_y = h * 4 + (1 - y) * 2 + c
        of_d = (1 - h) * 4 + (1 - y) * 2 + c
        sent = []

        def go(src, slot, index, device, half):
            copy = remote(src.at[half], out_ref.at[half, slot], sem, index, device)
            copy.start()
            sent.append(copy)

        go(x_ref, mine, 0, dev_x, 0)
        go(x_ref, mine, 1, dev_y, 1)
        go(x_ref, mine, 2, dev_x, 1)
        go(x_ref, mine, 3, dev_y, 0)
        go(x_ref, mine, 4, dev_c, 0)
        go(x_ref, mine, 5, dev_c, 1)
        yield
        out_ref[:, pl.ds(mine, 1)] = x_ref[...][:, None]

        def relay(slot, half, index, device, onward, to_core):
            landed(out_ref.at[half, slot], sem, index)
            if onward is not None:
                go(out_ref.at[:, slot], slot, onward, device, half)
            go(out_ref.at[:, slot], slot, to_core, dev_c, half)

        relay(of_x, 0, 0, dev_y, 6, 8)
        relay(of_y, 1, 1, dev_x, 7, 9)
        relay(of_x, 1, 2, None, None, 10)
        relay(of_y, 0, 3, None, None, 11)
        relay(of_d, 0, 6, None, None, 12)
        relay(of_d, 1, 7, None, None, 13)
        flip = 1 - 2 * c
        for slot, half, index in (
            (mine, 0, 4),
            (mine, 1, 5),
            (of_x, 0, 8),
            (of_y, 1, 9),
            (of_x, 1, 10),
            (of_y, 0, 11),
            (of_d, 0, 12),
            (of_d, 1, 13),
        ):
            landed(out_ref.at[half, slot + flip], sem, index)
        for copy in sent:
            copy.wait_send()

    return Part(run, [x], [((2, 8, r, n), x.dtype)], [sems(14)], [NEAR_X, NEAR_Y, NEAR_C])


def plane_scatter(x):
    two, eight, r, n = x.shape

    def run(ins, outs, own):
        (x_ref,), (out_ref,), (near, part, from_x, from_y, diag, sem) = ins, outs, own
        h, o, y, c = place()
        dev_x, dev_y, dev_c = peer(*NEAR_X), peer(*NEAR_Y), peer(*NEAR_C)
        mine = h * 4 + y * 2 + c
        of_x = (1 - h) * 4 + y * 2 + c
        of_y = h * 4 + (1 - y) * 2 + c
        of_d = (1 - h) * 4 + (1 - y) * 2 + c
        flip = 1 - 2 * c
        sent = []

        def go(src, dst, index, device):
            copy = remote(src, dst, sem, index, device)
            copy.start()
            sent.append(copy)

        order = (of_d, of_x, of_y, mine)
        for half in range(2):
            go(x_ref.at[half, of_d + flip], near.at[0, half], half, dev_c)
        go(x_ref.at[0, of_x + flip], near.at[1, 0], 2, dev_c)
        go(x_ref.at[1, of_y + flip], near.at[2, 1], 5, dev_c)
        go(x_ref.at[1, of_x + flip], near.at[1, 1], 3, dev_c)
        go(x_ref.at[0, of_y + flip], near.at[2, 0], 4, dev_c)
        for half in range(2):
            go(x_ref.at[half, mine + flip], near.at[3, half], 6 + half, dev_c)
        yield

        def add(k, half):
            landed(near.at[k, half], sem, 2 * k + half)
            return x_ref[half, order[k]].astype(F32) + near[k, half].astype(F32)

        part[0, 0] = add(0, 0).astype(BF16)
        go(part.at[0, 0], diag.at[0], 8, dev_x)
        part[0, 1] = add(0, 1).astype(BF16)
        go(part.at[0, 1], diag.at[1], 9, dev_y)
        part[1, 0] = add(1, 0).astype(BF16)
        go(part.at[1, 0], from_x.at[0], 10, dev_x)
        part[2, 1] = add(2, 1).astype(BF16)
        go(part.at[2, 1], from_y.at[1], 11, dev_y)
        kept_x = add(1, 1)
        landed(diag.at[1], sem, 9)
        part[1, 1] = (kept_x + diag[1].astype(F32)).astype(BF16)
        go(part.at[1, 1], from_x.at[1], 12, dev_x)
        kept_y = add(2, 0)
        landed(diag.at[0], sem, 8)
        part[2, 0] = (kept_y + diag[0].astype(F32)).astype(BF16)
        go(part.at[2, 0], from_y.at[0], 13, dev_y)
        for half in range(2):
            out_ref[half] = add(3, half)
        for half, ix, iy in ((0, 10, 13), (1, 12, 11)):
            landed(from_x.at[half], sem, ix)
            landed(from_y.at[half], sem, iy)
            out_ref[half] += from_x[half].astype(F32) + from_y[half].astype(F32)
        for copy in sent:
            copy.wait_send()

    return Part(
        run,
        [x],
        [((2, r, n), F32)],
        [
            pltpu.VMEM((4, 2, r, n), BF16),
            pltpu.VMEM((3, 2, r, n), BF16),
            pltpu.VMEM((2, r, n), BF16),
            pltpu.VMEM((2, r, n), BF16),
            pltpu.VMEM((2, r, n), BF16),
            sems(14),
        ],
        [NEAR_X, NEAR_Y, NEAR_C],
    )


def exchange(x, peers, out_lead, source, target):
    peers = list(peers)

    def coords(p):
        h, o, y, c = place()
        flip = lambda v, d: 1 - v if d else v
        return flip(h, p[0]), (o + p[1]) % 4 if p[1] else o, flip(y, p[2]), flip(c, p[3])

    def run(ins, outs, own):
        (x_ref,), (out_ref,), (sem,) = ins, outs, own
        me = place()
        copies = []
        for k, p in enumerate(peers):
            copy = remote(
                source(x_ref, coords(p)), target(out_ref, me), sem, k, peer(*p)
            )
            copy.start()
            copies.append(copy)
        yield
        target(out_ref, me)[...] = source(x_ref, me)[...]
        for copy in copies:
            copy.wait()

    return Part(run, [x], [(out_lead, x.dtype)], [sems(len(peers))], peers)


def line_gather(x):
    return exchange(x, COLUMN, (4,) + x.shape, lambda r, d: r, lambda r, s: r.at[s[1]])


def blk_exchange(x):
    return exchange(
        x,
        [(0, 0, 1, 0), (0, 0, 0, 1), (0, 0, 1, 1)],
        x.shape,
        lambda r, d: r.at[d[2] * 2 + d[3]],
        lambda r, s: r.at[s[2] * 2 + s[3]],
    )


def small_gather(x):
    peers = [
        (0, dz, dy, dc) for dz in range(4) for dy in range(2) for dc in range(2) if dz or dy or dc
    ]
    return exchange(x, peers, (16,) + x.shape, lambda r, d: r, lambda r, s: r.at[blk(*s[1:])])


def pair_copy(x):
    return exchange(x, [NEAR_X], (2,) + x.shape, lambda r, d: r, lambda r, s: r.at[s[0]])


def line_sum(x):
    block = x.shape[1:]

    def run(ins, outs, own):
        (x_ref,), (out_ref,), (held, sem) = ins, outs, own
        o = place()[1]
        copies = []
        for k, p in enumerate(COLUMN):
            copy = remote(x_ref.at[(o + k + 1) % 4], held.at[k], sem, k, peer(*p))
            copy.start()
            copies.append(copy)
        yield
        for copy in copies:
            copy.wait()
        total = x_ref[o].astype(F32)
        for k in range(3):
            total += held[k].astype(F32)
        out_ref[...] = total.astype(BF16)

    return Part(
        run, [x], [(block, BF16)], [pltpu.VMEM((3,) + block, BF16), sems(3)], COLUMN
    )


def plane_spread(x, width, spots):
    four, r, n = x.shape
    lanes = 128
    pieces = n // lanes

    def run(ins, outs, own):
        (x_ref,), (out_ref,), (sem,) = ins, outs, own
        h, o, y, c = place()
        t = h * 4 + y * 2 + c
        columns = [
            out_ref.at[:, pl.ds(pl.multiple_of(lane * lanes, lanes), lanes)] for lane in spots(t)
        ]
        copies = []
        for k, p in enumerate(PLANE):
            to = (1 - y if p[2] else y) * 2 + (1 - c if p[3] else c)
            for i in range(pieces):
                src = x_ref.at[to, :, pl.ds(i * lanes, lanes)]
                copy = remote(src, columns[i], sem, k * pieces + i, peer(*p))
                copy.start()
                copies.append(copy)
        yield
        for i in range(pieces):
            columns[i][...] = x_ref[y * 2 + c, :, i * lanes : (i + 1) * lanes]
        for copy in copies:
            copy.wait()

    return Part(run, [x], [((r, width), x.dtype)], [sems(7 * pieces)], PLANE)


def sum_spread(x, width, spots):
    planes, four, r, n = x.shape
    first = line_sum(x)
    second = plane_spread(jax.ShapeDtypeStruct((four, r, n), BF16), width, spots)

    def run(ins, outs, own):
        count = len(first.scratch)
        total = own[-1]
        yield from first.run(ins, (total,), own[:count])
        yield from second.run((total,), outs, own[count:-1])

    scratch = first.scratch + second.scratch + [pltpu.VMEM((four, r, n), BF16)]
    return Part(run, [x], second_outs(second, BF16), scratch, tuple(COLUMN) + tuple(PLANE))


def second_outs(part, dtype):
    return [(shape, dtype) for shape, _ in part.outs]


def place_copy(src, dst, send_sem, recv_sem, device):
    return pltpu.make_async_remote_copy(
        src_ref=src,
        dst_ref=dst,
        send_sem=send_sem,
        recv_sem=recv_sem,
        device_id=device,
        device_id_type=MESH,
    )


BLK = tuple(
    (0, dz, dy, dc) for dz in range(4) for dy in range(2) for dc in range(2) if dz or dy or dc
)


def out_weights(w):
    r, n = w.shape

    def run(ins, outs, own):
        (w_ref,), (out_ref,), (send, recv) = ins, outs, own
        h, o, y, c = place()
        has = o // 2 == h
        serves = (o % 2 == y) & (y == c)

        def each(act):
            for k in range(4):
                device = (h, blk((o + k) % 4, o % 2, y))
                copy = place_copy(w_ref, out_ref.at[c], send.at[k], recv.at[c], device)

                @pl.when(has if k else has & jnp.logical_not(serves))
                def _():
                    act(copy)

        each(lambda copy: copy.start())
        yield

        @pl.when(has & serves)
        def _():
            out_ref[pl.ds(c, 1)] = w_ref[...][None]

        each(lambda copy: copy.wait_send())
        for core in range(2):
            from_self = (o == 2 * h + y) & (y == c) & (c == core)
            ref = out_ref.at[core]

            @pl.when(jnp.logical_not(from_self))
            def _():
                place_copy(ref, ref, send.at[0], recv.at[core], (h, blk(o, y, c))).wait_recv()

    scratch = [pltpu.SemaphoreType.DMA((4,)), pltpu.SemaphoreType.DMA((2,))]
    return Part(run, [w], [((2, r, n), BF16)], scratch, BLK)


def out_grads(x):
    two, r, n = x.shape

    def run(ins, outs, own):
        (x_ref,), (out_ref,), (held, total, send, recv, pair) = ins, outs, own
        h, o, y, c = place()
        has = o // 2 == h

        def each(act):
            for j in range(2):
                device = (h, blk(2 * h + y, c, j))
                copy = place_copy(x_ref.at[j], held.at[o], send.at[j], recv.at[o], device)

                @pl.when(jnp.logical_not((o == 2 * h + y) & (y == c) & (c == j)))
                def _():
                    act(copy)

        each(lambda copy: copy.start())
        yield
        total[...] = jnp.zeros_like(total)
        for z in range(4):
            mine = (z == o) & (o % 2 == y) & (y == c)

            @pl.when(has & mine)
            def _():
                total[...] += x_ref[c].astype(F32)

            @pl.when(has & jnp.logical_not(mine))
            def _():
                ref = held.at[z]
                place_copy(ref, ref, send.at[0], recv.at[z], (h, blk(o, y, c))).wait_recv()
                total[...] += held[z].astype(F32)

        @pl.when(has)
        def _():
            out_ref[...] = total[...].astype(BF16)
            remote(out_ref, out_ref, pair, 0, peer(*NEAR_X)).start()

        yield
        each(lambda copy: copy.wait_send())

        @pl.when(has)
        def _():
            remote(out_ref, out_ref, pair, 0, peer(*NEAR_X)).wait_send()

        @pl.when(jnp.logical_not(has))
        def _():
            landed(out_ref, pair, 0)

    scratch = [
        pltpu.VMEM((4, r, n), BF16),
        pltpu.VMEM((r, n), F32),
        pltpu.SemaphoreType.DMA((2,)),
        pltpu.SemaphoreType.DMA((4,)),
        sems(1),
    ]
    return Part(run, [x], [((r, n), BF16)], scratch, BLK + (NEAR_X,))


def mirrored():
    o = place()[1]
    far = o // 2
    seen = lambda v: v * (1 - 2 * far) + 3 * far
    return seen(o), seen


def rows_scatter(x):
    r, n = x.shape[3:]

    def run(ins, outs, own):
        (x_ref,), (out_ref,), (near, part, from_y, term, ends, mids, last, csem, ysem, zsem) = (
            ins,
            outs,
            own,
        )
        h, o, y, c = place()
        at, seen = mirrored()
        dev_y, dev_c = peer(*NEAR_Y), peer(*NEAR_C)
        order = [seen(3), seen(2), seen(1 - at), o]
        end, inner, other = (h, blk(seen(0), y, c)), (h, blk(seen(1), y, c)), (h, blk(seen(2), y, c))
        sent = []
        for i, yy in enumerate((1 - y, y)):
            for j, z in enumerate(order):
                copy = remote(x_ref.at[z, yy, 1 - c], near.at[i, j], csem, i * 4 + j, dev_c)
                copy.start()
                sent.append(copy)
        yield
        for j, z in enumerate(order):
            landed(near.at[0, j], csem, j)
            part[j] = x_ref[z, 1 - y, c] + near[0, j]
            copy = remote(part.at[j], from_y.at[j], ysem, j, dev_y)
            copy.start()
            sent.append(copy)
        for j, z in enumerate(order):
            landed(near.at[1, j], csem, 4 + j)
            landed(from_y.at[j], ysem, j)
            term[j] = x_ref[z, y, c] + near[1, j] + from_y[j]
            if j < 3:

                @pl.when(at == 0)
                def _():
                    remote(term.at[j], ends.at[j], zsem, j, inner).start()

            if j < 2:

                @pl.when(at == 1)
                def _():
                    landed(ends.at[j], zsem, j)
                    term[j] += ends[j]
                    remote(term.at[j], mids.at[j], zsem, 3 + j, other).start()

        @pl.when(at == 1)
        def _():
            landed(mids.at[0], zsem, 3)
            term[2] += mids[0]
            remote(term.at[2], last, zsem, 5, end).start()
            landed(ends.at[2], zsem, 2)
            landed(mids.at[1], zsem, 4)
            out_ref[...] = (term[3] + ends[2] + mids[1]).astype(F32)
            for j in range(2):
                remote(term.at[j], mids.at[j], zsem, 3 + j, other).wait_send()
            remote(term.at[2], last, zsem, 5, end).wait_send()

        @pl.when(at == 0)
        def _():
            landed(last, zsem, 5)
            out_ref[...] = (term[3] + last[...]).astype(F32)
            for j in range(3):
                remote(term.at[j], ends.at[j], zsem, j, inner).wait_send()

        for copy in sent:
            copy.wait_send()

    block = (r, n)
    scratch = [
        pltpu.VMEM((2, 4) + block, BF16),
        pltpu.VMEM((4,) + block, BF16),
        pltpu.VMEM((4,) + block, BF16),
        pltpu.VMEM((4,) + block, BF16),
        pltpu.VMEM((3,) + block, BF16),
        pltpu.VMEM((2,) + block, BF16),
        pltpu.VMEM(block, BF16),
        sems(8),
        sems(4),
        sems(6),
    ]
    return Part(run, [x], [(block, F32)], scratch, (NEAR_Y, NEAR_C) + COLUMN)


def blk_gather(x):
    r, n = x.shape

    def run(ins, outs, own):
        (x_ref,), (out_ref,), (zsem, ysem, csem) = ins, outs, own
        h, o, y, c = place()
        at, seen = mirrored()
        dev_y, dev_c = peer(*NEAR_Y), peer(*NEAR_C)
        end, inner, other = (h, blk(seen(0), y, c)), (h, blk(seen(1), y, c)), (h, blk(seen(2), y, c))
        sent = []

        def spot(z, yy=y, cc=c):
            return out_ref.at[z, yy, cc]

        def go(src, z, yy, sem, index, device):
            copy = remote(src, spot(z, yy), sem, index, device)
            copy.start()
            sent.append(copy)

        def line(src, z, index, device):
            return remote(src, spot(z), zsem, index, device)

        @pl.when(at == 0)
        def _():
            line(x_ref, o, 0, inner).start()

        @pl.when(at == 1)
        def _():
            line(x_ref, o, 1, end).start()
            line(x_ref, o, 2, other).start()

        go(x_ref, o, y, ysem, 0, dev_y)
        go(x_ref, o, y, csem, 0, dev_c)
        yield
        out_ref[o, y, c] = x_ref[...]

        def onward(j, z):
            go(spot(z), z, y, ysem, j, dev_y)
            go(spot(z), z, y, csem, j, dev_c)

        first = seen(1 - at)

        @pl.when(at == 0)
        def _():
            landed(spot(seen(1)), zsem, 1)

        @pl.when(at == 1)
        def _():
            landed(spot(seen(0)), zsem, 0)
            line(spot(seen(0)), seen(0), 3, other).start()

        onward(1, first)

        @pl.when(at == 0)
        def _():
            landed(spot(seen(2)), zsem, 4)

        @pl.when(at == 1)
        def _():
            landed(spot(seen(2)), zsem, 2)
            line(spot(seen(2)), seen(2), 4, end).start()

        onward(2, seen(2))

        @pl.when(at == 0)
        def _():
            landed(spot(seen(3)), zsem, 5)

        @pl.when(at == 1)
        def _():
            landed(spot(seen(3)), zsem, 3)
            line(spot(seen(3)), seen(3), 5, end).start()

        onward(3, seen(3))
        for j, z in enumerate((o, first, seen(2), seen(3))):
            landed(spot(z, 1 - y), ysem, j)
            go(spot(z, 1 - y), z, 1 - y, csem, 4 + j, dev_c)
        for j, z in enumerate((o, first, seen(2), seen(3))):
            landed(spot(z, y, 1 - c), csem, j)
            landed(spot(z, 1 - y, 1 - c), csem, 4 + j)

        @pl.when(at == 0)
        def _():
            line(x_ref, o, 0, inner).wait_send()

        @pl.when(at == 1)
        def _():
            line(x_ref, o, 1, end).wait_send()
            line(x_ref, o, 2, other).wait_send()
            line(spot(seen(0)), seen(0), 3, other).wait_send()
            line(spot(seen(2)), seen(2), 4, end).wait_send()
            line(spot(seen(3)), seen(3), 5, end).wait_send()

        for copy in sent:
            copy.wait_send()

    return Part(
        run,
        [x],
        [((4, 2, 2, r, n), x.dtype)],
        [sems(6), sems(4), sems(8)],
        (NEAR_Y, NEAR_C) + COLUMN,
    )


def pair_sum(x):
    n = x.shape[0]

    def run(ins, outs, own):
        (x_ref,), (out_ref,), (held, sem) = ins, outs, own
        copies = [remote(x_ref.at[k], held.at[k], sem, k, peer(*NEAR_X)) for k in range(n)]
        for copy in copies:
            copy.start()
        yield
        for k, copy in enumerate(copies):
            copy.wait()
            out_ref[k] = x_ref[k].astype(F32) + held[k].astype(F32)

    return Part(
        run, [x], [(x.shape, F32)], [pltpu.VMEM(x.shape, x.dtype), sems(n)], [NEAR_X]
    )


def small_scatter(x):
    peers = [
        (dx, dz, dy, dc)
        for dx in range(2)
        for dz in range(4)
        for dy in range(2)
        for dc in range(2)
        if dx or dz or dy or dc
    ]
    block = x.shape[1:]

    def run(ins, outs, own):
        (x_ref,), (out_ref,), (held, sem) = ins, outs, own
        h, o, y, c = place()
        copies = []
        for k, p in enumerate(peers):
            to = peer(*p)
            copy = remote(x_ref.at[to[1]], held.at[k], sem, k, to)
            copy.start()
            copies.append(copy)
        yield
        for copy in copies:
            copy.wait()
        out_ref[...] = x_ref[blk(o, y, c)] + jnp.sum(held[...], axis=0)

    return Part(
        run, [x], [(block, F32)], [pltpu.VMEM((31,) + block, F32), sems(31)], peers
    )


def attend(x, scale, cols=256):
    three, two, e, wide = x.shape
    n = wide // 2
    length = 4 * n

    def run(ins, outs, own):
        (x_ref,), (back_ref, held, o_ref, lse_ref), (keys, low, isem, osem) = ins, outs, own
        o = place()[1]
        copies = []
        for k, p in enumerate(COLUMN):
            z = (o + k + 1) % 4
            copy = remote(
                x_ref.at[:, z % 2, :, pl.ds(pl.multiple_of((z // 2) * n, n), n)],
                held.at[:, :, pl.ds(pl.multiple_of(o * n, n), n)],
                isem,
                k,
                peer(*p),
            )
            copy.start()
            copies.append(copy)
        yield
        mine = pl.ds(pl.multiple_of((o // 2) * n, n), n)
        held[:, :, pl.ds(pl.multiple_of(o * n, n), n)] = x_ref[:, o % 2, :, mine]
        for copy in copies:
            copy.wait()
        keys[...] = held[1].astype(F32).T.astype(BF16)

        def back(i, z):
            return remote(
                low.at[:, pl.ds(pl.multiple_of(z * n, n), n)],
                back_ref.at[o % 2, :, mine],
                osem,
                i,
                (place()[0], z * 4 + lax.axis_index("blk") % 4),
            )

        @pl.loop(0, 4 * (n // cols))
        def _(step):
            i = step // (n // cols)
            z = (o + 1 + i) % 4
            at = pl.ds(pl.multiple_of(z * n + step % (n // cols) * cols, cols), cols)
            q = (held[0, :, at].astype(F32) * scale).astype(BF16)
            s = jnp.dot(keys[...], q, preferred_element_type=F32)
            peak = jnp.max(s, axis=0, keepdims=True)
            p = jnp.exp(s - peak)
            total = jnp.sum(p, axis=0, keepdims=True)
            out = jnp.dot(held[2], p.astype(BF16), preferred_element_type=F32) / total
            o_ref[:, at] = out
            low[:, at] = out.astype(BF16)
            lse_ref[:, at] = peak + jnp.log(total)

            @pl.when((step % (n // cols) == n // cols - 1) & (i < 3))
            def _():
                back(i, z).start()

        back_ref[o % 2, :, mine] = low[:, pl.ds(pl.multiple_of(o * n, n), n)]
        for i in range(3):
            back(i, (o + 1 + i) % 4).wait_send()
            z = (o + 3 - i) % 4
            ref = back_ref.at[z % 2, :, pl.ds(pl.multiple_of((z // 2) * n, n), n)]
            landed(ref, osem, i)

    return Part(
        run,
        [x],
        [
            ((two, e, wide), BF16),
            ((three, e, length), BF16),
            ((e, length), F32),
            ((1, length), F32),
        ],
        [pltpu.VMEM((length, e), BF16), pltpu.VMEM((e, length), BF16), sems(3), sems(3)],
        COLUMN,
    )


def attend_back(g, held, out, lse, scale, rows=256):
    three, e, length = held.shape
    n = length // 4

    def run(ins, outs, own):
        (g_ref, held_ref, o_ref, lse_ref), (back_ref,) = ins, outs
        gs, qs, q_rows, g_rows, dq, delta, low, isem, ksem, qsem = own
        o = place()[1]
        copies = []
        for k, p in enumerate(COLUMN):
            z = (o + k + 1) % 4
            copy = remote(
                g_ref.at[z % 2, :, pl.ds(pl.multiple_of((z // 2) * n, n), n)],
                gs.at[:, pl.ds(pl.multiple_of(o * n, n), n)],
                isem,
                k,
                peer(*p),
            )
            copy.start()
            copies.append(copy)
        yield
        mine = pl.ds(pl.multiple_of((o // 2) * n, n), n)
        gs[:, pl.ds(pl.multiple_of(o * n, n), n)] = g_ref[o % 2, :, mine]
        q32 = held_ref[0].astype(F32) * scale
        qs[...] = q32.astype(BF16)
        q_rows[...] = q32.T.astype(BF16)
        dq[...] = jnp.zeros_like(dq)
        for copy in copies:
            copy.wait()
        g32 = gs[...].astype(F32)
        g_rows[...] = g32.T.astype(BF16)
        delta[...] = jnp.sum(g32 * o_ref[...], axis=0, keepdims=True)

        def back(part, sem, i, z):
            return remote(
                low.at[part, :, pl.ds(pl.multiple_of(z * n, n), n)],
                back_ref.at[part, o % 2, :, mine],
                sem,
                i,
                (place()[0], z * 4 + lax.axis_index("blk") % 4),
            )

        late = pl.ds(1, 2)
        steps = n // rows

        @pl.loop(0, 4 * steps)
        def _(step):
            i = step // steps
            z = (o + 1 + i) % 4
            at = pl.ds(pl.multiple_of(z * n + step % steps * rows, rows), rows)
            k_cols = held_ref[1, :, at]
            k_rows = k_cols.astype(F32).T.astype(BF16)
            v_rows = held_ref[2, :, at].astype(F32).T.astype(BF16)
            s = jnp.dot(k_rows, qs[...], preferred_element_type=F32)
            p = jnp.exp(s - lse_ref[...])
            dv = jnp.dot(p.astype(BF16), g_rows[...], preferred_element_type=F32)
            dp = jnp.dot(v_rows, gs[...], preferred_element_type=F32)
            ds = (p * (dp - delta[...])).astype(BF16)
            dk = jnp.dot(ds, q_rows[...], preferred_element_type=F32)
            dq[...] += jnp.dot(k_cols, ds, preferred_element_type=F32)
            low[1, :, at] = dk.T.astype(BF16)
            low[2, :, at] = dv.T.astype(BF16)

            @pl.when((step % steps == steps - 1) & (i < 3))
            def _():
                back(late, ksem, i, z).start()

        low[0] = (dq[...] * scale).astype(BF16)
        for i in range(3):
            back(pl.ds(0, 1), qsem, i, (o + 1 + i) % 4).start()
        yield
        back_ref[:, o % 2, :, mine] = low[:, :, pl.ds(pl.multiple_of(o * n, n), n)]
        for i in range(3):
            back(late, ksem, i, (o + 1 + i) % 4).wait_send()
            back(pl.ds(0, 1), qsem, i, (o + 1 + i) % 4).wait_send()
            z = (o + 3 - i) % 4
            there = pl.ds(pl.multiple_of((z // 2) * n, n), n)
            landed(back_ref.at[late, z % 2, :, there], ksem, i)
            landed(back_ref.at[pl.ds(0, 1), z % 2, :, there], qsem, i)

    return Part(
        run,
        [g, held, out, lse],
        [((three,) + g.shape, BF16)],
        [
            pltpu.VMEM((e, length), BF16),
            pltpu.VMEM((e, length), BF16),
            pltpu.VMEM((length, e), BF16),
            pltpu.VMEM((length, e), BF16),
            pltpu.VMEM((e, length), F32),
            pltpu.VMEM((1, length), F32),
            pltpu.VMEM((three, e, length), BF16),
            sems(3),
            sems(3),
            sems(3),
        ],
        COLUMN,
    )


def gather_steps(src, dst, sem):
    h, o, y, c = place()
    dev_x, dev_y, dev_c = peer(*NEAR_X), peer(*NEAR_Y), peer(*NEAR_C)
    mine = h * 4 + y * 2 + c
    of_x = (1 - h) * 4 + y * 2 + c
    of_y = h * 4 + (1 - y) * 2 + c
    of_d = (1 - h) * 4 + (1 - y) * 2 + c
    flip = 1 - 2 * c
    sent = []

    def go(ref, slot, half, index, device):
        copy = remote(ref, dst(half, slot), sem, index, device)
        copy.start()
        sent.append(copy)

    go(src(0), mine, 0, 0, dev_x)
    go(src(1), mine, 1, 1, dev_y)
    go(src(1), mine, 1, 2, dev_x)
    go(src(0), mine, 0, 3, dev_y)
    go(src(0), mine, 0, 4, dev_c)
    go(src(1), mine, 1, 5, dev_c)
    for half in range(2):
        dst(half, mine)[...] = src(half)[...]

    def relay(slot, half, index, device, onward, to_core):
        landed(dst(half, slot), sem, index)
        if onward is not None:
            go(dst(half, slot), slot, half, onward, device)
        go(dst(half, slot), slot, half, to_core, dev_c)

    yield
    relay(of_x, 0, 0, dev_y, 6, 8)
    relay(of_y, 1, 1, dev_x, 7, 9)
    yield
    relay(of_x, 1, 2, None, None, 10)
    relay(of_y, 0, 3, None, None, 11)
    yield
    relay(of_d, 0, 6, None, None, 12)
    relay(of_d, 1, 7, None, None, 13)
    yield
    for slot, half, index in (
        (mine, 0, 4),
        (mine, 1, 5),
        (of_x, 0, 8),
        (of_y, 1, 9),
        (of_x, 1, 10),
        (of_y, 0, 11),
        (of_d, 0, 12),
        (of_d, 1, 13),
    ):
        landed(dst(half, slot + flip), sem, index)
    for copy in sent:
        copy.wait_send()


def scatter_steps(src, total, near, part, from_x, from_y, diag, sem):
    h, o, y, c = place()
    dev_x, dev_y, dev_c = peer(*NEAR_X), peer(*NEAR_Y), peer(*NEAR_C)
    mine = h * 4 + y * 2 + c
    of_x = (1 - h) * 4 + y * 2 + c
    of_y = h * 4 + (1 - y) * 2 + c
    of_d = (1 - h) * 4 + (1 - y) * 2 + c
    flip = 1 - 2 * c
    order = (of_d, of_x, of_y, mine)
    sent = []

    def go(ref, to, index, device):
        copy = remote(ref, to, sem, index, device)
        copy.start()
        sent.append(copy)

    for k, half in ((0, 0), (0, 1), (1, 0), (2, 1), (1, 1), (2, 0), (3, 0), (3, 1)):
        go(src(half, order[k] + flip), near.at[k, half], 2 * k + half, dev_c)

    def add(k, half):
        landed(near.at[k, half], sem, 2 * k + half)
        return src(half, order[k])[...].astype(F32) + near[k, half].astype(F32)

    yield
    part[0, 0] = add(0, 0).astype(BF16)
    go(part.at[0, 0], diag.at[0], 8, dev_x)
    part[0, 1] = add(0, 1).astype(BF16)
    go(part.at[0, 1], diag.at[1], 9, dev_y)
    part[1, 0] = add(1, 0).astype(BF16)
    go(part.at[1, 0], from_x.at[0], 10, dev_x)
    part[2, 1] = add(2, 1).astype(BF16)
    go(part.at[2, 1], from_y.at[1], 11, dev_y)
    yield
    kept_x = add(1, 1)
    landed(diag.at[1], sem, 9)
    part[1, 1] = (kept_x + diag[1].astype(F32)).astype(BF16)
    go(part.at[1, 1], from_x.at[1], 12, dev_x)
    kept_y = add(2, 0)
    landed(diag.at[0], sem, 8)
    part[2, 0] = (kept_y + diag[0].astype(F32)).astype(BF16)
    go(part.at[2, 0], from_y.at[0], 13, dev_y)
    yield
    own = [add(3, half) for half in range(2)]
    for half, ix, iy in ((0, 10, 13), (1, 12, 11)):
        landed(from_x.at[half], sem, ix)
        landed(from_y.at[half], sem, iy)
        total(half)[...] = own[half] + from_x[half].astype(F32) + from_y[half].astype(F32)
    for copy in sent:
        copy.wait_send()


def scatter_scratch(r, n):
    block = (2, r // 2, n)
    return [
        pltpu.VMEM((4,) + block, BF16),
        pltpu.VMEM((3,) + block, BF16),
        pltpu.VMEM(block, BF16),
        pltpu.VMEM(block, BF16),
        pltpu.VMEM(block, BF16),
        sems(14),
    ]


def norm_parts(r):
    centred = r - jnp.mean(r, axis=-1, keepdims=True)
    scale = lax.rsqrt(jnp.mean(centred * centred, axis=-1, keepdims=True) + 1e-12)
    return centred * scale, scale


def norm_back(xh, scale, dh):
    return (
        dh
        - jnp.mean(dh, axis=-1, keepdims=True)
        - xh * jnp.mean(dh * xh, axis=-1, keepdims=True)
    ) * scale


def dot_nt(a, b):
    return lax.dot_general(a, b, (((1,), (1,)), ((), ())), preferred_element_type=F32)


def dot_tn(a, b):
    return lax.dot_general(a, b, (((0,), (0,)), ((), ())), preferred_element_type=F32)


def middle(branch, embedded, cotangent, up_one, up_cut, down_one, down_cut, up_bias, vectors, lag):
    seqs, eight, r, d = branch.shape
    half = r // 2
    planes, four, e, fh = up_one.shape
    f = 2 * fh
    fcols = down_cut.shape[0]
    dh_cols = d // 2
    rows = 8 * r
    q_rows = rows // 2

    def run(ins, outs, own):
        (x_ref, emb_ref, cot_ref, up1, up_src, down1, down_src, bias_ref, vec_ref) = ins
        (out_ref, resid_ref, branch_out, down_sum, up_sum, sums_ref, bias_sum) = outs
        it = iter(own)
        up2, down2, up_sem, down_sem = (next(it) for _ in range(4))
        first_g, grad_g, second, third, act, slope, inner_grad = (next(it) for _ in range(7))
        first, xh_one, scale_one, grad_two, low, total = (next(it) for _ in range(6))
        down_part, down_held, sum_sem = (next(it) for _ in range(3))
        up_part, up_held, up_sum_sem = (next(it) for _ in range(3))
        streams = []
        for s in range(seqs):
            scatters = [[next(it) for _ in range(6)] for _ in range(3)]
            streams.append((scatters, [next(it) for _ in range(3)]))
        o = place()[1]

        weights = []
        for k, p in enumerate(COLUMN):
            for src, dst, sem in ((up_src, up2, up_sem), (down_src, down2, down_sem)):
                copy = remote(src, dst.at[o], sem, k, peer(*p))
                copy.start()
                weights.append(copy)
        up2[pl.ds(o, 1)] = up_src[...][None]
        down2[pl.ds(o, 1)] = down_src[...][None]
        sums_ref[...] = jnp.zeros_like(sums_ref)
        bias_sum[...] = jnp.zeros_like(bias_sum)
        yield

        ups = [lambda: up1[...].reshape(d, fh), lambda: up2[...].reshape(d, fh)]
        downs = [lambda: down1[...].reshape(f, dh_cols), lambda: down2[...].reshape(f, dh_cols)]
        vec = lambda k: vec_ref[k : k + 1]

        def piece(ref, s):
            return lambda i, slot: ref.at[s, slot, pl.ds(i * half, half)]

        def plain(ref, s):
            return lambda i: ref.at[s, pl.ds(i * half, half)]

        def quarter(ref, s, q):
            return ref[s, 4 * q : 4 * q + 4].reshape(q_rows, d)

        def note(k, value):
            sums_ref[k : k + 1] += jnp.sum(value, axis=0, keepdims=True)

        def stream(s):
            scatters, gathers = streams[s]
            at = lambda q: pl.ds(s * rows + q * q_rows, q_rows)
            yield from scatter_steps(piece(x_ref, s), plain(total, s), *scatters[0])
            xh, scale = norm_parts(emb_ref[s] + (total[s] + vec(0)))
            xh_one[s] = xh
            scale_one[s] = scale
            value = xh * vec(4) + vec(1)
            first[s] = value
            low[s] = value.astype(BF16)
            yield from gather_steps(plain(low, s), piece(first_g, s), gathers[0])
            if s == 0:
                for copy in weights:
                    copy.wait()
            for q in range(2):
                rows_in = quarter(first_g, s, q)
                for k in range(2):
                    cols = slice(k * fh, (k + 1) * fh)
                    inner = jnp.dot(rows_in, ups[k](), preferred_element_type=F32)
                    inner = inner + bias_ref[:, cols]
                    phi = 0.5 + 0.5 * lax.erf(inner * (0.5**0.5))
                    act[at(q), cols] = (inner * phi).astype(BF16)
                    bell = jnp.exp(inner * inner * -0.5) * (1.0 / math.sqrt(2.0 * math.pi))
                    slope[at(q), cols] = phi + inner * bell
                    yield
                for k in range(2):
                    part = jnp.dot(act[at(q)], downs[k](), preferred_element_type=F32)
                    second[s, 4 * q : 4 * q + 4, :, k * dh_cols : (k + 1) * dh_cols] = part.astype(
                        BF16
                    ).reshape(4, r, dh_cols)
                yield
            yield from scatter_steps(piece(second, s), plain(total, s), *scatters[1])
            xh, scale = norm_parts(first[s] + (total[s] + vec(2)))
            out_ref[s] = (xh * vec(5) + vec(3)).astype(BF16)
            cot = cot_ref[s].astype(F32)
            note(5, cot * xh)
            note(3, cot)
            grad = norm_back(xh, scale, cot * vec(5))
            grad_two[s] = grad
            low[s] = grad.astype(BF16)
            note(2, low[s].astype(F32))
            yield from gather_steps(plain(low, s), piece(grad_g, s), gathers[1])
            for q in range(2):
                rows_in = quarter(grad_g, s, q)
                back = dot_nt(rows_in[:, :dh_cols], downs[0]()) + dot_nt(
                    rows_in[:, dh_cols:], downs[1]()
                )
                back = (back * slope[at(q)]).astype(BF16)
                inner_grad[at(q)] = back
                bias_sum[...] += jnp.sum(back.astype(F32), axis=0, keepdims=True)
                yield
                part = dot_nt(back[:, :fh], ups[0]()) + dot_nt(back[:, fh:], ups[1]())
                third[s, 4 * q : 4 * q + 4] = part.astype(BF16).reshape(4, r, d)
                yield
            last = scatter_steps(piece(third, s), plain(total, s), *scatters[2])
            next(last)
            if s == seqs - 1:
                all_grads = grad_g[...].reshape(seqs * rows, d)
                for z in range(planes):
                    cols = slice(z * fcols, (z + 1) * fcols)
                    down_part[z] = dot_tn(act[:, cols], all_grads).astype(BF16)
                    if z % 2:
                        yield
                send_sums(down_part, down_held, sum_sem)
                for z in range(planes):
                    cols = slice(z * 4 * e, (z + 1) * 4 * e)
                    all_first = first_g[:, :, :, cols].reshape(seqs * rows, 4 * e)
                    up_part[z] = dot_tn(all_first, inner_grad[...]).astype(BF16)
                    if z % 2:
                        yield
                send_sums(up_part, up_held, up_sum_sem)
            yield from last
            grad = grad_two[s] + total[s]
            note(4, grad * xh_one[s])
            note(1, grad)
            grad = norm_back(xh_one[s], scale_one[s], grad * vec(4))
            resid_ref[s] = grad
            low[s] = grad.astype(BF16)
            note(0, low[s].astype(F32))
            yield from gather_steps(plain(low, s), piece(branch_out, s), gathers[2])

        def send_sums(part, held, sem):
            for k, p in enumerate(COLUMN):
                copy = remote(part.at[(o + k + 1) % 4], held.at[k], sem, k, peer(*p))
                copy.start()
                sums.append(copy)

        sums = []
        gens = [stream(s) for s in range(seqs)]
        for _ in range(lag):
            next(gens[0])
        while gens:
            for gen in list(gens):
                try:
                    next(gen)
                except StopIteration:
                    gens.remove(gen)
        for copy in sums:
            copy.wait()
        for part, held, out in ((down_part, down_held, down_sum), (up_part, up_held, up_sum)):
            value = part[o].astype(F32)
            for k in range(3):
                value += held[k].astype(F32)
            out[...] = value.astype(BF16)

    plane = (seqs, 8, r, d)
    per_stream = []
    for _ in range(seqs):
        for _ in range(3):
            per_stream += scatter_scratch(r, d)
        per_stream += [sems(14)] * 3
    return Part(
        run,
        [branch, embedded, cotangent, up_one, up_cut, down_one, down_cut, up_bias, vectors],
        [
            ((seqs, r, d), BF16),
            ((seqs, r, d), F32),
            (plane, BF16),
            ((fcols, d), BF16),
            ((4 * e, f), BF16),
            ((8, d), F32),
            ((1, f), F32),
        ],
        [
            pltpu.VMEM(up_one.shape, BF16),
            pltpu.VMEM(down_one.shape, BF16),
            sems(3),
            sems(3),
            pltpu.VMEM(plane, BF16),
            pltpu.VMEM(plane, BF16),
            pltpu.VMEM(plane, BF16),
            pltpu.VMEM(plane, BF16),
            pltpu.VMEM((seqs * rows, f), BF16),
            pltpu.VMEM((seqs * rows, f), F32),
            pltpu.VMEM((seqs * rows, f), BF16),
            pltpu.VMEM((seqs, r, d), F32),
            pltpu.VMEM((seqs, r, d), F32),
            pltpu.VMEM((seqs, r, 1), F32),
            pltpu.VMEM((seqs, r, d), F32),
            pltpu.VMEM((seqs, r, d), BF16),
            pltpu.VMEM((seqs, r, d), F32),
            pltpu.VMEM((planes, fcols, d), BF16),
            pltpu.VMEM((3, fcols, d), BF16),
            sems(3),
            pltpu.VMEM((planes, 4 * e, f), BF16),
            pltpu.VMEM((3, 4 * e, f), BF16),
            sems(3),
        ]
        + per_stream,
        (NEAR_X, NEAR_Y, NEAR_C) + COLUMN,
    )


def blk_gather_steps(src, spot_of, zsem, ysem, csem):
    h, o, y, c = place()
    at, seen = mirrored()
    dev_y, dev_c = peer(*NEAR_Y), peer(*NEAR_C)
    end, inner, other = (h, blk(seen(0), y, c)), (h, blk(seen(1), y, c)), (h, blk(seen(2), y, c))
    sent = []

    def spot(z, yy=y, cc=c):
        return spot_of(z, yy, cc)

    def go(ref, z, yy, sem, index, device):
        copy = remote(ref, spot(z, yy), sem, index, device)
        copy.start()
        sent.append(copy)

    def line(ref, z, index, device):
        return remote(ref, spot(z), zsem, index, device)

    @pl.when(at == 0)
    def _():
        line(src, o, 0, inner).start()

    @pl.when(at == 1)
    def _():
        line(src, o, 1, end).start()
        line(src, o, 2, other).start()

    go(src, o, y, ysem, 0, dev_y)
    go(src, o, y, csem, 0, dev_c)
    spot(o)[...] = src[...]

    def onward(j, z):
        go(spot(z), z, y, ysem, j, dev_y)
        go(spot(z), z, y, csem, j, dev_c)

    first = seen(1 - at)
    order = (o, first, seen(2), seen(3))

    def from_y(j):
        landed(spot(order[j], 1 - y), ysem, j)
        go(spot(order[j], 1 - y), order[j], 1 - y, csem, 4 + j, dev_c)

    yield

    @pl.when(at == 0)
    def _():
        landed(spot(seen(1)), zsem, 1)

    @pl.when(at == 1)
    def _():
        landed(spot(seen(0)), zsem, 0)
        line(spot(seen(0)), seen(0), 3, other).start()

    onward(1, first)

    @pl.when(at == 1)
    def _():
        landed(spot(seen(2)), zsem, 2)
        line(spot(seen(2)), seen(2), 4, end).start()

    yield
    from_y(0)

    @pl.when(at == 0)
    def _():
        landed(spot(seen(2)), zsem, 4)

    onward(2, seen(2))

    @pl.when(at == 1)
    def _():
        landed(spot(seen(3)), zsem, 3)
        line(spot(seen(3)), seen(3), 5, end).start()

    yield
    from_y(1)

    @pl.when(at == 0)
    def _():
        landed(spot(seen(3)), zsem, 5)

    onward(3, seen(3))
    yield
    from_y(2)
    yield
    from_y(3)
    yield
    for j, z in enumerate(order):
        landed(spot(z, y, 1 - c), csem, j)
        landed(spot(z, 1 - y, 1 - c), csem, 4 + j)

    @pl.when(at == 0)
    def _():
        line(src, o, 0, inner).wait_send()

    @pl.when(at == 1)
    def _():
        line(src, o, 1, end).wait_send()
        line(src, o, 2, other).wait_send()
        line(spot(seen(0)), seen(0), 3, other).wait_send()
        line(spot(seen(2)), seen(2), 4, end).wait_send()
        line(spot(seen(3)), seen(3), 5, end).wait_send()

    for copy in sent:
        copy.wait_send()


ALL = tuple(
    (dx, dz, dy, dc)
    for dx in range(2)
    for dz in range(4)
    for dy in range(2)
    for dc in range(2)
    if dx or dz or dy or dc
)


def closing(partial, resid, ids, second, slots, chunks, lag):
    seqs, eight, r, d = partial.shape
    rows = seqs * r
    w = d // chunks
    blks = 16

    def run(ins, outs, own):
        (x_ref, resid_ref, ids_ref, second_ref), (grad_ref, pos_ref, type_ref) = ins, outs
        it = iter(own)
        low, gathered, pick, part, held, types, slabs = (next(it) for _ in range(7))
        pair_sem, type_sem = next(it), next(it)
        per_chunk = [[next(it) for _ in range(9)] for _ in range(chunks)]
        h, o, y, c = place()

        def chunk(q):
            cols = pl.ds(q * w, w)
            scatter, (zsem, ysem, csem) = per_chunk[q][:6], per_chunk[q][6:]
            yield from scatter_steps(
                lambda half, slot: x_ref.at[half, slot, :, cols],
                lambda half: grad_ref.at[half, :, cols],
                *scatter,
            )
            grad = grad_ref[:, :, cols] + resid_ref[:, :, cols]
            grad_ref[:, :, cols] = grad
            grad = grad.reshape(rows, w)
            low[q] = grad.astype(BF16)
            late = jnp.sum(grad * second_ref[...], axis=0, keepdims=True)
            types[0:1, cols] = jnp.sum(grad * (1.0 - second_ref[...]), axis=0, keepdims=True)
            types[1:2, cols] = late
            yield from blk_gather_steps(
                low.at[q], lambda z, yy, cc: gathered.at[q, blk(z, yy, cc)], zsem, ysem, csem
            )
            total = jnp.dot(
                pick[...], gathered[q].reshape(blks * rows, w), preferred_element_type=F32
            )
            pos_ref[:, cols] = total
            part[q] = total.astype(BF16)
            copy = remote(part.at[q], held.at[q], pair_sem, q, peer(*NEAR_X))
            copy.start()
            pairs.append(copy)
            yield

        pairs = []
        gens = [chunk(q) for q in range(chunks)]
        next(gens[0])
        yield
        row = lax.broadcasted_iota(jnp.int32, (slots, 1), 0)
        pick[...] = (ids_ref[...] == row).astype(F32).astype(BF16)
        types[...] = jnp.zeros_like(types)
        active, waiting = [gens[0]], gens[1:]
        turn = 0
        while active or waiting:
            turn += 1
            if waiting and turn % lag == 0:
                active.append(waiting.pop(0))
            for gen in list(active):
                try:
                    next(gen)
                except StopIteration:
                    active.remove(gen)
            yield
        copies = []
        for k, p in enumerate(ALL):
            to = peer(*p)
            lanes = pl.ds(pl.multiple_of(to[1] // 2 * 128, 128), 128)
            copy = remote(types.at[:, lanes], slabs.at[k], type_sem, k, to)
            copy.start()
            copies.append(copy)
        yield
        for q, copy in enumerate(pairs):
            copy.wait()
            cols = pl.ds(q * w, w)
            pos_ref[:, cols] = pos_ref[:, cols] + held[q].astype(F32)
        for copy in copies:
            copy.wait()
        mine = pl.ds(pl.multiple_of(blk(o, y, c) // 2 * 128, 128), 128)
        type_ref[...] = types[:, mine] + jnp.sum(slabs[...], axis=0)

    scratch = [
        pltpu.VMEM((chunks, rows, w), BF16),
        pltpu.VMEM((chunks, blks, rows, w), BF16),
        pltpu.VMEM((slots, blks * rows), BF16),
        pltpu.VMEM((chunks, slots, w), BF16),
        pltpu.VMEM((chunks, slots, w), BF16),
        pltpu.VMEM((8, d), F32),
        pltpu.VMEM((31, 8, 128), F32),
        sems(chunks),
        sems(31),
    ]
    for _ in range(chunks):
        scratch += scatter_scratch(2 * r, w) + [sems(6), sems(4), sems(8)]
    return Part(
        run,
        [partial, resid, ids, second],
        [((seqs, r, d), F32), ((slots, d), F32), ((8, 128), F32)],
        scratch,
        ALL,
    )


def norm_layer(values_in, gain_row, offset_row):
    average = jnp.mean(values_in, axis=-1, keepdims=True)
    centred = values_in - average
    variance = jnp.mean(centred * centred, axis=-1, keepdims=True)
    return centred * lax.rsqrt(variance + 1e-12) * gain_row + offset_row


def gelu_exact(inner_product_sum):
    return jax.nn.gelu(inner_product_sum, approximate=False)


def widest_block(length, limit):
    return max(
        (candidate for candidate in range(1, min(length, limit) + 1) if length % candidate == 0)
    )


def block_scores(query_heads, key_block, score_scale):
    return (
        jnp.einsum("sqhe,skhe->shqk", query_heads, key_block, preferred_element_type=jnp.float32)
        * score_scale
    )


def key_side(query_block, grad_block, lse_block, delta_block, key_heads, value_heads, score_scale):
    scores = block_scores(query_block, key_heads, score_scale)
    weights = jnp.exp(scores - lse_block[..., None])
    more_values = jnp.einsum(
        "shqk,sqhe->shke",
        weights.astype(jnp.bfloat16),
        grad_block,
        preferred_element_type=jnp.float32,
    )
    grad_weights = jnp.einsum(
        "sqhe,skhe->shqk", grad_block, value_heads, preferred_element_type=jnp.float32
    )
    grad_scores = weights * (grad_weights - delta_block[..., None])
    more_keys = jnp.einsum(
        "shqk,sqhe->shke",
        grad_scores.astype(jnp.bfloat16),
        query_block,
        preferred_element_type=jnp.float32,
    )
    return (more_keys, more_values)


def forward_fold(query_heads, score_scale, head_count, head_size):

    def fold_keys(running, portion, offset):
        key_piece, value_piece = portion
        seq_count, length = (key_piece.shape[0], key_piece.shape[1])
        block_size = widest_block(length, 512)

        def one_step(block_index, carried):
            row_peak, row_total, weighted = carried
            row_start = block_index * block_size
            key_block = lax.dynamic_slice_in_dim(key_piece, row_start, block_size, 1).reshape(
                seq_count, block_size, head_count, head_size
            )
            value_block = lax.dynamic_slice_in_dim(value_piece, row_start, block_size, 1).reshape(
                seq_count, block_size, head_count, head_size
            )
            scores = block_scores(query_heads, key_block, score_scale)
            new_peak = jnp.maximum(row_peak, jnp.max(scores, axis=-1))
            shrink = jnp.exp(row_peak - new_peak)
            weights = jnp.exp(scores - new_peak[..., None])
            row_total = row_total * shrink + jnp.sum(weights, axis=-1)
            weighted = weighted * shrink[..., None] + jnp.einsum(
                "shqk,skhe->shqe",
                weights.astype(jnp.bfloat16),
                value_block,
                preferred_element_type=jnp.float32,
            )
            return (new_peak, row_total, weighted)

        return lax.fori_loop(0, length // block_size, one_step, running)

    return fold_keys


def query_fold(query_heads, grad_heads, log_totals, delta_rows, score_scale, head_count, head_size):

    def fold_keys(running, portion, offset):
        key_piece, value_piece = portion
        seq_count, length = (key_piece.shape[0], key_piece.shape[1])
        block_size = widest_block(length, 512)

        def one_step(block_index, weighted):
            row_start = block_index * block_size
            key_block = lax.dynamic_slice_in_dim(key_piece, row_start, block_size, 1).reshape(
                seq_count, block_size, head_count, head_size
            )
            value_block = lax.dynamic_slice_in_dim(value_piece, row_start, block_size, 1).reshape(
                seq_count, block_size, head_count, head_size
            )
            scores = block_scores(query_heads, key_block, score_scale)
            weights = jnp.exp(scores - log_totals[..., None])
            grad_weights = jnp.einsum(
                "sqhe,skhe->shqk", grad_heads, value_block, preferred_element_type=jnp.float32
            )
            grad_scores = weights * (grad_weights - delta_rows[..., None])
            return weighted + jnp.einsum(
                "shqk,skhe->shqe",
                grad_scores.astype(jnp.bfloat16),
                key_block,
                preferred_element_type=jnp.float32,
            )

        return lax.fori_loop(0, length // block_size, one_step, running)

    return fold_keys


def key_fold(key_heads, value_heads, score_scale, head_count, head_size):

    def fold_queries(running, portion, offset):
        query_piece, grad_piece, lse_piece, delta_piece = portion
        seq_count, length = (query_piece.shape[0], query_piece.shape[1])
        block_size = widest_block(length, 512)

        def one_step(block_index, carried):
            grad_keys, grad_values = carried
            row_start = block_index * block_size
            query_block = lax.dynamic_slice_in_dim(query_piece, row_start, block_size, 1).reshape(
                seq_count, block_size, head_count, head_size
            )
            grad_block = lax.dynamic_slice_in_dim(grad_piece, row_start, block_size, 1).reshape(
                seq_count, block_size, head_count, head_size
            )
            lse_block = lax.dynamic_slice_in_dim(lse_piece, row_start, block_size, 1).transpose(
                0, 2, 1
            )
            delta_block = lax.dynamic_slice_in_dim(delta_piece, row_start, block_size, 1).transpose(
                0, 2, 1
            )
            more_keys, more_values = key_side(
                query_block, grad_block, lse_block, delta_block, key_heads, value_heads, score_scale
            )
            return (grad_keys + more_keys, grad_values + more_values)

        return lax.fori_loop(0, length // block_size, one_step, running)

    return fold_queries


def layer_in_blocks(
    hidden,
    pos_ids,
    type_ids,
    cotangent,
    pos_table,
    type_table,
    query_key_value_weight,
    attention_output_weight,
    up_projection_weight,
    down_projection_weight,
    up_projection_bias,
    norm_gains,
    biases,
):
    seq_count, seg_tokens, model_width = hidden.shape
    row_count = seq_count * seg_tokens
    head_count = HEADS // lax.axis_size("head")
    head_size = model_width // HEADS
    local_width = head_count * head_size
    query_rows = lax.axis_size("head") * seg_tokens
    score_scale = 1.0 / math.sqrt(head_size)

    def fetch_weights():
        return (
            lax.all_gather(query_key_value_weight, "blk", axis=0, tiled=True),
            lax.all_gather(attention_output_weight, "blk", axis=0, tiled=True),
            lax.all_gather(up_projection_weight, "blk", axis=0, tiled=True),
            lax.all_gather(down_projection_weight, "blk", axis=0, tiled=True),
            lax.all_gather(up_projection_bias, "blk", axis=0, tiled=True),
            lax.all_gather(norm_gains, "blk", axis=1, tiled=True),
            lax.all_gather(biases, "blk", axis=1, tiled=True),
            lax.all_gather(type_table, "blk", axis=1, tiled=True),
        )

    qkv_full, out_full, up_full, down_full, up_bias_full, gain_full, bias_full, type_full = (
        fetch_weights()
    )
    bias_float = bias_full.astype(jnp.float32)
    gain_float = gain_full.astype(jnp.float32)
    flat_pos = pos_ids.reshape(row_count)
    portion = lax.all_gather(pos_table, "blk", axis=0, tiled=True)
    local_slots = flat_pos
    onehot = (
        local_slots[:, None] == jnp.arange(portion.shape[0], dtype=jnp.int32)[None, :]
    ).astype(jnp.bfloat16)
    positions = jnp.dot(onehot, portion, preferred_element_type=jnp.float32)
    is_second = type_ids.reshape(row_count, 1) == 1
    typed_rows = jnp.where(
        is_second, type_full[1].astype(jnp.float32), type_full[0].astype(jnp.float32)
    )
    embedded_tokens = (
        hidden.reshape(row_count, model_width).astype(jnp.float32) + positions + typed_rows
    )
    embedded_low = embedded_tokens.astype(jnp.bfloat16)
    projected_rows = jnp.dot(embedded_low, qkv_full, preferred_element_type=jnp.float32)
    token_shape = (seq_count, seg_tokens, model_width)
    queries = (
        (projected_rows[:, :model_width] + bias_float[0]).astype(jnp.bfloat16).reshape(token_shape)
    )
    keys_token = (
        projected_rows[:, model_width : 2 * model_width].astype(jnp.bfloat16).reshape(token_shape)
    )
    values_token = (
        (projected_rows[:, 2 * model_width :] + bias_float[1])
        .astype(jnp.bfloat16)
        .reshape(token_shape)
    )
    query_local, key_local, value_local = (
        lax.all_to_all(queries, "head", split_axis=2, concat_axis=1, tiled=True),
        lax.all_to_all(keys_token, "head", split_axis=2, concat_axis=1, tiled=True),
        lax.all_to_all(values_token, "head", split_axis=2, concat_axis=1, tiled=True),
    )
    head_shape = (seq_count, query_rows, head_count, head_size)
    query_heads = query_local.reshape(head_shape)
    key_heads = key_local.reshape(head_shape)
    value_heads = value_local.reshape(head_shape)
    start_peak = jnp.full((seq_count, head_count, query_rows), -jnp.inf, jnp.float32)
    start_total = jnp.zeros((seq_count, head_count, query_rows), jnp.float32)
    zero_heads = jnp.zeros((seq_count, head_count, query_rows, head_size), jnp.float32)
    fold_keys = forward_fold(query_heads, score_scale, head_count, head_size)
    row_peak, row_total, weighted = fold_keys(
        (start_peak, start_total, zero_heads),
        (
            lax.all_gather(key_local, "blk", axis=1, tiled=True),
            lax.all_gather(value_local, "blk", axis=1, tiled=True),
        ),
        jnp.int32(0),
    )
    log_totals = row_peak + jnp.log(row_total)
    attention_result = weighted / row_total[..., None]
    attended_low = (
        attention_result.transpose(0, 2, 1, 3)
        .reshape(seq_count, query_rows, local_width)
        .astype(jnp.bfloat16)
    )
    attended_token = lax.all_to_all(
        attended_low, "head", split_axis=1, concat_axis=2, tiled=True
    ).reshape(row_count, model_width)
    residual_branch = (
        jnp.dot(attended_token, out_full, preferred_element_type=jnp.float32) + bias_float[2]
    )
    first_layer_norm, first_pull = jax.vjp(
        norm_layer, embedded_tokens + residual_branch, gain_float[0], bias_float[3]
    )
    first_low = first_layer_norm.astype(jnp.bfloat16)
    inner_product_sum = jnp.dot(
        first_low, up_full, preferred_element_type=jnp.float32
    ) + up_bias_full.astype(jnp.float32)
    gelu_activations, gelu_pull = jax.vjp(gelu_exact, inner_product_sum)
    activated_low = gelu_activations.astype(jnp.bfloat16)
    second_layer_norm = (
        jnp.dot(activated_low, down_full, preferred_element_type=jnp.float32) + bias_float[4]
    )
    final_norm, final_pull = jax.vjp(
        norm_layer, first_layer_norm + second_layer_norm, gain_float[1], bias_float[5]
    )
    layer_out = final_norm.astype(jnp.bfloat16).reshape(token_shape)
    qkv_full, out_full, up_full, down_full, up_bias_full, gain_full, bias_full, type_full = (
        fetch_weights()
    )
    grad_final, grad_gain_two, grad_shift_two = final_pull(
        cotangent.reshape(row_count, model_width).astype(jnp.float32)
    )
    grad_second = grad_final.astype(jnp.bfloat16)
    grad_down = jnp.einsum(
        "rf,rd->fd", activated_low, grad_second, preferred_element_type=jnp.float32
    )
    grad_bias_second = jnp.sum(grad_second.astype(jnp.float32), axis=0)
    (grad_inner,) = gelu_pull(
        jnp.einsum("rd,fd->rf", grad_second, down_full, preferred_element_type=jnp.float32)
    )
    grad_inner_low = grad_inner.astype(jnp.bfloat16)
    grad_up = jnp.einsum("rd,rf->df", first_low, grad_inner_low, preferred_element_type=jnp.float32)
    grad_up_bias = jnp.sum(grad_inner_low.astype(jnp.float32), axis=0)
    grad_first = grad_final + jnp.einsum(
        "rf,df->rd", grad_inner_low, up_full, preferred_element_type=jnp.float32
    )
    grad_resid, grad_gain_one, grad_shift_one = first_pull(grad_first)
    grad_branch = grad_resid.astype(jnp.bfloat16)
    grad_out = jnp.einsum(
        "re,rd->ed", attended_token, grad_branch, preferred_element_type=jnp.float32
    )
    grad_bias_branch = jnp.sum(grad_branch.astype(jnp.float32), axis=0)
    grad_attended = (
        jnp.einsum("rd,ed->re", grad_branch, out_full, preferred_element_type=jnp.float32)
        .astype(jnp.bfloat16)
        .reshape(token_shape)
    )
    grad_local = lax.all_to_all(grad_attended, "head", split_axis=2, concat_axis=1, tiled=True)
    grad_heads = grad_local.reshape(head_shape)
    delta_rows = jnp.sum(
        grad_heads.astype(jnp.float32).transpose(0, 2, 1, 3) * attention_result, axis=-1
    )
    fold_queries = query_fold(
        query_heads, grad_heads, log_totals, delta_rows, score_scale, head_count, head_size
    )
    grad_query_sum = fold_queries(
        zero_heads,
        (
            lax.all_gather(key_local, "blk", axis=1, tiled=True),
            lax.all_gather(value_local, "blk", axis=1, tiled=True),
        ),
        jnp.int32(0),
    )
    fold_side = key_fold(key_heads, value_heads, score_scale, head_count, head_size)
    grad_key_sum, grad_value_sum = fold_side(
        (zero_heads, zero_heads),
        (
            lax.all_gather(query_local.astype(jnp.float32), "blk", axis=1, tiled=True).astype(
                jnp.bfloat16
            ),
            lax.all_gather(grad_local.astype(jnp.float32), "blk", axis=1, tiled=True).astype(
                jnp.bfloat16
            ),
            lax.all_gather(log_totals.transpose(0, 2, 1), "blk", axis=1, tiled=True),
            lax.all_gather(delta_rows.transpose(0, 2, 1), "blk", axis=1, tiled=True),
        ),
        jnp.int32(0),
    )
    grad_keys_local = (
        (grad_key_sum * score_scale)
        .transpose(0, 2, 1, 3)
        .reshape(seq_count, query_rows, local_width)
        .astype(jnp.bfloat16)
    )
    grad_values_local = (
        grad_value_sum.transpose(0, 2, 1, 3)
        .reshape(seq_count, query_rows, local_width)
        .astype(jnp.bfloat16)
    )
    grad_query_local = (
        (grad_query_sum * score_scale)
        .transpose(0, 2, 1, 3)
        .reshape(seq_count, query_rows, local_width)
        .astype(jnp.bfloat16)
    )
    grad_query_token, grad_key_token, grad_value_token = (
        lax.all_to_all(grad_query_local, "head", split_axis=1, concat_axis=2, tiled=True),
        lax.all_to_all(grad_keys_local, "head", split_axis=1, concat_axis=2, tiled=True),
        lax.all_to_all(grad_values_local, "head", split_axis=1, concat_axis=2, tiled=True),
    )
    grad_qkv = jnp.concatenate(
        [grad_query_token, grad_key_token, grad_value_token], axis=-1
    ).reshape(row_count, 3 * model_width)
    grad_qkv_full = jnp.einsum(
        "rd,rf->df", embedded_low, grad_qkv, preferred_element_type=jnp.float32
    )
    grad_bias_query = jnp.sum(
        grad_query_token.astype(jnp.float32).reshape(row_count, model_width), axis=0
    )
    grad_bias_value = jnp.sum(
        grad_value_token.astype(jnp.float32).reshape(row_count, model_width), axis=0
    )
    grad_embedded = grad_resid + jnp.einsum(
        "rf,df->rd", grad_qkv, qkv_full, preferred_element_type=jnp.float32
    )
    second_mask = is_second.astype(jnp.float32)
    grad_type_one = jnp.sum(grad_embedded * second_mask, axis=0)
    grad_type_zero = jnp.sum(grad_embedded * (1.0 - second_mask), axis=0)
    length = lax.axis_size("blk") * pos_table.shape[0]
    local_slots = flat_pos
    inside = (local_slots >= 0) & (local_slots < length)
    slot_index = jnp.where(inside, local_slots, length)
    buffer = jnp.zeros((length + 1, model_width), jnp.float32).at[slot_index].add(grad_embedded)
    grad_positions = lax.psum_scatter(buffer[:length], "blk", scatter_dimension=0, tiled=True)
    gain_stack = jnp.stack([grad_gain_one, grad_gain_two])
    bias_stack = jnp.stack(
        [
            grad_bias_query,
            grad_bias_value,
            grad_bias_branch,
            grad_shift_one,
            grad_bias_second,
            grad_shift_two,
        ]
    )
    type_stack = jnp.stack([grad_type_zero, grad_type_one])
    (
        shard_qkv,
        shard_out,
        shard_up,
        shard_down,
        shard_up_bias,
        shard_gains,
        shard_biases,
        shard_types,
    ) = (
        lax.psum_scatter(grad_qkv_full, "blk", scatter_dimension=0, tiled=True),
        lax.psum_scatter(grad_out, "blk", scatter_dimension=0, tiled=True),
        lax.psum_scatter(grad_up, "blk", scatter_dimension=0, tiled=True),
        lax.psum_scatter(grad_down, "blk", scatter_dimension=0, tiled=True),
        lax.psum_scatter(grad_up_bias, "blk", scatter_dimension=0, tiled=True),
        lax.psum_scatter(gain_stack, "blk", scatter_dimension=1, tiled=True),
        lax.psum_scatter(bias_stack, "blk", scatter_dimension=1, tiled=True),
        lax.psum_scatter(type_stack, "blk", scatter_dimension=1, tiled=True),
    )
    (
        total_qkv,
        total_out,
        total_up,
        total_down,
        total_up_bias,
        total_gains,
        total_biases,
        total_types,
        total_positions,
    ) = lax.psum(
        (
            shard_qkv,
            shard_out,
            shard_up,
            shard_down,
            shard_up_bias,
            shard_gains,
            shard_biases,
            shard_types,
            grad_positions,
        ),
        "head",
    )
    grad_hidden = grad_embedded.reshape(token_shape)
    return (
        layer_out,
        grad_hidden,
        total_positions,
        total_types,
        total_qkv,
        total_out,
        total_up,
        total_down,
        total_up_bias,
        total_gains,
        total_biases,
    )


BIG = 60 << 20
LAG = 3
CHUNKS = 4
CHUNK_LAG = 1


def layer_in_planes(
    hidden,
    pos_ids,
    type_ids,
    cotangent,
    pos_table,
    type_table,
    query_key_value_weight,
    attention_output_weight,
    up_projection_weight,
    down_projection_weight,
    up_projection_bias,
    norm_gains,
    biases,
):
    seqs, seg, width = hidden.shape
    blks = lax.axis_size("blk")
    h = lax.axis_index("head")
    b = lax.axis_index("blk")
    o, g = b // 4, b % 4
    rows = seqs * seg
    e = width // HEADS
    ff = up_projection_weight.shape[1]
    scale = 1.0 / math.sqrt(e)
    slots = pos_table.shape[0]
    fcols = ff // blks // 2
    plane_rows = 8 * rows

    small = jnp.concatenate(
        [
            biases.astype(F32),
            norm_gains.astype(F32),
            type_table.astype(F32),
            up_projection_bias.astype(F32).reshape(4, e),
        ]
    ).reshape(7, 2 * e)
    packed = jnp.concatenate([small, pos_ids.astype(F32).reshape(1, rows)])
    qkv_cut = query_key_value_weight.reshape(e, 3, 2, 4, 2 * e)
    qkv_cut = lax.dynamic_slice_in_dim(qkv_cut, h, 1, 2).reshape(e, 3, 4, 2 * e)
    qkv_cut = qkv_cut.transpose(2, 0, 1, 3).reshape(4, e, 6 * e)
    up_cut = up_projection_weight.reshape(e, 4, 4, 2, fcols)
    up_cut = lax.dynamic_slice_in_dim(up_cut, h, 1, 3).reshape(e, 4, 4, fcols)
    up_cut = up_cut.transpose(2, 0, 1, 3).reshape(4, e, 4 * fcols)
    down_cut = lax.dynamic_slice_in_dim(down_projection_weight, h * fcols, fcols, 0)
    half_down, half_up = width // 2, 2 * fcols
    (everyone,), (out_all,), (qkv_cut,), (up_cut,) = fused(
        "opening",
        0,
        [
            small_gather(packed),
            out_weights(attention_output_weight),
            blk_exchange(qkv_cut),
            blk_exchange(up_cut),
        ],
    )
    out_own = out_all.reshape(2 * e, width)
    params = everyone[:, :7].reshape(blks, 14, e).transpose(1, 0, 2)
    vectors = params[:10].reshape(10, width)
    bias_float, gain_float, type_float = vectors[:6], vectors[6:8], vectors[8:10]
    up_bias = lax.dynamic_slice_in_dim(
        params[10:].transpose(1, 0, 2).reshape(4, 4, 2, fcols), h, 1, 2
    )
    up_bias = lax.dynamic_slice_in_dim(up_bias, g, 1, 1).reshape(1, 4 * fcols)
    all_ids = everyone[:, 7].astype(jnp.int32)

    local_ids = all_ids.reshape(blks * rows, 1) - b * slots
    onehot = (local_ids == lax.broadcasted_iota(jnp.int32, (1, slots), 1)).astype(BF16)
    found = jnp.dot(onehot, pos_table, preferred_element_type=F32).astype(BF16)
    (positions,), (qkv_all,) = fused(
        "rows", 1, [rows_scatter(found.reshape(4, 2, 2, rows, width)), line_gather(qkv_cut)], BIG
    )
    qkv_own = qkv_all.reshape(width, 6 * e)
    is_second = type_ids.reshape(rows, 1) == 1
    typed = jnp.where(is_second, type_float[1], type_float[0])
    embedded = hidden.reshape(rows, width).astype(F32) + positions + typed
    token_shape = (seqs, seg, width)

    (plane_low,), (up_first,) = fused(
        "gather_tokens",
        2,
        [
            plane_gather(embedded.astype(BF16).reshape(token_shape)),
            line_gather(up_cut[:, :, :half_up]),
        ],
    )
    plane_low = plane_low.reshape(plane_rows, width)
    bias_heads = bias_float.reshape(6, 8, 2 * e)
    bias_heads = lax.dynamic_slice_in_dim(bias_heads, h * 4 + g, 1, 1)[:, 0]
    qkv_bias = jnp.concatenate(
        [bias_heads[0], jnp.zeros_like(bias_heads[0]), bias_heads[1]]
    ).reshape(6 * e, 1)
    projected = (
        jnp.einsum("kf,rk->fr", qkv_own, plane_low, preferred_element_type=F32) + qkv_bias
    ).astype(BF16)
    (attended, pair_qkv, pair_out, lse), (down_first,) = fused(
        "attend",
        3,
        [
            attend(projected.reshape(3, 2, e, plane_rows), scale),
            line_gather(down_cut[:, :half_down]),
        ],
        BIG,
    )
    attended = attended.reshape(2 * e, plane_rows)
    branch = jnp.einsum("fr,fd->rd", attended, out_own, preferred_element_type=F32).astype(BF16)
    vectors = jnp.concatenate([bias_float[2:6], gain_float, jnp.zeros((2, width), F32)])
    (
        (layer_out, grad_resid, plane_branch, got_down, up_total, norm_sums, grad_up_bias),
    ) = fused(
        "middle",
        4,
        [
            middle(
                branch.reshape(seqs, 8, seg, width),
                embedded.reshape(token_shape),
                cotangent,
                up_first,
                up_cut[:, :, half_up:],
                down_first,
                down_cut[:, half_down:],
                up_bias,
                vectors,
                LAG,
            )
        ],
        BIG,
    )
    grad_resid = grad_resid.reshape(rows, width)
    plane_branch = plane_branch.reshape(plane_rows, width)
    grad_out = jnp.einsum(
        "fr,rd->fd", attended, plane_branch, preferred_element_type=F32
    ).astype(BF16)
    grad_attended = jnp.einsum(
        "fd,rd->fr", out_own, plane_branch, preferred_element_type=F32
    ).astype(BF16)
    (grad_qkv,), (got_up,), (got_down,), (got_out,) = fused(
        "attend_back",
        5,
        [
            attend_back(grad_attended.reshape(2, e, plane_rows), pair_qkv, pair_out, lse, scale),
            plane_spread(
                up_total.reshape(4, e, 4 * fcols),
                ff,
                lambda t: [(i * 4 + t % 4) * 2 + t // 4 for i in range(4)],
            ),
            pair_copy(got_down),
            out_grads(grad_out.reshape(2, e, width)).on(0),
        ],
        BIG,
    )
    grad_qkv = grad_qkv.reshape(6 * e, plane_rows)
    grad_qkv_weight = jnp.einsum(
        "rk,fr->kf", plane_low, grad_qkv, preferred_element_type=F32
    ).astype(BF16)
    head_sums = jnp.sum(grad_qkv.astype(F32), axis=1).reshape(3, 2 * e)
    back = jnp.einsum("fr,kf->rk", grad_qkv, qkv_own, preferred_element_type=F32).astype(BF16)
    def spread(part):
        whole = lax.dynamic_update_slice(
            jnp.zeros((8, 2 * e), F32), part.reshape(1, 2 * e), (h * 4 + g, 0)
        )
        return whole.reshape(width)

    stacked = jnp.concatenate(
        [
            spread(head_sums[0])[None],
            spread(head_sums[2])[None],
            norm_sums,
        ]
    )
    up_spread = lax.dynamic_update_slice(
        jnp.zeros((4, 4, 2, fcols), F32), grad_up_bias.reshape(4, 1, 1, fcols), (0, g, h, 0)
    ).reshape(blks, 4, e)
    vector_pack = jnp.concatenate(
        [stacked.reshape(10, blks, e).transpose(1, 0, 2), up_spread], axis=1
    ).reshape(blks, 7, 2 * e)
    vector_pack = jnp.pad(vector_pack, ((0, 0), (0, 1), (0, 0)))

    flat_ids = all_ids.reshape(1, blks * rows) - b * slots
    (grad_hidden, total_pos, type_slab), (totals,), (got_qkv,) = fused(
        "closing",
        6,
        [
            closing(
                back.reshape(seqs, 8, seg, width),
                grad_resid.reshape(token_shape),
                flat_ids,
                is_second.astype(F32),
                slots,
                CHUNKS,
                CHUNK_LAG,
            ),
            small_scatter(vector_pack),
            sum_spread(
                grad_qkv_weight.reshape(4, 4, e, 6 * e),
                3 * width,
                lambda t: [i * 8 + t for i in range(3)],
            ).on(5),
        ],
        BIG,
    )
    totals = totals[:7].reshape(14, e)
    total_types = lax.dynamic_slice_in_dim(type_slab[:2], b % 2 * e, e, 1)
    total_qkv = got_qkv.astype(F32)
    total_up = got_up.astype(F32)
    total_down = got_down.reshape(2 * fcols, width).astype(F32)
    total_out = got_out.astype(F32)
    return (
        layer_out,
        grad_hidden,
        total_pos,
        total_types,
        total_qkv,
        total_out,
        total_up,
        total_down,
        totals[10:14].reshape(4 * e),
        totals[6:8],
        totals[:6],
    )


def planes_fit(hidden, head_axis, blk_axis):
    seqs, seg, width = hidden.shape
    return head_axis == 2 and blk_axis == HEADS and seqs == 2 and seqs * seg == 2 * width // HEADS


def on_device(hidden, *rest):
    if planes_fit(hidden, lax.axis_size("head"), lax.axis_size("blk")):
        return layer_in_planes(hidden, *rest)
    return layer_in_blocks(hidden, *rest)


def solution(mesh):
    in_specs = (
        P(None, ("head", "blk"), None),
        P(None, ("head", "blk")),
        P(None, ("head", "blk")),
        P(None, ("head", "blk"), None),
        P("blk", None),
        P(None, "blk"),
        P("blk", None),
        P("blk", None),
        P("blk", None),
        P("blk", None),
        P("blk"),
        P(None, "blk"),
        P(None, "blk"),
    )
    out_specs = (
        P(None, ("head", "blk"), None),
        P(None, ("head", "blk"), None),
        P("blk", None),
        P(None, "blk"),
        P("blk", None),
        P("blk", None),
        P("blk", None),
        P("blk", None),
        P("blk"),
        P(None, "blk"),
        P(None, "blk"),
    )
    return jax.shard_map(
        on_device, mesh=mesh, in_specs=in_specs, out_specs=out_specs, check_vma=False
    )
```

```python
import functools
import math
from types import SimpleNamespace

import jax
import jax.numpy as jnp
from jax import lax
from jax.experimental import pallas as pl
from jax.experimental.pallas import tpu as pltpu
from jax.sharding import PartitionSpec as P

HEADS = 16
MESH = pl.DeviceIdType.MESH
F32 = jnp.float32
BF16 = jnp.bfloat16
VSPEC = pl.BlockSpec(memory_space=pltpu.VMEM)


def place():
    h = lax.axis_index("head")
    b = lax.axis_index("blk")
    return h, b // 4, (b // 2) % 2, b % 2


def blk(o, y, c):
    return (o * 2 + y) * 2 + c


def peer(dx, dz, dy, dc):
    h, o, y, c = place()
    flip = lambda v, d: 1 - v if d else v
    return flip(h, dx), blk((o + dz) % 4 if dz else o, flip(y, dy), flip(c, dc))


def remote(src, dst, sems, index, device):
    return pltpu.make_async_remote_copy(
        src_ref=src,
        dst_ref=dst,
        send_sem=sems.at[0, index],
        recv_sem=sems.at[1, index],
        device_id=device,
        device_id_type=MESH,
    )


def landed(ref, sems, index):
    remote(ref, ref, sems, index, peer(1, 0, 0, 0)).wait_recv()


def sems(count):
    return pltpu.SemaphoreType.DMA((2, count))


NEAR_X, NEAR_Y, NEAR_C = (1, 0, 0, 0), (0, 0, 1, 0), (0, 0, 0, 1)
COLUMN = ((0, 1, 0, 0), (0, 2, 0, 0), (0, 3, 0, 0))
PLANE = tuple(
    (dx, 0, dy, dc) for dx in range(2) for dy in range(2) for dc in range(2) if dx or dy or dc
)


class Part:
    def __init__(self, run, ins, outs, scratch, peers):
        self.run, self.ins, self.outs, self.scratch, self.peers = run, ins, outs, scratch, peers
        self.turns = ()

    def on(self, *turns):
        self.turns = turns
        return self


def fused(name, cid, parts, limit=None):
    peers = sorted({p for part in parts for p in part.peers})
    ins = [x for part in parts for x in part.ins]
    outs = [s for part in parts for s in part.outs]
    scratch = [s for part in parts for s in part.scratch]

    def kernel(*refs):
        in_refs, out_refs = refs[: len(ins)], refs[len(ins) : len(ins) + len(outs)]
        own = refs[len(ins) + len(outs) :]
        gens = []
        i = j = k = 0
        for part in parts:
            gens.append(
                part.run(
                    in_refs[i : i + len(part.ins)],
                    out_refs[j : j + len(part.outs)],
                    own[k : k + len(part.scratch)],
                )
            )
            i, j, k = i + len(part.ins), j + len(part.outs), k + len(part.scratch)
        barrier = pltpu.get_barrier_semaphore()
        for p in peers:
            pl.semaphore_signal(barrier, inc=1, device_id=peer(*p), device_id_type=MESH)
        pl.semaphore_wait(barrier, len(peers))
        for gen in gens:
            next(gen)
        for turn, _ in enumerate(gens[0]):
            for part, gen in zip(parts, gens):
                if turn in part.turns:
                    next(gen)
        for gen in gens[1:]:
            for _ in gen:
                pass

    got = pl.pallas_call(
        kernel,
        name=name,
        out_shape=[jax.ShapeDtypeStruct(s, d) for s, d in outs],
        in_specs=[VSPEC] * len(ins),
        out_specs=[VSPEC] * len(outs),
        scratch_shapes=scratch,
        compiler_params=pltpu.CompilerParams(
            collective_id=cid, has_side_effects=True, vmem_limit_bytes=limit
        ),
    )(*ins)
    result = []
    for part in parts:
        result.append(got[: len(part.outs)])
        got = got[len(part.outs) :]
    return result


def exchange(x, peers, out_lead, source, target):
    peers = list(peers)

    def coords(p):
        h, o, y, c = place()
        flip = lambda v, d: 1 - v if d else v
        return flip(h, p[0]), (o + p[1]) % 4 if p[1] else o, flip(y, p[2]), flip(c, p[3])

    def run(ins, outs, own):
        (x_ref,), (out_ref,), (sem,) = ins, outs, own
        me = place()
        copies = []
        for k, p in enumerate(peers):
            copy = remote(
                source(x_ref, coords(p)), target(out_ref, me), sem, k, peer(*p)
            )
            copy.start()
            copies.append(copy)
        yield
        target(out_ref, me)[...] = source(x_ref, me)[...]
        for copy in copies:
            copy.wait()

    return Part(run, [x], [(out_lead, x.dtype)], [sems(len(peers))], peers)


def blk_exchange(x):
    return exchange(
        x,
        [(0, 0, 1, 0), (0, 0, 0, 1), (0, 0, 1, 1)],
        x.shape,
        lambda r, d: r.at[d[2] * 2 + d[3]],
        lambda r, s: r.at[s[2] * 2 + s[3]],
    )


def small_gather(x):
    peers = [
        (0, dz, dy, dc) for dz in range(4) for dy in range(2) for dc in range(2) if dz or dy or dc
    ]
    return exchange(x, peers, (16,) + x.shape, lambda r, d: r, lambda r, s: r.at[blk(*s[1:])])


def place_copy(src, dst, send_sem, recv_sem, device):
    return pltpu.make_async_remote_copy(
        src_ref=src,
        dst_ref=dst,
        send_sem=send_sem,
        recv_sem=recv_sem,
        device_id=device,
        device_id_type=MESH,
    )


BLK = tuple(
    (0, dz, dy, dc) for dz in range(4) for dy in range(2) for dc in range(2) if dz or dy or dc
)


def out_weights(w):
    r, n = w.shape

    def run(ins, outs, own):
        (w_ref,), (out_ref,), (send, recv) = ins, outs, own
        h, o, y, c = place()
        has = o // 2 == h
        serves = (o % 2 == y) & (y == c)

        def each(act):
            for k in range(4):
                device = (h, blk((o + k) % 4, o % 2, y))
                copy = place_copy(w_ref, out_ref.at[c], send.at[k], recv.at[c], device)

                @pl.when(has if k else has & jnp.logical_not(serves))
                def _():
                    act(copy)

        each(lambda copy: copy.start())
        yield

        @pl.when(has & serves)
        def _():
            out_ref[pl.ds(c, 1)] = w_ref[...][None]

        each(lambda copy: copy.wait_send())
        for core in range(2):
            from_self = (o == 2 * h + y) & (y == c) & (c == core)
            ref = out_ref.at[core]

            @pl.when(jnp.logical_not(from_self))
            def _():
                place_copy(ref, ref, send.at[0], recv.at[core], (h, blk(o, y, c))).wait_recv()

    scratch = [pltpu.SemaphoreType.DMA((4,)), pltpu.SemaphoreType.DMA((2,))]
    return Part(run, [w], [((2, r, n), BF16)], scratch, BLK)


def mirrored():
    o = place()[1]
    far = o // 2
    seen = lambda v: v * (1 - 2 * far) + 3 * far
    return seen(o), seen


def gather_steps(src, dst, sem):
    h, o, y, c = place()
    dev_x, dev_y, dev_c = peer(*NEAR_X), peer(*NEAR_Y), peer(*NEAR_C)
    mine = h * 4 + y * 2 + c
    of_x = (1 - h) * 4 + y * 2 + c
    of_y = h * 4 + (1 - y) * 2 + c
    of_d = (1 - h) * 4 + (1 - y) * 2 + c
    flip = 1 - 2 * c
    sent = []

    def go(ref, slot, half, index, device):
        copy = remote(ref, dst(half, slot), sem, index, device)
        copy.start()
        sent.append(copy)

    go(src(0), mine, 0, 0, dev_x)
    go(src(1), mine, 1, 1, dev_y)
    go(src(1), mine, 1, 2, dev_x)
    go(src(0), mine, 0, 3, dev_y)
    go(src(0), mine, 0, 4, dev_c)
    go(src(1), mine, 1, 5, dev_c)
    for half in range(2):
        dst(half, mine)[...] = src(half)[...]

    def relay(slot, half, index, device, onward, to_core):
        landed(dst(half, slot), sem, index)
        if onward is not None:
            go(dst(half, slot), slot, half, onward, device)
        go(dst(half, slot), slot, half, to_core, dev_c)

    yield
    relay(of_x, 0, 0, dev_y, 6, 8)
    relay(of_y, 1, 1, dev_x, 7, 9)
    yield
    relay(of_x, 1, 2, None, None, 10)
    relay(of_y, 0, 3, None, None, 11)
    yield
    relay(of_d, 0, 6, None, None, 12)
    relay(of_d, 1, 7, None, None, 13)
    yield
    for slot, half, index in (
        (mine, 0, 4),
        (mine, 1, 5),
        (of_x, 0, 8),
        (of_y, 1, 9),
        (of_x, 1, 10),
        (of_y, 0, 11),
        (of_d, 0, 12),
        (of_d, 1, 13),
    ):
        landed(dst(half, slot + flip), sem, index)
    for copy in sent:
        copy.wait_send()


def scatter_steps(src, total, near, part, from_x, from_y, diag, sem):
    h, o, y, c = place()
    dev_x, dev_y, dev_c = peer(*NEAR_X), peer(*NEAR_Y), peer(*NEAR_C)
    mine = h * 4 + y * 2 + c
    of_x = (1 - h) * 4 + y * 2 + c
    of_y = h * 4 + (1 - y) * 2 + c
    of_d = (1 - h) * 4 + (1 - y) * 2 + c
    flip = 1 - 2 * c
    order = (of_d, of_x, of_y, mine)
    sent = []

    def go(ref, to, index, device):
        copy = remote(ref, to, sem, index, device)
        copy.start()
        sent.append(copy)

    for k, half in ((0, 0), (0, 1), (1, 0), (2, 1), (1, 1), (2, 0), (3, 0), (3, 1)):
        go(src(half, order[k] + flip), near.at[k, half], 2 * k + half, dev_c)

    def add(k, half):
        landed(near.at[k, half], sem, 2 * k + half)
        return src(half, order[k])[...].astype(F32) + near[k, half].astype(F32)

    yield
    part[0, 0] = add(0, 0).astype(BF16)
    go(part.at[0, 0], diag.at[0], 8, dev_x)
    part[0, 1] = add(0, 1).astype(BF16)
    go(part.at[0, 1], diag.at[1], 9, dev_y)
    part[1, 0] = add(1, 0).astype(BF16)
    go(part.at[1, 0], from_x.at[0], 10, dev_x)
    part[2, 1] = add(2, 1).astype(BF16)
    go(part.at[2, 1], from_y.at[1], 11, dev_y)
    yield
    kept_x = add(1, 1)
    landed(diag.at[1], sem, 9)
    part[1, 1] = (kept_x + diag[1].astype(F32)).astype(BF16)
    go(part.at[1, 1], from_x.at[1], 12, dev_x)
    kept_y = add(2, 0)
    landed(diag.at[0], sem, 8)
    part[2, 0] = (kept_y + diag[0].astype(F32)).astype(BF16)
    go(part.at[2, 0], from_y.at[0], 13, dev_y)
    yield
    own = [add(3, half) for half in range(2)]
    for half, ix, iy in ((0, 10, 13), (1, 12, 11)):
        landed(from_x.at[half], sem, ix)
        landed(from_y.at[half], sem, iy)
        total(half)[...] = own[half] + from_x[half].astype(F32) + from_y[half].astype(F32)
    for copy in sent:
        copy.wait_send()


def scatter_scratch(r, n):
    block = (2, r // 2, n)
    return [
        pltpu.VMEM((4,) + block, BF16),
        pltpu.VMEM((3,) + block, BF16),
        pltpu.VMEM(block, BF16),
        pltpu.VMEM(block, BF16),
        pltpu.VMEM(block, BF16),
        sems(14),
    ]


def norm_parts(r):
    centred = r - jnp.mean(r, axis=-1, keepdims=True)
    scale = lax.rsqrt(jnp.mean(centred * centred, axis=-1, keepdims=True) + 1e-12)
    return centred * scale, scale


def norm_back(xh, scale, dh):
    return (
        dh
        - jnp.mean(dh, axis=-1, keepdims=True)
        - xh * jnp.mean(dh * xh, axis=-1, keepdims=True)
    ) * scale


def dot_nt(a, b):
    return lax.dot_general(a, b, (((1,), (1,)), ((), ())), preferred_element_type=F32)


def dot_tn(a, b):
    return lax.dot_general(a, b, (((0,), (0,)), ((), ())), preferred_element_type=F32)


def blk_gather_steps(src, spot_of, zsem, ysem, csem):
    h, o, y, c = place()
    at, seen = mirrored()
    dev_y, dev_c = peer(*NEAR_Y), peer(*NEAR_C)
    end, inner, other = (h, blk(seen(0), y, c)), (h, blk(seen(1), y, c)), (h, blk(seen(2), y, c))
    sent = []

    def spot(z, yy=y, cc=c):
        return spot_of(z, yy, cc)

    def go(ref, z, yy, sem, index, device):
        copy = remote(ref, spot(z, yy), sem, index, device)
        copy.start()
        sent.append(copy)

    def line(ref, z, index, device):
        return remote(ref, spot(z), zsem, index, device)

    @pl.when(at == 0)
    def _():
        line(src, o, 0, inner).start()

    @pl.when(at == 1)
    def _():
        line(src, o, 1, end).start()
        line(src, o, 2, other).start()

    go(src, o, y, ysem, 0, dev_y)
    go(src, o, y, csem, 0, dev_c)
    spot(o)[...] = src[...]

    def onward(j, z):
        go(spot(z), z, y, ysem, j, dev_y)
        go(spot(z), z, y, csem, j, dev_c)

    first = seen(1 - at)
    order = (o, first, seen(2), seen(3))

    def from_y(j):
        landed(spot(order[j], 1 - y), ysem, j)
        go(spot(order[j], 1 - y), order[j], 1 - y, csem, 4 + j, dev_c)

    yield

    @pl.when(at == 0)
    def _():
        landed(spot(seen(1)), zsem, 1)

    @pl.when(at == 1)
    def _():
        landed(spot(seen(0)), zsem, 0)
        line(spot(seen(0)), seen(0), 3, other).start()

    onward(1, first)

    @pl.when(at == 1)
    def _():
        landed(spot(seen(2)), zsem, 2)
        line(spot(seen(2)), seen(2), 4, end).start()

    yield
    from_y(0)

    @pl.when(at == 0)
    def _():
        landed(spot(seen(2)), zsem, 4)

    onward(2, seen(2))

    @pl.when(at == 1)
    def _():
        landed(spot(seen(3)), zsem, 3)
        line(spot(seen(3)), seen(3), 5, end).start()

    yield
    from_y(1)

    @pl.when(at == 0)
    def _():
        landed(spot(seen(3)), zsem, 5)

    onward(3, seen(3))
    yield
    from_y(2)
    yield
    from_y(3)
    yield
    for j, z in enumerate(order):
        landed(spot(z, y, 1 - c), csem, j)
        landed(spot(z, 1 - y, 1 - c), csem, 4 + j)

    @pl.when(at == 0)
    def _():
        line(src, o, 0, inner).wait_send()

    @pl.when(at == 1)
    def _():
        line(src, o, 1, end).wait_send()
        line(src, o, 2, other).wait_send()
        line(spot(seen(0)), seen(0), 3, other).wait_send()
        line(spot(seen(2)), seen(2), 4, end).wait_send()
        line(spot(seen(3)), seen(3), 5, end).wait_send()

    for copy in sent:
        copy.wait_send()


ALL = tuple(
    (dx, dz, dy, dc)
    for dx in range(2)
    for dz in range(4)
    for dy in range(2)
    for dc in range(2)
    if dx or dz or dy or dc
)


def line_sum_steps(term_of, out, terms, ends, mids, last, sem):
    h, o, y, c = place()
    at, seen = mirrored()
    end, inner, other = (h, blk(seen(0), y, c)), (h, blk(seen(1), y, c)), (h, blk(seen(2), y, c))
    order = [seen(3), seen(2), seen(1 - at)]
    plus = lambda a, b: a[...].astype(F32) + b[...].astype(F32)

    @pl.when(at == 0)
    def _():
        for j in range(3):
            remote(term_of(order[j]), ends.at[j], sem, j, inner).start()

    for j in range(2):
        yield

        @pl.when(at == 1)
        def _():
            landed(ends.at[j], sem, j)
            terms[j] = plus(term_of(order[j]), ends.at[j]).astype(BF16)
            remote(terms.at[j], mids.at[j], sem, 3 + j, other).start()

    yield

    @pl.when(at == 1)
    def _():
        landed(mids.at[0], sem, 3)
        terms[2] = plus(term_of(order[2]), mids.at[0]).astype(BF16)
        remote(terms.at[2], last, sem, 5, end).start()

    yield

    @pl.when(at == 1)
    def _():
        landed(ends.at[2], sem, 2)
        landed(mids.at[1], sem, 4)
        out[...] = (plus(term_of(o), ends.at[2]) + mids[1].astype(F32)).astype(BF16)
        for j in range(2):
            remote(terms.at[j], mids.at[j], sem, 3 + j, other).wait_send()
        remote(terms.at[2], last, sem, 5, end).wait_send()

    @pl.when(at == 0)
    def _():
        landed(last, sem, 5)
        out[...] = plus(term_of(o), last).astype(BF16)
        for j in range(3):
            remote(term_of(order[j]), ends.at[j], sem, j, inner).wait_send()


def line_sum_scratch(block):
    return [
        pltpu.VMEM((3,) + block, BF16),
        pltpu.VMEM((3,) + block, BF16),
        pltpu.VMEM((2,) + block, BF16),
        pltpu.VMEM(block, BF16),
        sems(6),
    ]


def spread_steps(rows_of, out, spots, sem):
    h, o, y, c = place()
    t = h * 4 + y * 2 + c
    columns = [
        out.at[:, pl.ds(pl.multiple_of(lane * 128, 128), 128)] for lane in spots(t)
    ]
    pieces = len(columns)
    copies = []
    for k, p in enumerate(PLANE):
        to = (1 - y if p[2] else y) * 2 + (1 - c if p[3] else c)
        for i in range(pieces):
            src = rows_of(to).at[:, pl.ds(i * 128, 128)]
            copy = remote(src, columns[i], sem, k * pieces + i, peer(*p))
            copy.start()
            copies.append(copy)
    for i in range(pieces):
        columns[i][...] = rows_of(y * 2 + c)[:, i * 128 : (i + 1) * 128]
    yield
    for copy in copies:
        copy.wait()


def second_half(x, consts):
    names = list(vars(x))
    seqs, r, d = x.embedded.shape
    planes, four, e, fh = x.up_one.shape
    f = 2 * fh
    fcols = x.down_cut.shape[0]
    half, half_d = r // 2, d // 2
    rows, q_rows = 8 * r, 4 * r
    three, he, length = x.held.shape
    n = length // 4
    slots, chunks, lag, chunk_lag, scale = consts
    own_rows, w, blks = seqs * r, d // chunks, 16
    key_rows = 256
    width_qkv = 3 * 2 * he

    need = []

    def scratch(shape, dtype):
        need.append(pltpu.VMEM(shape, dtype))
        return len(need) - 1

    def many(specs):
        start = len(need)
        need.extend(specs)
        return list(range(start, len(need)))

    plane = (seqs, 8, r, d)
    shapes = dict(
        partial=(plane, BF16),
        up_two=(x.up_one.shape, BF16),
        down_two=(x.down_one.shape, BF16),
        first_g=(plane, BF16),
        grad_g=(plane, BF16),
        branch_g=(plane, BF16),
        act=((seqs * rows, f), BF16),
        slope=((seqs * rows, f), F32),
        inner_grad=((seqs * rows, f), BF16),
        first=((seqs, r, d), F32),
        xh_one=((seqs, r, d), F32),
        scale_one=((seqs, r, 1), F32),
        grad_two=((seqs, r, d), F32),
        low=((seqs, r, d), BF16),
        total=((seqs, r, d), F32),
        resid=((seqs, r, d), F32),
        down_part=((planes, fcols, d), BF16),
        up_part=((planes, 4 * e, f), BF16),
        up_total=((4 * e, f), BF16),
        out_part=((2, he, d), BF16),
        out_held=((4, he, d), BF16),
        out_acc=((he, d), F32),
        sums=((16, d), F32),
        up_sums=((1, f), F32),
        up_spots=((32, 128), F32),
        go=((2, he, 2 * n), BF16),
        gs=((he, length), BF16),
        qs=((he, length), BF16),
        q_rows=((length, he), BF16),
        g_rows=((length, he), BF16),
        dq=((he, length), F32),
        delta=((1, length), F32),
        pair_low=((three, he, length), BF16),
        dqkv=((three, 2, he, 2 * n), BF16),
        qkv_part=((planes, 4 * e, width_qkv), BF16),
        qkv_total=((4 * e, width_qkv), BF16),
        own=((chunks, own_rows, w), BF16),
        gathered=((chunks, blks, own_rows, w), BF16),
        pick=((slots, blks * own_rows), BF16),
        pos_low=((chunks, slots, w), BF16),
        pos_held=((chunks, slots, w), BF16),
        pack=((blks, 24, 128), F32),
        packs=((31, 24, 128), F32),
    )
    ids = {name: scratch(*spec) for name, spec in shapes.items()}
    counts = dict(
        up_sem=3,
        down_sem=3,
        ksem=3,
        qsem=3,
        down_pair=1,
        up_spread=28,
        qkv_spread=21,
        out_pair=1,
        pair_sem=chunks,
        pack_sem=31,
    )
    sem_ids = {k: many([sems(v)])[0] for k, v in counts.items()}
    for k, v in dict(go_send=4, go_recv=4, out_send=2, out_recv=4).items():
        sem_ids[k] = many([pltpu.SemaphoreType.DMA((v,))])[0]
    stream_ids = [
        ([many(scatter_scratch(r, d)) for _ in range(3)], [many([sems(14)])[0] for _ in range(3)])
        for _ in range(seqs)
    ]
    chunk_ids = [
        (many(scatter_scratch(2 * r, w)), many([sems(6), sems(4), sems(8)])) for _ in range(chunks)
    ]
    down_line = many(line_sum_scratch((fcols, d)))
    up_line = many(line_sum_scratch((4 * e, f)))
    qkv_line = many(line_sum_scratch((4 * e, width_qkv)))

    def run(ins, outs, own):
        src = SimpleNamespace(**dict(zip(names, ins)))
        out_ref, grad_ref, pos_ref, got_down, got_up, got_qkv, got_out, totals = outs
        m = SimpleNamespace(**{k: own[v] for k, v in ids.items()})
        sem = SimpleNamespace(**{k: own[v] for k, v in sem_ids.items()})
        pick_refs = lambda some: [own[i] for i in some]
        h, o, y, c = place()
        g = y * 2 + c
        t = h * 4 + g
        tail = []

        up_more = src.up_cut.at[:, :, pl.ds(fh, fh)]
        down_more = src.down_cut.at[:, pl.ds(half_d, half_d)]
        weights = []
        for k, p in enumerate(COLUMN):
            for ref, dst, s in (
                (up_more, m.up_two, sem.up_sem),
                (down_more, m.down_two, sem.down_sem),
            ):
                copy = remote(ref, dst.at[o], s, k, peer(*p))
                copy.start()
                weights.append(copy)
        m.up_two[pl.ds(o, 1)] = up_more[...][None]
        m.down_two[pl.ds(o, 1)] = down_more[...][None]
        for ref in (m.sums, m.up_sums, m.up_spots, m.dq):
            ref[...] = jnp.zeros_like(ref)
        yield

        ups = [lambda k=k: src.up_one[...].reshape(d, fh) if k == 0 else m.up_two[...].reshape(d, fh) for k in range(2)]
        downs = [lambda k=k: src.down_one[...].reshape(f, half_d) if k == 0 else m.down_two[...].reshape(f, half_d) for k in range(2)]
        vec = lambda k: src.vectors[k + 2 : k + 3]
        partial, low, total = m.partial, m.low, m.total

        def piece(ref, s):
            return lambda i, slot: ref.at[s, slot, pl.ds(i * half, half)]

        def plain(ref, s):
            return lambda i: ref.at[s, pl.ds(i * half, half)]

        def quarter(ref, s, q):
            return ref[s, 4 * q : 4 * q + 4].reshape(q_rows, d)

        def note(k, value):
            m.sums[k : k + 1] += jnp.sum(value, axis=0, keepdims=True)

        def step(*some):
            for gen in some:
                next(gen, None)

        def down_sums():
            yield from line_sum_steps(
                lambda z: m.down_part.at[z], got_down.at[h], *pick_refs(down_line)
            )
            copy = remote(got_down.at[h], got_down.at[h], sem.down_pair, 0, peer(*NEAR_X))
            copy.start()
            yield
            copy.wait_send()
            landed(got_down.at[1 - h], sem.down_pair, 0)

        def up_sums():
            yield from line_sum_steps(lambda z: m.up_part.at[z], m.up_total, *pick_refs(up_line))
            yield from spread_steps(
                lambda k: m.up_total.at[pl.ds(k * e, e)],
                got_up,
                lambda k: [(i * 4 + k % 4) * 2 + k // 4 for i in range(4)],
                sem.up_spread,
            )

        def qkv_sums():
            yield from line_sum_steps(
                lambda z: m.qkv_part.at[z], m.qkv_total, *pick_refs(qkv_line)
            )
            yield from spread_steps(
                lambda k: m.qkv_total.at[pl.ds(k * e, e)],
                got_qkv,
                lambda k: [i * 8 + k for i in range(3)],
                sem.qkv_spread,
            )

        def out_sums():
            has = o // 2 == h
            held, acc, send, recv = m.out_held, m.out_acc, sem.out_send, sem.out_recv

            def each(act):
                for j in range(2):
                    device = (h, blk(2 * h + y, c, j))
                    copy = place_copy(m.out_part.at[j], held.at[o], send.at[j], recv.at[o], device)

                    @pl.when(jnp.logical_not((o == 2 * h + y) & (y == c) & (c == j)))
                    def _():
                        act(copy)

            each(lambda copy: copy.start())
            yield
            acc[...] = jnp.zeros_like(acc)
            for z in range(4):
                mine = (z == o) & (o % 2 == y) & (y == c)

                @pl.when(has & mine)
                def _():
                    acc[...] += m.out_part[c].astype(F32)

                @pl.when(has & jnp.logical_not(mine))
                def _():
                    ref = held.at[z]
                    place_copy(ref, ref, send.at[0], recv.at[z], (h, blk(o, y, c))).wait_recv()
                    acc[...] += held[z].astype(F32)

            pair = remote(got_out, got_out, sem.out_pair, 0, peer(*NEAR_X))

            @pl.when(has)
            def _():
                got_out[...] = acc[...].astype(BF16)
                pair.start()

            yield
            each(lambda copy: copy.wait_send())

            @pl.when(has)
            def _():
                pair.wait_send()

            @pl.when(jnp.logical_not(has))
            def _():
                landed(got_out, sem.out_pair, 0)

        def go_copy(s, j):
            z = 2 * s + j
            return place_copy(
                m.go.at[j, :, pl.ds(s * n, n)],
                m.gs.at[:, pl.ds(pl.multiple_of(o * n, n), n)],
                sem.go_send.at[z],
                sem.go_recv.at[o],
                (h, z * 4 + g),
            )

        def stream(s):
            scatters = [pick_refs(i) for i in stream_ids[s][0]]
            gathers = pick_refs(stream_ids[s][1])
            at = lambda q: pl.ds(s * rows + q * q_rows, q_rows)
            branch = dot_tn(
                src.attended[:, :, s * n : (s + 1) * n].reshape(2 * he, n), src.out_own[...]
            )
            partial[s] = branch.astype(BF16).reshape(8, r, d)
            yield from scatter_steps(piece(partial, s), plain(total, s), *scatters[0])
            xh, scale_r = norm_parts(src.embedded[s] + (total[s] + vec(0)))
            m.xh_one[s] = xh
            m.scale_one[s] = scale_r
            value = xh * vec(4) + vec(1)
            m.first[s] = value
            low[s] = value.astype(BF16)
            yield from gather_steps(plain(low, s), piece(m.first_g, s), gathers[0])
            if s == 0:
                for copy in weights:
                    copy.wait()
            for q in range(2):
                rows_in = quarter(m.first_g, s, q)
                for k in range(2):
                    cols = slice(k * fh, (k + 1) * fh)
                    inner = jnp.dot(rows_in, ups[k](), preferred_element_type=F32)
                    inner = inner + src.up_bias[:, cols]
                    phi = 0.5 + 0.5 * lax.erf(inner * (0.5**0.5))
                    m.act[at(q), cols] = (inner * phi).astype(BF16)
                    bell = jnp.exp(inner * inner * -0.5) * (1.0 / math.sqrt(2.0 * math.pi))
                    m.slope[at(q), cols] = phi + inner * bell
                    yield
                for k in range(2):
                    part = jnp.dot(m.act[at(q)], downs[k](), preferred_element_type=F32)
                    partial[s, 4 * q : 4 * q + 4, :, k * half_d : (k + 1) * half_d] = part.astype(
                        BF16
                    ).reshape(4, r, half_d)
                yield
            yield from scatter_steps(piece(partial, s), plain(total, s), *scatters[1])
            xh, scale_r = norm_parts(m.first[s] + (total[s] + vec(2)))
            out_ref[s] = (xh * vec(5) + vec(3)).astype(BF16)
            cot = src.cotangent[s].astype(F32)
            note(5, cot * xh)
            note(3, cot)
            grad = norm_back(xh, scale_r, cot * vec(5))
            m.grad_two[s] = grad
            low[s] = grad.astype(BF16)
            note(2, low[s].astype(F32))
            yield from gather_steps(plain(low, s), piece(m.grad_g, s), gathers[1])
            for q in range(2):
                rows_in = quarter(m.grad_g, s, q)
                back = dot_nt(rows_in[:, :half_d], downs[0]()) + dot_nt(
                    rows_in[:, half_d:], downs[1]()
                )
                back = (back * m.slope[at(q)]).astype(BF16)
                m.inner_grad[at(q)] = back
                m.up_sums[...] += jnp.sum(back.astype(F32), axis=0, keepdims=True)
                yield
                part = dot_nt(back[:, :fh], ups[0]()) + dot_nt(back[:, fh:], ups[1]())
                partial[s, 4 * q : 4 * q + 4] = part.astype(BF16).reshape(4, r, d)
                yield
            last = scatter_steps(piece(partial, s), plain(total, s), *scatters[2])
            next(last)
            if s == seqs - 1:
                all_grads = m.grad_g[...].reshape(seqs * rows, d)
                for z in range(planes):
                    cols = slice(z * fcols, (z + 1) * fcols)
                    m.down_part[z] = dot_tn(m.act[:, cols], all_grads).astype(BF16)
                step(down)
                yield
                for z in range(planes):
                    cols = slice(z * 4 * e, (z + 1) * 4 * e)
                    all_first = m.first_g[:, :, :, cols].reshape(seqs * rows, 4 * e)
                    m.up_part[z] = dot_tn(all_first, m.inner_grad[...]).astype(BF16)
                yield
            yield from last
            grad = m.grad_two[s] + total[s]
            note(4, grad * m.xh_one[s])
            note(1, grad)
            grad = norm_back(m.xh_one[s], m.scale_one[s], grad * vec(4))
            m.resid[s] = grad
            low[s] = grad.astype(BF16)
            note(0, low[s].astype(F32))
            for k, _ in enumerate(gather_steps(plain(low, s), piece(m.branch_g, s), gathers[2])):
                yield
                if s == seqs - 1 and k in EARLY:
                    step(down)
            go = dot_nt(src.out_own[...], m.branch_g[s].reshape(rows, d))
            m.go[:, :, s * n : (s + 1) * n] = go.astype(BF16).reshape(2, he, n)
            for j in range(2):

                @pl.when(o != 2 * s + j)
                def _():
                    go_copy(s, j).start()

                @pl.when(o == 2 * s + j)
                def _():
                    m.gs[:, pl.ds(pl.multiple_of(o * n, n), n)] = m.go[
                        j, :, s * n : (s + 1) * n
                    ]

            yield

        down, up, out, qkv = down_sums(), up_sums(), out_sums(), qkv_sums()
        gens = [stream(s) for s in range(seqs)]
        for _ in range(lag):
            next(gens[0])
        while gens:
            for gen in list(gens):
                try:
                    next(gen)
                except StopIteration:
                    gens.remove(gen)

        step(up)
        grad_out = jnp.dot(
            src.attended[...].reshape(2 * he, 2 * n),
            m.branch_g[...].reshape(seqs * rows, d),
            preferred_element_type=F32,
        )
        m.out_part[...] = grad_out.astype(BF16).reshape(2, he, d)
        held = src.held
        gs, qs, q_t, g_t, dq, delta, pair_low = (
            m.gs, m.qs, m.q_rows, m.g_rows, m.dq, m.delta, m.pair_low
        )
        q32 = held[0].astype(F32) * scale
        qs[...] = q32.astype(BF16)
        q_t[...] = q32.T.astype(BF16)
        row = lax.broadcasted_iota(jnp.int32, (slots, 1), 0)
        m.pick[...] = (src.ids[...] == row).astype(F32).astype(BF16)
        for z in range(4):

            @pl.when(z != o)
            def _():
                ref = gs.at[:, pl.ds(z * n, n)]
                place_copy(
                    ref, ref, sem.go_send.at[0], sem.go_recv.at[z], peer(*NEAR_X)
                ).wait_recv()

        g32 = gs[...].astype(F32)
        g_t[...] = g32.T.astype(BF16)
        delta[...] = jnp.sum(g32 * src.pair_out[...], axis=0, keepdims=True)
        mine = pl.ds(pl.multiple_of((o // 2) * n, n), n)
        dqkv = m.dqkv

        def back(part, which, i, z):
            return remote(
                pair_low.at[part, :, pl.ds(pl.multiple_of(z * n, n), n)],
                dqkv.at[part, o % 2, :, mine],
                which,
                i,
                (h, z * 4 + g),
            )

        late = pl.ds(1, 2)
        for i in range(4):
            z = (o + 1 + i) % 4

            @pl.loop(0, n // key_rows)
            def _(step):
                at = pl.ds(pl.multiple_of(z * n + step * key_rows, key_rows), key_rows)
                k_cols = held[1, :, at]
                k_rows = k_cols.astype(F32).T.astype(BF16)
                v_rows = held[2, :, at].astype(F32).T.astype(BF16)
                s = jnp.dot(k_rows, qs[...], preferred_element_type=F32)
                p = jnp.exp(s - src.lse[...])
                dv = jnp.dot(p.astype(BF16), g_t[...], preferred_element_type=F32)
                dp = jnp.dot(v_rows, gs[...], preferred_element_type=F32)
                ds = (p * (dp - delta[...])).astype(BF16)
                dk = jnp.dot(ds, q_t[...], preferred_element_type=F32)
                dq[...] += jnp.dot(k_cols, ds, preferred_element_type=F32)
                pair_low[1, :, at] = dk.T.astype(BF16)
                pair_low[2, :, at] = dv.T.astype(BF16)

            if i < 3:
                back(late, sem.ksem, i, z).start()
            if i == 0:
                step(*[down] * (3 - len(EARLY)))
            if i == 2:
                step(up)
        pair_low[0] = (dq[...] * scale).astype(BF16)
        for i in range(3):
            back(pl.ds(0, 1), sem.qsem, i, (o + 1 + i) % 4).start()
        dqkv[:, o % 2, :, mine] = pair_low[:, :, pl.ds(pl.multiple_of(o * n, n), n)]
        step(down, up)
        for i in range(3):
            z = (o + 3 - i) % 4
            there = pl.ds(pl.multiple_of((z // 2) * n, n), n)
            landed(dqkv.at[late, z % 2, :, there], sem.ksem, i)
            landed(dqkv.at[pl.ds(0, 1), z % 2, :, there], sem.qsem, i)

        all_dqkv = lambda: dqkv[...].reshape(width_qkv, 2 * n)

        def back_chunk(q):
            part = lax.dot_general(
                all_dqkv(),
                src.qkv_own[q * w : (q + 1) * w],
                (((0,), (1,)), ((), ())),
                preferred_element_type=F32,
            )
            partial[:, :, :, q * w : (q + 1) * w] = part.astype(BF16).reshape(seqs, 8, r, w)

        def chunk(q):
            cols = pl.ds(q * w, w)
            scatter, (zsem, ysem, csem) = pick_refs(chunk_ids[q][0]), pick_refs(chunk_ids[q][1])
            back_chunk(q)
            yield from scatter_steps(
                lambda i, slot: partial.at[i, slot, :, cols],
                lambda i: grad_ref.at[i, :, cols],
                *scatter,
            )
            grad = grad_ref[:, :, cols] + m.resid[:, :, cols]
            grad_ref[:, :, cols] = grad
            grad = grad.reshape(own_rows, w)
            m.own[q] = grad.astype(BF16)
            second = src.second[...]
            m.sums[6:7, cols] = jnp.sum(grad * (1.0 - second), axis=0, keepdims=True)
            m.sums[7:8, cols] = jnp.sum(grad * second, axis=0, keepdims=True)
            yield from blk_gather_steps(
                m.own.at[q],
                lambda z, yy, cc: m.gathered.at[q, blk(z, yy, cc)],
                zsem,
                ysem,
                csem,
            )
            found = jnp.dot(
                m.pick[...],
                m.gathered[q].reshape(blks * own_rows, w),
                preferred_element_type=F32,
            )
            pos_ref[:, cols] = found
            m.pos_low[q] = found.astype(BF16)
            copy = remote(
                m.pos_low.at[q], m.pos_held.at[q], sem.pair_sem, q, peer(*NEAR_X)
            )
            copy.start()
            pairs.append(copy)
            yield

        pairs = []
        active, waiting = [], [chunk(q) for q in range(chunks)]
        turn = 0
        while active or waiting:
            if waiting and turn % chunk_lag == 0:
                active.append(waiting.pop(0))
            for gen in list(active):
                try:
                    next(gen)
                except StopIteration:
                    active.remove(gen)
            if turn == 0:
                low_all = src.plane_low[...].reshape(seqs * rows, d)
                for z in range(planes):
                    cols = slice(z * 4 * e, (z + 1) * 4 * e)
                    part = lax.dot_general(
                        low_all[:, cols],
                        all_dqkv(),
                        (((0,), (1,)), ((), ())),
                        preferred_element_type=F32,
                    )
                    m.qkv_part[z] = part.astype(BF16)
                step(qkv)
                ones = jnp.ones((8, 2 * n), BF16)
                heads = dot_nt(ones, all_dqkv())
                own_lanes = pl.ds(pl.multiple_of(t * 128, 128), 128)
                m.sums[8:9, own_lanes] = heads[0:1, 0:128]
                m.sums[9:10, own_lanes] = heads[0:1, 256:384]
                for i in range(4):
                    m.up_spots[pl.ds((i * 4 + g) * 2 + h, 1)] = m.up_sums[
                        :, i * 128 : (i + 1) * 128
                    ]
            for when, gen in zip(TURNS, (up, qkv, out)):
                if turn in when:
                    step(gen)
            turn += 1
        for b in range(blks):
            m.pack[b, 0:16] = m.sums[:, b // 2 * 128 : (b // 2 + 1) * 128]
            m.pack[b, 16:18] = m.up_spots[2 * b : 2 * b + 2]
            m.pack[b, 18:24] = jnp.zeros((6, 128), F32)
        copies = []
        for k, p in enumerate(ALL):
            to = peer(*p)
            copy = remote(m.pack.at[to[1]], m.packs.at[k], sem.pack_sem, k, to)
            copy.start()
            copies.append(copy)
        for gen in (down, up, out, qkv):
            for _ in gen:
                pass
        for q, copy in enumerate(pairs):
            copy.wait()
            cols = pl.ds(q * w, w)
            pos_ref[:, cols] = pos_ref[:, cols] + m.pos_held[q].astype(F32)
        for copy in copies:
            copy.wait()
        totals[...] = m.pack[blk(o, y, c)] + jnp.sum(m.packs[...], axis=0)
        for i in range(3):
            back(late, sem.ksem, i, (o + 1 + i) % 4).wait_send()
            back(pl.ds(0, 1), sem.qsem, i, (o + 1 + i) % 4).wait_send()
        for s in range(seqs):
            for j in range(2):

                @pl.when(o != 2 * s + j)
                def _():
                    go_copy(s, j).wait_send()

    return Part(
        run,
        list(vars(x).values()),
        [
            ((seqs, r, d), BF16),
            ((seqs, r, d), F32),
            ((slots, d), F32),
            ((2, fcols, d), BF16),
            ((e, 8 * f), BF16),
            ((e, 3 * d), BF16),
            ((he, d), BF16),
            ((24, 128), F32),
        ],
        need,
        ALL,
    )


def rows_steps(own_of, near, part, from_y, term, ends, mids, last, csem, ysem, zsem, out):
    h, o, y, c = place()
    at, seen = mirrored()
    dev_y = peer(*NEAR_Y)
    order = [seen(3), seen(2), seen(1 - at), o]
    end, inner, other = (h, blk(seen(0), y, c)), (h, blk(seen(1), y, c)), (h, blk(seen(2), y, c))
    sent = []
    for j, z in enumerate(order):
        landed(near.at[0, j], csem, j)
        part[j] = own_of(z, 1 - y)[...] + near[0, j]
        copy = remote(part.at[j], from_y.at[j], ysem, j, dev_y)
        copy.start()
        sent.append(copy)
    for j, z in enumerate(order):
        yield
        landed(near.at[1, j], csem, 4 + j)
        landed(from_y.at[j], ysem, j)
        term[j] = own_of(z, y)[...] + near[1, j] + from_y[j]
        if j < 3:

            @pl.when(at == 0)
            def _():
                remote(term.at[j], ends.at[j], zsem, j, inner).start()

        if j < 2:

            @pl.when(at == 1)
            def _():
                landed(ends.at[j], zsem, j)
                term[j] += ends[j]
                remote(term.at[j], mids.at[j], zsem, 3 + j, other).start()

    yield

    @pl.when(at == 1)
    def _():
        landed(mids.at[0], zsem, 3)
        term[2] += mids[0]
        remote(term.at[2], last, zsem, 5, end).start()

    yield

    @pl.when(at == 1)
    def _():
        landed(ends.at[2], zsem, 2)
        landed(mids.at[1], zsem, 4)
        out[...] = (term[3] + ends[2] + mids[1]).astype(F32)
        for j in range(2):
            remote(term.at[j], mids.at[j], zsem, 3 + j, other).wait_send()
        remote(term.at[2], last, zsem, 5, end).wait_send()

    @pl.when(at == 0)
    def _():
        landed(last, zsem, 5)
        out[...] = (term[3] + last[...]).astype(F32)
        for j in range(3):
            remote(term.at[j], ends.at[j], zsem, j, inner).wait_send()

    for copy in sent:
        copy.wait_send()


def first_half(x, scale, lag):
    names = list(vars(x))
    seqs, r, d = x.hidden.shape
    slots = x.table.shape[0]
    four, e, wq = x.qkv_cut.shape
    f = x.up_cut.shape[2]
    fcols = x.down_cut.shape[0]
    he = wq // 6
    n = 8 * r
    length = 4 * n
    half, fh, half_d = r // 2, f // 2, d // 2
    blks = 16
    cols = 256
    small = small_gather(x.packed)
    outw = out_weights(x.out_weight)
    trade_qkv, trade_up = blk_exchange(x.qkv_cut), blk_exchange(x.up_cut)
    need = []

    def many(specs):
        start = len(need)
        need.extend(specs)
        return list(range(start, len(need)))

    block = (r, d)
    shapes = dict(
        everyone=((blks,) + x.packed.shape, F32),
        found=((4, 2, 2, seqs, r, d), BF16),
        rows=((seqs, r, d), F32),
        low=((seqs, r, d), BF16),
        qkv_in=(x.qkv_cut.shape, BF16),
        projected=((3, 2, he, 2 * n), BF16),
        keys=((length, he), BF16),
        pair_low=((he, length), BF16),
    )
    ids = {k: many([pltpu.VMEM(*v)])[0] for k, v in shapes.items()}
    counts = dict(qkv_sem=3, up_sem=3, down_sem=3, back_sem=3)
    sem_ids = {k: many([sems(v)])[0] for k, v in counts.items()}
    for k in ("send", "recv"):
        sem_ids[k] = many([pltpu.SemaphoreType.DMA((4,))])[0]
    small_ids, outw_ids = many(small.scratch), many(outw.scratch)
    trade_ids = many(trade_qkv.scratch), many(trade_up.scratch)
    row_ids = [
        many(
            [
                pltpu.VMEM((2, 4) + block, BF16),
                pltpu.VMEM((4,) + block, BF16),
                pltpu.VMEM((4,) + block, BF16),
                pltpu.VMEM((4,) + block, BF16),
                pltpu.VMEM((3,) + block, BF16),
                pltpu.VMEM((2,) + block, BF16),
                pltpu.VMEM(block, BF16),
                sems(8),
                sems(4),
                sems(6),
            ]
        )
        for _ in range(seqs)
    ]
    gather_ids = [many([sems(14)])[0] for _ in range(seqs)]

    def run(ins, outs, own):
        src = SimpleNamespace(**dict(zip(names, ins)))
        attended, held, o_ref, lse_ref, emb_ref, plane_ref, qkv_ref = outs[:7]
        outw_ref, up_one, up_in, down_one, vec_ref, bias_ref, ids_ref = outs[7:]
        m = SimpleNamespace(**{k: own[v] for k, v in ids.items()})
        sem = SimpleNamespace(**{k: own[v] for k, v in sem_ids.items()})
        pick_refs = lambda some: [own[i] for i in some]
        h, o, y, c = place()
        g = y * 2 + c
        t = h * 4 + g
        gather_small = small.run((src.packed,), (m.everyone,), pick_refs(small_ids))
        trades = [
            trade_qkv.run((src.qkv_cut,), (m.qkv_in,), pick_refs(trade_ids[0])),
            trade_up.run((src.up_cut,), (up_in,), pick_refs(trade_ids[1])),
        ]
        weights = outw.run((src.out_weight,), (outw_ref,), pick_refs(outw_ids))
        next(gather_small)
        next(trades[0])
        yield
        next(trades[1])
        bulk = []

        def line(ref, dst, s):
            for k, p in enumerate(COLUMN):
                copy = remote(ref, dst.at[o], s, k, peer(*p))
                copy.start()
                bulk.append(copy)
            dst[pl.ds(o, 1)] = ref[...][None]

        for _ in gather_small:
            pass

        at, seen = mirrored()
        order = [seen(3), seen(2), seen(1 - at), o]
        b = blk(o, y, c)
        row = lax.broadcasted_iota(jnp.int32, (slots, 1), 0).astype(F32)
        base = (b * slots).astype(F32)
        streams = [pick_refs(i) for i in row_ids]
        core = []
        for i, yy in enumerate((1 - y, y)):
            for j, z in enumerate(order):
                hot = jnp.concatenate(
                    [
                        (m.everyone[blk(z, yy, cc), 7:8] - base == row).astype(F32).astype(BF16)
                        for cc in range(2)
                    ],
                    axis=1,
                )
                rows_of = dot_tn(hot, src.table[...]).astype(BF16)
                m.found[z, yy] = rows_of.reshape(2, seqs, r, d)
                for s in range(seqs):
                    near, csem = streams[s][0], streams[s][7]
                    copy = remote(
                        m.found.at[z, yy, 1 - c, s],
                        near.at[i, j],
                        csem,
                        i * 4 + j,
                        peer(*NEAR_C),
                    )
                    copy.start()
                    core.append(copy)
            if i == 0:
                for gen in trades:
                    for _ in gen:
                        pass
                line(m.qkv_in, qkv_ref, sem.qkv_sem)

        lane = lax.broadcasted_iota(jnp.int32, (1, 128), 1)
        for k in range(5):
            for i in range(blks // 2):
                one, two = m.everyone[2 * i, k : k + 1], m.everyone[2 * i + 1, k : k + 1]
                lanes = slice(i * 128, (i + 1) * 128)
                vec_ref[2 * k : 2 * k + 1, lanes] = jnp.where(
                    lane < 64, one, pltpu.roll(two, 64, 1)
                )
                vec_ref[2 * k + 1 : 2 * k + 2, lanes] = jnp.where(
                    lane < 64, pltpu.roll(one, 64, 1), two
                )
        for i in range(blks):
            ids_ref[:, i * 128 : (i + 1) * 128] = (m.everyone[i, 7:8] - base).astype(jnp.int32)
        for i in range(4):
            bias_ref[:, i * 128 : (i + 1) * 128] = m.everyone[i * 4 + g, pl.ds(5 + h, 1)]
        eye = lax.broadcasted_iota(jnp.int32, (128, 128), 0) == lax.broadcasted_iota(
            jnp.int32, (128, 128), 1
        )

        def column(k):
            lanes = vec_ref[k : k + 1, pl.ds(pl.multiple_of(t * 128, 128), 128)]
            return jnp.sum(jnp.where(eye, lanes, 0.0), axis=1, keepdims=True)

        def send_pair(s, j):
            z = 2 * s + j
            return place_copy(
                m.projected.at[:, j, :, pl.ds(s * n, n)],
                held.at[:, :, pl.ds(pl.multiple_of(o * n, n), n)],
                sem.send.at[z],
                sem.recv.at[o],
                (h, z * 4 + g),
            )

        def stream(s):
            yield from rows_steps(
                lambda z, yy: m.found.at[z, yy, c, s], *streams[s], m.rows.at[s]
            )
            second = src.second[s * r : (s + 1) * r]
            typed = vec_ref[8:9] * (1.0 - second) + vec_ref[9:10] * second
            value = src.hidden[s].astype(F32) + m.rows[s] + typed
            emb_ref[s] = value
            m.low[s] = value.astype(BF16)
            yield from gather_steps(
                lambda i: m.low.at[s, pl.ds(i * half, half)],
                lambda i, slot: plane_ref.at[s, slot, pl.ds(i * half, half)],
                own[gather_ids[s]],
            )
            if s == 0:
                for copy in bulk:
                    copy.wait()
                bulk.clear()
                line(up_in.at[:, :, pl.ds(0, fh)], up_one, sem.up_sem)
            part = lax.dot_general(
                qkv_ref[...].reshape(d, wq),
                plane_ref[s].reshape(n, d),
                (((0,), (1,)), ((), ())),
                preferred_element_type=F32,
            )
            here = slice(s * n, (s + 1) * n)
            third = wq // 3
            m.projected[0, :, :, here] = (part[:third] + column(0)).astype(BF16).reshape(2, he, n)
            m.projected[1, :, :, here] = part[third : 2 * third].astype(BF16).reshape(2, he, n)
            m.projected[2, :, :, here] = (
                (part[2 * third :] + column(1)).astype(BF16).reshape(2, he, n)
            )
            for j in range(2):

                @pl.when(o != 2 * s + j)
                def _():
                    send_pair(s, j).start()

                @pl.when(o == 2 * s + j)
                def _():
                    held[:, :, pl.ds(pl.multiple_of(o * n, n), n)] = m.projected[:, j, :, here]

            yield

        gens = [stream(s) for s in range(seqs)]
        for _ in range(lag):
            next(gens[0])
        while gens:
            for gen in list(gens):
                try:
                    next(gen)
                except StopIteration:
                    gens.remove(gen)
        next(weights)
        for z in range(4):

            @pl.when(z != o)
            def _():
                ref = held.at[:, :, pl.ds(z * n, n)]
                place_copy(ref, ref, sem.send.at[0], sem.recv.at[z], peer(*NEAR_X)).wait_recv()

        line(src.down_cut.at[:, pl.ds(0, half_d)], down_one, sem.down_sem)
        m.keys[...] = held[1].astype(F32).T.astype(BF16)
        mine = pl.ds(pl.multiple_of((o // 2) * n, n), n)

        def back(i, z):
            return remote(
                m.pair_low.at[:, pl.ds(pl.multiple_of(z * n, n), n)],
                attended.at[o % 2, :, mine],
                sem.back_sem,
                i,
                (h, z * 4 + g),
            )

        @pl.loop(0, 4 * (n // cols))
        def _(step):
            i = step // (n // cols)
            z = (o + 1 + i) % 4
            here = pl.ds(pl.multiple_of(z * n + step % (n // cols) * cols, cols), cols)
            q = (held[0, :, here].astype(F32) * scale).astype(BF16)
            s = jnp.dot(m.keys[...], q, preferred_element_type=F32)
            peak = jnp.max(s, axis=0, keepdims=True)
            p = jnp.exp(s - peak)
            total = jnp.sum(p, axis=0, keepdims=True)
            out = jnp.dot(held[2], p.astype(BF16), preferred_element_type=F32) / total
            o_ref[:, here] = out
            m.pair_low[:, here] = out.astype(BF16)
            lse_ref[:, here] = peak + jnp.log(total)

            @pl.when((step % (n // cols) == n // cols - 1) & (i < 3))
            def _():
                back(i, z).start()

        attended[o % 2, :, mine] = m.pair_low[:, pl.ds(pl.multiple_of(o * n, n), n)]
        for i in range(3):
            back(i, (o + 1 + i) % 4).wait_send()
            z = (o + 3 - i) % 4
            landed(attended.at[z % 2, :, pl.ds(pl.multiple_of((z // 2) * n, n), n)], sem.back_sem, i)
        for _ in weights:
            pass
        for copy in bulk:
            copy.wait()
        for copy in core:
            copy.wait_send()
        for s in range(seqs):
            for j in range(2):

                @pl.when(o != 2 * s + j)
                def _():
                    send_pair(s, j).wait_send()

    return Part(
        run,
        list(vars(x).values()),
        [
            ((2, he, 2 * n), BF16),
            ((3, he, length), BF16),
            ((he, length), F32),
            ((1, length), F32),
            ((seqs, r, d), F32),
            ((seqs, 8, r, d), BF16),
            ((4,) + x.qkv_cut.shape, BF16),
            ((2,) + x.out_weight.shape, BF16),
            ((4, four, e, fh), BF16),
            (x.up_cut.shape, BF16),
            ((4, fcols, half_d), BF16),
            ((10, d), F32),
            ((1, f), F32),
            ((1, blks * seqs * r), jnp.int32),
        ],
        need,
        ALL,
    )


def finish_kernel(odd, layer, hid, pos, down, up, qkv, out, totals, *outs):
    o_layer, o_hid, o_pos, o_types, o_qkv, o_out, o_up, o_down, o_upb, o_gains, o_bias = outs
    o_layer[...] = layer[...]
    o_hid[...] = hid[...]
    o_pos[...] = pos[...]
    o_qkv[...] = qkv[...].astype(F32)
    o_out[...] = out[...].astype(F32)
    o_up[...] = up[...].astype(F32)
    o_down[...] = down[...].astype(F32)
    t = totals[...]
    mine = jnp.where(odd[0] == 1, t[:, 64:], t[:, :64])
    o_types[...] = mine[6:8]
    o_gains[...] = mine[4:6]
    o_bias[0:1] = mine[8:9]
    o_bias[1:2] = mine[9:10]
    o_bias[2:6] = mine[0:4]
    o_upb[...] = t[16:18]


def finish(odd, layer, hid, pos, down, up, qkv, out, totals):
    like = lambda a, dtype=F32: jax.ShapeDtypeStruct(a.shape, dtype)
    e = out.shape[0]
    return pl.pallas_call(
        finish_kernel,
        name="finish",
        out_shape=[
            like(layer, BF16),
            like(hid),
            like(pos),
            jax.ShapeDtypeStruct((2, e), F32),
            like(qkv),
            like(out),
            like(up),
            like(down),
            jax.ShapeDtypeStruct((2, 128), F32),
            jax.ShapeDtypeStruct((2, e), F32),
            jax.ShapeDtypeStruct((6, e), F32),
        ],
        in_specs=[pl.BlockSpec(memory_space=pltpu.SMEM)] + [VSPEC] * 8,
        out_specs=[VSPEC] * 11,
        compiler_params=pltpu.CompilerParams(vmem_limit_bytes=48 << 20),
    )(odd, layer, hid, pos, down, up, qkv, out, totals)
def norm_layer(values_in, gain_row, offset_row):
    average = jnp.mean(values_in, axis=-1, keepdims=True)
    centred = values_in - average
    variance = jnp.mean(centred * centred, axis=-1, keepdims=True)
    return centred * lax.rsqrt(variance + 1e-12) * gain_row + offset_row


def gelu_exact(inner_product_sum):
    return jax.nn.gelu(inner_product_sum, approximate=False)


def widest_block(length, limit):
    return max(
        (candidate for candidate in range(1, min(length, limit) + 1) if length % candidate == 0)
    )


def block_scores(query_heads, key_block, score_scale):
    return (
        jnp.einsum("sqhe,skhe->shqk", query_heads, key_block, preferred_element_type=jnp.float32)
        * score_scale
    )


def key_side(query_block, grad_block, lse_block, delta_block, key_heads, value_heads, score_scale):
    scores = block_scores(query_block, key_heads, score_scale)
    weights = jnp.exp(scores - lse_block[..., None])
    more_values = jnp.einsum(
        "shqk,sqhe->shke",
        weights.astype(jnp.bfloat16),
        grad_block,
        preferred_element_type=jnp.float32,
    )
    grad_weights = jnp.einsum(
        "sqhe,skhe->shqk", grad_block, value_heads, preferred_element_type=jnp.float32
    )
    grad_scores = weights * (grad_weights - delta_block[..., None])
    more_keys = jnp.einsum(
        "shqk,sqhe->shke",
        grad_scores.astype(jnp.bfloat16),
        query_block,
        preferred_element_type=jnp.float32,
    )
    return (more_keys, more_values)


def forward_fold(query_heads, score_scale, head_count, head_size):

    def fold_keys(running, portion, offset):
        key_piece, value_piece = portion
        seq_count, length = (key_piece.shape[0], key_piece.shape[1])
        block_size = widest_block(length, 512)

        def one_step(block_index, carried):
            row_peak, row_total, weighted = carried
            row_start = block_index * block_size
            key_block = lax.dynamic_slice_in_dim(key_piece, row_start, block_size, 1).reshape(
                seq_count, block_size, head_count, head_size
            )
            value_block = lax.dynamic_slice_in_dim(value_piece, row_start, block_size, 1).reshape(
                seq_count, block_size, head_count, head_size
            )
            scores = block_scores(query_heads, key_block, score_scale)
            new_peak = jnp.maximum(row_peak, jnp.max(scores, axis=-1))
            shrink = jnp.exp(row_peak - new_peak)
            weights = jnp.exp(scores - new_peak[..., None])
            row_total = row_total * shrink + jnp.sum(weights, axis=-1)
            weighted = weighted * shrink[..., None] + jnp.einsum(
                "shqk,skhe->shqe",
                weights.astype(jnp.bfloat16),
                value_block,
                preferred_element_type=jnp.float32,
            )
            return (new_peak, row_total, weighted)

        return lax.fori_loop(0, length // block_size, one_step, running)

    return fold_keys


def query_fold(query_heads, grad_heads, log_totals, delta_rows, score_scale, head_count, head_size):

    def fold_keys(running, portion, offset):
        key_piece, value_piece = portion
        seq_count, length = (key_piece.shape[0], key_piece.shape[1])
        block_size = widest_block(length, 512)

        def one_step(block_index, weighted):
            row_start = block_index * block_size
            key_block = lax.dynamic_slice_in_dim(key_piece, row_start, block_size, 1).reshape(
                seq_count, block_size, head_count, head_size
            )
            value_block = lax.dynamic_slice_in_dim(value_piece, row_start, block_size, 1).reshape(
                seq_count, block_size, head_count, head_size
            )
            scores = block_scores(query_heads, key_block, score_scale)
            weights = jnp.exp(scores - log_totals[..., None])
            grad_weights = jnp.einsum(
                "sqhe,skhe->shqk", grad_heads, value_block, preferred_element_type=jnp.float32
            )
            grad_scores = weights * (grad_weights - delta_rows[..., None])
            return weighted + jnp.einsum(
                "shqk,skhe->shqe",
                grad_scores.astype(jnp.bfloat16),
                key_block,
                preferred_element_type=jnp.float32,
            )

        return lax.fori_loop(0, length // block_size, one_step, running)

    return fold_keys


def key_fold(key_heads, value_heads, score_scale, head_count, head_size):

    def fold_queries(running, portion, offset):
        query_piece, grad_piece, lse_piece, delta_piece = portion
        seq_count, length = (query_piece.shape[0], query_piece.shape[1])
        block_size = widest_block(length, 512)

        def one_step(block_index, carried):
            grad_keys, grad_values = carried
            row_start = block_index * block_size
            query_block = lax.dynamic_slice_in_dim(query_piece, row_start, block_size, 1).reshape(
                seq_count, block_size, head_count, head_size
            )
            grad_block = lax.dynamic_slice_in_dim(grad_piece, row_start, block_size, 1).reshape(
                seq_count, block_size, head_count, head_size
            )
            lse_block = lax.dynamic_slice_in_dim(lse_piece, row_start, block_size, 1).transpose(
                0, 2, 1
            )
            delta_block = lax.dynamic_slice_in_dim(delta_piece, row_start, block_size, 1).transpose(
                0, 2, 1
            )
            more_keys, more_values = key_side(
                query_block, grad_block, lse_block, delta_block, key_heads, value_heads, score_scale
            )
            return (grad_keys + more_keys, grad_values + more_values)

        return lax.fori_loop(0, length // block_size, one_step, running)

    return fold_queries


def layer_in_blocks(
    hidden,
    pos_ids,
    type_ids,
    cotangent,
    pos_table,
    type_table,
    query_key_value_weight,
    attention_output_weight,
    up_projection_weight,
    down_projection_weight,
    up_projection_bias,
    norm_gains,
    biases,
):
    seq_count, seg_tokens, model_width = hidden.shape
    row_count = seq_count * seg_tokens
    head_count = HEADS // lax.axis_size("head")
    head_size = model_width // HEADS
    local_width = head_count * head_size
    query_rows = lax.axis_size("head") * seg_tokens
    score_scale = 1.0 / math.sqrt(head_size)

    def fetch_weights():
        return (
            lax.all_gather(query_key_value_weight, "blk", axis=0, tiled=True),
            lax.all_gather(attention_output_weight, "blk", axis=0, tiled=True),
            lax.all_gather(up_projection_weight, "blk", axis=0, tiled=True),
            lax.all_gather(down_projection_weight, "blk", axis=0, tiled=True),
            lax.all_gather(up_projection_bias, "blk", axis=0, tiled=True),
            lax.all_gather(norm_gains, "blk", axis=1, tiled=True),
            lax.all_gather(biases, "blk", axis=1, tiled=True),
            lax.all_gather(type_table, "blk", axis=1, tiled=True),
        )

    qkv_full, out_full, up_full, down_full, up_bias_full, gain_full, bias_full, type_full = (
        fetch_weights()
    )
    bias_float = bias_full.astype(jnp.float32)
    gain_float = gain_full.astype(jnp.float32)
    flat_pos = pos_ids.reshape(row_count)
    portion = lax.all_gather(pos_table, "blk", axis=0, tiled=True)
    local_slots = flat_pos
    onehot = (
        local_slots[:, None] == jnp.arange(portion.shape[0], dtype=jnp.int32)[None, :]
    ).astype(jnp.bfloat16)
    positions = jnp.dot(onehot, portion, preferred_element_type=jnp.float32)
    is_second = type_ids.reshape(row_count, 1) == 1
    typed_rows = jnp.where(
        is_second, type_full[1].astype(jnp.float32), type_full[0].astype(jnp.float32)
    )
    embedded_tokens = (
        hidden.reshape(row_count, model_width).astype(jnp.float32) + positions + typed_rows
    )
    embedded_low = embedded_tokens.astype(jnp.bfloat16)
    projected_rows = jnp.dot(embedded_low, qkv_full, preferred_element_type=jnp.float32)
    token_shape = (seq_count, seg_tokens, model_width)
    queries = (
        (projected_rows[:, :model_width] + bias_float[0]).astype(jnp.bfloat16).reshape(token_shape)
    )
    keys_token = (
        projected_rows[:, model_width : 2 * model_width].astype(jnp.bfloat16).reshape(token_shape)
    )
    values_token = (
        (projected_rows[:, 2 * model_width :] + bias_float[1])
        .astype(jnp.bfloat16)
        .reshape(token_shape)
    )
    query_local, key_local, value_local = (
        lax.all_to_all(queries, "head", split_axis=2, concat_axis=1, tiled=True),
        lax.all_to_all(keys_token, "head", split_axis=2, concat_axis=1, tiled=True),
        lax.all_to_all(values_token, "head", split_axis=2, concat_axis=1, tiled=True),
    )
    head_shape = (seq_count, query_rows, head_count, head_size)
    query_heads = query_local.reshape(head_shape)
    key_heads = key_local.reshape(head_shape)
    value_heads = value_local.reshape(head_shape)
    start_peak = jnp.full((seq_count, head_count, query_rows), -jnp.inf, jnp.float32)
    start_total = jnp.zeros((seq_count, head_count, query_rows), jnp.float32)
    zero_heads = jnp.zeros((seq_count, head_count, query_rows, head_size), jnp.float32)
    fold_keys = forward_fold(query_heads, score_scale, head_count, head_size)
    row_peak, row_total, weighted = fold_keys(
        (start_peak, start_total, zero_heads),
        (
            lax.all_gather(key_local, "blk", axis=1, tiled=True),
            lax.all_gather(value_local, "blk", axis=1, tiled=True),
        ),
        jnp.int32(0),
    )
    log_totals = row_peak + jnp.log(row_total)
    attention_result = weighted / row_total[..., None]
    attended_low = (
        attention_result.transpose(0, 2, 1, 3)
        .reshape(seq_count, query_rows, local_width)
        .astype(jnp.bfloat16)
    )
    attended_token = lax.all_to_all(
        attended_low, "head", split_axis=1, concat_axis=2, tiled=True
    ).reshape(row_count, model_width)
    residual_branch = (
        jnp.dot(attended_token, out_full, preferred_element_type=jnp.float32) + bias_float[2]
    )
    first_layer_norm, first_pull = jax.vjp(
        norm_layer, embedded_tokens + residual_branch, gain_float[0], bias_float[3]
    )
    first_low = first_layer_norm.astype(jnp.bfloat16)
    inner_product_sum = jnp.dot(
        first_low, up_full, preferred_element_type=jnp.float32
    ) + up_bias_full.astype(jnp.float32)
    gelu_activations, gelu_pull = jax.vjp(gelu_exact, inner_product_sum)
    activated_low = gelu_activations.astype(jnp.bfloat16)
    second_layer_norm = (
        jnp.dot(activated_low, down_full, preferred_element_type=jnp.float32) + bias_float[4]
    )
    final_norm, final_pull = jax.vjp(
        norm_layer, first_layer_norm + second_layer_norm, gain_float[1], bias_float[5]
    )
    layer_out = final_norm.astype(jnp.bfloat16).reshape(token_shape)
    qkv_full, out_full, up_full, down_full, up_bias_full, gain_full, bias_full, type_full = (
        fetch_weights()
    )
    grad_final, grad_gain_two, grad_shift_two = final_pull(
        cotangent.reshape(row_count, model_width).astype(jnp.float32)
    )
    grad_second = grad_final.astype(jnp.bfloat16)
    grad_down = jnp.einsum(
        "rf,rd->fd", activated_low, grad_second, preferred_element_type=jnp.float32
    )
    grad_bias_second = jnp.sum(grad_second.astype(jnp.float32), axis=0)
    (grad_inner,) = gelu_pull(
        jnp.einsum("rd,fd->rf", grad_second, down_full, preferred_element_type=jnp.float32)
    )
    grad_inner_low = grad_inner.astype(jnp.bfloat16)
    grad_up = jnp.einsum("rd,rf->df", first_low, grad_inner_low, preferred_element_type=jnp.float32)
    grad_up_bias = jnp.sum(grad_inner_low.astype(jnp.float32), axis=0)
    grad_first = grad_final + jnp.einsum(
        "rf,df->rd", grad_inner_low, up_full, preferred_element_type=jnp.float32
    )
    grad_resid, grad_gain_one, grad_shift_one = first_pull(grad_first)
    grad_branch = grad_resid.astype(jnp.bfloat16)
    grad_out = jnp.einsum(
        "re,rd->ed", attended_token, grad_branch, preferred_element_type=jnp.float32
    )
    grad_bias_branch = jnp.sum(grad_branch.astype(jnp.float32), axis=0)
    grad_attended = (
        jnp.einsum("rd,ed->re", grad_branch, out_full, preferred_element_type=jnp.float32)
        .astype(jnp.bfloat16)
        .reshape(token_shape)
    )
    grad_local = lax.all_to_all(grad_attended, "head", split_axis=2, concat_axis=1, tiled=True)
    grad_heads = grad_local.reshape(head_shape)
    delta_rows = jnp.sum(
        grad_heads.astype(jnp.float32).transpose(0, 2, 1, 3) * attention_result, axis=-1
    )
    fold_queries = query_fold(
        query_heads, grad_heads, log_totals, delta_rows, score_scale, head_count, head_size
    )
    grad_query_sum = fold_queries(
        zero_heads,
        (
            lax.all_gather(key_local, "blk", axis=1, tiled=True),
            lax.all_gather(value_local, "blk", axis=1, tiled=True),
        ),
        jnp.int32(0),
    )
    fold_side = key_fold(key_heads, value_heads, score_scale, head_count, head_size)
    grad_key_sum, grad_value_sum = fold_side(
        (zero_heads, zero_heads),
        (
            lax.all_gather(query_local.astype(jnp.float32), "blk", axis=1, tiled=True).astype(
                jnp.bfloat16
            ),
            lax.all_gather(grad_local.astype(jnp.float32), "blk", axis=1, tiled=True).astype(
                jnp.bfloat16
            ),
            lax.all_gather(log_totals.transpose(0, 2, 1), "blk", axis=1, tiled=True),
            lax.all_gather(delta_rows.transpose(0, 2, 1), "blk", axis=1, tiled=True),
        ),
        jnp.int32(0),
    )
    grad_keys_local = (
        (grad_key_sum * score_scale)
        .transpose(0, 2, 1, 3)
        .reshape(seq_count, query_rows, local_width)
        .astype(jnp.bfloat16)
    )
    grad_values_local = (
        grad_value_sum.transpose(0, 2, 1, 3)
        .reshape(seq_count, query_rows, local_width)
        .astype(jnp.bfloat16)
    )
    grad_query_local = (
        (grad_query_sum * score_scale)
        .transpose(0, 2, 1, 3)
        .reshape(seq_count, query_rows, local_width)
        .astype(jnp.bfloat16)
    )
    grad_query_token, grad_key_token, grad_value_token = (
        lax.all_to_all(grad_query_local, "head", split_axis=1, concat_axis=2, tiled=True),
        lax.all_to_all(grad_keys_local, "head", split_axis=1, concat_axis=2, tiled=True),
        lax.all_to_all(grad_values_local, "head", split_axis=1, concat_axis=2, tiled=True),
    )
    grad_qkv = jnp.concatenate(
        [grad_query_token, grad_key_token, grad_value_token], axis=-1
    ).reshape(row_count, 3 * model_width)
    grad_qkv_full = jnp.einsum(
        "rd,rf->df", embedded_low, grad_qkv, preferred_element_type=jnp.float32
    )
    grad_bias_query = jnp.sum(
        grad_query_token.astype(jnp.float32).reshape(row_count, model_width), axis=0
    )
    grad_bias_value = jnp.sum(
        grad_value_token.astype(jnp.float32).reshape(row_count, model_width), axis=0
    )
    grad_embedded = grad_resid + jnp.einsum(
        "rf,df->rd", grad_qkv, qkv_full, preferred_element_type=jnp.float32
    )
    second_mask = is_second.astype(jnp.float32)
    grad_type_one = jnp.sum(grad_embedded * second_mask, axis=0)
    grad_type_zero = jnp.sum(grad_embedded * (1.0 - second_mask), axis=0)
    length = lax.axis_size("blk") * pos_table.shape[0]
    local_slots = flat_pos
    inside = (local_slots >= 0) & (local_slots < length)
    slot_index = jnp.where(inside, local_slots, length)
    buffer = jnp.zeros((length + 1, model_width), jnp.float32).at[slot_index].add(grad_embedded)
    grad_positions = lax.psum_scatter(buffer[:length], "blk", scatter_dimension=0, tiled=True)
    gain_stack = jnp.stack([grad_gain_one, grad_gain_two])
    bias_stack = jnp.stack(
        [
            grad_bias_query,
            grad_bias_value,
            grad_bias_branch,
            grad_shift_one,
            grad_bias_second,
            grad_shift_two,
        ]
    )
    type_stack = jnp.stack([grad_type_zero, grad_type_one])
    (
        shard_qkv,
        shard_out,
        shard_up,
        shard_down,
        shard_up_bias,
        shard_gains,
        shard_biases,
        shard_types,
    ) = (
        lax.psum_scatter(grad_qkv_full, "blk", scatter_dimension=0, tiled=True),
        lax.psum_scatter(grad_out, "blk", scatter_dimension=0, tiled=True),
        lax.psum_scatter(grad_up, "blk", scatter_dimension=0, tiled=True),
        lax.psum_scatter(grad_down, "blk", scatter_dimension=0, tiled=True),
        lax.psum_scatter(grad_up_bias, "blk", scatter_dimension=0, tiled=True),
        lax.psum_scatter(gain_stack, "blk", scatter_dimension=1, tiled=True),
        lax.psum_scatter(bias_stack, "blk", scatter_dimension=1, tiled=True),
        lax.psum_scatter(type_stack, "blk", scatter_dimension=1, tiled=True),
    )
    (
        total_qkv,
        total_out,
        total_up,
        total_down,
        total_up_bias,
        total_gains,
        total_biases,
        total_types,
        total_positions,
    ) = lax.psum(
        (
            shard_qkv,
            shard_out,
            shard_up,
            shard_down,
            shard_up_bias,
            shard_gains,
            shard_biases,
            shard_types,
            grad_positions,
        ),
        "head",
    )
    grad_hidden = grad_embedded.reshape(token_shape)
    return (
        layer_out,
        grad_hidden,
        total_positions,
        total_types,
        total_qkv,
        total_out,
        total_up,
        total_down,
        total_up_bias,
        total_gains,
        total_biases,
    )


BIG = 56 << 20
WHOLE = 67043328
LAG = 3
CHUNKS = 4
CHUNK_LAG = 1
EARLY = (1, 3)
TURNS = ((1, 3), (2, 4, 6, 8), (6, 12))


def layer_in_planes(
    hidden,
    pos_ids,
    type_ids,
    cotangent,
    pos_table,
    type_table,
    query_key_value_weight,
    attention_output_weight,
    up_projection_weight,
    down_projection_weight,
    up_projection_bias,
    norm_gains,
    biases,
):
    seqs, seg, width = hidden.shape
    blks = lax.axis_size("blk")
    h = lax.axis_index("head")
    b = lax.axis_index("blk")
    o, g = b // 4, b % 4
    rows = seqs * seg
    e = width // HEADS
    ff = up_projection_weight.shape[1]
    scale = 1.0 / math.sqrt(e)
    slots = pos_table.shape[0]
    fcols = ff // blks // 2
    plane_rows = 8 * rows

    small = jnp.concatenate(
        [
            biases.astype(F32),
            norm_gains.astype(F32),
            type_table.astype(F32),
            up_projection_bias.astype(F32).reshape(4, e),
        ]
    ).reshape(7, 2 * e)
    packed = jnp.concatenate([small, pos_ids.astype(F32).reshape(1, rows)])
    qkv_cut = query_key_value_weight.reshape(e, 3, 2, 4, 2 * e)
    qkv_cut = lax.dynamic_slice_in_dim(qkv_cut, h, 1, 2).reshape(e, 3, 4, 2 * e)
    qkv_cut = qkv_cut.transpose(2, 0, 1, 3).reshape(4, e, 6 * e)
    up_cut = up_projection_weight.reshape(e, 4, 4, 2, fcols)
    up_cut = lax.dynamic_slice_in_dim(up_cut, h, 1, 3).reshape(e, 4, 4, fcols)
    up_cut = up_cut.transpose(2, 0, 1, 3).reshape(4, e, 4 * fcols)
    down_cut = lax.dynamic_slice_in_dim(down_projection_weight, h * fcols, fcols, 0)
    is_second = (type_ids.reshape(rows, 1) == 1).astype(F32)
    begin = SimpleNamespace(
        packed=packed,
        out_weight=attention_output_weight,
        qkv_cut=qkv_cut,
        up_cut=up_cut,
        down_cut=down_cut,
        table=pos_table,
        hidden=hidden,
        second=is_second,
    )
    (
        (
            attended,
            held,
            pair_out,
            lse,
            embedded,
            plane_low,
            qkv_own,
            out_own,
            up_one,
            up_cut,
            down_one,
            vectors,
            up_bias,
            pos_all,
        ),
    ) = fused("first_half", 0, [first_half(begin, scale, LAG)], WHOLE)
    parts = SimpleNamespace(
        attended=attended,
        out_own=out_own.reshape(2 * e, width),
        embedded=embedded,
        cotangent=cotangent,
        up_one=up_one,
        up_cut=up_cut,
        down_one=down_one,
        down_cut=down_cut,
        up_bias=up_bias,
        vectors=vectors,
        held=held,
        pair_out=pair_out,
        lse=lse,
        qkv_own=qkv_own.reshape(width, 6 * e),
        plane_low=plane_low,
        ids=pos_all,
        second=is_second,
    )
    sizes = (slots, CHUNKS, LAG, CHUNK_LAG, scale)
    ((layer_out, grad_hidden, pos, down, up, qkv, out, totals),) = fused(
        "second_half", 4, [second_half(parts, sizes)], WHOLE
    )
    outs = finish(
        (b % 2).reshape(1),
        layer_out,
        grad_hidden,
        pos,
        down.reshape(2 * fcols, width),
        up,
        qkv,
        out,
        totals,
    )
    return (*outs[:8], outs[8].reshape(4 * e), *outs[9:])


def planes_fit(hidden, head_axis, blk_axis):
    seqs, seg, width = hidden.shape
    return head_axis == 2 and blk_axis == HEADS and seqs == 2 and seqs * seg == 2 * width // HEADS


def on_device(hidden, *rest):
    if planes_fit(hidden, lax.axis_size("head"), lax.axis_size("blk")):
        return layer_in_planes(hidden, *rest)
    return layer_in_blocks(hidden, *rest)


def solution(mesh):
    in_specs = (
        P(None, ("head", "blk"), None),
        P(None, ("head", "blk")),
        P(None, ("head", "blk")),
        P(None, ("head", "blk"), None),
        P("blk", None),
        P(None, "blk"),
        P("blk", None),
        P("blk", None),
        P("blk", None),
        P("blk", None),
        P("blk"),
        P(None, "blk"),
        P(None, "blk"),
    )
    out_specs = (
        P(None, ("head", "blk"), None),
        P(None, ("head", "blk"), None),
        P("blk", None),
        P(None, "blk"),
        P("blk", None),
        P("blk", None),
        P("blk", None),
        P("blk", None),
        P("blk"),
        P(None, "blk"),
        P(None, "blk"),
    )
    return jax.shard_map(
        on_device, mesh=mesh, in_specs=in_specs, out_specs=out_specs, check_vma=False
    )
```

```python
import functools
import math
from types import SimpleNamespace

import jax
import jax.numpy as jnp
from jax import lax
from jax.experimental import pallas as pl
from jax.experimental.pallas import tpu as pltpu
from jax.sharding import PartitionSpec as P

HEADS = 16
MESH = pl.DeviceIdType.MESH
F32 = jnp.float32
BF16 = jnp.bfloat16
VSPEC = pl.BlockSpec(memory_space=pltpu.VMEM)


def place():
    h = lax.axis_index("head")
    b = lax.axis_index("blk")
    return h, b // 4, (b // 2) % 2, b % 2


def blk(o, y, c):
    return (o * 2 + y) * 2 + c


def peer(dx, dz, dy, dc):
    h, o, y, c = place()
    flip = lambda v, d: 1 - v if d else v
    return flip(h, dx), blk((o + dz) % 4 if dz else o, flip(y, dy), flip(c, dc))


def remote(src, dst, sems, index, device):
    return pltpu.make_async_remote_copy(
        src_ref=src,
        dst_ref=dst,
        send_sem=sems.at[0, index],
        recv_sem=sems.at[1, index],
        device_id=device,
        device_id_type=MESH,
    )


def landed(ref, sems, index):
    remote(ref, ref, sems, index, peer(1, 0, 0, 0)).wait_recv()


def sems(count):
    return pltpu.SemaphoreType.DMA((2, count))


NEAR_X, NEAR_Y, NEAR_C = (1, 0, 0, 0), (0, 0, 1, 0), (0, 0, 0, 1)
COLUMN = ((0, 1, 0, 0), (0, 2, 0, 0), (0, 3, 0, 0))
PLANE = tuple(
    (dx, 0, dy, dc) for dx in range(2) for dy in range(2) for dc in range(2) if dx or dy or dc
)


class Part:
    def __init__(self, run, ins, outs, scratch, peers):
        self.run, self.ins, self.outs, self.scratch, self.peers = run, ins, outs, scratch, peers
        self.turns = ()

    def on(self, *turns):
        self.turns = turns
        return self


def fused(name, cid, parts, limit=None):
    peers = sorted({p for part in parts for p in part.peers})
    ins = [x for part in parts for x in part.ins]
    outs = [s for part in parts for s in part.outs]
    scratch = [s for part in parts for s in part.scratch]

    def kernel(*refs):
        in_refs, out_refs = refs[: len(ins)], refs[len(ins) : len(ins) + len(outs)]
        own = refs[len(ins) + len(outs) :]
        gens = []
        i = j = k = 0
        for part in parts:
            gens.append(
                part.run(
                    in_refs[i : i + len(part.ins)],
                    out_refs[j : j + len(part.outs)],
                    own[k : k + len(part.scratch)],
                )
            )
            i, j, k = i + len(part.ins), j + len(part.outs), k + len(part.scratch)
        barrier = pltpu.get_barrier_semaphore()
        for p in peers:
            pl.semaphore_signal(barrier, inc=1, device_id=peer(*p), device_id_type=MESH)
        pl.semaphore_wait(barrier, len(peers))
        for gen in gens:
            next(gen)
        for turn, _ in enumerate(gens[0]):
            for part, gen in zip(parts, gens):
                if turn in part.turns:
                    next(gen)
        for gen in gens[1:]:
            for _ in gen:
                pass

    got = pl.pallas_call(
        kernel,
        name=name,
        out_shape=[jax.ShapeDtypeStruct(s, d) for s, d in outs],
        in_specs=[VSPEC] * len(ins),
        out_specs=[VSPEC] * len(outs),
        scratch_shapes=scratch,
        compiler_params=pltpu.CompilerParams(
            collective_id=cid, has_side_effects=True, vmem_limit_bytes=limit
        ),
    )(*ins)
    result = []
    for part in parts:
        result.append(got[: len(part.outs)])
        got = got[len(part.outs) :]
    return result


def exchange(x, peers, out_lead, source, target):
    peers = list(peers)

    def coords(p):
        h, o, y, c = place()
        flip = lambda v, d: 1 - v if d else v
        return flip(h, p[0]), (o + p[1]) % 4 if p[1] else o, flip(y, p[2]), flip(c, p[3])

    def run(ins, outs, own):
        (x_ref,), (out_ref,), (sem,) = ins, outs, own
        me = place()
        copies = []
        for k, p in enumerate(peers):
            copy = remote(
                source(x_ref, coords(p)), target(out_ref, me), sem, k, peer(*p)
            )
            copy.start()
            copies.append(copy)
        yield
        target(out_ref, me)[...] = source(x_ref, me)[...]
        for copy in copies:
            copy.wait()

    return Part(run, [x], [(out_lead, x.dtype)], [sems(len(peers))], peers)


def small_gather(x):
    peers = [
        (0, dz, dy, dc) for dz in range(4) for dy in range(2) for dc in range(2) if dz or dy or dc
    ]
    return exchange(x, peers, (16,) + x.shape, lambda r, d: r, lambda r, s: r.at[blk(*s[1:])])


def place_copy(src, dst, send_sem, recv_sem, device):
    return pltpu.make_async_remote_copy(
        src_ref=src,
        dst_ref=dst,
        send_sem=send_sem,
        recv_sem=recv_sem,
        device_id=device,
        device_id_type=MESH,
    )


BLK = tuple(
    (0, dz, dy, dc) for dz in range(4) for dy in range(2) for dc in range(2) if dz or dy or dc
)


def out_weights(w):
    r, n = w.shape

    def run(ins, outs, own):
        (w_ref,), (out_ref,), (send, recv) = ins, outs, own
        h, o, y, c = place()
        has = o // 2 == h
        serves = (o % 2 == y) & (y == c)

        def each(act):
            for k in range(4):
                device = (h, blk((o + k) % 4, o % 2, y))
                copy = place_copy(w_ref, out_ref.at[c], send.at[k], recv.at[c], device)

                @pl.when(has if k else has & jnp.logical_not(serves))
                def _():
                    act(copy)

        each(lambda copy: copy.start())
        yield

        @pl.when(has & serves)
        def _():
            out_ref[pl.ds(c, 1)] = w_ref[...][None]

        each(lambda copy: copy.wait_send())
        for core in range(2):
            from_self = (o == 2 * h + y) & (y == c) & (c == core)
            ref = out_ref.at[core]

            @pl.when(jnp.logical_not(from_self))
            def _():
                place_copy(ref, ref, send.at[0], recv.at[core], (h, blk(o, y, c))).wait_recv()

    scratch = [pltpu.SemaphoreType.DMA((4,)), pltpu.SemaphoreType.DMA((2,))]
    return Part(run, [w], [((2, r, n), BF16)], scratch, BLK)


def mirrored():
    o = place()[1]
    far = o // 2
    seen = lambda v: v * (1 - 2 * far) + 3 * far
    return seen(o), seen


def gather_steps(src, dst, sem):
    h, o, y, c = place()
    dev_x, dev_y, dev_c = peer(*NEAR_X), peer(*NEAR_Y), peer(*NEAR_C)
    mine = h * 4 + y * 2 + c
    of_x = (1 - h) * 4 + y * 2 + c
    of_y = h * 4 + (1 - y) * 2 + c
    of_d = (1 - h) * 4 + (1 - y) * 2 + c
    flip = 1 - 2 * c
    sent = []

    def go(ref, slot, half, index, device):
        copy = remote(ref, dst(half, slot), sem, index, device)
        copy.start()
        sent.append(copy)

    go(src(0), mine, 0, 0, dev_x)
    go(src(1), mine, 1, 1, dev_y)
    go(src(1), mine, 1, 2, dev_x)
    go(src(0), mine, 0, 3, dev_y)
    go(src(0), mine, 0, 4, dev_c)
    go(src(1), mine, 1, 5, dev_c)
    for half in range(2):
        dst(half, mine)[...] = src(half)[...]

    def relay(slot, half, index, device, onward, to_core):
        landed(dst(half, slot), sem, index)
        if onward is not None:
            go(dst(half, slot), slot, half, onward, device)
        go(dst(half, slot), slot, half, to_core, dev_c)

    yield
    relay(of_x, 0, 0, dev_y, 6, 8)
    relay(of_y, 1, 1, dev_x, 7, 9)
    yield
    relay(of_x, 1, 2, None, None, 10)
    relay(of_y, 0, 3, None, None, 11)
    yield
    relay(of_d, 0, 6, None, None, 12)
    relay(of_d, 1, 7, None, None, 13)
    yield
    for slot, half, index in (
        (mine, 0, 4),
        (mine, 1, 5),
        (of_x, 0, 8),
        (of_y, 1, 9),
        (of_x, 1, 10),
        (of_y, 0, 11),
        (of_d, 0, 12),
        (of_d, 1, 13),
    ):
        landed(dst(half, slot + flip), sem, index)
    for copy in sent:
        copy.wait_send()


def scatter_steps(src, total, near, part, from_x, from_y, diag, sem):
    h, o, y, c = place()
    dev_x, dev_y, dev_c = peer(*NEAR_X), peer(*NEAR_Y), peer(*NEAR_C)
    mine = h * 4 + y * 2 + c
    of_x = (1 - h) * 4 + y * 2 + c
    of_y = h * 4 + (1 - y) * 2 + c
    of_d = (1 - h) * 4 + (1 - y) * 2 + c
    flip = 1 - 2 * c
    order = (of_d, of_x, of_y, mine)
    sent = []

    def go(ref, to, index, device):
        copy = remote(ref, to, sem, index, device)
        copy.start()
        sent.append(copy)

    for k, half in ((0, 0), (0, 1), (1, 0), (2, 1), (1, 1), (2, 0), (3, 0), (3, 1)):
        go(src(half, order[k] + flip), near.at[k, half], 2 * k + half, dev_c)

    def add(k, half):
        landed(near.at[k, half], sem, 2 * k + half)
        return src(half, order[k])[...].astype(F32) + near[k, half].astype(F32)

    yield
    part[0, 0] = add(0, 0).astype(BF16)
    go(part.at[0, 0], diag.at[0], 8, dev_x)
    part[0, 1] = add(0, 1).astype(BF16)
    go(part.at[0, 1], diag.at[1], 9, dev_y)
    part[1, 0] = add(1, 0).astype(BF16)
    go(part.at[1, 0], from_x.at[0], 10, dev_x)
    part[2, 1] = add(2, 1).astype(BF16)
    go(part.at[2, 1], from_y.at[1], 11, dev_y)
    yield
    kept_x = add(1, 1)
    landed(diag.at[1], sem, 9)
    part[1, 1] = (kept_x + diag[1].astype(F32)).astype(BF16)
    go(part.at[1, 1], from_x.at[1], 12, dev_x)
    kept_y = add(2, 0)
    landed(diag.at[0], sem, 8)
    part[2, 0] = (kept_y + diag[0].astype(F32)).astype(BF16)
    go(part.at[2, 0], from_y.at[0], 13, dev_y)
    yield
    own = [add(3, half) for half in range(2)]
    for half, ix, iy in ((0, 10, 13), (1, 12, 11)):
        landed(from_x.at[half], sem, ix)
        landed(from_y.at[half], sem, iy)
        total(half)[...] = own[half] + from_x[half].astype(F32) + from_y[half].astype(F32)
    for copy in sent:
        copy.wait_send()


def scatter_scratch(r, n):
    block = (2, r // 2, n)
    return [
        pltpu.VMEM((4,) + block, BF16),
        pltpu.VMEM((3,) + block, BF16),
        pltpu.VMEM(block, BF16),
        pltpu.VMEM(block, BF16),
        pltpu.VMEM(block, BF16),
        sems(14),
    ]


def norm_parts(r):
    centred = r - jnp.mean(r, axis=-1, keepdims=True)
    scale = lax.rsqrt(jnp.mean(centred * centred, axis=-1, keepdims=True) + 1e-12)
    return centred * scale, scale


def norm_back(xh, scale, dh):
    return (
        dh
        - jnp.mean(dh, axis=-1, keepdims=True)
        - xh * jnp.mean(dh * xh, axis=-1, keepdims=True)
    ) * scale


def dot_nt(a, b):
    return lax.dot_general(a, b, (((1,), (1,)), ((), ())), preferred_element_type=F32)


def dot_tn(a, b):
    return lax.dot_general(a, b, (((0,), (0,)), ((), ())), preferred_element_type=F32)


def blk_gather_steps(src, spot_of, zsem, ysem, csem):
    h, o, y, c = place()
    at, seen = mirrored()
    dev_y, dev_c = peer(*NEAR_Y), peer(*NEAR_C)
    end, inner, other = (h, blk(seen(0), y, c)), (h, blk(seen(1), y, c)), (h, blk(seen(2), y, c))
    sent = []

    def spot(z, yy=y, cc=c):
        return spot_of(z, yy, cc)

    def go(ref, z, yy, sem, index, device):
        copy = remote(ref, spot(z, yy), sem, index, device)
        copy.start()
        sent.append(copy)

    def line(ref, z, index, device):
        return remote(ref, spot(z), zsem, index, device)

    @pl.when(at == 0)
    def _():
        line(src, o, 0, inner).start()

    @pl.when(at == 1)
    def _():
        line(src, o, 1, end).start()
        line(src, o, 2, other).start()

    go(src, o, y, ysem, 0, dev_y)
    go(src, o, y, csem, 0, dev_c)
    spot(o)[...] = src[...]

    def onward(j, z):
        go(spot(z), z, y, ysem, j, dev_y)
        go(spot(z), z, y, csem, j, dev_c)

    first = seen(1 - at)
    order = (o, first, seen(2), seen(3))

    def from_y(j):
        landed(spot(order[j], 1 - y), ysem, j)
        go(spot(order[j], 1 - y), order[j], 1 - y, csem, 4 + j, dev_c)

    yield

    @pl.when(at == 0)
    def _():
        landed(spot(seen(1)), zsem, 1)

    @pl.when(at == 1)
    def _():
        landed(spot(seen(0)), zsem, 0)
        line(spot(seen(0)), seen(0), 3, other).start()

    onward(1, first)

    @pl.when(at == 1)
    def _():
        landed(spot(seen(2)), zsem, 2)
        line(spot(seen(2)), seen(2), 4, end).start()

    yield
    from_y(0)

    @pl.when(at == 0)
    def _():
        landed(spot(seen(2)), zsem, 4)

    onward(2, seen(2))

    @pl.when(at == 1)
    def _():
        landed(spot(seen(3)), zsem, 3)
        line(spot(seen(3)), seen(3), 5, end).start()

    yield
    from_y(1)

    @pl.when(at == 0)
    def _():
        landed(spot(seen(3)), zsem, 5)

    onward(3, seen(3))
    yield
    from_y(2)
    yield
    from_y(3)
    yield
    for j, z in enumerate(order):
        landed(spot(z, y, 1 - c), csem, j)
        landed(spot(z, 1 - y, 1 - c), csem, 4 + j)

    @pl.when(at == 0)
    def _():
        line(src, o, 0, inner).wait_send()

    @pl.when(at == 1)
    def _():
        line(src, o, 1, end).wait_send()
        line(src, o, 2, other).wait_send()
        line(spot(seen(0)), seen(0), 3, other).wait_send()
        line(spot(seen(2)), seen(2), 4, end).wait_send()
        line(spot(seen(3)), seen(3), 5, end).wait_send()

    for copy in sent:
        copy.wait_send()


ALL = tuple(
    (dx, dz, dy, dc)
    for dx in range(2)
    for dz in range(4)
    for dy in range(2)
    for dc in range(2)
    if dx or dz or dy or dc
)


def line_sum_steps(term_of, out, terms, ends, mids, last, sem):
    h, o, y, c = place()
    at, seen = mirrored()
    end, inner, other = (h, blk(seen(0), y, c)), (h, blk(seen(1), y, c)), (h, blk(seen(2), y, c))
    order = [seen(3), seen(2), seen(1 - at)]
    plus = lambda a, b: a[...].astype(F32) + b[...].astype(F32)

    @pl.when(at == 0)
    def _():
        for j in range(3):
            remote(term_of(order[j]), ends.at[j], sem, j, inner).start()

    for j in range(2):
        yield

        @pl.when(at == 1)
        def _():
            landed(ends.at[j], sem, j)
            terms[j] = plus(term_of(order[j]), ends.at[j]).astype(BF16)
            remote(terms.at[j], mids.at[j], sem, 3 + j, other).start()

    yield

    @pl.when(at == 1)
    def _():
        landed(mids.at[0], sem, 3)
        terms[2] = plus(term_of(order[2]), mids.at[0]).astype(BF16)
        remote(terms.at[2], last, sem, 5, end).start()

    yield

    @pl.when(at == 1)
    def _():
        landed(ends.at[2], sem, 2)
        landed(mids.at[1], sem, 4)
        out[...] = (plus(term_of(o), ends.at[2]) + mids[1].astype(F32)).astype(BF16)
        for j in range(2):
            remote(terms.at[j], mids.at[j], sem, 3 + j, other).wait_send()
        remote(terms.at[2], last, sem, 5, end).wait_send()

    @pl.when(at == 0)
    def _():
        landed(last, sem, 5)
        out[...] = plus(term_of(o), last).astype(BF16)
        for j in range(3):
            remote(term_of(order[j]), ends.at[j], sem, j, inner).wait_send()


def line_sum_scratch(block):
    return [
        pltpu.VMEM((3,) + block, BF16),
        pltpu.VMEM((3,) + block, BF16),
        pltpu.VMEM((2,) + block, BF16),
        pltpu.VMEM(block, BF16),
        sems(6),
    ]


def spread_steps(rows_of, out, spots, sem):
    h, o, y, c = place()
    t = h * 4 + y * 2 + c
    columns = [
        out.at[:, pl.ds(pl.multiple_of(lane * 128, 128), 128)] for lane in spots(t)
    ]
    pieces = len(columns)
    copies = []
    for k, p in enumerate(PLANE):
        to = (1 - y if p[2] else y) * 2 + (1 - c if p[3] else c)
        for i in range(pieces):
            src = rows_of(to).at[:, pl.ds(i * 128, 128)]
            copy = remote(src, columns[i], sem, k * pieces + i, peer(*p))
            copy.start()
            copies.append(copy)
    for i in range(pieces):
        columns[i][...] = rows_of(y * 2 + c)[:, i * 128 : (i + 1) * 128]
    yield
    for copy in copies:
        copy.wait()


def second_half(x, consts):
    names = list(vars(x))
    seqs, r, d = x.embedded.shape
    planes, four, e, fh = x.up_one.shape
    f = 2 * fh
    fcols = x.down_weight.shape[0] // 2
    half, half_d = r // 2, d // 2
    rows, q_rows = 8 * r, 4 * r
    three, he, length = x.held.shape
    n = length // 4
    slots, chunks, lag, chunk_lag, scale = consts
    own_rows, w, blks = seqs * r, d // chunks, 16
    key_rows = 256
    width_qkv = 3 * 2 * he

    need = []

    def scratch(shape, dtype):
        need.append(pltpu.VMEM(shape, dtype))
        return len(need) - 1

    def many(specs):
        start = len(need)
        need.extend(specs)
        return list(range(start, len(need)))

    plane = (seqs, 8, r, d)
    shapes = dict(
        partial=(plane, BF16),
        up_two=(x.up_one.shape, BF16),
        down_two=(x.down_one.shape, BF16),
        first_g=(plane, BF16),
        grad_g=(plane, BF16),
        branch_g=(plane, BF16),
        act=((seqs * rows, f), BF16),
        slope=((seqs * rows, f), F32),
        inner_grad=((seqs * rows, f), BF16),
        first=((seqs, r, d), F32),
        xh_one=((seqs, r, d), F32),
        scale_one=((seqs, r, 1), F32),
        grad_two=((seqs, r, d), F32),
        low=((seqs, r, d), BF16),
        total=((seqs, r, d), F32),
        resid=((seqs, r, d), F32),
        down_part=((planes, fcols, d), BF16),
        up_part=((planes, 4 * e, f), BF16),
        up_total=((4 * e, f), BF16),
        out_part=((2, he, d), BF16),
        out_held=((4, he, d), BF16),
        out_acc=((he, d), F32),
        sums=((16, d), F32),
        up_sums=((1, f), F32),
        up_spots=((32, 128), F32),
        go=((2, he, 2 * n), BF16),
        gs=((he, length), BF16),
        qs=((he, length), BF16),
        q_rows=((length, he), BF16),
        g_rows=((length, he), BF16),
        dq=((he, length), F32),
        delta=((1, length), F32),
        pair_low=((three, he, length), BF16),
        dqkv=((three, 2, he, 2 * n), BF16),
        qkv_part=((planes, 4 * e, width_qkv), BF16),
        qkv_total=((4 * e, width_qkv), BF16),
        own=((chunks, own_rows, w), BF16),
        gathered=((chunks, blks, own_rows, w), BF16),
        pick=((slots, blks * own_rows), BF16),
        pos_low=((chunks, slots, w), BF16),
        pos_held=((chunks, slots, w), BF16),
        pack=((blks, 24, 128), F32),
        packs=((31, 24, 128), F32),
    )
    ids = {name: scratch(*spec) for name, spec in shapes.items()}
    counts = dict(
        up_sem=3,
        down_sem=3,
        ksem=3,
        qsem=3,
        down_pair=1,
        up_spread=28,
        qkv_spread=21,
        out_pair=1,
        pair_sem=chunks,
        pack_sem=31,
    )
    sem_ids = {k: many([sems(v)])[0] for k, v in counts.items()}
    for k, v in dict(go_send=4, go_recv=4, out_send=2, out_recv=4).items():
        sem_ids[k] = many([pltpu.SemaphoreType.DMA((v,))])[0]
    stream_ids = [
        ([many(scatter_scratch(r, d)) for _ in range(3)], [many([sems(14)])[0] for _ in range(3)])
        for _ in range(seqs)
    ]
    chunk_ids = [
        (many(scatter_scratch(2 * r, w)), many([sems(6), sems(4), sems(8)])) for _ in range(chunks)
    ]
    down_line = many(line_sum_scratch((fcols, d)))
    up_line = many(line_sum_scratch((4 * e, f)))
    qkv_line = many(line_sum_scratch((4 * e, width_qkv)))

    def run(ins, outs, own):
        src = SimpleNamespace(**dict(zip(names, ins)))
        out_ref, grad_ref, pos_ref, got_down, got_up, got_qkv, got_out, totals = outs
        m = SimpleNamespace(**{k: own[v] for k, v in ids.items()})
        sem = SimpleNamespace(**{k: own[v] for k, v in sem_ids.items()})
        pick_refs = lambda some: [own[i] for i in some]
        h, o, y, c = place()
        g = y * 2 + c
        t = h * 4 + g
        tail = []

        up_more = src.up_cut.at[:, :, pl.ds(fh, fh)]
        down_rows = pl.ds(pl.multiple_of(h * fcols, fcols), fcols)
        down_more = src.down_weight.at[down_rows, pl.ds(half_d, half_d)]
        weights = []
        for k, p in enumerate(COLUMN):
            for ref, dst, s in (
                (up_more, m.up_two, sem.up_sem),
                (down_more, m.down_two, sem.down_sem),
            ):
                copy = remote(ref, dst.at[o], s, k, peer(*p))
                copy.start()
                weights.append(copy)
        m.up_two[pl.ds(o, 1)] = up_more[...][None]
        m.down_two[pl.ds(o, 1)] = down_more[...][None]
        for ref in (m.sums, m.up_sums, m.up_spots, m.dq):
            ref[...] = jnp.zeros_like(ref)
        yield

        ups = [lambda k=k: src.up_one[...].reshape(d, fh) if k == 0 else m.up_two[...].reshape(d, fh) for k in range(2)]
        downs = [lambda k=k: src.down_one[...].reshape(f, half_d) if k == 0 else m.down_two[...].reshape(f, half_d) for k in range(2)]
        vec = lambda k: src.vectors[k + 2 : k + 3]
        partial, low, total = m.partial, m.low, m.total

        def piece(ref, s):
            return lambda i, slot: ref.at[s, slot, pl.ds(i * half, half)]

        def plain(ref, s):
            return lambda i: ref.at[s, pl.ds(i * half, half)]

        def quarter(ref, s, q):
            return ref[s, 4 * q : 4 * q + 4].reshape(q_rows, d)

        def note(k, value):
            m.sums[k : k + 1] += jnp.sum(value, axis=0, keepdims=True)

        def step(*some):
            for gen in some:
                next(gen, None)

        def down_sums():
            yield from line_sum_steps(
                lambda z: m.down_part.at[z], got_down.at[h], *pick_refs(down_line)
            )
            copy = remote(got_down.at[h], got_down.at[h], sem.down_pair, 0, peer(*NEAR_X))
            copy.start()
            yield
            copy.wait_send()
            landed(got_down.at[1 - h], sem.down_pair, 0)

        def up_sums():
            yield from line_sum_steps(lambda z: m.up_part.at[z], m.up_total, *pick_refs(up_line))
            yield from spread_steps(
                lambda k: m.up_total.at[pl.ds(k * e, e)],
                got_up,
                lambda k: [(i * 4 + k % 4) * 2 + k // 4 for i in range(4)],
                sem.up_spread,
            )

        def qkv_sums():
            yield from line_sum_steps(
                lambda z: m.qkv_part.at[z], m.qkv_total, *pick_refs(qkv_line)
            )
            yield from spread_steps(
                lambda k: m.qkv_total.at[pl.ds(k * e, e)],
                got_qkv,
                lambda k: [i * 8 + k for i in range(3)],
                sem.qkv_spread,
            )

        def out_sums():
            has = o // 2 == h
            held, acc, send, recv = m.out_held, m.out_acc, sem.out_send, sem.out_recv

            def each(act):
                for j in range(2):
                    device = (h, blk(2 * h + y, c, j))
                    copy = place_copy(m.out_part.at[j], held.at[o], send.at[j], recv.at[o], device)

                    @pl.when(jnp.logical_not((o == 2 * h + y) & (y == c) & (c == j)))
                    def _():
                        act(copy)

            each(lambda copy: copy.start())
            yield
            acc[...] = jnp.zeros_like(acc)
            for z in range(4):
                mine = (z == o) & (o % 2 == y) & (y == c)

                @pl.when(has & mine)
                def _():
                    acc[...] += m.out_part[c].astype(F32)

                @pl.when(has & jnp.logical_not(mine))
                def _():
                    ref = held.at[z]
                    place_copy(ref, ref, send.at[0], recv.at[z], (h, blk(o, y, c))).wait_recv()
                    acc[...] += held[z].astype(F32)

            pair = remote(got_out, got_out, sem.out_pair, 0, peer(*NEAR_X))

            @pl.when(has)
            def _():
                got_out[...] = acc[...].astype(BF16)
                pair.start()

            yield
            each(lambda copy: copy.wait_send())

            @pl.when(has)
            def _():
                pair.wait_send()

            @pl.when(jnp.logical_not(has))
            def _():
                landed(got_out, sem.out_pair, 0)

        def go_copy(s, j):
            z = 2 * s + j
            return place_copy(
                m.go.at[j, :, pl.ds(s * n, n)],
                m.gs.at[:, pl.ds(pl.multiple_of(o * n, n), n)],
                sem.go_send.at[z],
                sem.go_recv.at[o],
                (h, z * 4 + g),
            )

        def stream(s):
            scatters = [pick_refs(i) for i in stream_ids[s][0]]
            gathers = pick_refs(stream_ids[s][1])
            at = lambda q: pl.ds(s * rows + q * q_rows, q_rows)
            branch = dot_tn(
                src.attended[:, :, s * n : (s + 1) * n].reshape(2 * he, n), src.out_own[...]
            )
            partial[s] = branch.astype(BF16).reshape(8, r, d)
            yield from scatter_steps(piece(partial, s), plain(total, s), *scatters[0])
            xh, scale_r = norm_parts(src.embedded[s] + (total[s] + vec(0)))
            m.xh_one[s] = xh
            m.scale_one[s] = scale_r
            value = xh * vec(4) + vec(1)
            m.first[s] = value
            low[s] = value.astype(BF16)
            yield from gather_steps(plain(low, s), piece(m.first_g, s), gathers[0])
            if s == 0:
                for copy in weights:
                    copy.wait()
            for q in range(2):
                rows_in = quarter(m.first_g, s, q)
                for k in range(2):
                    cols = slice(k * fh, (k + 1) * fh)
                    inner = jnp.dot(rows_in, ups[k](), preferred_element_type=F32)
                    inner = inner + src.up_bias[:, cols]
                    phi = 0.5 + 0.5 * lax.erf(inner * (0.5**0.5))
                    m.act[at(q), cols] = (inner * phi).astype(BF16)
                    bell = jnp.exp(inner * inner * -0.5) * (1.0 / math.sqrt(2.0 * math.pi))
                    m.slope[at(q), cols] = phi + inner * bell
                    yield
                for k in range(2):
                    part = jnp.dot(m.act[at(q)], downs[k](), preferred_element_type=F32)
                    partial[s, 4 * q : 4 * q + 4, :, k * half_d : (k + 1) * half_d] = part.astype(
                        BF16
                    ).reshape(4, r, half_d)
                yield
            yield from scatter_steps(piece(partial, s), plain(total, s), *scatters[1])
            xh, scale_r = norm_parts(m.first[s] + (total[s] + vec(2)))
            out_ref[s] = (xh * vec(5) + vec(3)).astype(BF16)
            cot = src.cotangent[s].astype(F32)
            note(5, cot * xh)
            note(3, cot)
            grad = norm_back(xh, scale_r, cot * vec(5))
            m.grad_two[s] = grad
            low[s] = grad.astype(BF16)
            note(2, low[s].astype(F32))
            yield from gather_steps(plain(low, s), piece(m.grad_g, s), gathers[1])
            for q in range(2):
                rows_in = quarter(m.grad_g, s, q)
                back = dot_nt(rows_in[:, :half_d], downs[0]()) + dot_nt(
                    rows_in[:, half_d:], downs[1]()
                )
                back = (back * m.slope[at(q)]).astype(BF16)
                m.inner_grad[at(q)] = back
                m.up_sums[...] += jnp.sum(back.astype(F32), axis=0, keepdims=True)
                yield
                part = dot_nt(back[:, :fh], ups[0]()) + dot_nt(back[:, fh:], ups[1]())
                partial[s, 4 * q : 4 * q + 4] = part.astype(BF16).reshape(4, r, d)
                yield
            last = scatter_steps(piece(partial, s), plain(total, s), *scatters[2])
            next(last)
            if s == seqs - 1:
                @pl.loop(0, planes)
                def _(z):
                    cols = pl.ds(pl.multiple_of(z * fcols, fcols), fcols)
                    all_grads = m.grad_g[...].reshape(seqs * rows, d)
                    m.down_part[z] = dot_tn(m.act[:, cols], all_grads).astype(BF16)

                step(down)
                yield

                @pl.loop(0, planes)
                def _(z):
                    cols = pl.ds(pl.multiple_of(z * 4 * e, 4 * e), 4 * e)
                    all_first = m.first_g[:, :, :, cols].reshape(seqs * rows, 4 * e)
                    m.up_part[z] = dot_tn(all_first, m.inner_grad[...]).astype(BF16)

                yield
            yield from last
            grad = m.grad_two[s] + total[s]
            note(4, grad * m.xh_one[s])
            note(1, grad)
            grad = norm_back(m.xh_one[s], m.scale_one[s], grad * vec(4))
            m.resid[s] = grad
            low[s] = grad.astype(BF16)
            note(0, low[s].astype(F32))
            for k, _ in enumerate(gather_steps(plain(low, s), piece(m.branch_g, s), gathers[2])):
                yield
                if s == seqs - 1 and k in EARLY:
                    step(down)
            go = dot_nt(src.out_own[...], m.branch_g[s].reshape(rows, d))
            m.go[:, :, s * n : (s + 1) * n] = go.astype(BF16).reshape(2, he, n)
            for j in range(2):

                @pl.when(o != 2 * s + j)
                def _():
                    go_copy(s, j).start()

                @pl.when(o == 2 * s + j)
                def _():
                    m.gs[:, pl.ds(pl.multiple_of(o * n, n), n)] = m.go[
                        j, :, s * n : (s + 1) * n
                    ]

            yield

        down, up, out, qkv = down_sums(), up_sums(), out_sums(), qkv_sums()
        gens = [stream(s) for s in range(seqs)]
        for _ in range(lag):
            next(gens[0])
        while gens:
            for gen in list(gens):
                try:
                    next(gen)
                except StopIteration:
                    gens.remove(gen)

        step(up)
        grad_out = jnp.dot(
            src.attended[...].reshape(2 * he, 2 * n),
            m.branch_g[...].reshape(seqs * rows, d),
            preferred_element_type=F32,
        )
        m.out_part[...] = grad_out.astype(BF16).reshape(2, he, d)
        held = src.held
        gs, qs, q_t, g_t, dq, delta, pair_low = (
            m.gs, m.qs, m.q_rows, m.g_rows, m.dq, m.delta, m.pair_low
        )
        q32 = held[0].astype(F32) * scale
        qs[...] = q32.astype(BF16)
        q_t[...] = q32.T.astype(BF16)

        @pl.loop(0, slots // 64)
        def _(k):
            row = lax.broadcasted_iota(jnp.int32, (64, 1), 0) + k * 64
            some = pl.ds(pl.multiple_of(k * 64, 64), 64)
            m.pick[some] = (src.ids[...] == row).astype(F32).astype(BF16)

        for z in range(4):

            @pl.when(z != o)
            def _():
                ref = gs.at[:, pl.ds(z * n, n)]
                place_copy(
                    ref, ref, sem.go_send.at[0], sem.go_recv.at[z], peer(*NEAR_X)
                ).wait_recv()

        g32 = gs[...].astype(F32)
        g_t[...] = g32.T.astype(BF16)
        delta[...] = jnp.sum(g32 * src.pair_out[...], axis=0, keepdims=True)
        mine = pl.ds(pl.multiple_of((o // 2) * n, n), n)
        dqkv = m.dqkv

        def back(part, which, i, z):
            return remote(
                pair_low.at[part, :, pl.ds(pl.multiple_of(z * n, n), n)],
                dqkv.at[part, o % 2, :, mine],
                which,
                i,
                (h, z * 4 + g),
            )

        late = pl.ds(1, 2)
        for i in range(4):
            z = (o + 1 + i) % 4

            @pl.loop(0, n // key_rows)
            def _(step):
                at = pl.ds(pl.multiple_of(z * n + step * key_rows, key_rows), key_rows)
                k_cols = held[1, :, at]
                k_rows = k_cols.astype(F32).T.astype(BF16)
                v_rows = held[2, :, at].astype(F32).T.astype(BF16)
                s = jnp.dot(k_rows, qs[...], preferred_element_type=F32)
                p = jnp.exp(s - src.lse[...])
                dv = jnp.dot(p.astype(BF16), g_t[...], preferred_element_type=F32)
                dp = jnp.dot(v_rows, gs[...], preferred_element_type=F32)
                ds = (p * (dp - delta[...])).astype(BF16)
                dk = jnp.dot(ds, q_t[...], preferred_element_type=F32)
                dq[...] += jnp.dot(k_cols, ds, preferred_element_type=F32)
                pair_low[1, :, at] = dk.T.astype(BF16)
                pair_low[2, :, at] = dv.T.astype(BF16)

            if i < 3:
                back(late, sem.ksem, i, z).start()
            if i == 0:
                step(*[down] * (3 - len(EARLY)))
            if i == 2:
                step(up)
        pair_low[0] = (dq[...] * scale).astype(BF16)
        for i in range(3):
            back(pl.ds(0, 1), sem.qsem, i, (o + 1 + i) % 4).start()
        dqkv[:, o % 2, :, mine] = pair_low[:, :, pl.ds(pl.multiple_of(o * n, n), n)]
        step(down, up)
        for i in range(3):
            z = (o + 3 - i) % 4
            there = pl.ds(pl.multiple_of((z // 2) * n, n), n)
            landed(dqkv.at[late, z % 2, :, there], sem.ksem, i)
            landed(dqkv.at[pl.ds(0, 1), z % 2, :, there], sem.qsem, i)

        all_dqkv = lambda: dqkv[...].reshape(width_qkv, 2 * n)

        def back_chunk(q):
            part = lax.dot_general(
                all_dqkv(),
                src.qkv_own[q * w : (q + 1) * w],
                (((0,), (1,)), ((), ())),
                preferred_element_type=F32,
            )
            partial[:, :, :, q * w : (q + 1) * w] = part.astype(BF16).reshape(seqs, 8, r, w)

        def chunk(q):
            cols = pl.ds(q * w, w)
            scatter, (zsem, ysem, csem) = pick_refs(chunk_ids[q][0]), pick_refs(chunk_ids[q][1])
            back_chunk(q)
            yield from scatter_steps(
                lambda i, slot: partial.at[i, slot, :, cols],
                lambda i: grad_ref.at[i, :, cols],
                *scatter,
            )
            grad = grad_ref[:, :, cols] + m.resid[:, :, cols]
            grad_ref[:, :, cols] = grad
            grad = grad.reshape(own_rows, w)
            m.own[q] = grad.astype(BF16)
            second = src.second[...]
            m.sums[6:7, cols] = jnp.sum(grad * (1.0 - second), axis=0, keepdims=True)
            m.sums[7:8, cols] = jnp.sum(grad * second, axis=0, keepdims=True)
            yield from blk_gather_steps(
                m.own.at[q],
                lambda z, yy, cc: m.gathered.at[q, blk(z, yy, cc)],
                zsem,
                ysem,
                csem,
            )

            @pl.loop(0, slots // 128)
            def _(k):
                some = pl.ds(pl.multiple_of(k * 128, 128), 128)
                found = jnp.dot(
                    m.pick[some],
                    m.gathered[q].reshape(blks * own_rows, w),
                    preferred_element_type=F32,
                )
                pos_ref[some, cols] = found
                m.pos_low[q, some] = found.astype(BF16)

            copy = remote(
                m.pos_low.at[q], m.pos_held.at[q], sem.pair_sem, q, peer(*NEAR_X)
            )
            copy.start()
            pairs.append(copy)
            yield

        pairs = []
        active, waiting = [], [chunk(q) for q in range(chunks)]
        turn = 0
        while active or waiting:
            if waiting and turn % chunk_lag == 0:
                active.append(waiting.pop(0))
            for gen in list(active):
                try:
                    next(gen)
                except StopIteration:
                    active.remove(gen)
            if turn == 0:
                @pl.loop(0, planes)
                def _(z):
                    cols = pl.ds(pl.multiple_of(z * 4 * e, 4 * e), 4 * e)
                    part = lax.dot_general(
                        src.plane_low[:, :, :, cols].reshape(seqs * rows, 4 * e),
                        all_dqkv(),
                        (((0,), (1,)), ((), ())),
                        preferred_element_type=F32,
                    )
                    m.qkv_part[z] = part.astype(BF16)

                step(qkv)
                ones = jnp.ones((8, 2 * n), BF16)
                heads = dot_nt(ones, all_dqkv())
                own_lanes = pl.ds(pl.multiple_of(t * 128, 128), 128)
                m.sums[8:9, own_lanes] = heads[0:1, 0:128]
                m.sums[9:10, own_lanes] = heads[0:1, 256:384]
                for i in range(4):
                    m.up_spots[pl.ds((i * 4 + g) * 2 + h, 1)] = m.up_sums[
                        :, i * 128 : (i + 1) * 128
                    ]
            for when, gen in zip(TURNS, (up, qkv, out)):
                if turn in when:
                    step(gen)
            turn += 1
        for b in range(blks):
            m.pack[b, 0:16] = m.sums[:, b // 2 * 128 : (b // 2 + 1) * 128]
            m.pack[b, 16:18] = m.up_spots[2 * b : 2 * b + 2]
            m.pack[b, 18:24] = jnp.zeros((6, 128), F32)
        copies = []
        for k, p in enumerate(ALL):
            to = peer(*p)
            copy = remote(m.pack.at[to[1]], m.packs.at[k], sem.pack_sem, k, to)
            copy.start()
            copies.append(copy)
        for gen in (down, up, out, qkv):
            for _ in gen:
                pass
        for q, copy in enumerate(pairs):
            copy.wait()
            cols = pl.ds(q * w, w)
            pos_ref[:, cols] = pos_ref[:, cols] + m.pos_held[q].astype(F32)
        for copy in copies:
            copy.wait()
        totals[...] = m.pack[blk(o, y, c)] + jnp.sum(m.packs[...], axis=0)
        for i in range(3):
            back(late, sem.ksem, i, (o + 1 + i) % 4).wait_send()
            back(pl.ds(0, 1), sem.qsem, i, (o + 1 + i) % 4).wait_send()
        for s in range(seqs):
            for j in range(2):

                @pl.when(o != 2 * s + j)
                def _():
                    go_copy(s, j).wait_send()

    return Part(
        run,
        list(vars(x).values()),
        [
            ((seqs, r, d), BF16),
            ((seqs, r, d), F32),
            ((slots, d), F32),
            ((2, fcols, d), BF16),
            ((e, 8 * f), BF16),
            ((e, 3 * d), BF16),
            ((he, d), BF16),
            ((24, 128), F32),
        ],
        need,
        ALL,
    )


def rows_steps(own_of, near, part, from_y, term, ends, mids, last, csem, ysem, zsem, out):
    h, o, y, c = place()
    at, seen = mirrored()
    dev_y = peer(*NEAR_Y)
    order = [seen(3), seen(2), seen(1 - at), o]
    end, inner, other = (h, blk(seen(0), y, c)), (h, blk(seen(1), y, c)), (h, blk(seen(2), y, c))
    sent = []
    for j, z in enumerate(order):
        landed(near.at[0, j], csem, j)
        part[j] = own_of(z, 1 - y)[...] + near[0, j]
        copy = remote(part.at[j], from_y.at[j], ysem, j, dev_y)
        copy.start()
        sent.append(copy)
    for j, z in enumerate(order):
        yield
        landed(near.at[1, j], csem, 4 + j)
        landed(from_y.at[j], ysem, j)
        term[j] = own_of(z, y)[...] + near[1, j] + from_y[j]
        if j < 3:

            @pl.when(at == 0)
            def _():
                remote(term.at[j], ends.at[j], zsem, j, inner).start()

        if j < 2:

            @pl.when(at == 1)
            def _():
                landed(ends.at[j], zsem, j)
                term[j] += ends[j]
                remote(term.at[j], mids.at[j], zsem, 3 + j, other).start()

    yield

    @pl.when(at == 1)
    def _():
        landed(mids.at[0], zsem, 3)
        term[2] += mids[0]
        remote(term.at[2], last, zsem, 5, end).start()

    yield

    @pl.when(at == 1)
    def _():
        landed(ends.at[2], zsem, 2)
        landed(mids.at[1], zsem, 4)
        out[...] = (term[3] + ends[2] + mids[1]).astype(F32)
        for j in range(2):
            remote(term.at[j], mids.at[j], zsem, 3 + j, other).wait_send()
        remote(term.at[2], last, zsem, 5, end).wait_send()

    @pl.when(at == 0)
    def _():
        landed(last, zsem, 5)
        out[...] = (term[3] + last[...]).astype(F32)
        for j in range(3):
            remote(term.at[j], ends.at[j], zsem, j, inner).wait_send()

    for copy in sent:
        copy.wait_send()


def first_half(x, scale, lag):
    names = list(vars(x))
    seqs, r, d = x.hidden.shape
    slots = x.table.shape[0]
    e = x.qkv_weight.shape[0]
    four, wq, f = 4, x.qkv_weight.shape[1] // 8, x.up_weight.shape[1] // 8
    fcols = x.down_weight.shape[0] // 2
    he = wq // 6
    n = 8 * r
    length = 4 * n
    half, fh, half_d = r // 2, f // 2, d // 2
    blks = 16
    cols = 256
    small = small_gather(jax.ShapeDtypeStruct((8, 128), F32))
    outw = out_weights(x.out_weight)
    need = []

    def many(specs):
        start = len(need)
        need.extend(specs)
        return list(range(start, len(need)))

    block = (r, d)
    shapes = dict(
        packed=((8, 128), F32),
        everyone=((blks, 8, 128), F32),
        found=((4, 2, 2, seqs, r, d), BF16),
        rows=((seqs, r, d), F32),
        low=((seqs, r, d), BF16),
        qkv_in=((four, e, wq), BF16),
        projected=((3, 2, he, 2 * n), BF16),
        keys=((length, he), BF16),
        pair_low=((he, length), BF16),
    )
    ids = {k: many([pltpu.VMEM(*v)])[0] for k, v in shapes.items()}
    counts = dict(qkv_sem=3, up_sem=3, down_sem=3, back_sem=3, qkv_trade=9, up_trade=12)
    sem_ids = {k: many([sems(v)])[0] for k, v in counts.items()}
    for k in ("send", "recv"):
        sem_ids[k] = many([pltpu.SemaphoreType.DMA((4,))])[0]
    small_ids, outw_ids = many(small.scratch), many(outw.scratch)
    row_ids = [
        many(
            [
                pltpu.VMEM((2, 4) + block, BF16),
                pltpu.VMEM((4,) + block, BF16),
                pltpu.VMEM((4,) + block, BF16),
                pltpu.VMEM((4,) + block, BF16),
                pltpu.VMEM((3,) + block, BF16),
                pltpu.VMEM((2,) + block, BF16),
                pltpu.VMEM(block, BF16),
                sems(8),
                sems(4),
                sems(6),
            ]
        )
        for _ in range(seqs)
    ]
    gather_ids = [many([sems(14)])[0] for _ in range(seqs)]

    def run(ins, outs, own):
        src = SimpleNamespace(**dict(zip(names, ins)))
        attended, held, o_ref, lse_ref, emb_ref, plane_ref, qkv_ref = outs[:7]
        outw_ref, up_one, up_in, down_one, vec_ref, bias_ref, ids_ref, second_ref = outs[7:]
        m = SimpleNamespace(**{k: own[v] for k, v in ids.items()})
        sem = SimpleNamespace(**{k: own[v] for k, v in sem_ids.items()})
        pick_refs = lambda some: [own[i] for i in some]
        h, o, y, c = place()
        g = y * 2 + c
        t = h * 4 + g
        side = lambda a: jnp.concatenate([a[0:1], a[1:2]], axis=1).astype(F32)
        for k in range(3):
            m.packed[k : k + 1] = side(src.biases[2 * k : 2 * k + 2])
        m.packed[3:4] = side(src.gains[...])
        m.packed[4:5] = side(src.types[...])
        m.packed[5:7] = src.up_bias[...].astype(F32)
        m.packed[7:8] = side(src.pos_ids[...])
        gather_small = small.run((m.packed,), (m.everyone,), pick_refs(small_ids))
        trades = []

        def trade(ref, dst, s, lanes_of):
            count = len(lanes_of(0))
            for k, p in enumerate(((0, 0, 1, 0), (0, 0, 0, 1), (0, 0, 1, 1))):
                to = (1 - y if p[2] else y) * 2 + (1 - c if p[3] else c)
                for i, lane in enumerate(lanes_of(to)):
                    copy = remote(
                        ref.at[:, pl.ds(pl.multiple_of(lane * 128, 128), 128)],
                        dst.at[g, :, pl.ds(i * 128, 128)],
                        s,
                        k * count + i,
                        peer(*p),
                    )
                    copy.start()
                    trades.append(copy)
            for i, lane in enumerate(lanes_of(g)):
                dst[g, :, i * 128 : (i + 1) * 128] = ref[
                    :, pl.ds(pl.multiple_of(lane * 128, 128), 128)
                ]

        weights = outw.run((src.out_weight,), (outw_ref,), pick_refs(outw_ids))
        qkv_lanes = lambda k: [i * 8 + h * 4 + k for i in range(3)]
        up_lanes = lambda k: [(i * 4 + k) * 2 + h for i in range(4)]
        trade(src.qkv_weight, m.qkv_in, sem.qkv_trade, qkv_lanes)
        next(gather_small)
        yield
        trade(src.up_weight, up_in, sem.up_trade, up_lanes)
        bulk = []

        def line(ref, dst, s):
            for k, p in enumerate(COLUMN):
                copy = remote(ref, dst.at[o], s, k, peer(*p))
                copy.start()
                bulk.append(copy)
            dst[pl.ds(o, 1)] = ref[...][None]

        for _ in gather_small:
            pass

        at, seen = mirrored()
        order = [seen(3), seen(2), seen(1 - at), o]
        b = blk(o, y, c)
        row = lax.broadcasted_iota(jnp.int32, (slots, 1), 0).astype(F32)
        base = (b * slots).astype(F32)
        streams = [pick_refs(i) for i in row_ids]
        core = []
        for i, yy in enumerate((1 - y, y)):
            for j, z in enumerate(order):
                hot = jnp.concatenate(
                    [
                        (m.everyone[blk(z, yy, cc), 7:8] - base == row).astype(F32).astype(BF16)
                        for cc in range(2)
                    ],
                    axis=1,
                )
                rows_of = dot_tn(hot, src.table[...]).astype(BF16)
                m.found[z, yy] = rows_of.reshape(2, seqs, r, d)
                for s in range(seqs):
                    near, csem = streams[s][0], streams[s][7]
                    copy = remote(
                        m.found.at[z, yy, 1 - c, s],
                        near.at[i, j],
                        csem,
                        i * 4 + j,
                        peer(*NEAR_C),
                    )
                    copy.start()
                    core.append(copy)
            if i == 0:
                for copy in trades:
                    copy.wait()
                line(m.qkv_in, qkv_ref, sem.qkv_sem)

        lane = lax.broadcasted_iota(jnp.int32, (1, 128), 1)
        for k in range(5):
            for i in range(blks // 2):
                one, two = m.everyone[2 * i, k : k + 1], m.everyone[2 * i + 1, k : k + 1]
                lanes = slice(i * 128, (i + 1) * 128)
                vec_ref[2 * k : 2 * k + 1, lanes] = jnp.where(
                    lane < 64, one, pltpu.roll(two, 64, 1)
                )
                vec_ref[2 * k + 1 : 2 * k + 2, lanes] = jnp.where(
                    lane < 64, pltpu.roll(one, 64, 1), two
                )
        for i in range(blks):
            ids_ref[:, i * 128 : (i + 1) * 128] = (m.everyone[i, 7:8] - base).astype(jnp.int32)
        for i in range(4):
            bias_ref[:, i * 128 : (i + 1) * 128] = m.everyone[i * 4 + g, pl.ds(5 + h, 1)]
        eye = lax.broadcasted_iota(jnp.int32, (128, 128), 0) == lax.broadcasted_iota(
            jnp.int32, (128, 128), 1
        )

        def upright(lanes):
            return jnp.sum(jnp.where(eye, lanes, 0.0), axis=1, keepdims=True)

        def column(k):
            return upright(vec_ref[k : k + 1, pl.ds(pl.multiple_of(t * 128, 128), 128)])

        second_ref[...] = upright(side(src.type_ids[...]))

        def send_pair(s, j):
            z = 2 * s + j
            return place_copy(
                m.projected.at[:, j, :, pl.ds(s * n, n)],
                held.at[:, :, pl.ds(pl.multiple_of(o * n, n), n)],
                sem.send.at[z],
                sem.recv.at[o],
                (h, z * 4 + g),
            )

        def stream(s):
            yield from rows_steps(
                lambda z, yy: m.found.at[z, yy, c, s], *streams[s], m.rows.at[s]
            )
            second = second_ref[s * r : (s + 1) * r]
            typed = vec_ref[8:9] * (1.0 - second) + vec_ref[9:10] * second
            value = src.hidden[s].astype(F32) + m.rows[s] + typed
            emb_ref[s] = value
            m.low[s] = value.astype(BF16)
            yield from gather_steps(
                lambda i: m.low.at[s, pl.ds(i * half, half)],
                lambda i, slot: plane_ref.at[s, slot, pl.ds(i * half, half)],
                own[gather_ids[s]],
            )
            if s == 0:
                for copy in bulk:
                    copy.wait()
                bulk.clear()
                line(up_in.at[:, :, pl.ds(0, fh)], up_one, sem.up_sem)
            part = lax.dot_general(
                qkv_ref[...].reshape(d, wq),
                plane_ref[s].reshape(n, d),
                (((0,), (1,)), ((), ())),
                preferred_element_type=F32,
            )
            here = slice(s * n, (s + 1) * n)
            third = wq // 3
            m.projected[0, :, :, here] = (part[:third] + column(0)).astype(BF16).reshape(2, he, n)
            m.projected[1, :, :, here] = part[third : 2 * third].astype(BF16).reshape(2, he, n)
            m.projected[2, :, :, here] = (
                (part[2 * third :] + column(1)).astype(BF16).reshape(2, he, n)
            )
            for j in range(2):

                @pl.when(o != 2 * s + j)
                def _():
                    send_pair(s, j).start()

                @pl.when(o == 2 * s + j)
                def _():
                    held[:, :, pl.ds(pl.multiple_of(o * n, n), n)] = m.projected[:, j, :, here]

            yield

        gens = [stream(s) for s in range(seqs)]
        for _ in range(lag):
            next(gens[0])
        while gens:
            for gen in list(gens):
                try:
                    next(gen)
                except StopIteration:
                    gens.remove(gen)
        next(weights)
        for z in range(4):

            @pl.when(z != o)
            def _():
                ref = held.at[:, :, pl.ds(z * n, n)]
                place_copy(ref, ref, sem.send.at[0], sem.recv.at[z], peer(*NEAR_X)).wait_recv()

        down_rows = pl.ds(pl.multiple_of(h * fcols, fcols), fcols)
        line(src.down_weight.at[down_rows, pl.ds(0, half_d)], down_one, sem.down_sem)
        m.keys[...] = held[1].astype(F32).T.astype(BF16)
        mine = pl.ds(pl.multiple_of((o // 2) * n, n), n)

        def back(i, z):
            return remote(
                m.pair_low.at[:, pl.ds(pl.multiple_of(z * n, n), n)],
                attended.at[o % 2, :, mine],
                sem.back_sem,
                i,
                (h, z * 4 + g),
            )

        @pl.loop(0, 4 * (n // cols))
        def _(step):
            i = step // (n // cols)
            z = (o + 1 + i) % 4
            here = pl.ds(pl.multiple_of(z * n + step % (n // cols) * cols, cols), cols)
            q = (held[0, :, here].astype(F32) * scale).astype(BF16)
            s = jnp.dot(m.keys[...], q, preferred_element_type=F32)
            peak = jnp.max(s, axis=0, keepdims=True)
            p = jnp.exp(s - peak)
            total = jnp.sum(p, axis=0, keepdims=True)
            out = jnp.dot(held[2], p.astype(BF16), preferred_element_type=F32) / total
            o_ref[:, here] = out
            m.pair_low[:, here] = out.astype(BF16)
            lse_ref[:, here] = peak + jnp.log(total)

            @pl.when((step % (n // cols) == n // cols - 1) & (i < 3))
            def _():
                back(i, z).start()

        attended[o % 2, :, mine] = m.pair_low[:, pl.ds(pl.multiple_of(o * n, n), n)]
        for i in range(3):
            back(i, (o + 1 + i) % 4).wait_send()
            z = (o + 3 - i) % 4
            landed(attended.at[z % 2, :, pl.ds(pl.multiple_of((z // 2) * n, n), n)], sem.back_sem, i)
        for _ in weights:
            pass
        for copy in bulk:
            copy.wait()
        for copy in core:
            copy.wait_send()
        for s in range(seqs):
            for j in range(2):

                @pl.when(o != 2 * s + j)
                def _():
                    send_pair(s, j).wait_send()

    return Part(
        run,
        list(vars(x).values()),
        [
            ((2, he, 2 * n), BF16),
            ((3, he, length), BF16),
            ((he, length), F32),
            ((1, length), F32),
            ((seqs, r, d), F32),
            ((seqs, 8, r, d), BF16),
            ((4, four, e, wq), BF16),
            ((2,) + x.out_weight.shape, BF16),
            ((4, four, e, fh), BF16),
            ((four, e, f), BF16),
            ((4, fcols, half_d), BF16),
            ((10, d), F32),
            ((1, f), F32),
            ((1, blks * seqs * r), jnp.int32),
            ((seqs * r, 1), F32),
        ],
        need,
        ALL,
    )


def finish_kernel(odd, layer, hid, pos, down, up, qkv, out, totals, *outs):
    o_layer, o_hid, o_pos, o_types, o_qkv, o_out, o_up, o_down, o_upb, o_gains, o_bias = outs
    o_layer[...] = layer[...]
    o_hid[...] = hid[...]
    o_pos[...] = pos[...]
    o_qkv[...] = qkv[...].astype(F32)
    o_out[...] = out[...].astype(F32)
    o_up[...] = up[...].astype(F32)
    o_down[...] = down[...].astype(F32)
    t = totals[...]
    mine = jnp.where(odd[0] == 1, t[:, 64:], t[:, :64])
    o_types[...] = mine[6:8]
    o_gains[...] = mine[4:6]
    o_bias[0:1] = mine[8:9]
    o_bias[1:2] = mine[9:10]
    o_bias[2:6] = mine[0:4]
    o_upb[...] = t[16:18]


def finish(odd, layer, hid, pos, down, up, qkv, out, totals, steps=4):
    e = out.shape[0]
    large = [(layer, BF16), (hid, F32), (pos, F32), (qkv, F32), (out, F32), (up, F32), (down, F32)]

    def cut(a):
        return pl.BlockSpec((a.shape[0] // steps, a.shape[1]), lambda i: (i, 0))

    def whole(*shape):
        return pl.BlockSpec(shape, lambda i: (0, 0))

    like = {id(a): jax.ShapeDtypeStruct(a.shape, dtype) for a, dtype in large}
    full = lambda *shape: jax.ShapeDtypeStruct(shape, F32)
    return pl.pallas_call(
        finish_kernel,
        name="finish",
        grid=(steps,),
        out_shape=[like[id(a)] for a in (layer, hid, pos)]
        + [full(2, e)]
        + [like[id(a)] for a in (qkv, out, up, down)]
        + [full(2, 128), full(2, e), full(6, e)],
        in_specs=[pl.BlockSpec(memory_space=pltpu.SMEM)]
        + [cut(a) for a in (layer, hid, pos, down, up, qkv, out)]
        + [whole(24, 128)],
        out_specs=[cut(a) for a in (layer, hid, pos)]
        + [whole(2, e)]
        + [cut(a) for a in (qkv, out, up, down)]
        + [whole(2, 128), whole(2, e), whole(6, e)],
    )(odd, layer, hid, pos, down, up, qkv, out, totals)


def norm_layer(values_in, gain_row, offset_row):
    average = jnp.mean(values_in, axis=-1, keepdims=True)
    centred = values_in - average
    variance = jnp.mean(centred * centred, axis=-1, keepdims=True)
    return centred * lax.rsqrt(variance + 1e-12) * gain_row + offset_row


def gelu_exact(inner_product_sum):
    return jax.nn.gelu(inner_product_sum, approximate=False)


def widest_block(length, limit):
    return max(
        (candidate for candidate in range(1, min(length, limit) + 1) if length % candidate == 0)
    )


def block_scores(query_heads, key_block, score_scale):
    return (
        jnp.einsum("sqhe,skhe->shqk", query_heads, key_block, preferred_element_type=jnp.float32)
        * score_scale
    )


def key_side(query_block, grad_block, lse_block, delta_block, key_heads, value_heads, score_scale):
    scores = block_scores(query_block, key_heads, score_scale)
    weights = jnp.exp(scores - lse_block[..., None])
    more_values = jnp.einsum(
        "shqk,sqhe->shke",
        weights.astype(jnp.bfloat16),
        grad_block,
        preferred_element_type=jnp.float32,
    )
    grad_weights = jnp.einsum(
        "sqhe,skhe->shqk", grad_block, value_heads, preferred_element_type=jnp.float32
    )
    grad_scores = weights * (grad_weights - delta_block[..., None])
    more_keys = jnp.einsum(
        "shqk,sqhe->shke",
        grad_scores.astype(jnp.bfloat16),
        query_block,
        preferred_element_type=jnp.float32,
    )
    return (more_keys, more_values)


def forward_fold(query_heads, score_scale, head_count, head_size):

    def fold_keys(running, portion, offset):
        key_piece, value_piece = portion
        seq_count, length = (key_piece.shape[0], key_piece.shape[1])
        block_size = widest_block(length, 512)

        def one_step(block_index, carried):
            row_peak, row_total, weighted = carried
            row_start = block_index * block_size
            key_block = lax.dynamic_slice_in_dim(key_piece, row_start, block_size, 1).reshape(
                seq_count, block_size, head_count, head_size
            )
            value_block = lax.dynamic_slice_in_dim(value_piece, row_start, block_size, 1).reshape(
                seq_count, block_size, head_count, head_size
            )
            scores = block_scores(query_heads, key_block, score_scale)
            new_peak = jnp.maximum(row_peak, jnp.max(scores, axis=-1))
            shrink = jnp.exp(row_peak - new_peak)
            weights = jnp.exp(scores - new_peak[..., None])
            row_total = row_total * shrink + jnp.sum(weights, axis=-1)
            weighted = weighted * shrink[..., None] + jnp.einsum(
                "shqk,skhe->shqe",
                weights.astype(jnp.bfloat16),
                value_block,
                preferred_element_type=jnp.float32,
            )
            return (new_peak, row_total, weighted)

        return lax.fori_loop(0, length // block_size, one_step, running)

    return fold_keys


def query_fold(query_heads, grad_heads, log_totals, delta_rows, score_scale, head_count, head_size):

    def fold_keys(running, portion, offset):
        key_piece, value_piece = portion
        seq_count, length = (key_piece.shape[0], key_piece.shape[1])
        block_size = widest_block(length, 512)

        def one_step(block_index, weighted):
            row_start = block_index * block_size
            key_block = lax.dynamic_slice_in_dim(key_piece, row_start, block_size, 1).reshape(
                seq_count, block_size, head_count, head_size
            )
            value_block = lax.dynamic_slice_in_dim(value_piece, row_start, block_size, 1).reshape(
                seq_count, block_size, head_count, head_size
            )
            scores = block_scores(query_heads, key_block, score_scale)
            weights = jnp.exp(scores - log_totals[..., None])
            grad_weights = jnp.einsum(
                "sqhe,skhe->shqk", grad_heads, value_block, preferred_element_type=jnp.float32
            )
            grad_scores = weights * (grad_weights - delta_rows[..., None])
            return weighted + jnp.einsum(
                "shqk,skhe->shqe",
                grad_scores.astype(jnp.bfloat16),
                key_block,
                preferred_element_type=jnp.float32,
            )

        return lax.fori_loop(0, length // block_size, one_step, running)

    return fold_keys


def key_fold(key_heads, value_heads, score_scale, head_count, head_size):

    def fold_queries(running, portion, offset):
        query_piece, grad_piece, lse_piece, delta_piece = portion
        seq_count, length = (query_piece.shape[0], query_piece.shape[1])
        block_size = widest_block(length, 512)

        def one_step(block_index, carried):
            grad_keys, grad_values = carried
            row_start = block_index * block_size
            query_block = lax.dynamic_slice_in_dim(query_piece, row_start, block_size, 1).reshape(
                seq_count, block_size, head_count, head_size
            )
            grad_block = lax.dynamic_slice_in_dim(grad_piece, row_start, block_size, 1).reshape(
                seq_count, block_size, head_count, head_size
            )
            lse_block = lax.dynamic_slice_in_dim(lse_piece, row_start, block_size, 1).transpose(
                0, 2, 1
            )
            delta_block = lax.dynamic_slice_in_dim(delta_piece, row_start, block_size, 1).transpose(
                0, 2, 1
            )
            more_keys, more_values = key_side(
                query_block, grad_block, lse_block, delta_block, key_heads, value_heads, score_scale
            )
            return (grad_keys + more_keys, grad_values + more_values)

        return lax.fori_loop(0, length // block_size, one_step, running)

    return fold_queries


def layer_in_blocks(
    hidden,
    pos_ids,
    type_ids,
    cotangent,
    pos_table,
    type_table,
    query_key_value_weight,
    attention_output_weight,
    up_projection_weight,
    down_projection_weight,
    up_projection_bias,
    norm_gains,
    biases,
):
    seq_count, seg_tokens, model_width = hidden.shape
    row_count = seq_count * seg_tokens
    head_count = HEADS // lax.axis_size("head")
    head_size = model_width // HEADS
    local_width = head_count * head_size
    query_rows = lax.axis_size("head") * seg_tokens
    score_scale = 1.0 / math.sqrt(head_size)

    def fetch_weights():
        return (
            lax.all_gather(query_key_value_weight, "blk", axis=0, tiled=True),
            lax.all_gather(attention_output_weight, "blk", axis=0, tiled=True),
            lax.all_gather(up_projection_weight, "blk", axis=0, tiled=True),
            lax.all_gather(down_projection_weight, "blk", axis=0, tiled=True),
            lax.all_gather(up_projection_bias, "blk", axis=0, tiled=True),
            lax.all_gather(norm_gains, "blk", axis=1, tiled=True),
            lax.all_gather(biases, "blk", axis=1, tiled=True),
            lax.all_gather(type_table, "blk", axis=1, tiled=True),
        )

    qkv_full, out_full, up_full, down_full, up_bias_full, gain_full, bias_full, type_full = (
        fetch_weights()
    )
    bias_float = bias_full.astype(jnp.float32)
    gain_float = gain_full.astype(jnp.float32)
    flat_pos = pos_ids.reshape(row_count)
    portion = lax.all_gather(pos_table, "blk", axis=0, tiled=True)
    local_slots = flat_pos
    onehot = (
        local_slots[:, None] == jnp.arange(portion.shape[0], dtype=jnp.int32)[None, :]
    ).astype(jnp.bfloat16)
    positions = jnp.dot(onehot, portion, preferred_element_type=jnp.float32)
    is_second = type_ids.reshape(row_count, 1) == 1
    typed_rows = jnp.where(
        is_second, type_full[1].astype(jnp.float32), type_full[0].astype(jnp.float32)
    )
    embedded_tokens = (
        hidden.reshape(row_count, model_width).astype(jnp.float32) + positions + typed_rows
    )
    embedded_low = embedded_tokens.astype(jnp.bfloat16)
    projected_rows = jnp.dot(embedded_low, qkv_full, preferred_element_type=jnp.float32)
    token_shape = (seq_count, seg_tokens, model_width)
    queries = (
        (projected_rows[:, :model_width] + bias_float[0]).astype(jnp.bfloat16).reshape(token_shape)
    )
    keys_token = (
        projected_rows[:, model_width : 2 * model_width].astype(jnp.bfloat16).reshape(token_shape)
    )
    values_token = (
        (projected_rows[:, 2 * model_width :] + bias_float[1])
        .astype(jnp.bfloat16)
        .reshape(token_shape)
    )
    query_local, key_local, value_local = (
        lax.all_to_all(queries, "head", split_axis=2, concat_axis=1, tiled=True),
        lax.all_to_all(keys_token, "head", split_axis=2, concat_axis=1, tiled=True),
        lax.all_to_all(values_token, "head", split_axis=2, concat_axis=1, tiled=True),
    )
    head_shape = (seq_count, query_rows, head_count, head_size)
    query_heads = query_local.reshape(head_shape)
    key_heads = key_local.reshape(head_shape)
    value_heads = value_local.reshape(head_shape)
    start_peak = jnp.full((seq_count, head_count, query_rows), -jnp.inf, jnp.float32)
    start_total = jnp.zeros((seq_count, head_count, query_rows), jnp.float32)
    zero_heads = jnp.zeros((seq_count, head_count, query_rows, head_size), jnp.float32)
    fold_keys = forward_fold(query_heads, score_scale, head_count, head_size)
    row_peak, row_total, weighted = fold_keys(
        (start_peak, start_total, zero_heads),
        (
            lax.all_gather(key_local, "blk", axis=1, tiled=True),
            lax.all_gather(value_local, "blk", axis=1, tiled=True),
        ),
        jnp.int32(0),
    )
    log_totals = row_peak + jnp.log(row_total)
    attention_result = weighted / row_total[..., None]
    attended_low = (
        attention_result.transpose(0, 2, 1, 3)
        .reshape(seq_count, query_rows, local_width)
        .astype(jnp.bfloat16)
    )
    attended_token = lax.all_to_all(
        attended_low, "head", split_axis=1, concat_axis=2, tiled=True
    ).reshape(row_count, model_width)
    residual_branch = (
        jnp.dot(attended_token, out_full, preferred_element_type=jnp.float32) + bias_float[2]
    )
    first_layer_norm, first_pull = jax.vjp(
        norm_layer, embedded_tokens + residual_branch, gain_float[0], bias_float[3]
    )
    first_low = first_layer_norm.astype(jnp.bfloat16)
    inner_product_sum = jnp.dot(
        first_low, up_full, preferred_element_type=jnp.float32
    ) + up_bias_full.astype(jnp.float32)
    gelu_activations, gelu_pull = jax.vjp(gelu_exact, inner_product_sum)
    activated_low = gelu_activations.astype(jnp.bfloat16)
    second_layer_norm = (
        jnp.dot(activated_low, down_full, preferred_element_type=jnp.float32) + bias_float[4]
    )
    final_norm, final_pull = jax.vjp(
        norm_layer, first_layer_norm + second_layer_norm, gain_float[1], bias_float[5]
    )
    layer_out = final_norm.astype(jnp.bfloat16).reshape(token_shape)
    qkv_full, out_full, up_full, down_full, up_bias_full, gain_full, bias_full, type_full = (
        fetch_weights()
    )
    grad_final, grad_gain_two, grad_shift_two = final_pull(
        cotangent.reshape(row_count, model_width).astype(jnp.float32)
    )
    grad_second = grad_final.astype(jnp.bfloat16)
    grad_down = jnp.einsum(
        "rf,rd->fd", activated_low, grad_second, preferred_element_type=jnp.float32
    )
    grad_bias_second = jnp.sum(grad_second.astype(jnp.float32), axis=0)
    (grad_inner,) = gelu_pull(
        jnp.einsum("rd,fd->rf", grad_second, down_full, preferred_element_type=jnp.float32)
    )
    grad_inner_low = grad_inner.astype(jnp.bfloat16)
    grad_up = jnp.einsum("rd,rf->df", first_low, grad_inner_low, preferred_element_type=jnp.float32)
    grad_up_bias = jnp.sum(grad_inner_low.astype(jnp.float32), axis=0)
    grad_first = grad_final + jnp.einsum(
        "rf,df->rd", grad_inner_low, up_full, preferred_element_type=jnp.float32
    )
    grad_resid, grad_gain_one, grad_shift_one = first_pull(grad_first)
    grad_branch = grad_resid.astype(jnp.bfloat16)
    grad_out = jnp.einsum(
        "re,rd->ed", attended_token, grad_branch, preferred_element_type=jnp.float32
    )
    grad_bias_branch = jnp.sum(grad_branch.astype(jnp.float32), axis=0)
    grad_attended = (
        jnp.einsum("rd,ed->re", grad_branch, out_full, preferred_element_type=jnp.float32)
        .astype(jnp.bfloat16)
        .reshape(token_shape)
    )
    grad_local = lax.all_to_all(grad_attended, "head", split_axis=2, concat_axis=1, tiled=True)
    grad_heads = grad_local.reshape(head_shape)
    delta_rows = jnp.sum(
        grad_heads.astype(jnp.float32).transpose(0, 2, 1, 3) * attention_result, axis=-1
    )
    fold_queries = query_fold(
        query_heads, grad_heads, log_totals, delta_rows, score_scale, head_count, head_size
    )
    grad_query_sum = fold_queries(
        zero_heads,
        (
            lax.all_gather(key_local, "blk", axis=1, tiled=True),
            lax.all_gather(value_local, "blk", axis=1, tiled=True),
        ),
        jnp.int32(0),
    )
    fold_side = key_fold(key_heads, value_heads, score_scale, head_count, head_size)
    grad_key_sum, grad_value_sum = fold_side(
        (zero_heads, zero_heads),
        (
            lax.all_gather(query_local.astype(jnp.float32), "blk", axis=1, tiled=True).astype(
                jnp.bfloat16
            ),
            lax.all_gather(grad_local.astype(jnp.float32), "blk", axis=1, tiled=True).astype(
                jnp.bfloat16
            ),
            lax.all_gather(log_totals.transpose(0, 2, 1), "blk", axis=1, tiled=True),
            lax.all_gather(delta_rows.transpose(0, 2, 1), "blk", axis=1, tiled=True),
        ),
        jnp.int32(0),
    )
    grad_keys_local = (
        (grad_key_sum * score_scale)
        .transpose(0, 2, 1, 3)
        .reshape(seq_count, query_rows, local_width)
        .astype(jnp.bfloat16)
    )
    grad_values_local = (
        grad_value_sum.transpose(0, 2, 1, 3)
        .reshape(seq_count, query_rows, local_width)
        .astype(jnp.bfloat16)
    )
    grad_query_local = (
        (grad_query_sum * score_scale)
        .transpose(0, 2, 1, 3)
        .reshape(seq_count, query_rows, local_width)
        .astype(jnp.bfloat16)
    )
    grad_query_token, grad_key_token, grad_value_token = (
        lax.all_to_all(grad_query_local, "head", split_axis=1, concat_axis=2, tiled=True),
        lax.all_to_all(grad_keys_local, "head", split_axis=1, concat_axis=2, tiled=True),
        lax.all_to_all(grad_values_local, "head", split_axis=1, concat_axis=2, tiled=True),
    )
    grad_qkv = jnp.concatenate(
        [grad_query_token, grad_key_token, grad_value_token], axis=-1
    ).reshape(row_count, 3 * model_width)
    grad_qkv_full = jnp.einsum(
        "rd,rf->df", embedded_low, grad_qkv, preferred_element_type=jnp.float32
    )
    grad_bias_query = jnp.sum(
        grad_query_token.astype(jnp.float32).reshape(row_count, model_width), axis=0
    )
    grad_bias_value = jnp.sum(
        grad_value_token.astype(jnp.float32).reshape(row_count, model_width), axis=0
    )
    grad_embedded = grad_resid + jnp.einsum(
        "rf,df->rd", grad_qkv, qkv_full, preferred_element_type=jnp.float32
    )
    second_mask = is_second.astype(jnp.float32)
    grad_type_one = jnp.sum(grad_embedded * second_mask, axis=0)
    grad_type_zero = jnp.sum(grad_embedded * (1.0 - second_mask), axis=0)
    length = lax.axis_size("blk") * pos_table.shape[0]
    local_slots = flat_pos
    inside = (local_slots >= 0) & (local_slots < length)
    slot_index = jnp.where(inside, local_slots, length)
    buffer = jnp.zeros((length + 1, model_width), jnp.float32).at[slot_index].add(grad_embedded)
    grad_positions = lax.psum_scatter(buffer[:length], "blk", scatter_dimension=0, tiled=True)
    gain_stack = jnp.stack([grad_gain_one, grad_gain_two])
    bias_stack = jnp.stack(
        [
            grad_bias_query,
            grad_bias_value,
            grad_bias_branch,
            grad_shift_one,
            grad_bias_second,
            grad_shift_two,
        ]
    )
    type_stack = jnp.stack([grad_type_zero, grad_type_one])
    (
        shard_qkv,
        shard_out,
        shard_up,
        shard_down,
        shard_up_bias,
        shard_gains,
        shard_biases,
        shard_types,
    ) = (
        lax.psum_scatter(grad_qkv_full, "blk", scatter_dimension=0, tiled=True),
        lax.psum_scatter(grad_out, "blk", scatter_dimension=0, tiled=True),
        lax.psum_scatter(grad_up, "blk", scatter_dimension=0, tiled=True),
        lax.psum_scatter(grad_down, "blk", scatter_dimension=0, tiled=True),
        lax.psum_scatter(grad_up_bias, "blk", scatter_dimension=0, tiled=True),
        lax.psum_scatter(gain_stack, "blk", scatter_dimension=1, tiled=True),
        lax.psum_scatter(bias_stack, "blk", scatter_dimension=1, tiled=True),
        lax.psum_scatter(type_stack, "blk", scatter_dimension=1, tiled=True),
    )
    (
        total_qkv,
        total_out,
        total_up,
        total_down,
        total_up_bias,
        total_gains,
        total_biases,
        total_types,
        total_positions,
    ) = lax.psum(
        (
            shard_qkv,
            shard_out,
            shard_up,
            shard_down,
            shard_up_bias,
            shard_gains,
            shard_biases,
            shard_types,
            grad_positions,
        ),
        "head",
    )
    grad_hidden = grad_embedded.reshape(token_shape)
    return (
        layer_out,
        grad_hidden,
        total_positions,
        total_types,
        total_qkv,
        total_out,
        total_up,
        total_down,
        total_up_bias,
        total_gains,
        total_biases,
    )


BIG = 56 << 20
WHOLE = 67043328
LAG = 1
CHUNKS = 4
CHUNK_LAG = 1
EARLY = (1, 3)
TURNS = ((1, 3), (2, 4, 6, 8), (6, 12))


def layer_in_planes(
    hidden,
    pos_ids,
    type_ids,
    cotangent,
    pos_table,
    type_table,
    query_key_value_weight,
    attention_output_weight,
    up_projection_weight,
    down_projection_weight,
    up_projection_bias,
    norm_gains,
    biases,
):
    seqs, seg, width = hidden.shape
    b = lax.axis_index("blk")
    rows = seqs * seg
    e = width // HEADS
    scale = 1.0 / math.sqrt(e)
    slots = pos_table.shape[0]
    fcols = down_projection_weight.shape[0] // 2

    token_shape = (seqs, seg, width)
    begin = SimpleNamespace(
        biases=biases,
        gains=norm_gains,
        types=type_table,
        up_bias=up_projection_bias.reshape(2, 2 * e),
        pos_ids=pos_ids,
        type_ids=type_ids,
        qkv_weight=query_key_value_weight,
        out_weight=attention_output_weight,
        up_weight=up_projection_weight,
        down_weight=down_projection_weight,
        table=pos_table,
        hidden=hidden,
    )
    (
        (
            attended,
            held,
            pair_out,
            lse,
            embedded,
            plane_low,
            qkv_own,
            out_own,
            up_one,
            up_cut,
            down_one,
            vectors,
            up_bias,
            pos_all,
            is_second,
        ),
    ) = fused("first_half", 0, [first_half(begin, scale, LAG)], WHOLE)
    parts = SimpleNamespace(
        attended=attended,
        out_own=out_own.reshape(2 * e, width),
        embedded=embedded,
        cotangent=cotangent,
        up_one=up_one,
        up_cut=up_cut,
        down_one=down_one,
        down_weight=down_projection_weight,
        up_bias=up_bias,
        vectors=vectors,
        held=held,
        pair_out=pair_out,
        lse=lse,
        qkv_own=qkv_own.reshape(width, 6 * e),
        plane_low=plane_low,
        ids=pos_all,
        second=is_second,
    )
    sizes = (slots, CHUNKS, LAG, CHUNK_LAG, scale)
    ((layer_out, grad_hidden, pos, down, up, qkv, out, totals),) = fused(
        "second_half", 4, [second_half(parts, sizes)], WHOLE
    )
    outs = finish(
        (b % 2).reshape(1),
        layer_out.reshape(rows, width),
        grad_hidden.reshape(rows, width),
        pos,
        down.reshape(2 * fcols, width),
        up,
        qkv,
        out,
        totals,
    )
    return (
        outs[0].reshape(token_shape),
        outs[1].reshape(token_shape),
        *outs[2:8],
        outs[8].reshape(4 * e),
        *outs[9:],
    )


def planes_fit(hidden, head_axis, blk_axis):
    seqs, seg, width = hidden.shape
    return head_axis == 2 and blk_axis == HEADS and seqs == 2 and seqs * seg == 2 * width // HEADS


def on_device(hidden, *rest):
    if planes_fit(hidden, lax.axis_size("head"), lax.axis_size("blk")):
        return layer_in_planes(hidden, *rest)
    return layer_in_blocks(hidden, *rest)


def solution(mesh):
    in_specs = (
        P(None, ("head", "blk"), None),
        P(None, ("head", "blk")),
        P(None, ("head", "blk")),
        P(None, ("head", "blk"), None),
        P("blk", None),
        P(None, "blk"),
        P("blk", None),
        P("blk", None),
        P("blk", None),
        P("blk", None),
        P("blk"),
        P(None, "blk"),
        P(None, "blk"),
    )
    out_specs = (
        P(None, ("head", "blk"), None),
        P(None, ("head", "blk"), None),
        P("blk", None),
        P(None, "blk"),
        P("blk", None),
        P("blk", None),
        P("blk", None),
        P("blk", None),
        P("blk"),
        P(None, "blk"),
        P(None, "blk"),
    )
    return jax.shard_map(
        on_device, mesh=mesh, in_specs=in_specs, out_specs=out_specs, check_vma=False
    )
```

```python
import functools
import math
from types import SimpleNamespace

import jax
import jax.numpy as jnp
from jax import lax
from jax.experimental import pallas as pl
from jax.experimental.pallas import tpu as pltpu
from jax.sharding import PartitionSpec as P

HEADS = 16
MESH = pl.DeviceIdType.MESH
F32 = jnp.float32
BF16 = jnp.bfloat16
VSPEC = pl.BlockSpec(memory_space=pltpu.VMEM)


def place():
    h = lax.axis_index("head")
    b = lax.axis_index("blk")
    return h, b // 4, (b // 2) % 2, b % 2


def blk(o, y, c):
    return (o * 2 + y) * 2 + c


def peer(dx, dz, dy, dc):
    h, o, y, c = place()
    flip = lambda v, d: 1 - v if d else v
    return flip(h, dx), blk((o + dz) % 4 if dz else o, flip(y, dy), flip(c, dc))


def remote(src, dst, sems, index, device):
    return pltpu.make_async_remote_copy(
        src_ref=src,
        dst_ref=dst,
        send_sem=sems.at[0, index],
        recv_sem=sems.at[1, index],
        device_id=device,
        device_id_type=MESH,
    )


def landed(ref, sems, index):
    remote(ref, ref, sems, index, peer(1, 0, 0, 0)).wait_recv()


def sems(count):
    return pltpu.SemaphoreType.DMA((2, count))


NEAR_X, NEAR_Y, NEAR_C = (1, 0, 0, 0), (0, 0, 1, 0), (0, 0, 0, 1)
COLUMN = ((0, 1, 0, 0), (0, 2, 0, 0), (0, 3, 0, 0))
PLANE = tuple(
    (dx, 0, dy, dc) for dx in range(2) for dy in range(2) for dc in range(2) if dx or dy or dc
)


class Part:
    def __init__(self, run, ins, outs, scratch, peers):
        self.run, self.ins, self.outs, self.scratch, self.peers = run, ins, outs, scratch, peers
        self.turns = ()

    def on(self, *turns):
        self.turns = turns
        return self


def fused(name, cid, parts, limit=None):
    peers = sorted({p for part in parts for p in part.peers})
    ins = [x for part in parts for x in part.ins]
    outs = [s for part in parts for s in part.outs]
    scratch = [s for part in parts for s in part.scratch]

    def kernel(*refs):
        in_refs, out_refs = refs[: len(ins)], refs[len(ins) : len(ins) + len(outs)]
        own = refs[len(ins) + len(outs) :]
        gens = []
        i = j = k = 0
        for part in parts:
            gens.append(
                part.run(
                    in_refs[i : i + len(part.ins)],
                    out_refs[j : j + len(part.outs)],
                    own[k : k + len(part.scratch)],
                )
            )
            i, j, k = i + len(part.ins), j + len(part.outs), k + len(part.scratch)
        barrier = pltpu.get_barrier_semaphore()
        for p in peers:
            pl.semaphore_signal(barrier, inc=1, device_id=peer(*p), device_id_type=MESH)
        pl.semaphore_wait(barrier, len(peers))
        for gen in gens:
            next(gen)
        for turn, _ in enumerate(gens[0]):
            for part, gen in zip(parts, gens):
                if turn in part.turns:
                    next(gen)
        for gen in gens[1:]:
            for _ in gen:
                pass

    got = pl.pallas_call(
        kernel,
        name=name,
        out_shape=[jax.ShapeDtypeStruct(s, d) for s, d in outs],
        in_specs=[VSPEC] * len(ins),
        out_specs=[VSPEC] * len(outs),
        scratch_shapes=scratch,
        compiler_params=pltpu.CompilerParams(
            collective_id=cid, has_side_effects=True, vmem_limit_bytes=limit
        ),
    )(*ins)
    result = []
    for part in parts:
        result.append(got[: len(part.outs)])
        got = got[len(part.outs) :]
    return result


def exchange(x, peers, out_lead, source, target):
    peers = list(peers)

    def coords(p):
        h, o, y, c = place()
        flip = lambda v, d: 1 - v if d else v
        return flip(h, p[0]), (o + p[1]) % 4 if p[1] else o, flip(y, p[2]), flip(c, p[3])

    def run(ins, outs, own):
        (x_ref,), (out_ref,), (sem,) = ins, outs, own
        me = place()
        copies = []
        for k, p in enumerate(peers):
            copy = remote(
                source(x_ref, coords(p)), target(out_ref, me), sem, k, peer(*p)
            )
            copy.start()
            copies.append(copy)
        yield
        target(out_ref, me)[...] = source(x_ref, me)[...]
        for copy in copies:
            copy.wait()

    return Part(run, [x], [(out_lead, x.dtype)], [sems(len(peers))], peers)


def small_gather(x):
    peers = [
        (0, dz, dy, dc) for dz in range(4) for dy in range(2) for dc in range(2) if dz or dy or dc
    ]
    return exchange(x, peers, (16,) + x.shape, lambda r, d: r, lambda r, s: r.at[blk(*s[1:])])


def place_copy(src, dst, send_sem, recv_sem, device):
    return pltpu.make_async_remote_copy(
        src_ref=src,
        dst_ref=dst,
        send_sem=send_sem,
        recv_sem=recv_sem,
        device_id=device,
        device_id_type=MESH,
    )


BLK = tuple(
    (0, dz, dy, dc) for dz in range(4) for dy in range(2) for dc in range(2) if dz or dy or dc
)


def out_weights(w):
    r, n = w.shape

    def run(ins, outs, own):
        (w_ref,), (out_ref,), (send, recv) = ins, outs, own
        h, o, y, c = place()
        has = o // 2 == h
        serves = (o % 2 == y) & (y == c)

        def each(act):
            for k in range(4):
                device = (h, blk((o + k) % 4, o % 2, y))
                copy = place_copy(w_ref, out_ref.at[c], send.at[k], recv.at[c], device)

                @pl.when(has if k else has & jnp.logical_not(serves))
                def _():
                    act(copy)

        each(lambda copy: copy.start())
        yield

        @pl.when(has & serves)
        def _():
            out_ref[pl.ds(c, 1)] = w_ref[...][None]

        each(lambda copy: copy.wait_send())
        for core in range(2):
            from_self = (o == 2 * h + y) & (y == c) & (c == core)
            ref = out_ref.at[core]

            @pl.when(jnp.logical_not(from_self))
            def _():
                place_copy(ref, ref, send.at[0], recv.at[core], (h, blk(o, y, c))).wait_recv()

    scratch = [pltpu.SemaphoreType.DMA((4,)), pltpu.SemaphoreType.DMA((2,))]
    return Part(run, [w], [((2, r, n), BF16)], scratch, BLK)


def mirrored():
    o = place()[1]
    far = o // 2
    seen = lambda v: v * (1 - 2 * far) + 3 * far
    return seen(o), seen


def gather_steps(src, dst, sem):
    h, o, y, c = place()
    dev_x, dev_y, dev_c = peer(*NEAR_X), peer(*NEAR_Y), peer(*NEAR_C)
    mine = h * 4 + y * 2 + c
    of_x = (1 - h) * 4 + y * 2 + c
    of_y = h * 4 + (1 - y) * 2 + c
    of_d = (1 - h) * 4 + (1 - y) * 2 + c
    flip = 1 - 2 * c
    sent = []

    def go(ref, slot, half, index, device):
        copy = remote(ref, dst(half, slot), sem, index, device)
        copy.start()
        sent.append(copy)

    go(src(0), mine, 0, 0, dev_x)
    go(src(1), mine, 1, 1, dev_y)
    go(src(1), mine, 1, 2, dev_x)
    go(src(0), mine, 0, 3, dev_y)
    go(src(0), mine, 0, 4, dev_c)
    go(src(1), mine, 1, 5, dev_c)
    for half in range(2):
        dst(half, mine)[...] = src(half)[...]

    def relay(slot, half, index, device, onward, to_core):
        landed(dst(half, slot), sem, index)
        if onward is not None:
            go(dst(half, slot), slot, half, onward, device)
        go(dst(half, slot), slot, half, to_core, dev_c)

    yield
    relay(of_x, 0, 0, dev_y, 6, 8)
    relay(of_y, 1, 1, dev_x, 7, 9)
    yield
    relay(of_x, 1, 2, None, None, 10)
    relay(of_y, 0, 3, None, None, 11)
    yield
    relay(of_d, 0, 6, None, None, 12)
    relay(of_d, 1, 7, None, None, 13)
    yield
    for slot, half, index in (
        (mine, 0, 4),
        (mine, 1, 5),
        (of_x, 0, 8),
        (of_y, 1, 9),
        (of_x, 1, 10),
        (of_y, 0, 11),
        (of_d, 0, 12),
        (of_d, 1, 13),
    ):
        landed(dst(half, slot + flip), sem, index)
    for copy in sent:
        copy.wait_send()


def scatter_steps(src, total, near, part, from_x, from_y, diag, sem):
    h, o, y, c = place()
    dev_x, dev_y, dev_c = peer(*NEAR_X), peer(*NEAR_Y), peer(*NEAR_C)
    mine = h * 4 + y * 2 + c
    of_x = (1 - h) * 4 + y * 2 + c
    of_y = h * 4 + (1 - y) * 2 + c
    of_d = (1 - h) * 4 + (1 - y) * 2 + c
    flip = 1 - 2 * c
    order = (of_d, of_x, of_y, mine)
    sent = []

    def go(ref, to, index, device):
        copy = remote(ref, to, sem, index, device)
        copy.start()
        sent.append(copy)

    for k, half in ((0, 0), (0, 1), (1, 0), (2, 1), (1, 1), (2, 0), (3, 0), (3, 1)):
        go(src(half, order[k] + flip), near.at[k, half], 2 * k + half, dev_c)

    def add(k, half):
        landed(near.at[k, half], sem, 2 * k + half)
        return src(half, order[k])[...].astype(F32) + near[k, half].astype(F32)

    yield
    part[0, 0] = add(0, 0).astype(BF16)
    go(part.at[0, 0], diag.at[0], 8, dev_x)
    part[0, 1] = add(0, 1).astype(BF16)
    go(part.at[0, 1], diag.at[1], 9, dev_y)
    part[1, 0] = add(1, 0).astype(BF16)
    go(part.at[1, 0], from_x.at[0], 10, dev_x)
    part[2, 1] = add(2, 1).astype(BF16)
    go(part.at[2, 1], from_y.at[1], 11, dev_y)
    yield
    kept_x = add(1, 1)
    landed(diag.at[1], sem, 9)
    part[1, 1] = (kept_x + diag[1].astype(F32)).astype(BF16)
    go(part.at[1, 1], from_x.at[1], 12, dev_x)
    kept_y = add(2, 0)
    landed(diag.at[0], sem, 8)
    part[2, 0] = (kept_y + diag[0].astype(F32)).astype(BF16)
    go(part.at[2, 0], from_y.at[0], 13, dev_y)
    yield
    own = [add(3, half) for half in range(2)]
    for half, ix, iy in ((0, 10, 13), (1, 12, 11)):
        landed(from_x.at[half], sem, ix)
        landed(from_y.at[half], sem, iy)
        total(half)[...] = own[half] + from_x[half].astype(F32) + from_y[half].astype(F32)
    for copy in sent:
        copy.wait_send()


def scatter_scratch(r, n):
    block = (2, r // 2, n)
    return [
        pltpu.VMEM((4,) + block, BF16),
        pltpu.VMEM((3,) + block, BF16),
        pltpu.VMEM(block, BF16),
        pltpu.VMEM(block, BF16),
        pltpu.VMEM(block, BF16),
        sems(14),
    ]


def norm_parts(r):
    centred = r - jnp.mean(r, axis=-1, keepdims=True)
    scale = lax.rsqrt(jnp.mean(centred * centred, axis=-1, keepdims=True) + 1e-12)
    return centred * scale, scale


def norm_back(xh, scale, dh):
    return (
        dh
        - jnp.mean(dh, axis=-1, keepdims=True)
        - xh * jnp.mean(dh * xh, axis=-1, keepdims=True)
    ) * scale


def dot_nt(a, b):
    return lax.dot_general(a, b, (((1,), (1,)), ((), ())), preferred_element_type=F32)


def dot_tn(a, b):
    return lax.dot_general(a, b, (((0,), (0,)), ((), ())), preferred_element_type=F32)


def blk_gather_steps(src, spot_of, zsem, ysem, csem):
    h, o, y, c = place()
    at, seen = mirrored()
    dev_y, dev_c = peer(*NEAR_Y), peer(*NEAR_C)
    end, inner, other = (h, blk(seen(0), y, c)), (h, blk(seen(1), y, c)), (h, blk(seen(2), y, c))
    sent = []

    def spot(z, yy=y, cc=c):
        return spot_of(z, yy, cc)

    def go(ref, z, yy, sem, index, device):
        copy = remote(ref, spot(z, yy), sem, index, device)
        copy.start()
        sent.append(copy)

    def line(ref, z, index, device):
        return remote(ref, spot(z), zsem, index, device)

    @pl.when(at == 0)
    def _():
        line(src, o, 0, inner).start()

    @pl.when(at == 1)
    def _():
        line(src, o, 1, end).start()
        line(src, o, 2, other).start()

    go(src, o, y, ysem, 0, dev_y)
    go(src, o, y, csem, 0, dev_c)
    spot(o)[...] = src[...]

    def onward(j, z):
        go(spot(z), z, y, ysem, j, dev_y)
        go(spot(z), z, y, csem, j, dev_c)

    first = seen(1 - at)
    order = (o, first, seen(2), seen(3))

    def from_y(j):
        landed(spot(order[j], 1 - y), ysem, j)
        go(spot(order[j], 1 - y), order[j], 1 - y, csem, 4 + j, dev_c)

    yield

    @pl.when(at == 0)
    def _():
        landed(spot(seen(1)), zsem, 1)

    @pl.when(at == 1)
    def _():
        landed(spot(seen(0)), zsem, 0)
        line(spot(seen(0)), seen(0), 3, other).start()

    onward(1, first)

    @pl.when(at == 1)
    def _():
        landed(spot(seen(2)), zsem, 2)
        line(spot(seen(2)), seen(2), 4, end).start()

    yield
    from_y(0)

    @pl.when(at == 0)
    def _():
        landed(spot(seen(2)), zsem, 4)

    onward(2, seen(2))

    @pl.when(at == 1)
    def _():
        landed(spot(seen(3)), zsem, 3)
        line(spot(seen(3)), seen(3), 5, end).start()

    yield
    from_y(1)

    @pl.when(at == 0)
    def _():
        landed(spot(seen(3)), zsem, 5)

    onward(3, seen(3))
    yield
    from_y(2)
    yield
    from_y(3)
    yield
    for j, z in enumerate(order):
        landed(spot(z, y, 1 - c), csem, j)
        landed(spot(z, 1 - y, 1 - c), csem, 4 + j)

    @pl.when(at == 0)
    def _():
        line(src, o, 0, inner).wait_send()

    @pl.when(at == 1)
    def _():
        line(src, o, 1, end).wait_send()
        line(src, o, 2, other).wait_send()
        line(spot(seen(0)), seen(0), 3, other).wait_send()
        line(spot(seen(2)), seen(2), 4, end).wait_send()
        line(spot(seen(3)), seen(3), 5, end).wait_send()

    for copy in sent:
        copy.wait_send()


ALL = tuple(
    (dx, dz, dy, dc)
    for dx in range(2)
    for dz in range(4)
    for dy in range(2)
    for dc in range(2)
    if dx or dz or dy or dc
)


def line_gather_steps(src, spot, sem):
    h, o, y, c = place()
    at, seen = mirrored()
    end, inner, other = (h, blk(seen(0), y, c)), (h, blk(seen(1), y, c)), (h, blk(seen(2), y, c))

    def line(ref, z, index, device):
        return remote(ref, spot(z), sem, index, device)

    @pl.when(at == 0)
    def _():
        line(src, o, 0, inner).start()

    @pl.when(at == 1)
    def _():
        line(src, o, 2, other).start()
        line(src, o, 1, end).start()

    spot(o)[...] = src[...]
    for k, (z, to, device) in enumerate(((0, 3, other), (2, 4, end), (3, 5, end))):
        yield

        @pl.when(at == 1)
        def _():
            landed(spot(seen(z)), sem, (0, 2, 3)[k])
            line(spot(seen(z)), seen(z), to, device).start()

    yield

    @pl.when(at == 0)
    def _():
        for z, index in ((1, 1), (2, 4), (3, 5)):
            landed(spot(seen(z)), sem, index)
        line(src, o, 0, inner).wait_send()

    @pl.when(at == 1)
    def _():
        line(src, o, 1, end).wait_send()
        line(src, o, 2, other).wait_send()
        for z, to, device in ((0, 3, other), (2, 4, end), (3, 5, end)):
            line(spot(seen(z)), seen(z), to, device).wait_send()


def line_sum_steps(term_of, out, terms, ends, mids, last, sem):
    h, o, y, c = place()
    at, seen = mirrored()
    end, inner, other = (h, blk(seen(0), y, c)), (h, blk(seen(1), y, c)), (h, blk(seen(2), y, c))
    order = [seen(3), seen(2), seen(1 - at)]
    plus = lambda a, b: a[...].astype(F32) + b[...].astype(F32)

    @pl.when(at == 0)
    def _():
        for j in range(3):
            remote(term_of(order[j]), ends.at[j], sem, j, inner).start()

    for j in range(2):
        yield

        @pl.when(at == 1)
        def _():
            landed(ends.at[j], sem, j)
            terms[j] = plus(term_of(order[j]), ends.at[j]).astype(BF16)
            remote(terms.at[j], mids.at[j], sem, 3 + j, other).start()

    yield

    @pl.when(at == 1)
    def _():
        landed(mids.at[0], sem, 3)
        terms[2] = plus(term_of(order[2]), mids.at[0]).astype(BF16)
        remote(terms.at[2], last, sem, 5, end).start()

    yield

    @pl.when(at == 1)
    def _():
        landed(ends.at[2], sem, 2)
        landed(mids.at[1], sem, 4)
        out[...] = (plus(term_of(o), ends.at[2]) + mids[1].astype(F32)).astype(BF16)
        for j in range(2):
            remote(terms.at[j], mids.at[j], sem, 3 + j, other).wait_send()
        remote(terms.at[2], last, sem, 5, end).wait_send()

    @pl.when(at == 0)
    def _():
        landed(last, sem, 5)
        out[...] = plus(term_of(o), last).astype(BF16)
        for j in range(3):
            remote(term_of(order[j]), ends.at[j], sem, j, inner).wait_send()


def line_sum_scratch(block):
    return [
        pltpu.VMEM((3,) + block, BF16),
        pltpu.VMEM((3,) + block, BF16),
        pltpu.VMEM((2,) + block, BF16),
        pltpu.VMEM(block, BF16),
        sems(6),
    ]


def spread_steps(rows_of, out, spots, sem):
    h, o, y, c = place()
    t = h * 4 + y * 2 + c
    columns = [
        out.at[:, pl.ds(pl.multiple_of(lane * 128, 128), 128)] for lane in spots(t)
    ]
    pieces = len(columns)
    copies = []
    for k, p in enumerate(PLANE):
        to = (1 - y if p[2] else y) * 2 + (1 - c if p[3] else c)
        for i in range(pieces):
            src = rows_of(to).at[:, pl.ds(i * 128, 128)]
            copy = remote(src, columns[i], sem, k * pieces + i, peer(*p))
            copy.start()
            copies.append(copy)
    for i in range(pieces):
        columns[i][...] = rows_of(y * 2 + c)[:, i * 128 : (i + 1) * 128]
    yield
    for copy in copies:
        copy.wait()


def second_half(x, consts):
    names = list(vars(x))
    seqs, r, d = x.embedded.shape
    planes, four, e, fh = x.up_one.shape
    f = 2 * fh
    fcols = x.down_weight.shape[0] // 2
    half_d = d // 2
    rows, q_rows = 8 * r, 4 * r
    three, he, length = x.held.shape
    n = length // 4
    slots, chunks, chunk_lag, scale = consts
    own_rows, w, blks = seqs * r, d // chunks, 16
    key_rows = 256
    width_qkv = 3 * 2 * he

    need = []

    def scratch(shape, dtype):
        need.append(pltpu.VMEM(shape, dtype))
        return len(need) - 1

    def many(specs):
        start = len(need)
        need.extend(specs)
        return list(range(start, len(need)))

    plane = (seqs, 8, r, d)
    shapes = dict(
        partial=(plane, BF16),
        up_two=(x.up_one.shape, BF16),
        down_all=((planes, fcols, d), BF16),
        first_g=(plane, BF16),
        grad_g=(plane, BF16),
        branch_g=(plane, BF16),
        act=((seqs * rows, f), BF16),
        slope=((seqs * rows, f), F32),
        inner_grad=((seqs * rows, f), BF16),
        first=((seqs, r, d), F32),
        xh_one=((seqs, r, d), F32),
        scale_one=((seqs, r, 1), F32),
        grad_two=((seqs, r, d), F32),
        low=((seqs, r, d), BF16),
        total=((seqs, r, d), F32),
        resid=((seqs, r, d), F32),
        down_part=((planes, fcols, d), BF16),
        up_part=((planes, 4 * e, f), BF16),
        up_total=((4 * e, f), BF16),
        out_part=((2, he, d), BF16),
        out_held=((4, he, d), BF16),
        out_acc=((he, d), F32),
        sums=((16, d), F32),
        up_sums=((1, f), F32),
        up_spots=((32, 128), F32),
        go=((2, he, 2 * n), BF16),
        gs=((he, length), BF16),
        qs=((he, length), BF16),
        q_rows=((length, he), BF16),
        g_rows=((length, he), BF16),
        dq=((he, length), F32),
        delta=((1, length), F32),
        pair_low=((three, he, length), BF16),
        dqkv=((three, 2, he, 2 * n), BF16),
        qkv_part=((planes, 4 * e, width_qkv), BF16),
        qkv_total=((4 * e, width_qkv), BF16),
        own=((chunks, own_rows, w), BF16),
        gathered=((chunks, blks, own_rows, w), BF16),
        pick=((slots, blks * own_rows), BF16),
        pos_low=((chunks, slots, w), BF16),
        pos_held=((chunks, slots, w), BF16),
        pack=((blks, 24, 128), F32),
        packs=((31, 24, 128), F32),
    )
    ids = {name: scratch(*spec) for name, spec in shapes.items()}
    counts = dict(
        up_sem=6,
        down_sem=6,
        ksem=3,
        qsem=3,
        down_pair=1,
        up_spread=28,
        qkv_spread=21,
        out_pair=1,
        pair_sem=chunks,
        pack_sem=31,
    )
    sem_ids = {k: many([sems(v)])[0] for k, v in counts.items()}
    for k, v in dict(go_send=4, go_recv=4, out_send=2, out_recv=4).items():
        sem_ids[k] = many([pltpu.SemaphoreType.DMA((v,))])[0]
    stream_ids = [
        ([many(scatter_scratch(2 * r, d)) for _ in range(3)], [many([sems(14)])[0] for _ in range(3)])
    ]
    chunk_ids = [
        (many(scatter_scratch(2 * r, w)), many([sems(6), sems(4), sems(8)])) for _ in range(chunks)
    ]
    down_line = many(line_sum_scratch((fcols, d)))
    up_line = many(line_sum_scratch((4 * e, f)))
    qkv_line = many(line_sum_scratch((4 * e, width_qkv)))

    def run(ins, outs, own):
        src = SimpleNamespace(**dict(zip(names, ins)))
        out_ref, grad_ref, pos_ref, got_down, got_up, got_qkv, got_out, totals = outs
        m = SimpleNamespace(**{k: own[v] for k, v in ids.items()})
        sem = SimpleNamespace(**{k: own[v] for k, v in sem_ids.items()})
        pick_refs = lambda some: [own[i] for i in some]
        h, o, y, c = place()
        g = y * 2 + c
        t = h * 4 + g
        tail = []

        up_more = src.up_cut.at[:, :, pl.ds(fh, fh)]
        down_rows = pl.ds(pl.multiple_of(h * fcols, fcols), fcols)
        down_more = src.down_weight.at[down_rows]
        up_line_in = line_gather_steps(up_more, lambda z: m.up_two.at[z], sem.up_sem)
        down_line_in = line_gather_steps(down_more, lambda z: m.down_all.at[z], sem.down_sem)
        next(up_line_in)
        next(down_line_in)
        for ref in (m.sums, m.up_sums, m.up_spots, m.dq):
            ref[...] = jnp.zeros_like(ref)
        yield

        ups = [lambda k=k: src.up_one[...].reshape(d, fh) if k == 0 else m.up_two[...].reshape(d, fh) for k in range(2)]
        downs = [
            lambda k=k: m.down_all[:, :, k * half_d : (k + 1) * half_d].reshape(f, half_d)
            for k in range(2)
        ]
        vec = lambda k: src.vectors[k + 2 : k + 3]
        partial, low, total = m.partial, m.low, m.total

        both = range(seqs)

        def piece(ref):
            return lambda i, slot: ref.at[i, slot]

        def plain(ref):
            return lambda i: ref.at[i]

        def quarter(ref, s, q):
            return ref[s, 4 * q : 4 * q + 4].reshape(q_rows, d)

        def note(k, value):
            m.sums[k : k + 1] += jnp.sum(value, axis=0, keepdims=True)

        def step(*some):
            for gen in some:
                next(gen, None)

        def down_sums():
            yield from line_sum_steps(
                lambda z: m.down_part.at[z], got_down.at[h], *pick_refs(down_line)
            )
            copy = remote(got_down.at[h], got_down.at[h], sem.down_pair, 0, peer(*NEAR_X))
            copy.start()
            yield
            copy.wait_send()
            landed(got_down.at[1 - h], sem.down_pair, 0)

        def up_sums():
            yield from line_sum_steps(lambda z: m.up_part.at[z], m.up_total, *pick_refs(up_line))
            yield from spread_steps(
                lambda k: m.up_total.at[pl.ds(k * e, e)],
                got_up,
                lambda k: [(i * 4 + k % 4) * 2 + k // 4 for i in range(4)],
                sem.up_spread,
            )

        def qkv_sums():
            yield from line_sum_steps(
                lambda z: m.qkv_part.at[z], m.qkv_total, *pick_refs(qkv_line)
            )
            yield from spread_steps(
                lambda k: m.qkv_total.at[pl.ds(k * e, e)],
                got_qkv,
                lambda k: [i * 8 + k for i in range(3)],
                sem.qkv_spread,
            )

        def out_sums():
            has = o // 2 == h
            held, acc, send, recv = m.out_held, m.out_acc, sem.out_send, sem.out_recv

            def each(act):
                for j in range(2):
                    device = (h, blk(2 * h + y, c, j))
                    copy = place_copy(m.out_part.at[j], held.at[o], send.at[j], recv.at[o], device)

                    @pl.when(jnp.logical_not((o == 2 * h + y) & (y == c) & (c == j)))
                    def _():
                        act(copy)

            each(lambda copy: copy.start())
            yield
            acc[...] = jnp.zeros_like(acc)
            for z in range(4):
                mine = (z == o) & (o % 2 == y) & (y == c)

                @pl.when(has & mine)
                def _():
                    acc[...] += m.out_part[c].astype(F32)

                @pl.when(has & jnp.logical_not(mine))
                def _():
                    ref = held.at[z]
                    place_copy(ref, ref, send.at[0], recv.at[z], (h, blk(o, y, c))).wait_recv()
                    acc[...] += held[z].astype(F32)

            pair = remote(got_out, got_out, sem.out_pair, 0, peer(*NEAR_X))

            @pl.when(has)
            def _():
                got_out[...] = acc[...].astype(BF16)
                pair.start()

            yield
            each(lambda copy: copy.wait_send())

            @pl.when(has)
            def _():
                pair.wait_send()

            @pl.when(jnp.logical_not(has))
            def _():
                landed(got_out, sem.out_pair, 0)

        def go_copy(s, j):
            z = 2 * s + j
            return place_copy(
                m.go.at[j, :, pl.ds(s * n, n)],
                m.gs.at[:, pl.ds(pl.multiple_of(o * n, n), n)],
                sem.go_send.at[z],
                sem.go_recv.at[o],
                (h, z * 4 + g),
            )

        def stream():
            scatters = [pick_refs(i) for i in stream_ids[0][0]]
            gathers = pick_refs(stream_ids[0][1])
            at = lambda s, q: pl.ds(s * rows + q * q_rows, q_rows)
            for s in both:
                branch = dot_tn(
                    src.attended[:, :, s * n : (s + 1) * n].reshape(2 * he, n), src.out_own[...]
                )
                partial[s] = branch.astype(BF16).reshape(8, r, d)
            for k, _ in enumerate(scatter_steps(piece(partial), plain(total), *scatters[0])):
                if k > 0:
                    step(up_line_in)
                yield
            for s in both:
                xh, scale_r = norm_parts(src.embedded[s] + (total[s] + vec(0)))
                m.xh_one[s] = xh
                m.scale_one[s] = scale_r
                value = xh * vec(4) + vec(1)
                m.first[s] = value
                low[s] = value.astype(BF16)
            step(up_line_in, down_line_in)
            for k, _ in enumerate(gather_steps(plain(low), piece(m.first_g), gathers[0])):
                if k in (1, 3):
                    step(down_line_in)
                yield
            for _ in up_line_in:
                pass
            for s in both:
                for q in range(2):
                    rows_in = quarter(m.first_g, s, q)
                    for k in range(2):
                        cols = slice(k * fh, (k + 1) * fh)
                        inner = jnp.dot(rows_in, ups[k](), preferred_element_type=F32)
                        inner = inner + src.up_bias[:, cols]
                        phi = 0.5 + 0.5 * lax.erf(inner * (0.5**0.5))
                        m.act[at(s, q), cols] = (inner * phi).astype(BF16)
                        bell = jnp.exp(inner * inner * -0.5) * (1.0 / math.sqrt(2.0 * math.pi))
                        m.slope[at(s, q), cols] = phi + inner * bell
            for _ in down_line_in:
                pass
            for s in both:
                for k in range(2):
                    part = jnp.dot(
                        m.act[s * rows : (s + 1) * rows], downs[k](), preferred_element_type=F32
                    )
                    partial[s, :, :, k * half_d : (k + 1) * half_d] = part.astype(BF16).reshape(
                        8, r, half_d
                    )
            yield from scatter_steps(piece(partial), plain(total), *scatters[1])
            for s in both:
                xh, scale_r = norm_parts(m.first[s] + (total[s] + vec(2)))
                out_ref[s] = (xh * vec(5) + vec(3)).astype(BF16)
                cot = src.cotangent[s].astype(F32)
                note(5, cot * xh)
                note(3, cot)
                grad = norm_back(xh, scale_r, cot * vec(5))
                m.grad_two[s] = grad
                low[s] = grad.astype(BF16)
                note(2, low[s].astype(F32))
            yield from gather_steps(plain(low), piece(m.grad_g), gathers[1])
            for s in both:
                for q in range(2):
                    rows_in = quarter(m.grad_g, s, q)
                    back = dot_nt(rows_in[:, :half_d], downs[0]()) + dot_nt(
                        rows_in[:, half_d:], downs[1]()
                    )
                    back = (back * m.slope[at(s, q)]).astype(BF16)
                    m.inner_grad[at(s, q)] = back
                    m.up_sums[...] += jnp.sum(back.astype(F32), axis=0, keepdims=True)
                    part = dot_nt(back[:, :fh], ups[0]()) + dot_nt(back[:, fh:], ups[1]())
                    partial[s, 4 * q : 4 * q + 4] = part.astype(BF16).reshape(4, r, d)
            last = scatter_steps(piece(partial), plain(total), *scatters[2])
            next(last)

            @pl.loop(0, planes)
            def _(z):
                cols = pl.ds(pl.multiple_of(z * fcols, fcols), fcols)
                all_grads = m.grad_g[...].reshape(seqs * rows, d)
                m.down_part[z] = dot_tn(m.act[:, cols], all_grads).astype(BF16)

            step(down)
            next(last)

            @pl.loop(0, planes)
            def _(z):
                cols = pl.ds(pl.multiple_of(z * 4 * e, 4 * e), 4 * e)
                all_first = m.first_g[:, :, :, cols].reshape(seqs * rows, 4 * e)
                m.up_part[z] = dot_tn(all_first, m.inner_grad[...]).astype(BF16)

            yield from last
            for s in both:
                grad = m.grad_two[s] + total[s]
                note(4, grad * m.xh_one[s])
                note(1, grad)
                grad = norm_back(m.xh_one[s], m.scale_one[s], grad * vec(4))
                m.resid[s] = grad
                low[s] = grad.astype(BF16)
                note(0, low[s].astype(F32))
            for k, _ in enumerate(gather_steps(plain(low), piece(m.branch_g), gathers[2])):
                yield
                if k in EARLY:
                    step(down)
            for s in both:
                go = dot_nt(src.out_own[...], m.branch_g[s].reshape(rows, d))
                m.go[:, :, s * n : (s + 1) * n] = go.astype(BF16).reshape(2, he, n)
                for j in range(2):

                    @pl.when(o != 2 * s + j)
                    def _():
                        go_copy(s, j).start()

                    @pl.when(o == 2 * s + j)
                    def _():
                        m.gs[:, pl.ds(pl.multiple_of(o * n, n), n)] = m.go[
                            j, :, s * n : (s + 1) * n
                        ]

        down, up, out, qkv = down_sums(), up_sums(), out_sums(), qkv_sums()
        for _ in stream():
            pass
        step(up)
        grad_out = jnp.dot(
            src.attended[...].reshape(2 * he, 2 * n),
            m.branch_g[...].reshape(seqs * rows, d),
            preferred_element_type=F32,
        )
        m.out_part[...] = grad_out.astype(BF16).reshape(2, he, d)
        held = src.held
        gs, qs, q_t, g_t, dq, delta, pair_low = (
            m.gs, m.qs, m.q_rows, m.g_rows, m.dq, m.delta, m.pair_low
        )
        q32 = held[0].astype(F32) * scale
        qs[...] = q32.astype(BF16)
        q_t[...] = q32.T.astype(BF16)

        @pl.loop(0, slots // 64)
        def _(k):
            row = lax.broadcasted_iota(jnp.int32, (64, 1), 0) + k * 64
            some = pl.ds(pl.multiple_of(k * 64, 64), 64)
            m.pick[some] = (src.ids[...] == row).astype(F32).astype(BF16)

        for z in range(4):

            @pl.when(z != o)
            def _():
                ref = gs.at[:, pl.ds(z * n, n)]
                place_copy(
                    ref, ref, sem.go_send.at[0], sem.go_recv.at[z], peer(*NEAR_X)
                ).wait_recv()

        g32 = gs[...].astype(F32)
        g_t[...] = g32.T.astype(BF16)
        delta[...] = jnp.sum(g32 * src.pair_out[...], axis=0, keepdims=True)
        mine = pl.ds(pl.multiple_of((o // 2) * n, n), n)
        dqkv = m.dqkv

        def back(part, which, i, z):
            return remote(
                pair_low.at[part, :, pl.ds(pl.multiple_of(z * n, n), n)],
                dqkv.at[part, o % 2, :, mine],
                which,
                i,
                (h, z * 4 + g),
            )

        late = pl.ds(1, 2)
        for i in range(4):
            z = (o + 1 + i) % 4

            @pl.loop(0, n // key_rows)
            def _(step):
                at = pl.ds(pl.multiple_of(z * n + step * key_rows, key_rows), key_rows)
                k_cols = held[1, :, at]
                k_rows = k_cols.astype(F32).T.astype(BF16)
                v_rows = held[2, :, at].astype(F32).T.astype(BF16)
                s = jnp.dot(k_rows, qs[...], preferred_element_type=F32)
                p = jnp.exp(s - src.lse[...])
                dv = jnp.dot(p.astype(BF16), g_t[...], preferred_element_type=F32)
                dp = jnp.dot(v_rows, gs[...], preferred_element_type=F32)
                ds = (p * (dp - delta[...])).astype(BF16)
                dk = jnp.dot(ds, q_t[...], preferred_element_type=F32)
                dq[...] += jnp.dot(k_cols, ds, preferred_element_type=F32)
                pair_low[1, :, at] = dk.T.astype(BF16)
                pair_low[2, :, at] = dv.T.astype(BF16)

            if i < 3:
                back(late, sem.ksem, i, z).start()
            if i == 0:
                step(*[down] * (3 - len(EARLY)))
            if i == 2:
                step(up)
        pair_low[0] = (dq[...] * scale).astype(BF16)
        for i in range(3):
            back(pl.ds(0, 1), sem.qsem, i, (o + 1 + i) % 4).start()
        dqkv[:, o % 2, :, mine] = pair_low[:, :, pl.ds(pl.multiple_of(o * n, n), n)]
        step(down, up)
        for i in range(3):
            z = (o + 3 - i) % 4
            there = pl.ds(pl.multiple_of((z // 2) * n, n), n)
            landed(dqkv.at[late, z % 2, :, there], sem.ksem, i)
            landed(dqkv.at[pl.ds(0, 1), z % 2, :, there], sem.qsem, i)

        all_dqkv = lambda: dqkv[...].reshape(width_qkv, 2 * n)

        def back_chunk(q):
            part = lax.dot_general(
                all_dqkv(),
                src.qkv_own[q * w : (q + 1) * w],
                (((0,), (1,)), ((), ())),
                preferred_element_type=F32,
            )
            partial[:, :, :, q * w : (q + 1) * w] = part.astype(BF16).reshape(seqs, 8, r, w)

        def chunk(q):
            cols = pl.ds(q * w, w)
            scatter, (zsem, ysem, csem) = pick_refs(chunk_ids[q][0]), pick_refs(chunk_ids[q][1])
            back_chunk(q)
            yield from scatter_steps(
                lambda i, slot: partial.at[i, slot, :, cols],
                lambda i: grad_ref.at[i, :, cols],
                *scatter,
            )
            grad = grad_ref[:, :, cols] + m.resid[:, :, cols]
            grad_ref[:, :, cols] = grad
            grad = grad.reshape(own_rows, w)
            m.own[q] = grad.astype(BF16)
            second = src.second[...]
            m.sums[6:7, cols] = jnp.sum(grad * (1.0 - second), axis=0, keepdims=True)
            m.sums[7:8, cols] = jnp.sum(grad * second, axis=0, keepdims=True)
            yield from blk_gather_steps(
                m.own.at[q],
                lambda z, yy, cc: m.gathered.at[q, blk(z, yy, cc)],
                zsem,
                ysem,
                csem,
            )

            @pl.loop(0, slots // 128)
            def _(k):
                some = pl.ds(pl.multiple_of(k * 128, 128), 128)
                found = jnp.dot(
                    m.pick[some],
                    m.gathered[q].reshape(blks * own_rows, w),
                    preferred_element_type=F32,
                )
                pos_ref[some, cols] = found
                m.pos_low[q, some] = found.astype(BF16)

            copy = remote(
                m.pos_low.at[q], m.pos_held.at[q], sem.pair_sem, q, peer(*NEAR_X)
            )
            copy.start()
            pairs.append(copy)
            yield

        pairs = []
        active, waiting = [], [chunk(q) for q in range(chunks)]
        turn = 0
        while active or waiting:
            if waiting and turn % chunk_lag == 0:
                active.append(waiting.pop(0))
            for gen in list(active):
                try:
                    next(gen)
                except StopIteration:
                    active.remove(gen)
            if turn == 0:
                @pl.loop(0, planes)
                def _(z):
                    cols = pl.ds(pl.multiple_of(z * 4 * e, 4 * e), 4 * e)
                    part = lax.dot_general(
                        src.plane_low[:, :, :, cols].reshape(seqs * rows, 4 * e),
                        all_dqkv(),
                        (((0,), (1,)), ((), ())),
                        preferred_element_type=F32,
                    )
                    m.qkv_part[z] = part.astype(BF16)

                step(qkv)
                ones = jnp.ones((8, 2 * n), BF16)
                heads = dot_nt(ones, all_dqkv())
                own_lanes = pl.ds(pl.multiple_of(t * 128, 128), 128)
                m.sums[8:9, own_lanes] = heads[0:1, 0:128]
                m.sums[9:10, own_lanes] = heads[0:1, 256:384]
                for i in range(4):
                    m.up_spots[pl.ds((i * 4 + g) * 2 + h, 1)] = m.up_sums[
                        :, i * 128 : (i + 1) * 128
                    ]
            for when, gen in zip(TURNS, (up, qkv, out)):
                if turn in when:
                    step(gen)
            turn += 1
        for b in range(blks):
            m.pack[b, 0:16] = m.sums[:, b // 2 * 128 : (b // 2 + 1) * 128]
            m.pack[b, 16:18] = m.up_spots[2 * b : 2 * b + 2]
            m.pack[b, 18:24] = jnp.zeros((6, 128), F32)
        copies = []
        for k, p in enumerate(ALL):
            to = peer(*p)
            copy = remote(m.pack.at[to[1]], m.packs.at[k], sem.pack_sem, k, to)
            copy.start()
            copies.append(copy)
        for gen in (down, up, out, qkv):
            for _ in gen:
                pass
        for q, copy in enumerate(pairs):
            copy.wait()
            cols = pl.ds(q * w, w)
            pos_ref[:, cols] = pos_ref[:, cols] + m.pos_held[q].astype(F32)
        for copy in copies:
            copy.wait()
        totals[...] = m.pack[blk(o, y, c)] + jnp.sum(m.packs[...], axis=0)
        for i in range(3):
            back(late, sem.ksem, i, (o + 1 + i) % 4).wait_send()
            back(pl.ds(0, 1), sem.qsem, i, (o + 1 + i) % 4).wait_send()
        for s in range(seqs):
            for j in range(2):

                @pl.when(o != 2 * s + j)
                def _():
                    go_copy(s, j).wait_send()

    return Part(
        run,
        list(vars(x).values()),
        [
            ((seqs, r, d), BF16),
            ((seqs, r, d), F32),
            ((slots, d), F32),
            ((2, fcols, d), BF16),
            ((e, 8 * f), BF16),
            ((e, 3 * d), BF16),
            ((he, d), BF16),
            ((24, 128), F32),
        ],
        need,
        ALL,
    )


def rows_steps(own_of, near, part, from_y, term, ends, mids, last, csem, ysem, zsem, out):
    h, o, y, c = place()
    at, seen = mirrored()
    dev_y = peer(*NEAR_Y)
    order = [seen(3), seen(2), seen(1 - at), o]
    end, inner, other = (h, blk(seen(0), y, c)), (h, blk(seen(1), y, c)), (h, blk(seen(2), y, c))
    sent = []
    for j, z in enumerate(order):
        landed(near.at[0, j], csem, j)
        part[j] = own_of(z, 1 - y)[...] + near[0, j]
        copy = remote(part.at[j], from_y.at[j], ysem, j, dev_y)
        copy.start()
        sent.append(copy)
    for j, z in enumerate(order):
        yield
        landed(near.at[1, j], csem, 4 + j)
        landed(from_y.at[j], ysem, j)
        term[j] = own_of(z, y)[...] + near[1, j] + from_y[j]
        if j < 3:

            @pl.when(at == 0)
            def _():
                remote(term.at[j], ends.at[j], zsem, j, inner).start()

        if j < 2:

            @pl.when(at == 1)
            def _():
                landed(ends.at[j], zsem, j)
                term[j] += ends[j]
                remote(term.at[j], mids.at[j], zsem, 3 + j, other).start()

    yield

    @pl.when(at == 1)
    def _():
        landed(mids.at[0], zsem, 3)
        term[2] += mids[0]
        remote(term.at[2], last, zsem, 5, end).start()

    yield

    @pl.when(at == 1)
    def _():
        landed(ends.at[2], zsem, 2)
        landed(mids.at[1], zsem, 4)
        out[...] = (term[3] + ends[2] + mids[1]).astype(F32)
        for j in range(2):
            remote(term.at[j], mids.at[j], zsem, 3 + j, other).wait_send()
        remote(term.at[2], last, zsem, 5, end).wait_send()

    @pl.when(at == 0)
    def _():
        landed(last, zsem, 5)
        out[...] = (term[3] + last[...]).astype(F32)
        for j in range(3):
            remote(term.at[j], ends.at[j], zsem, j, inner).wait_send()

    for copy in sent:
        copy.wait_send()


def first_half(x, scale, lag):
    names = list(vars(x))
    seqs, r, d = x.hidden.shape
    slots = x.table.shape[0]
    e = x.qkv_weight.shape[0]
    four, wq, f = 4, x.qkv_weight.shape[1] // 8, x.up_weight.shape[1] // 8
    he = wq // 6
    n = 8 * r
    length = 4 * n
    half, fh = r // 2, f // 2
    blks = 16
    cols = 256
    small = small_gather(jax.ShapeDtypeStruct((8, 128), F32))
    outw = out_weights(x.out_weight)
    need = []

    def many(specs):
        start = len(need)
        need.extend(specs)
        return list(range(start, len(need)))

    block = (r, d)
    shapes = dict(
        packed=((8, 128), F32),
        everyone=((blks, 8, 128), F32),
        found=((4, 2, 2, seqs, r, d), BF16),
        rows=((seqs, r, d), F32),
        low=((seqs, r, d), BF16),
        qkv_in=((four, e, wq), BF16),
        projected=((3, 2, he, 2 * n), BF16),
        keys=((length, he), BF16),
        pair_low=((he, length), BF16),
    )
    ids = {k: many([pltpu.VMEM(*v)])[0] for k, v in shapes.items()}
    counts = dict(qkv_sem=3, up_sem=3, back_sem=3, qkv_trade=9, up_trade=12)
    sem_ids = {k: many([sems(v)])[0] for k, v in counts.items()}
    for k in ("send", "recv"):
        sem_ids[k] = many([pltpu.SemaphoreType.DMA((4,))])[0]
    small_ids, outw_ids = many(small.scratch), many(outw.scratch)
    row_ids = [
        many(
            [
                pltpu.VMEM((2, 4) + block, BF16),
                pltpu.VMEM((4,) + block, BF16),
                pltpu.VMEM((4,) + block, BF16),
                pltpu.VMEM((4,) + block, BF16),
                pltpu.VMEM((3,) + block, BF16),
                pltpu.VMEM((2,) + block, BF16),
                pltpu.VMEM(block, BF16),
                sems(8),
                sems(4),
                sems(6),
            ]
        )
        for _ in range(seqs)
    ]
    gather_ids = [many([sems(14)])[0] for _ in range(seqs)]

    def run(ins, outs, own):
        src = SimpleNamespace(**dict(zip(names, ins)))
        attended, held, o_ref, lse_ref, emb_ref, plane_ref, qkv_ref = outs[:7]
        outw_ref, up_one, up_in, vec_ref, bias_ref, ids_ref, second_ref = outs[7:]
        m = SimpleNamespace(**{k: own[v] for k, v in ids.items()})
        sem = SimpleNamespace(**{k: own[v] for k, v in sem_ids.items()})
        pick_refs = lambda some: [own[i] for i in some]
        h, o, y, c = place()
        g = y * 2 + c
        t = h * 4 + g
        side = lambda a: jnp.concatenate([a[0:1], a[1:2]], axis=1).astype(F32)
        for k in range(3):
            m.packed[k : k + 1] = side(src.biases[2 * k : 2 * k + 2])
        m.packed[3:4] = side(src.gains[...])
        m.packed[4:5] = side(src.types[...])
        m.packed[5:7] = src.up_bias[...].astype(F32)
        m.packed[7:8] = side(src.pos_ids[...])
        gather_small = small.run((m.packed,), (m.everyone,), pick_refs(small_ids))
        trades = []

        def trade(ref, dst, s, lanes_of):
            count = len(lanes_of(0))
            for k, p in enumerate(((0, 0, 1, 0), (0, 0, 0, 1), (0, 0, 1, 1))):
                to = (1 - y if p[2] else y) * 2 + (1 - c if p[3] else c)
                for i, lane in enumerate(lanes_of(to)):
                    copy = remote(
                        ref.at[:, pl.ds(pl.multiple_of(lane * 128, 128), 128)],
                        dst.at[g, :, pl.ds(i * 128, 128)],
                        s,
                        k * count + i,
                        peer(*p),
                    )
                    copy.start()
                    trades.append(copy)
            for i, lane in enumerate(lanes_of(g)):
                dst[g, :, i * 128 : (i + 1) * 128] = ref[
                    :, pl.ds(pl.multiple_of(lane * 128, 128), 128)
                ]

        weights = outw.run((src.out_weight,), (outw_ref,), pick_refs(outw_ids))
        qkv_lanes = lambda k: [i * 8 + h * 4 + k for i in range(3)]
        up_lanes = lambda k: [(i * 4 + k) * 2 + h for i in range(4)]
        trade(src.qkv_weight, m.qkv_in, sem.qkv_trade, qkv_lanes)
        next(gather_small)
        yield
        next(weights)
        trade(src.up_weight, up_in, sem.up_trade, up_lanes)
        bulk = []

        def line(ref, dst, s):
            for k, p in enumerate(COLUMN):
                copy = remote(ref, dst.at[o], s, k, peer(*p))
                copy.start()
                bulk.append(copy)
            dst[pl.ds(o, 1)] = ref[...][None]

        for _ in gather_small:
            pass

        at, seen = mirrored()
        order = [seen(3), seen(2), seen(1 - at), o]
        b = blk(o, y, c)
        row = lax.broadcasted_iota(jnp.int32, (slots, 1), 0).astype(F32)
        base = (b * slots).astype(F32)
        streams = [pick_refs(i) for i in row_ids]
        core = []
        for i, yy in enumerate((1 - y, y)):
            for j, z in enumerate(order):
                hot = jnp.concatenate(
                    [
                        (m.everyone[blk(z, yy, cc), 7:8] - base == row).astype(F32).astype(BF16)
                        for cc in range(2)
                    ],
                    axis=1,
                )
                rows_of = dot_tn(hot, src.table[...]).astype(BF16)
                m.found[z, yy] = rows_of.reshape(2, seqs, r, d)
                for s in range(seqs):
                    near, csem = streams[s][0], streams[s][7]
                    copy = remote(
                        m.found.at[z, yy, 1 - c, s],
                        near.at[i, j],
                        csem,
                        i * 4 + j,
                        peer(*NEAR_C),
                    )
                    copy.start()
                    core.append(copy)
            if i == 0:
                for copy in trades:
                    copy.wait()
                line(m.qkv_in, qkv_ref, sem.qkv_sem)

        lane = lax.broadcasted_iota(jnp.int32, (1, 128), 1)
        for k in range(5):
            for i in range(blks // 2):
                one, two = m.everyone[2 * i, k : k + 1], m.everyone[2 * i + 1, k : k + 1]
                lanes = slice(i * 128, (i + 1) * 128)
                vec_ref[2 * k : 2 * k + 1, lanes] = jnp.where(
                    lane < 64, one, pltpu.roll(two, 64, 1)
                )
                vec_ref[2 * k + 1 : 2 * k + 2, lanes] = jnp.where(
                    lane < 64, pltpu.roll(one, 64, 1), two
                )
        for i in range(blks):
            ids_ref[:, i * 128 : (i + 1) * 128] = (m.everyone[i, 7:8] - base).astype(jnp.int32)
        for i in range(4):
            bias_ref[:, i * 128 : (i + 1) * 128] = m.everyone[i * 4 + g, pl.ds(5 + h, 1)]
        eye = lax.broadcasted_iota(jnp.int32, (128, 128), 0) == lax.broadcasted_iota(
            jnp.int32, (128, 128), 1
        )

        def upright(lanes):
            return jnp.sum(jnp.where(eye, lanes, 0.0), axis=1, keepdims=True)

        def column(k):
            return upright(vec_ref[k : k + 1, pl.ds(pl.multiple_of(t * 128, 128), 128)])

        second_ref[...] = upright(side(src.type_ids[...]))

        def send_pair(s, j):
            z = 2 * s + j
            return place_copy(
                m.projected.at[:, j, :, pl.ds(s * n, n)],
                held.at[:, :, pl.ds(pl.multiple_of(o * n, n), n)],
                sem.send.at[z],
                sem.recv.at[o],
                (h, z * 4 + g),
            )

        def stream(s):
            yield from rows_steps(
                lambda z, yy: m.found.at[z, yy, c, s], *streams[s], m.rows.at[s]
            )
            if s == seqs - 1:
                line(up_in.at[:, :, pl.ds(0, fh)], up_one, sem.up_sem)
            second = second_ref[s * r : (s + 1) * r]
            typed = vec_ref[8:9] * (1.0 - second) + vec_ref[9:10] * second
            value = src.hidden[s].astype(F32) + m.rows[s] + typed
            emb_ref[s] = value
            m.low[s] = value.astype(BF16)
            yield from gather_steps(
                lambda i: m.low.at[s, pl.ds(i * half, half)],
                lambda i, slot: plane_ref.at[s, slot, pl.ds(i * half, half)],
                own[gather_ids[s]],
            )
            if s == 0:
                for copy in bulk[:3]:
                    copy.wait()
                del bulk[:3]
            part = lax.dot_general(
                qkv_ref[...].reshape(d, wq),
                plane_ref[s].reshape(n, d),
                (((0,), (1,)), ((), ())),
                preferred_element_type=F32,
            )
            here = slice(s * n, (s + 1) * n)
            third = wq // 3
            m.projected[0, :, :, here] = (part[:third] + column(0)).astype(BF16).reshape(2, he, n)
            m.projected[1, :, :, here] = part[third : 2 * third].astype(BF16).reshape(2, he, n)
            m.projected[2, :, :, here] = (
                (part[2 * third :] + column(1)).astype(BF16).reshape(2, he, n)
            )
            for j in range(2):

                @pl.when(o != 2 * s + j)
                def _():
                    send_pair(s, j).start()

                @pl.when(o == 2 * s + j)
                def _():
                    held[:, :, pl.ds(pl.multiple_of(o * n, n), n)] = m.projected[:, j, :, here]

            yield

        gens = [stream(s) for s in range(seqs)]
        for _ in range(lag):
            next(gens[0])
        while gens:
            for gen in list(gens):
                try:
                    next(gen)
                except StopIteration:
                    gens.remove(gen)
        for z in range(4):

            @pl.when(z != o)
            def _():
                ref = held.at[:, :, pl.ds(z * n, n)]
                place_copy(ref, ref, sem.send.at[0], sem.recv.at[z], peer(*NEAR_X)).wait_recv()

        m.keys[...] = held[1].astype(F32).T.astype(BF16)
        mine = pl.ds(pl.multiple_of((o // 2) * n, n), n)

        def back(i, z):
            return remote(
                m.pair_low.at[:, pl.ds(pl.multiple_of(z * n, n), n)],
                attended.at[o % 2, :, mine],
                sem.back_sem,
                i,
                (h, z * 4 + g),
            )

        @pl.loop(0, 4 * (n // cols))
        def _(step):
            i = step // (n // cols)
            z = (o + 1 + i) % 4
            here = pl.ds(pl.multiple_of(z * n + step % (n // cols) * cols, cols), cols)
            q = (held[0, :, here].astype(F32) * scale).astype(BF16)
            s = jnp.dot(m.keys[...], q, preferred_element_type=F32)
            peak = jnp.max(s, axis=0, keepdims=True)
            p = jnp.exp(s - peak)
            total = jnp.sum(p, axis=0, keepdims=True)
            out = jnp.dot(held[2], p.astype(BF16), preferred_element_type=F32) / total
            o_ref[:, here] = out
            m.pair_low[:, here] = out.astype(BF16)
            lse_ref[:, here] = peak + jnp.log(total)

            @pl.when((step % (n // cols) == n // cols - 1) & (i < 3))
            def _():
                back(i, z).start()

        attended[o % 2, :, mine] = m.pair_low[:, pl.ds(pl.multiple_of(o * n, n), n)]
        for i in range(3):
            back(i, (o + 1 + i) % 4).wait_send()
            z = (o + 3 - i) % 4
            landed(attended.at[z % 2, :, pl.ds(pl.multiple_of((z // 2) * n, n), n)], sem.back_sem, i)
        for _ in weights:
            pass
        for copy in bulk:
            copy.wait()
        for copy in core:
            copy.wait_send()
        for s in range(seqs):
            for j in range(2):

                @pl.when(o != 2 * s + j)
                def _():
                    send_pair(s, j).wait_send()

    return Part(
        run,
        list(vars(x).values()),
        [
            ((2, he, 2 * n), BF16),
            ((3, he, length), BF16),
            ((he, length), F32),
            ((1, length), F32),
            ((seqs, r, d), F32),
            ((seqs, 8, r, d), BF16),
            ((4, four, e, wq), BF16),
            ((2,) + x.out_weight.shape, BF16),
            ((4, four, e, fh), BF16),
            ((four, e, f), BF16),
            ((10, d), F32),
            ((1, f), F32),
            ((1, blks * seqs * r), jnp.int32),
            ((seqs * r, 1), F32),
        ],
        need,
        ALL,
    )


def finish_kernel(odd, layer, hid, pos, down, up, qkv, out, totals, *outs):
    o_layer, o_hid, o_pos, o_types, o_qkv, o_out, o_up, o_down, o_upb, o_gains, o_bias = outs
    o_layer[...] = layer[...]
    o_hid[...] = hid[...]
    o_pos[...] = pos[...]
    o_qkv[...] = qkv[...].astype(F32)
    o_out[...] = out[...].astype(F32)
    o_up[...] = up[...].astype(F32)
    o_down[...] = down[...].astype(F32)
    t = totals[...]
    mine = jnp.where(odd[0] == 1, t[:, 64:], t[:, :64])
    o_types[...] = mine[6:8]
    o_gains[...] = mine[4:6]
    o_bias[0:1] = mine[8:9]
    o_bias[1:2] = mine[9:10]
    o_bias[2:6] = mine[0:4]
    o_upb[...] = t[16:18]


def finish(odd, layer, hid, pos, down, up, qkv, out, totals, steps=4):
    e = out.shape[0]
    large = [(layer, BF16), (hid, F32), (pos, F32), (qkv, F32), (out, F32), (up, F32), (down, F32)]

    def cut(a):
        return pl.BlockSpec((a.shape[0] // steps, a.shape[1]), lambda i: (i, 0))

    def whole(*shape):
        return pl.BlockSpec(shape, lambda i: (0, 0))

    like = {id(a): jax.ShapeDtypeStruct(a.shape, dtype) for a, dtype in large}
    full = lambda *shape: jax.ShapeDtypeStruct(shape, F32)
    return pl.pallas_call(
        finish_kernel,
        name="finish",
        grid=(steps,),
        out_shape=[like[id(a)] for a in (layer, hid, pos)]
        + [full(2, e)]
        + [like[id(a)] for a in (qkv, out, up, down)]
        + [full(2, 128), full(2, e), full(6, e)],
        in_specs=[pl.BlockSpec(memory_space=pltpu.SMEM)]
        + [cut(a) for a in (layer, hid, pos, down, up, qkv, out)]
        + [whole(24, 128)],
        out_specs=[cut(a) for a in (layer, hid, pos)]
        + [whole(2, e)]
        + [cut(a) for a in (qkv, out, up, down)]
        + [whole(2, 128), whole(2, e), whole(6, e)],
    )(odd, layer, hid, pos, down, up, qkv, out, totals)


def norm_layer(values_in, gain_row, offset_row):
    average = jnp.mean(values_in, axis=-1, keepdims=True)
    centred = values_in - average
    variance = jnp.mean(centred * centred, axis=-1, keepdims=True)
    return centred * lax.rsqrt(variance + 1e-12) * gain_row + offset_row


def gelu_exact(inner_product_sum):
    return jax.nn.gelu(inner_product_sum, approximate=False)


def widest_block(length, limit):
    return max(
        (candidate for candidate in range(1, min(length, limit) + 1) if length % candidate == 0)
    )


def block_scores(query_heads, key_block, score_scale):
    return (
        jnp.einsum("sqhe,skhe->shqk", query_heads, key_block, preferred_element_type=jnp.float32)
        * score_scale
    )


def key_side(query_block, grad_block, lse_block, delta_block, key_heads, value_heads, score_scale):
    scores = block_scores(query_block, key_heads, score_scale)
    weights = jnp.exp(scores - lse_block[..., None])
    more_values = jnp.einsum(
        "shqk,sqhe->shke",
        weights.astype(jnp.bfloat16),
        grad_block,
        preferred_element_type=jnp.float32,
    )
    grad_weights = jnp.einsum(
        "sqhe,skhe->shqk", grad_block, value_heads, preferred_element_type=jnp.float32
    )
    grad_scores = weights * (grad_weights - delta_block[..., None])
    more_keys = jnp.einsum(
        "shqk,sqhe->shke",
        grad_scores.astype(jnp.bfloat16),
        query_block,
        preferred_element_type=jnp.float32,
    )
    return (more_keys, more_values)


def forward_fold(query_heads, score_scale, head_count, head_size):

    def fold_keys(running, portion, offset):
        key_piece, value_piece = portion
        seq_count, length = (key_piece.shape[0], key_piece.shape[1])
        block_size = widest_block(length, 512)

        def one_step(block_index, carried):
            row_peak, row_total, weighted = carried
            row_start = block_index * block_size
            key_block = lax.dynamic_slice_in_dim(key_piece, row_start, block_size, 1).reshape(
                seq_count, block_size, head_count, head_size
            )
            value_block = lax.dynamic_slice_in_dim(value_piece, row_start, block_size, 1).reshape(
                seq_count, block_size, head_count, head_size
            )
            scores = block_scores(query_heads, key_block, score_scale)
            new_peak = jnp.maximum(row_peak, jnp.max(scores, axis=-1))
            shrink = jnp.exp(row_peak - new_peak)
            weights = jnp.exp(scores - new_peak[..., None])
            row_total = row_total * shrink + jnp.sum(weights, axis=-1)
            weighted = weighted * shrink[..., None] + jnp.einsum(
                "shqk,skhe->shqe",
                weights.astype(jnp.bfloat16),
                value_block,
                preferred_element_type=jnp.float32,
            )
            return (new_peak, row_total, weighted)

        return lax.fori_loop(0, length // block_size, one_step, running)

    return fold_keys


def query_fold(query_heads, grad_heads, log_totals, delta_rows, score_scale, head_count, head_size):

    def fold_keys(running, portion, offset):
        key_piece, value_piece = portion
        seq_count, length = (key_piece.shape[0], key_piece.shape[1])
        block_size = widest_block(length, 512)

        def one_step(block_index, weighted):
            row_start = block_index * block_size
            key_block = lax.dynamic_slice_in_dim(key_piece, row_start, block_size, 1).reshape(
                seq_count, block_size, head_count, head_size
            )
            value_block = lax.dynamic_slice_in_dim(value_piece, row_start, block_size, 1).reshape(
                seq_count, block_size, head_count, head_size
            )
            scores = block_scores(query_heads, key_block, score_scale)
            weights = jnp.exp(scores - log_totals[..., None])
            grad_weights = jnp.einsum(
                "sqhe,skhe->shqk", grad_heads, value_block, preferred_element_type=jnp.float32
            )
            grad_scores = weights * (grad_weights - delta_rows[..., None])
            return weighted + jnp.einsum(
                "shqk,skhe->shqe",
                grad_scores.astype(jnp.bfloat16),
                key_block,
                preferred_element_type=jnp.float32,
            )

        return lax.fori_loop(0, length // block_size, one_step, running)

    return fold_keys


def key_fold(key_heads, value_heads, score_scale, head_count, head_size):

    def fold_queries(running, portion, offset):
        query_piece, grad_piece, lse_piece, delta_piece = portion
        seq_count, length = (query_piece.shape[0], query_piece.shape[1])
        block_size = widest_block(length, 512)

        def one_step(block_index, carried):
            grad_keys, grad_values = carried
            row_start = block_index * block_size
            query_block = lax.dynamic_slice_in_dim(query_piece, row_start, block_size, 1).reshape(
                seq_count, block_size, head_count, head_size
            )
            grad_block = lax.dynamic_slice_in_dim(grad_piece, row_start, block_size, 1).reshape(
                seq_count, block_size, head_count, head_size
            )
            lse_block = lax.dynamic_slice_in_dim(lse_piece, row_start, block_size, 1).transpose(
                0, 2, 1
            )
            delta_block = lax.dynamic_slice_in_dim(delta_piece, row_start, block_size, 1).transpose(
                0, 2, 1
            )
            more_keys, more_values = key_side(
                query_block, grad_block, lse_block, delta_block, key_heads, value_heads, score_scale
            )
            return (grad_keys + more_keys, grad_values + more_values)

        return lax.fori_loop(0, length // block_size, one_step, running)

    return fold_queries


def layer_in_blocks(
    hidden,
    pos_ids,
    type_ids,
    cotangent,
    pos_table,
    type_table,
    query_key_value_weight,
    attention_output_weight,
    up_projection_weight,
    down_projection_weight,
    up_projection_bias,
    norm_gains,
    biases,
):
    seq_count, seg_tokens, model_width = hidden.shape
    row_count = seq_count * seg_tokens
    head_count = HEADS // lax.axis_size("head")
    head_size = model_width // HEADS
    local_width = head_count * head_size
    query_rows = lax.axis_size("head") * seg_tokens
    score_scale = 1.0 / math.sqrt(head_size)

    def fetch_weights():
        return (
            lax.all_gather(query_key_value_weight, "blk", axis=0, tiled=True),
            lax.all_gather(attention_output_weight, "blk", axis=0, tiled=True),
            lax.all_gather(up_projection_weight, "blk", axis=0, tiled=True),
            lax.all_gather(down_projection_weight, "blk", axis=0, tiled=True),
            lax.all_gather(up_projection_bias, "blk", axis=0, tiled=True),
            lax.all_gather(norm_gains, "blk", axis=1, tiled=True),
            lax.all_gather(biases, "blk", axis=1, tiled=True),
            lax.all_gather(type_table, "blk", axis=1, tiled=True),
        )

    qkv_full, out_full, up_full, down_full, up_bias_full, gain_full, bias_full, type_full = (
        fetch_weights()
    )
    bias_float = bias_full.astype(jnp.float32)
    gain_float = gain_full.astype(jnp.float32)
    flat_pos = pos_ids.reshape(row_count)
    portion = lax.all_gather(pos_table, "blk", axis=0, tiled=True)
    local_slots = flat_pos
    onehot = (
        local_slots[:, None] == jnp.arange(portion.shape[0], dtype=jnp.int32)[None, :]
    ).astype(jnp.bfloat16)
    positions = jnp.dot(onehot, portion, preferred_element_type=jnp.float32)
    is_second = type_ids.reshape(row_count, 1) == 1
    typed_rows = jnp.where(
        is_second, type_full[1].astype(jnp.float32), type_full[0].astype(jnp.float32)
    )
    embedded_tokens = (
        hidden.reshape(row_count, model_width).astype(jnp.float32) + positions + typed_rows
    )
    embedded_low = embedded_tokens.astype(jnp.bfloat16)
    projected_rows = jnp.dot(embedded_low, qkv_full, preferred_element_type=jnp.float32)
    token_shape = (seq_count, seg_tokens, model_width)
    queries = (
        (projected_rows[:, :model_width] + bias_float[0]).astype(jnp.bfloat16).reshape(token_shape)
    )
    keys_token = (
        projected_rows[:, model_width : 2 * model_width].astype(jnp.bfloat16).reshape(token_shape)
    )
    values_token = (
        (projected_rows[:, 2 * model_width :] + bias_float[1])
        .astype(jnp.bfloat16)
        .reshape(token_shape)
    )
    query_local, key_local, value_local = (
        lax.all_to_all(queries, "head", split_axis=2, concat_axis=1, tiled=True),
        lax.all_to_all(keys_token, "head", split_axis=2, concat_axis=1, tiled=True),
        lax.all_to_all(values_token, "head", split_axis=2, concat_axis=1, tiled=True),
    )
    head_shape = (seq_count, query_rows, head_count, head_size)
    query_heads = query_local.reshape(head_shape)
    key_heads = key_local.reshape(head_shape)
    value_heads = value_local.reshape(head_shape)
    start_peak = jnp.full((seq_count, head_count, query_rows), -jnp.inf, jnp.float32)
    start_total = jnp.zeros((seq_count, head_count, query_rows), jnp.float32)
    zero_heads = jnp.zeros((seq_count, head_count, query_rows, head_size), jnp.float32)
    fold_keys = forward_fold(query_heads, score_scale, head_count, head_size)
    row_peak, row_total, weighted = fold_keys(
        (start_peak, start_total, zero_heads),
        (
            lax.all_gather(key_local, "blk", axis=1, tiled=True),
            lax.all_gather(value_local, "blk", axis=1, tiled=True),
        ),
        jnp.int32(0),
    )
    log_totals = row_peak + jnp.log(row_total)
    attention_result = weighted / row_total[..., None]
    attended_low = (
        attention_result.transpose(0, 2, 1, 3)
        .reshape(seq_count, query_rows, local_width)
        .astype(jnp.bfloat16)
    )
    attended_token = lax.all_to_all(
        attended_low, "head", split_axis=1, concat_axis=2, tiled=True
    ).reshape(row_count, model_width)
    residual_branch = (
        jnp.dot(attended_token, out_full, preferred_element_type=jnp.float32) + bias_float[2]
    )
    first_layer_norm, first_pull = jax.vjp(
        norm_layer, embedded_tokens + residual_branch, gain_float[0], bias_float[3]
    )
    first_low = first_layer_norm.astype(jnp.bfloat16)
    inner_product_sum = jnp.dot(
        first_low, up_full, preferred_element_type=jnp.float32
    ) + up_bias_full.astype(jnp.float32)
    gelu_activations, gelu_pull = jax.vjp(gelu_exact, inner_product_sum)
    activated_low = gelu_activations.astype(jnp.bfloat16)
    second_layer_norm = (
        jnp.dot(activated_low, down_full, preferred_element_type=jnp.float32) + bias_float[4]
    )
    final_norm, final_pull = jax.vjp(
        norm_layer, first_layer_norm + second_layer_norm, gain_float[1], bias_float[5]
    )
    layer_out = final_norm.astype(jnp.bfloat16).reshape(token_shape)
    qkv_full, out_full, up_full, down_full, up_bias_full, gain_full, bias_full, type_full = (
        fetch_weights()
    )
    grad_final, grad_gain_two, grad_shift_two = final_pull(
        cotangent.reshape(row_count, model_width).astype(jnp.float32)
    )
    grad_second = grad_final.astype(jnp.bfloat16)
    grad_down = jnp.einsum(
        "rf,rd->fd", activated_low, grad_second, preferred_element_type=jnp.float32
    )
    grad_bias_second = jnp.sum(grad_second.astype(jnp.float32), axis=0)
    (grad_inner,) = gelu_pull(
        jnp.einsum("rd,fd->rf", grad_second, down_full, preferred_element_type=jnp.float32)
    )
    grad_inner_low = grad_inner.astype(jnp.bfloat16)
    grad_up = jnp.einsum("rd,rf->df", first_low, grad_inner_low, preferred_element_type=jnp.float32)
    grad_up_bias = jnp.sum(grad_inner_low.astype(jnp.float32), axis=0)
    grad_first = grad_final + jnp.einsum(
        "rf,df->rd", grad_inner_low, up_full, preferred_element_type=jnp.float32
    )
    grad_resid, grad_gain_one, grad_shift_one = first_pull(grad_first)
    grad_branch = grad_resid.astype(jnp.bfloat16)
    grad_out = jnp.einsum(
        "re,rd->ed", attended_token, grad_branch, preferred_element_type=jnp.float32
    )
    grad_bias_branch = jnp.sum(grad_branch.astype(jnp.float32), axis=0)
    grad_attended = (
        jnp.einsum("rd,ed->re", grad_branch, out_full, preferred_element_type=jnp.float32)
        .astype(jnp.bfloat16)
        .reshape(token_shape)
    )
    grad_local = lax.all_to_all(grad_attended, "head", split_axis=2, concat_axis=1, tiled=True)
    grad_heads = grad_local.reshape(head_shape)
    delta_rows = jnp.sum(
        grad_heads.astype(jnp.float32).transpose(0, 2, 1, 3) * attention_result, axis=-1
    )
    fold_queries = query_fold(
        query_heads, grad_heads, log_totals, delta_rows, score_scale, head_count, head_size
    )
    grad_query_sum = fold_queries(
        zero_heads,
        (
            lax.all_gather(key_local, "blk", axis=1, tiled=True),
            lax.all_gather(value_local, "blk", axis=1, tiled=True),
        ),
        jnp.int32(0),
    )
    fold_side = key_fold(key_heads, value_heads, score_scale, head_count, head_size)
    grad_key_sum, grad_value_sum = fold_side(
        (zero_heads, zero_heads),
        (
            lax.all_gather(query_local.astype(jnp.float32), "blk", axis=1, tiled=True).astype(
                jnp.bfloat16
            ),
            lax.all_gather(grad_local.astype(jnp.float32), "blk", axis=1, tiled=True).astype(
                jnp.bfloat16
            ),
            lax.all_gather(log_totals.transpose(0, 2, 1), "blk", axis=1, tiled=True),
            lax.all_gather(delta_rows.transpose(0, 2, 1), "blk", axis=1, tiled=True),
        ),
        jnp.int32(0),
    )
    grad_keys_local = (
        (grad_key_sum * score_scale)
        .transpose(0, 2, 1, 3)
        .reshape(seq_count, query_rows, local_width)
        .astype(jnp.bfloat16)
    )
    grad_values_local = (
        grad_value_sum.transpose(0, 2, 1, 3)
        .reshape(seq_count, query_rows, local_width)
        .astype(jnp.bfloat16)
    )
    grad_query_local = (
        (grad_query_sum * score_scale)
        .transpose(0, 2, 1, 3)
        .reshape(seq_count, query_rows, local_width)
        .astype(jnp.bfloat16)
    )
    grad_query_token, grad_key_token, grad_value_token = (
        lax.all_to_all(grad_query_local, "head", split_axis=1, concat_axis=2, tiled=True),
        lax.all_to_all(grad_keys_local, "head", split_axis=1, concat_axis=2, tiled=True),
        lax.all_to_all(grad_values_local, "head", split_axis=1, concat_axis=2, tiled=True),
    )
    grad_qkv = jnp.concatenate(
        [grad_query_token, grad_key_token, grad_value_token], axis=-1
    ).reshape(row_count, 3 * model_width)
    grad_qkv_full = jnp.einsum(
        "rd,rf->df", embedded_low, grad_qkv, preferred_element_type=jnp.float32
    )
    grad_bias_query = jnp.sum(
        grad_query_token.astype(jnp.float32).reshape(row_count, model_width), axis=0
    )
    grad_bias_value = jnp.sum(
        grad_value_token.astype(jnp.float32).reshape(row_count, model_width), axis=0
    )
    grad_embedded = grad_resid + jnp.einsum(
        "rf,df->rd", grad_qkv, qkv_full, preferred_element_type=jnp.float32
    )
    second_mask = is_second.astype(jnp.float32)
    grad_type_one = jnp.sum(grad_embedded * second_mask, axis=0)
    grad_type_zero = jnp.sum(grad_embedded * (1.0 - second_mask), axis=0)
    length = lax.axis_size("blk") * pos_table.shape[0]
    local_slots = flat_pos
    inside = (local_slots >= 0) & (local_slots < length)
    slot_index = jnp.where(inside, local_slots, length)
    buffer = jnp.zeros((length + 1, model_width), jnp.float32).at[slot_index].add(grad_embedded)
    grad_positions = lax.psum_scatter(buffer[:length], "blk", scatter_dimension=0, tiled=True)
    gain_stack = jnp.stack([grad_gain_one, grad_gain_two])
    bias_stack = jnp.stack(
        [
            grad_bias_query,
            grad_bias_value,
            grad_bias_branch,
            grad_shift_one,
            grad_bias_second,
            grad_shift_two,
        ]
    )
    type_stack = jnp.stack([grad_type_zero, grad_type_one])
    (
        shard_qkv,
        shard_out,
        shard_up,
        shard_down,
        shard_up_bias,
        shard_gains,
        shard_biases,
        shard_types,
    ) = (
        lax.psum_scatter(grad_qkv_full, "blk", scatter_dimension=0, tiled=True),
        lax.psum_scatter(grad_out, "blk", scatter_dimension=0, tiled=True),
        lax.psum_scatter(grad_up, "blk", scatter_dimension=0, tiled=True),
        lax.psum_scatter(grad_down, "blk", scatter_dimension=0, tiled=True),
        lax.psum_scatter(grad_up_bias, "blk", scatter_dimension=0, tiled=True),
        lax.psum_scatter(gain_stack, "blk", scatter_dimension=1, tiled=True),
        lax.psum_scatter(bias_stack, "blk", scatter_dimension=1, tiled=True),
        lax.psum_scatter(type_stack, "blk", scatter_dimension=1, tiled=True),
    )
    (
        total_qkv,
        total_out,
        total_up,
        total_down,
        total_up_bias,
        total_gains,
        total_biases,
        total_types,
        total_positions,
    ) = lax.psum(
        (
            shard_qkv,
            shard_out,
            shard_up,
            shard_down,
            shard_up_bias,
            shard_gains,
            shard_biases,
            shard_types,
            grad_positions,
        ),
        "head",
    )
    grad_hidden = grad_embedded.reshape(token_shape)
    return (
        layer_out,
        grad_hidden,
        total_positions,
        total_types,
        total_qkv,
        total_out,
        total_up,
        total_down,
        total_up_bias,
        total_gains,
        total_biases,
    )


BIG = 56 << 20
WHOLE = 67043328
LAG = 1
CHUNKS = 4
CHUNK_LAG = 1
EARLY = (1, 3)
TURNS = ((1, 3), (2, 4, 6, 8), (6, 12))


def layer_in_planes(
    hidden,
    pos_ids,
    type_ids,
    cotangent,
    pos_table,
    type_table,
    query_key_value_weight,
    attention_output_weight,
    up_projection_weight,
    down_projection_weight,
    up_projection_bias,
    norm_gains,
    biases,
):
    seqs, seg, width = hidden.shape
    b = lax.axis_index("blk")
    rows = seqs * seg
    e = width // HEADS
    scale = 1.0 / math.sqrt(e)
    slots = pos_table.shape[0]
    fcols = down_projection_weight.shape[0] // 2

    token_shape = (seqs, seg, width)
    begin = SimpleNamespace(
        biases=biases,
        gains=norm_gains,
        types=type_table,
        up_bias=up_projection_bias.reshape(2, 2 * e),
        pos_ids=pos_ids,
        type_ids=type_ids,
        qkv_weight=query_key_value_weight,
        out_weight=attention_output_weight,
        up_weight=up_projection_weight,
        table=pos_table,
        hidden=hidden,
    )
    (
        (
            attended,
            held,
            pair_out,
            lse,
            embedded,
            plane_low,
            qkv_own,
            out_own,
            up_one,
            up_cut,
            vectors,
            up_bias,
            pos_all,
            is_second,
        ),
    ) = fused("first_half", 0, [first_half(begin, scale, LAG)], WHOLE)
    parts = SimpleNamespace(
        attended=attended,
        out_own=out_own.reshape(2 * e, width),
        embedded=embedded,
        cotangent=cotangent,
        up_one=up_one,
        up_cut=up_cut,
        down_weight=down_projection_weight,
        up_bias=up_bias,
        vectors=vectors,
        held=held,
        pair_out=pair_out,
        lse=lse,
        qkv_own=qkv_own.reshape(width, 6 * e),
        plane_low=plane_low,
        ids=pos_all,
        second=is_second,
    )
    sizes = (slots, CHUNKS, CHUNK_LAG, scale)
    ((layer_out, grad_hidden, pos, down, up, qkv, out, totals),) = fused(
        "second_half", 4, [second_half(parts, sizes)], WHOLE
    )
    outs = finish(
        (b % 2).reshape(1),
        layer_out.reshape(rows, width),
        grad_hidden.reshape(rows, width),
        pos,
        down.reshape(2 * fcols, width),
        up,
        qkv,
        out,
        totals,
    )
    return (
        outs[0].reshape(token_shape),
        outs[1].reshape(token_shape),
        *outs[2:8],
        outs[8].reshape(4 * e),
        *outs[9:],
    )


def planes_fit(hidden, head_axis, blk_axis):
    seqs, seg, width = hidden.shape
    return head_axis == 2 and blk_axis == HEADS and seqs == 2 and seqs * seg == 2 * width // HEADS


def on_device(hidden, *rest):
    if planes_fit(hidden, lax.axis_size("head"), lax.axis_size("blk")):
        return layer_in_planes(hidden, *rest)
    return layer_in_blocks(hidden, *rest)


def solution(mesh):
    in_specs = (
        P(None, ("head", "blk"), None),
        P(None, ("head", "blk")),
        P(None, ("head", "blk")),
        P(None, ("head", "blk"), None),
        P("blk", None),
        P(None, "blk"),
        P("blk", None),
        P("blk", None),
        P("blk", None),
        P("blk", None),
        P("blk"),
        P(None, "blk"),
        P(None, "blk"),
    )
    out_specs = (
        P(None, ("head", "blk"), None),
        P(None, ("head", "blk"), None),
        P("blk", None),
        P(None, "blk"),
        P("blk", None),
        P("blk", None),
        P("blk", None),
        P("blk", None),
        P("blk"),
        P(None, "blk"),
        P(None, "blk"),
    )
    return jax.shard_map(
        on_device, mesh=mesh, in_specs=in_specs, out_specs=out_specs, check_vma=False
    )
```

```python
import functools
import math
from types import SimpleNamespace

import jax
import jax.numpy as jnp
from jax import lax
from jax.experimental import pallas as pl
from jax.experimental.pallas import tpu as pltpu
from jax.sharding import PartitionSpec as P

HEADS = 16
MESH = pl.DeviceIdType.MESH
F32 = jnp.float32
BF16 = jnp.bfloat16
VSPEC = pl.BlockSpec(memory_space=pltpu.VMEM)


def place():
    h = lax.axis_index("head")
    b = lax.axis_index("blk")
    return h, b // 4, (b // 2) % 2, b % 2


def blk(o, y, c):
    return (o * 2 + y) * 2 + c


def peer(dx, dz, dy, dc):
    h, o, y, c = place()
    flip = lambda v, d: 1 - v if d else v
    return flip(h, dx), blk((o + dz) % 4 if dz else o, flip(y, dy), flip(c, dc))


def remote(src, dst, sems, index, device):
    return pltpu.make_async_remote_copy(
        src_ref=src,
        dst_ref=dst,
        send_sem=sems.at[0, index],
        recv_sem=sems.at[1, index],
        device_id=device,
        device_id_type=MESH,
    )


def landed(ref, sems, index):
    remote(ref, ref, sems, index, peer(1, 0, 0, 0)).wait_recv()


def sems(count):
    return pltpu.SemaphoreType.DMA((2, count))


NEAR_X, NEAR_Y, NEAR_C = (1, 0, 0, 0), (0, 0, 1, 0), (0, 0, 0, 1)
COLUMN = ((0, 1, 0, 0), (0, 2, 0, 0), (0, 3, 0, 0))
PLANE = tuple(
    (dx, 0, dy, dc) for dx in range(2) for dy in range(2) for dc in range(2) if dx or dy or dc
)


class Part:
    def __init__(self, run, ins, outs, scratch, peers):
        self.run, self.ins, self.outs, self.scratch, self.peers = run, ins, outs, scratch, peers
        self.turns = ()

    def on(self, *turns):
        self.turns = turns
        return self


def fused(name, cid, parts, limit=None):
    peers = sorted({p for part in parts for p in part.peers})
    ins = [x for part in parts for x in part.ins]
    outs = [s for part in parts for s in part.outs]
    scratch = [s for part in parts for s in part.scratch]

    def kernel(*refs):
        in_refs, out_refs = refs[: len(ins)], refs[len(ins) : len(ins) + len(outs)]
        own = refs[len(ins) + len(outs) :]
        gens = []
        i = j = k = 0
        for part in parts:
            gens.append(
                part.run(
                    in_refs[i : i + len(part.ins)],
                    out_refs[j : j + len(part.outs)],
                    own[k : k + len(part.scratch)],
                )
            )
            i, j, k = i + len(part.ins), j + len(part.outs), k + len(part.scratch)
        barrier = pltpu.get_barrier_semaphore()
        for p in peers:
            pl.semaphore_signal(barrier, inc=1, device_id=peer(*p), device_id_type=MESH)
        pl.semaphore_wait(barrier, len(peers))
        for gen in gens:
            next(gen)
        for turn, _ in enumerate(gens[0]):
            for part, gen in zip(parts, gens):
                if turn in part.turns:
                    next(gen)
        for gen in gens[1:]:
            for _ in gen:
                pass

    got = pl.pallas_call(
        kernel,
        name=name,
        out_shape=[jax.ShapeDtypeStruct(s, d) for s, d in outs],
        in_specs=[VSPEC] * len(ins),
        out_specs=[VSPEC] * len(outs),
        scratch_shapes=scratch,
        compiler_params=pltpu.CompilerParams(
            collective_id=cid, has_side_effects=True, vmem_limit_bytes=limit
        ),
    )(*ins)
    result = []
    for part in parts:
        result.append(got[: len(part.outs)])
        got = got[len(part.outs) :]
    return result


def exchange(x, peers, out_lead, source, target):
    peers = list(peers)

    def coords(p):
        h, o, y, c = place()
        flip = lambda v, d: 1 - v if d else v
        return flip(h, p[0]), (o + p[1]) % 4 if p[1] else o, flip(y, p[2]), flip(c, p[3])

    def run(ins, outs, own):
        (x_ref,), (out_ref,), (sem,) = ins, outs, own
        me = place()
        copies = []
        for k, p in enumerate(peers):
            copy = remote(
                source(x_ref, coords(p)), target(out_ref, me), sem, k, peer(*p)
            )
            copy.start()
            copies.append(copy)
        yield
        target(out_ref, me)[...] = source(x_ref, me)[...]
        for copy in copies:
            copy.wait()

    return Part(run, [x], [(out_lead, x.dtype)], [sems(len(peers))], peers)


def small_gather(x):
    peers = [
        (0, dz, dy, dc) for dz in range(4) for dy in range(2) for dc in range(2) if dz or dy or dc
    ]
    return exchange(x, peers, (16,) + x.shape, lambda r, d: r, lambda r, s: r.at[blk(*s[1:])])


def place_copy(src, dst, send_sem, recv_sem, device):
    return pltpu.make_async_remote_copy(
        src_ref=src,
        dst_ref=dst,
        send_sem=send_sem,
        recv_sem=recv_sem,
        device_id=device,
        device_id_type=MESH,
    )


BLK = tuple(
    (0, dz, dy, dc) for dz in range(4) for dy in range(2) for dc in range(2) if dz or dy or dc
)


def out_weights(w):
    r, n = w.shape

    def run(ins, outs, own):
        (w_ref,), (out_ref,), (send, recv) = ins, outs, own
        h, o, y, c = place()
        has = o // 2 == h
        serves = (o % 2 == y) & (y == c)

        def each(act):
            for k in range(4):
                device = (h, blk((o + k) % 4, o % 2, y))
                copy = place_copy(w_ref, out_ref.at[c], send.at[k], recv.at[c], device)

                @pl.when(has if k else has & jnp.logical_not(serves))
                def _():
                    act(copy)

        each(lambda copy: copy.start())
        yield

        @pl.when(has & serves)
        def _():
            out_ref[pl.ds(c, 1)] = w_ref[...][None]

        each(lambda copy: copy.wait_send())
        for core in range(2):
            from_self = (o == 2 * h + y) & (y == c) & (c == core)
            ref = out_ref.at[core]

            @pl.when(jnp.logical_not(from_self))
            def _():
                place_copy(ref, ref, send.at[0], recv.at[core], (h, blk(o, y, c))).wait_recv()

    scratch = [pltpu.SemaphoreType.DMA((4,)), pltpu.SemaphoreType.DMA((2,))]
    return Part(run, [w], [((2, r, n), BF16)], scratch, BLK)


def mirrored():
    o = place()[1]
    far = o // 2
    seen = lambda v: v * (1 - 2 * far) + 3 * far
    return seen(o), seen


def gather_steps(src, dst, sem):
    h, o, y, c = place()
    dev_x, dev_y, dev_c = peer(*NEAR_X), peer(*NEAR_Y), peer(*NEAR_C)
    mine = h * 4 + y * 2 + c
    of_x = (1 - h) * 4 + y * 2 + c
    of_y = h * 4 + (1 - y) * 2 + c
    of_d = (1 - h) * 4 + (1 - y) * 2 + c
    flip = 1 - 2 * c
    sent = []

    def go(ref, slot, half, index, device):
        copy = remote(ref, dst(half, slot), sem, index, device)
        copy.start()
        sent.append(copy)

    go(src(0), mine, 0, 0, dev_x)
    go(src(1), mine, 1, 1, dev_y)
    go(src(1), mine, 1, 2, dev_x)
    go(src(0), mine, 0, 3, dev_y)
    go(src(0), mine, 0, 4, dev_c)
    go(src(1), mine, 1, 5, dev_c)
    for half in range(2):
        dst(half, mine)[...] = src(half)[...]

    def relay(slot, half, index, device, onward, to_core):
        landed(dst(half, slot), sem, index)
        if onward is not None:
            go(dst(half, slot), slot, half, onward, device)
        go(dst(half, slot), slot, half, to_core, dev_c)

    yield
    relay(of_x, 0, 0, dev_y, 6, 8)
    relay(of_y, 1, 1, dev_x, 7, 9)
    yield
    relay(of_x, 1, 2, None, None, 10)
    relay(of_y, 0, 3, None, None, 11)
    yield
    relay(of_d, 0, 6, None, None, 12)
    relay(of_d, 1, 7, None, None, 13)
    yield
    for slot, half, index in (
        (mine, 0, 4),
        (mine, 1, 5),
        (of_x, 0, 8),
        (of_y, 1, 9),
        (of_x, 1, 10),
        (of_y, 0, 11),
        (of_d, 0, 12),
        (of_d, 1, 13),
    ):
        landed(dst(half, slot + flip), sem, index)
    for copy in sent:
        copy.wait_send()


def scatter_steps(src, total, near, part, from_x, from_y, diag, sem):
    h, o, y, c = place()
    dev_x, dev_y, dev_c = peer(*NEAR_X), peer(*NEAR_Y), peer(*NEAR_C)
    mine = h * 4 + y * 2 + c
    of_x = (1 - h) * 4 + y * 2 + c
    of_y = h * 4 + (1 - y) * 2 + c
    of_d = (1 - h) * 4 + (1 - y) * 2 + c
    flip = 1 - 2 * c
    order = (of_d, of_x, of_y, mine)
    sent = []

    def go(ref, to, index, device):
        copy = remote(ref, to, sem, index, device)
        copy.start()
        sent.append(copy)

    for k, half in ((0, 0), (0, 1), (1, 0), (2, 1), (1, 1), (2, 0), (3, 0), (3, 1)):
        go(src(half, order[k] + flip), near.at[k, half], 2 * k + half, dev_c)

    def add(k, half):
        landed(near.at[k, half], sem, 2 * k + half)
        return src(half, order[k])[...].astype(F32) + near[k, half].astype(F32)

    yield
    part[0, 0] = add(0, 0).astype(BF16)
    go(part.at[0, 0], diag.at[0], 8, dev_x)
    part[0, 1] = add(0, 1).astype(BF16)
    go(part.at[0, 1], diag.at[1], 9, dev_y)
    part[1, 0] = add(1, 0).astype(BF16)
    go(part.at[1, 0], from_x.at[0], 10, dev_x)
    part[2, 1] = add(2, 1).astype(BF16)
    go(part.at[2, 1], from_y.at[1], 11, dev_y)
    yield
    kept_x = add(1, 1)
    landed(diag.at[1], sem, 9)
    part[1, 1] = (kept_x + diag[1].astype(F32)).astype(BF16)
    go(part.at[1, 1], from_x.at[1], 12, dev_x)
    kept_y = add(2, 0)
    landed(diag.at[0], sem, 8)
    part[2, 0] = (kept_y + diag[0].astype(F32)).astype(BF16)
    go(part.at[2, 0], from_y.at[0], 13, dev_y)
    yield
    own = [add(3, half) for half in range(2)]
    for half, ix, iy in ((0, 10, 13), (1, 12, 11)):
        landed(from_x.at[half], sem, ix)
        landed(from_y.at[half], sem, iy)
        total(half)[...] = own[half] + from_x[half].astype(F32) + from_y[half].astype(F32)
    for copy in sent:
        copy.wait_send()


def scatter_scratch(r, n):
    block = (2, r // 2, n)
    return [
        pltpu.VMEM((4,) + block, BF16),
        pltpu.VMEM((3,) + block, BF16),
        pltpu.VMEM(block, BF16),
        pltpu.VMEM(block, BF16),
        pltpu.VMEM(block, BF16),
        sems(14),
    ]


def norm_parts(r):
    centred = r - jnp.mean(r, axis=-1, keepdims=True)
    scale = lax.rsqrt(jnp.mean(centred * centred, axis=-1, keepdims=True) + 1e-12)
    return centred * scale, scale


def norm_back(xh, scale, dh):
    return (
        dh
        - jnp.mean(dh, axis=-1, keepdims=True)
        - xh * jnp.mean(dh * xh, axis=-1, keepdims=True)
    ) * scale


def dot_nt(a, b):
    return lax.dot_general(a, b, (((1,), (1,)), ((), ())), preferred_element_type=F32)


def dot_tn(a, b):
    return lax.dot_general(a, b, (((0,), (0,)), ((), ())), preferred_element_type=F32)


def blk_gather_steps(src, spot_of, zsem, ysem, csem):
    h, o, y, c = place()
    at, seen = mirrored()
    dev_y, dev_c = peer(*NEAR_Y), peer(*NEAR_C)
    end, inner, other = (h, blk(seen(0), y, c)), (h, blk(seen(1), y, c)), (h, blk(seen(2), y, c))
    sent = []

    def spot(z, yy=y, cc=c):
        return spot_of(z, yy, cc)

    def go(ref, z, yy, sem, index, device):
        copy = remote(ref, spot(z, yy), sem, index, device)
        copy.start()
        sent.append(copy)

    def line(ref, z, index, device):
        return remote(ref, spot(z), zsem, index, device)

    @pl.when(at == 0)
    def _():
        line(src, o, 0, inner).start()

    @pl.when(at == 1)
    def _():
        line(src, o, 1, end).start()
        line(src, o, 2, other).start()

    go(src, o, y, ysem, 0, dev_y)
    go(src, o, y, csem, 0, dev_c)
    spot(o)[...] = src[...]

    def onward(j, z):
        go(spot(z), z, y, ysem, j, dev_y)
        go(spot(z), z, y, csem, j, dev_c)

    first = seen(1 - at)
    order = (o, first, seen(2), seen(3))

    def from_y(j):
        landed(spot(order[j], 1 - y), ysem, j)
        go(spot(order[j], 1 - y), order[j], 1 - y, csem, 4 + j, dev_c)

    yield

    @pl.when(at == 0)
    def _():
        landed(spot(seen(1)), zsem, 1)

    @pl.when(at == 1)
    def _():
        landed(spot(seen(0)), zsem, 0)
        line(spot(seen(0)), seen(0), 3, other).start()

    onward(1, first)

    @pl.when(at == 1)
    def _():
        landed(spot(seen(2)), zsem, 2)
        line(spot(seen(2)), seen(2), 4, end).start()

    yield
    from_y(0)

    @pl.when(at == 0)
    def _():
        landed(spot(seen(2)), zsem, 4)

    onward(2, seen(2))

    @pl.when(at == 1)
    def _():
        landed(spot(seen(3)), zsem, 3)
        line(spot(seen(3)), seen(3), 5, end).start()

    yield
    from_y(1)

    @pl.when(at == 0)
    def _():
        landed(spot(seen(3)), zsem, 5)

    onward(3, seen(3))
    yield
    from_y(2)
    yield
    from_y(3)
    yield
    for j, z in enumerate(order):
        landed(spot(z, y, 1 - c), csem, j)
        landed(spot(z, 1 - y, 1 - c), csem, 4 + j)

    @pl.when(at == 0)
    def _():
        line(src, o, 0, inner).wait_send()

    @pl.when(at == 1)
    def _():
        line(src, o, 1, end).wait_send()
        line(src, o, 2, other).wait_send()
        line(spot(seen(0)), seen(0), 3, other).wait_send()
        line(spot(seen(2)), seen(2), 4, end).wait_send()
        line(spot(seen(3)), seen(3), 5, end).wait_send()

    for copy in sent:
        copy.wait_send()


ALL = tuple(
    (dx, dz, dy, dc)
    for dx in range(2)
    for dz in range(4)
    for dy in range(2)
    for dc in range(2)
    if dx or dz or dy or dc
)


def line_gather_steps(src, spot, sem):
    h, o, y, c = place()
    at, seen = mirrored()
    end, inner, other = (h, blk(seen(0), y, c)), (h, blk(seen(1), y, c)), (h, blk(seen(2), y, c))

    def line(ref, z, index, device):
        return remote(ref, spot(z), sem, index, device)

    @pl.when(at == 0)
    def _():
        line(src, o, 0, inner).start()

    @pl.when(at == 1)
    def _():
        line(src, o, 2, other).start()
        line(src, o, 1, end).start()

    spot(o)[...] = src[...]
    for k, (z, to, device) in enumerate(((0, 3, other), (2, 4, end), (3, 5, end))):
        yield

        @pl.when(at == 1)
        def _():
            landed(spot(seen(z)), sem, (0, 2, 3)[k])
            line(spot(seen(z)), seen(z), to, device).start()

    yield

    @pl.when(at == 0)
    def _():
        for z, index in ((1, 1), (2, 4), (3, 5)):
            landed(spot(seen(z)), sem, index)
        line(src, o, 0, inner).wait_send()

    @pl.when(at == 1)
    def _():
        line(src, o, 1, end).wait_send()
        line(src, o, 2, other).wait_send()
        for z, to, device in ((0, 3, other), (2, 4, end), (3, 5, end)):
            line(spot(seen(z)), seen(z), to, device).wait_send()


def line_sum_steps(term_of, out, terms, ends, mids, last, sem):
    h, o, y, c = place()
    at, seen = mirrored()
    end, inner, other = (h, blk(seen(0), y, c)), (h, blk(seen(1), y, c)), (h, blk(seen(2), y, c))
    order = [seen(3), seen(2), seen(1 - at)]
    plus = lambda a, b: a[...].astype(F32) + b[...].astype(F32)

    @pl.when(at == 0)
    def _():
        for j in range(3):
            remote(term_of(order[j]), ends.at[j], sem, j, inner).start()

    for j in range(2):
        yield

        @pl.when(at == 1)
        def _():
            landed(ends.at[j], sem, j)
            terms[j] = plus(term_of(order[j]), ends.at[j]).astype(BF16)
            remote(terms.at[j], mids.at[j], sem, 3 + j, other).start()

    yield

    @pl.when(at == 1)
    def _():
        landed(mids.at[0], sem, 3)
        terms[2] = plus(term_of(order[2]), mids.at[0]).astype(BF16)
        remote(terms.at[2], last, sem, 5, end).start()

    yield

    @pl.when(at == 1)
    def _():
        landed(ends.at[2], sem, 2)
        landed(mids.at[1], sem, 4)
        out[...] = (plus(term_of(o), ends.at[2]) + mids[1].astype(F32)).astype(BF16)
        for j in range(2):
            remote(terms.at[j], mids.at[j], sem, 3 + j, other).wait_send()
        remote(terms.at[2], last, sem, 5, end).wait_send()

    @pl.when(at == 0)
    def _():
        landed(last, sem, 5)
        out[...] = plus(term_of(o), last).astype(BF16)
        for j in range(3):
            remote(term_of(order[j]), ends.at[j], sem, j, inner).wait_send()


def line_sum_scratch(block):
    return [
        pltpu.VMEM((3,) + block, BF16),
        pltpu.VMEM((3,) + block, BF16),
        pltpu.VMEM((2,) + block, BF16),
        pltpu.VMEM(block, BF16),
        sems(6),
    ]


def spread_steps(rows_of, out, spots, sem):
    h, o, y, c = place()
    t = h * 4 + y * 2 + c
    columns = [
        out.at[:, pl.ds(pl.multiple_of(lane * 128, 128), 128)] for lane in spots(t)
    ]
    pieces = len(columns)
    copies = []
    for k, p in enumerate(PLANE):
        to = (1 - y if p[2] else y) * 2 + (1 - c if p[3] else c)
        for i in range(pieces):
            src = rows_of(to).at[:, pl.ds(i * 128, 128)]
            copy = remote(src, columns[i], sem, k * pieces + i, peer(*p))
            copy.start()
            copies.append(copy)
    for i in range(pieces):
        columns[i][...] = rows_of(y * 2 + c)[:, i * 128 : (i + 1) * 128]
    yield
    for copy in copies:
        copy.wait()


def second_half(x, consts):
    names = list(vars(x))
    seqs, r, d = x.embedded.shape
    planes, four, e, fh = x.up_one.shape
    f = 2 * fh
    fcols = x.down_weight.shape[0] // 2
    half_d = d // 2
    rows, q_rows = 8 * r, 4 * r
    three, he, length = x.held.shape
    n = length // 4
    slots, chunks, chunk_lag, scale = consts
    own_rows, w, blks = seqs * r, d // chunks, 16
    key_rows = 256
    width_qkv = 3 * 2 * he

    need = []

    def scratch(shape, dtype):
        need.append(pltpu.VMEM(shape, dtype))
        return len(need) - 1

    def many(specs):
        start = len(need)
        need.extend(specs)
        return list(range(start, len(need)))

    plane = (seqs, 8, r, d)
    shapes = dict(
        partial=(plane, BF16),
        up_two=(x.up_one.shape, BF16),
        down_all=((planes, fcols, d), BF16),
        first_g=(plane, BF16),
        grad_g=(plane, BF16),
        branch_g=(plane, BF16),
        act=((seqs * rows, f), BF16),
        slope=((seqs * rows, f), F32),
        inner_grad=((seqs * rows, f), BF16),
        first=((seqs, r, d), F32),
        xh_one=((seqs, r, d), F32),
        scale_one=((seqs, r, 1), F32),
        grad_two=((seqs, r, d), F32),
        low=((seqs, r, d), BF16),
        total=((seqs, r, d), F32),
        resid=((seqs, r, d), F32),
        down_part=((planes, fcols, d), BF16),
        up_part=((planes, 4 * e, f), BF16),
        up_total=((4 * e, f), BF16),
        out_part=((2, he, d), BF16),
        out_held=((4, he, d), BF16),
        out_acc=((he, d), F32),
        sums=((16, d), F32),
        up_sums=((1, f), F32),
        up_spots=((32, 128), F32),
        go=((2, he, 2 * n), BF16),
        gs=((he, length), BF16),
        qs=((he, length), BF16),
        q_rows=((length, he), BF16),
        g_rows=((length, he), BF16),
        dq=((he, length), F32),
        delta=((1, length), F32),
        pair_low=((three, he, length), BF16),
        dqkv=((three, 2, he, 2 * n), BF16),
        qkv_part=((planes, 4 * e, width_qkv), BF16),
        qkv_total=((4 * e, width_qkv), BF16),
        own=((chunks, own_rows, w), BF16),
        gathered=((chunks, blks, own_rows, w), BF16),
        pick=((slots, blks * own_rows), BF16),
        pos_low=((chunks, slots, w), BF16),
        pos_held=((chunks, slots, w), BF16),
        pack=((blks, 24, 128), F32),
        packs=((31, 24, 128), F32),
    )
    ids = {name: scratch(*spec) for name, spec in shapes.items()}
    counts = dict(
        up_sem=6,
        down_sem=6,
        ksem=3,
        qsem=3,
        down_pair=1,
        up_spread=28,
        qkv_spread=21,
        out_pair=1,
        pair_sem=chunks,
        pack_sem=31,
    )
    sem_ids = {k: many([sems(v)])[0] for k, v in counts.items()}
    for k, v in dict(go_send=4, go_recv=4, out_send=2, out_recv=4).items():
        sem_ids[k] = many([pltpu.SemaphoreType.DMA((v,))])[0]
    stream_ids = [
        ([many(scatter_scratch(2 * r, d)) for _ in range(3)], [many([sems(14)])[0] for _ in range(3)])
    ]
    chunk_ids = [
        (many(scatter_scratch(2 * r, w)), many([sems(6), sems(4), sems(8)])) for _ in range(chunks)
    ]
    down_line = many(line_sum_scratch((fcols, d)))
    up_line = many(line_sum_scratch((4 * e, f)))
    qkv_line = many(line_sum_scratch((4 * e, width_qkv)))

    def run(ins, outs, own):
        src = SimpleNamespace(**dict(zip(names, ins)))
        out_ref, grad_ref, pos_ref, got_down, got_up, got_qkv, got_out, totals = outs
        m = SimpleNamespace(**{k: own[v] for k, v in ids.items()})
        sem = SimpleNamespace(**{k: own[v] for k, v in sem_ids.items()})
        pick_refs = lambda some: [own[i] for i in some]
        h, o, y, c = place()
        g = y * 2 + c
        t = h * 4 + g
        tail = []

        up_more = src.up_cut.at[:, :, pl.ds(fh, fh)]
        down_rows = pl.ds(pl.multiple_of(h * fcols, fcols), fcols)
        down_more = src.down_weight.at[down_rows]
        up_line_in = line_gather_steps(up_more, lambda z: m.up_two.at[z], sem.up_sem)
        down_line_in = line_gather_steps(down_more, lambda z: m.down_all.at[z], sem.down_sem)
        next(up_line_in)
        next(down_line_in)
        for ref in (m.sums, m.up_sums, m.up_spots, m.dq):
            ref[...] = jnp.zeros_like(ref)
        yield

        ups = [lambda k=k: src.up_one[...].reshape(d, fh) if k == 0 else m.up_two[...].reshape(d, fh) for k in range(2)]
        downs = [
            lambda k=k: m.down_all[:, :, k * half_d : (k + 1) * half_d].reshape(f, half_d)
            for k in range(2)
        ]
        vec = lambda k: src.vectors[k + 2 : k + 3]
        partial, low, total = m.partial, m.low, m.total

        both = range(seqs)

        def piece(ref):
            return lambda i, slot: ref.at[i, slot]

        def plain(ref):
            return lambda i: ref.at[i]

        def quarter(ref, s, q):
            return ref[s, 4 * q : 4 * q + 4].reshape(q_rows, d)

        def note(k, value):
            m.sums[k : k + 1] += jnp.sum(value, axis=0, keepdims=True)

        def step(*some):
            for gen in some:
                next(gen, None)

        def down_sums():
            yield from line_sum_steps(
                lambda z: m.down_part.at[z], got_down.at[h], *pick_refs(down_line)
            )
            copy = remote(got_down.at[h], got_down.at[h], sem.down_pair, 0, peer(*NEAR_X))
            copy.start()
            yield
            copy.wait_send()
            landed(got_down.at[1 - h], sem.down_pair, 0)

        def up_sums():
            yield from line_sum_steps(lambda z: m.up_part.at[z], m.up_total, *pick_refs(up_line))
            yield from spread_steps(
                lambda k: m.up_total.at[pl.ds(k * e, e)],
                got_up,
                lambda k: [(i * 4 + k % 4) * 2 + k // 4 for i in range(4)],
                sem.up_spread,
            )

        def qkv_sums():
            yield from line_sum_steps(
                lambda z: m.qkv_part.at[z], m.qkv_total, *pick_refs(qkv_line)
            )
            yield from spread_steps(
                lambda k: m.qkv_total.at[pl.ds(k * e, e)],
                got_qkv,
                lambda k: [i * 8 + k for i in range(3)],
                sem.qkv_spread,
            )

        def out_sums():
            has = o // 2 == h
            held, acc, send, recv = m.out_held, m.out_acc, sem.out_send, sem.out_recv

            def each(act):
                for j in range(2):
                    device = (h, blk(2 * h + y, c, j))
                    copy = place_copy(m.out_part.at[j], held.at[o], send.at[j], recv.at[o], device)

                    @pl.when(jnp.logical_not((o == 2 * h + y) & (y == c) & (c == j)))
                    def _():
                        act(copy)

            each(lambda copy: copy.start())
            yield
            acc[...] = jnp.zeros_like(acc)
            for z in range(4):
                mine = (z == o) & (o % 2 == y) & (y == c)

                @pl.when(has & mine)
                def _():
                    acc[...] += m.out_part[c].astype(F32)

                @pl.when(has & jnp.logical_not(mine))
                def _():
                    ref = held.at[z]
                    place_copy(ref, ref, send.at[0], recv.at[z], (h, blk(o, y, c))).wait_recv()
                    acc[...] += held[z].astype(F32)

            pair = remote(got_out, got_out, sem.out_pair, 0, peer(*NEAR_X))

            @pl.when(has)
            def _():
                got_out[...] = acc[...].astype(BF16)
                pair.start()

            yield
            each(lambda copy: copy.wait_send())

            @pl.when(has)
            def _():
                pair.wait_send()

            @pl.when(jnp.logical_not(has))
            def _():
                landed(got_out, sem.out_pair, 0)

        def go_copy(s, j):
            z = 2 * s + j
            return place_copy(
                m.go.at[j, :, pl.ds(s * n, n)],
                m.gs.at[:, pl.ds(pl.multiple_of(o * n, n), n)],
                sem.go_send.at[z],
                sem.go_recv.at[o],
                (h, z * 4 + g),
            )

        def stream():
            scatters = [pick_refs(i) for i in stream_ids[0][0]]
            gathers = pick_refs(stream_ids[0][1])
            at = lambda s, q: pl.ds(s * rows + q * q_rows, q_rows)
            for s in both:
                branch = dot_tn(
                    src.attended[:, :, s * n : (s + 1) * n].reshape(2 * he, n), src.out_own[...]
                )
                partial[s] = branch.astype(BF16).reshape(8, r, d)
            for k, _ in enumerate(scatter_steps(piece(partial), plain(total), *scatters[0])):
                if k > 0:
                    step(up_line_in)
                yield
            for s in both:
                xh, scale_r = norm_parts(src.embedded[s] + (total[s] + vec(0)))
                m.xh_one[s] = xh
                m.scale_one[s] = scale_r
                value = xh * vec(4) + vec(1)
                m.first[s] = value
                low[s] = value.astype(BF16)
            step(up_line_in, down_line_in)
            for k, _ in enumerate(gather_steps(plain(low), piece(m.first_g), gathers[0])):
                if k in (1, 3):
                    step(down_line_in)
                yield
            for _ in up_line_in:
                pass
            for s in both:
                for q in range(2):
                    rows_in = quarter(m.first_g, s, q)
                    for k in range(2):
                        cols = slice(k * fh, (k + 1) * fh)
                        inner = jnp.dot(rows_in, ups[k](), preferred_element_type=F32)
                        inner = inner + src.up_bias[:, cols]
                        phi = 0.5 + 0.5 * lax.erf(inner * (0.5**0.5))
                        m.act[at(s, q), cols] = (inner * phi).astype(BF16)
                        bell = jnp.exp(inner * inner * -0.5) * (1.0 / math.sqrt(2.0 * math.pi))
                        m.slope[at(s, q), cols] = phi + inner * bell
            for _ in down_line_in:
                pass
            for s in both:
                for k in range(2):
                    part = jnp.dot(
                        m.act[s * rows : (s + 1) * rows], downs[k](), preferred_element_type=F32
                    )
                    partial[s, :, :, k * half_d : (k + 1) * half_d] = part.astype(BF16).reshape(
                        8, r, half_d
                    )
            yield from scatter_steps(piece(partial), plain(total), *scatters[1])
            for s in both:
                xh, scale_r = norm_parts(m.first[s] + (total[s] + vec(2)))
                out_ref[s] = (xh * vec(5) + vec(3)).astype(BF16)
                cot = src.cotangent[s].astype(F32)
                note(5, cot * xh)
                note(3, cot)
                grad = norm_back(xh, scale_r, cot * vec(5))
                m.grad_two[s] = grad
                low[s] = grad.astype(BF16)
                note(2, low[s].astype(F32))
            yield from gather_steps(plain(low), piece(m.grad_g), gathers[1])
            for s in both:
                for q in range(2):
                    rows_in = quarter(m.grad_g, s, q)
                    back = dot_nt(rows_in[:, :half_d], downs[0]()) + dot_nt(
                        rows_in[:, half_d:], downs[1]()
                    )
                    back = (back * m.slope[at(s, q)]).astype(BF16)
                    m.inner_grad[at(s, q)] = back
                    m.up_sums[...] += jnp.sum(back.astype(F32), axis=0, keepdims=True)
                    part = dot_nt(back[:, :fh], ups[0]()) + dot_nt(back[:, fh:], ups[1]())
                    partial[s, 4 * q : 4 * q + 4] = part.astype(BF16).reshape(4, r, d)
            last = scatter_steps(piece(partial), plain(total), *scatters[2])
            next(last)

            @pl.loop(0, planes)
            def _(z):
                cols = pl.ds(pl.multiple_of(z * fcols, fcols), fcols)
                all_grads = m.grad_g[...].reshape(seqs * rows, d)
                m.down_part[z] = dot_tn(m.act[:, cols], all_grads).astype(BF16)

            step(down)
            next(last)

            @pl.loop(0, planes)
            def _(z):
                cols = pl.ds(pl.multiple_of(z * 4 * e, 4 * e), 4 * e)
                all_first = m.first_g[:, :, :, cols].reshape(seqs * rows, 4 * e)
                m.up_part[z] = dot_tn(all_first, m.inner_grad[...]).astype(BF16)

            yield from last
            for s in both:
                grad = m.grad_two[s] + total[s]
                note(4, grad * m.xh_one[s])
                note(1, grad)
                grad = norm_back(m.xh_one[s], m.scale_one[s], grad * vec(4))
                m.resid[s] = grad
                low[s] = grad.astype(BF16)
                note(0, low[s].astype(F32))
            for k, _ in enumerate(gather_steps(plain(low), piece(m.branch_g), gathers[2])):
                yield
                if k in EARLY:
                    step(down)
            for s in both:
                go = dot_nt(src.out_own[...], m.branch_g[s].reshape(rows, d))
                m.go[:, :, s * n : (s + 1) * n] = go.astype(BF16).reshape(2, he, n)
                for j in range(2):

                    @pl.when(o != 2 * s + j)
                    def _():
                        go_copy(s, j).start()

                    @pl.when(o == 2 * s + j)
                    def _():
                        m.gs[:, pl.ds(pl.multiple_of(o * n, n), n)] = m.go[
                            j, :, s * n : (s + 1) * n
                        ]

        down, up, out, qkv = down_sums(), up_sums(), out_sums(), qkv_sums()
        for _ in stream():
            pass
        step(up)
        grad_out = jnp.dot(
            src.attended[...].reshape(2 * he, 2 * n),
            m.branch_g[...].reshape(seqs * rows, d),
            preferred_element_type=F32,
        )
        m.out_part[...] = grad_out.astype(BF16).reshape(2, he, d)
        held = src.held
        gs, qs, q_t, g_t, dq, delta, pair_low = (
            m.gs, m.qs, m.q_rows, m.g_rows, m.dq, m.delta, m.pair_low
        )
        q32 = held[0].astype(F32) * scale
        qs[...] = q32.astype(BF16)
        q_t[...] = q32.T.astype(BF16)

        @pl.loop(0, slots // 64)
        def _(k):
            row = lax.broadcasted_iota(jnp.int32, (64, 1), 0) + k * 64
            some = pl.ds(pl.multiple_of(k * 64, 64), 64)
            m.pick[some] = (src.ids[...] == row).astype(F32).astype(BF16)

        for z in range(4):

            @pl.when(z != o)
            def _():
                ref = gs.at[:, pl.ds(z * n, n)]
                place_copy(
                    ref, ref, sem.go_send.at[0], sem.go_recv.at[z], peer(*NEAR_X)
                ).wait_recv()

        g32 = gs[...].astype(F32)
        g_t[...] = g32.T.astype(BF16)
        delta[...] = jnp.sum(g32 * src.pair_out[...], axis=0, keepdims=True)
        mine = pl.ds(pl.multiple_of((o // 2) * n, n), n)
        dqkv = m.dqkv

        def back(part, which, i, z):
            return remote(
                pair_low.at[part, :, pl.ds(pl.multiple_of(z * n, n), n)],
                dqkv.at[part, o % 2, :, mine],
                which,
                i,
                (h, z * 4 + g),
            )

        late = pl.ds(1, 2)
        for i in range(4):
            z = (o + 1 + i) % 4

            @pl.loop(0, n // key_rows)
            def _(step):
                at = pl.ds(pl.multiple_of(z * n + step * key_rows, key_rows), key_rows)
                k_cols = held[1, :, at]
                k_rows = k_cols.astype(F32).T.astype(BF16)
                v_rows = held[2, :, at].astype(F32).T.astype(BF16)
                s = jnp.dot(k_rows, qs[...], preferred_element_type=F32)
                p = jnp.exp(s - src.lse[...])
                dv = jnp.dot(p.astype(BF16), g_t[...], preferred_element_type=F32)
                dp = jnp.dot(v_rows, gs[...], preferred_element_type=F32)
                ds = (p * (dp - delta[...])).astype(BF16)
                dk = jnp.dot(ds, q_t[...], preferred_element_type=F32)
                dq[...] += jnp.dot(k_cols, ds, preferred_element_type=F32)
                pair_low[1, :, at] = dk.T.astype(BF16)
                pair_low[2, :, at] = dv.T.astype(BF16)

            if i < 3:
                back(late, sem.ksem, i, z).start()
            if i == 0:
                step(*[down] * (3 - len(EARLY)))
            if i == 2:
                step(up)
        pair_low[0] = (dq[...] * scale).astype(BF16)
        for i in range(3):
            back(pl.ds(0, 1), sem.qsem, i, (o + 1 + i) % 4).start()
        dqkv[:, o % 2, :, mine] = pair_low[:, :, pl.ds(pl.multiple_of(o * n, n), n)]
        step(down, up)
        for i in range(3):
            z = (o + 3 - i) % 4
            there = pl.ds(pl.multiple_of((z // 2) * n, n), n)
            landed(dqkv.at[late, z % 2, :, there], sem.ksem, i)
            landed(dqkv.at[pl.ds(0, 1), z % 2, :, there], sem.qsem, i)

        all_dqkv = lambda: dqkv[...].reshape(width_qkv, 2 * n)

        def back_chunk(q):
            part = lax.dot_general(
                all_dqkv(),
                src.qkv_own[q * w : (q + 1) * w],
                (((0,), (1,)), ((), ())),
                preferred_element_type=F32,
            )
            partial[:, :, :, q * w : (q + 1) * w] = part.astype(BF16).reshape(seqs, 8, r, w)

        def chunk(q):
            cols = pl.ds(q * w, w)
            scatter, (zsem, ysem, csem) = pick_refs(chunk_ids[q][0]), pick_refs(chunk_ids[q][1])
            back_chunk(q)
            yield from scatter_steps(
                lambda i, slot: partial.at[i, slot, :, cols],
                lambda i: grad_ref.at[i, :, cols],
                *scatter,
            )
            grad = grad_ref[:, :, cols] + m.resid[:, :, cols]
            grad_ref[:, :, cols] = grad
            grad = grad.reshape(own_rows, w)
            m.own[q] = grad.astype(BF16)
            second = src.second[...]
            m.sums[6:7, cols] = jnp.sum(grad * (1.0 - second), axis=0, keepdims=True)
            m.sums[7:8, cols] = jnp.sum(grad * second, axis=0, keepdims=True)
            yield from blk_gather_steps(
                m.own.at[q],
                lambda z, yy, cc: m.gathered.at[q, blk(z, yy, cc)],
                zsem,
                ysem,
                csem,
            )

            @pl.loop(0, slots // 128)
            def _(k):
                some = pl.ds(pl.multiple_of(k * 128, 128), 128)
                found = jnp.dot(
                    m.pick[some],
                    m.gathered[q].reshape(blks * own_rows, w),
                    preferred_element_type=F32,
                )
                pos_ref[some, cols] = found
                m.pos_low[q, some] = found.astype(BF16)

            copy = remote(
                m.pos_low.at[q], m.pos_held.at[q], sem.pair_sem, q, peer(*NEAR_X)
            )
            copy.start()
            pairs.append(copy)
            yield

        pairs = []
        active, waiting = [], [chunk(q) for q in range(chunks)]
        turn = 0
        while active or waiting:
            if waiting and turn % chunk_lag == 0:
                active.append(waiting.pop(0))
            for gen in list(active):
                try:
                    next(gen)
                except StopIteration:
                    active.remove(gen)
            if turn == 0:
                @pl.loop(0, planes)
                def _(z):
                    cols = pl.ds(pl.multiple_of(z * 4 * e, 4 * e), 4 * e)
                    part = lax.dot_general(
                        src.plane_low[:, :, :, cols].reshape(seqs * rows, 4 * e),
                        all_dqkv(),
                        (((0,), (1,)), ((), ())),
                        preferred_element_type=F32,
                    )
                    m.qkv_part[z] = part.astype(BF16)

                step(qkv)
                ones = jnp.ones((8, 2 * n), BF16)
                heads = dot_nt(ones, all_dqkv())
                own_lanes = pl.ds(pl.multiple_of(t * 128, 128), 128)
                m.sums[8:9, own_lanes] = heads[0:1, 0:128]
                m.sums[9:10, own_lanes] = heads[0:1, 256:384]
                for i in range(4):
                    m.up_spots[pl.ds((i * 4 + g) * 2 + h, 1)] = m.up_sums[
                        :, i * 128 : (i + 1) * 128
                    ]
            for when, gen in zip(TURNS, (up, qkv, out)):
                if turn in when:
                    step(gen)
            turn += 1
        for b in range(blks):
            m.pack[b, 0:16] = m.sums[:, b // 2 * 128 : (b // 2 + 1) * 128]
            m.pack[b, 16:18] = m.up_spots[2 * b : 2 * b + 2]
            m.pack[b, 18:24] = jnp.zeros((6, 128), F32)
        copies = []
        for k, p in enumerate(ALL):
            to = peer(*p)
            copy = remote(m.pack.at[to[1]], m.packs.at[k], sem.pack_sem, k, to)
            copy.start()
            copies.append(copy)
        for gen in (down, up, out, qkv):
            for _ in gen:
                pass
        for q, copy in enumerate(pairs):
            copy.wait()
            cols = pl.ds(q * w, w)
            pos_ref[:, cols] = pos_ref[:, cols] + m.pos_held[q].astype(F32)
        for copy in copies:
            copy.wait()
        totals[...] = m.pack[blk(o, y, c)] + jnp.sum(m.packs[...], axis=0)
        for i in range(3):
            back(late, sem.ksem, i, (o + 1 + i) % 4).wait_send()
            back(pl.ds(0, 1), sem.qsem, i, (o + 1 + i) % 4).wait_send()
        for s in range(seqs):
            for j in range(2):

                @pl.when(o != 2 * s + j)
                def _():
                    go_copy(s, j).wait_send()

    return Part(
        run,
        list(vars(x).values()),
        [
            ((seqs, r, d), BF16),
            ((seqs, r, d), F32),
            ((slots, d), F32),
            ((2, fcols, d), BF16),
            ((e, 8 * f), BF16),
            ((e, 3 * d), BF16),
            ((he, d), BF16),
            ((24, 128), F32),
        ],
        need,
        ALL,
    )


def rows_steps(own_of, near, part, from_y, term, ends, mids, last, csem, ysem, zsem, out):
    h, o, y, c = place()
    at, seen = mirrored()
    dev_y = peer(*NEAR_Y)
    order = [seen(3), seen(2), seen(1 - at), o]
    end, inner, other = (h, blk(seen(0), y, c)), (h, blk(seen(1), y, c)), (h, blk(seen(2), y, c))
    sent = []
    for j, z in enumerate(order):
        landed(near.at[0, j], csem, j)
        part[j] = own_of(z, 1 - y)[...] + near[0, j]
        copy = remote(part.at[j], from_y.at[j], ysem, j, dev_y)
        copy.start()
        sent.append(copy)
    for j, z in enumerate(order):
        yield
        landed(near.at[1, j], csem, 4 + j)
        landed(from_y.at[j], ysem, j)
        term[j] = own_of(z, y)[...] + near[1, j] + from_y[j]
        if j < 3:

            @pl.when(at == 0)
            def _():
                remote(term.at[j], ends.at[j], zsem, j, inner).start()

        if j < 2:

            @pl.when(at == 1)
            def _():
                landed(ends.at[j], zsem, j)
                term[j] += ends[j]
                remote(term.at[j], mids.at[j], zsem, 3 + j, other).start()

    yield

    @pl.when(at == 1)
    def _():
        landed(mids.at[0], zsem, 3)
        term[2] += mids[0]
        remote(term.at[2], last, zsem, 5, end).start()

    yield

    @pl.when(at == 1)
    def _():
        landed(ends.at[2], zsem, 2)
        landed(mids.at[1], zsem, 4)
        out[...] = (term[3] + ends[2] + mids[1]).astype(F32)
        for j in range(2):
            remote(term.at[j], mids.at[j], zsem, 3 + j, other).wait_send()
        remote(term.at[2], last, zsem, 5, end).wait_send()

    @pl.when(at == 0)
    def _():
        landed(last, zsem, 5)
        out[...] = (term[3] + last[...]).astype(F32)
        for j in range(3):
            remote(term.at[j], ends.at[j], zsem, j, inner).wait_send()

    for copy in sent:
        copy.wait_send()


def first_half(x, scale, lag):
    names = list(vars(x))
    seqs, r, d = x.hidden.shape
    slots = x.table.shape[0]
    e = x.qkv_weight.shape[0]
    four, wq, f = 4, x.qkv_weight.shape[1] // 8, x.up_weight.shape[1] // 8
    he = wq // 6
    n = 8 * r
    length = 4 * n
    half, fh = r // 2, f // 2
    blks = 16
    cols = 256
    small = small_gather(jax.ShapeDtypeStruct((8, 128), F32))
    outw = out_weights(x.out_weight)
    need = []

    def many(specs):
        start = len(need)
        need.extend(specs)
        return list(range(start, len(need)))

    block = (r, d)
    shapes = dict(
        packed=((8, 128), F32),
        everyone=((blks, 8, 128), F32),
        found=((4, 2, 2, seqs, r, d), BF16),
        rows=((seqs, r, d), F32),
        low=((seqs, r, d), BF16),
        qkv_in=((four, e, wq), BF16),
        projected=((3, 2, he, 2 * n), BF16),
        keys=((length, he), BF16),
        pair_low=((he, length), BF16),
    )
    ids = {k: many([pltpu.VMEM(*v)])[0] for k, v in shapes.items()}
    counts = dict(qkv_sem=6, up_sem=6, back_sem=3, qkv_trade=9, up_trade=12)
    sem_ids = {k: many([sems(v)])[0] for k, v in counts.items()}
    for k in ("send", "recv"):
        sem_ids[k] = many([pltpu.SemaphoreType.DMA((4,))])[0]
    small_ids, outw_ids = many(small.scratch), many(outw.scratch)
    row_ids = [
        many(
            [
                pltpu.VMEM((2, 4) + block, BF16),
                pltpu.VMEM((4,) + block, BF16),
                pltpu.VMEM((4,) + block, BF16),
                pltpu.VMEM((4,) + block, BF16),
                pltpu.VMEM((3,) + block, BF16),
                pltpu.VMEM((2,) + block, BF16),
                pltpu.VMEM(block, BF16),
                sems(8),
                sems(4),
                sems(6),
            ]
        )
        for _ in range(seqs)
    ]
    gather_ids = [many([sems(14)])[0] for _ in range(seqs)]

    def run(ins, outs, own):
        src = SimpleNamespace(**dict(zip(names, ins)))
        attended, held, o_ref, lse_ref, emb_ref, plane_ref, qkv_ref = outs[:7]
        outw_ref, up_one, up_in, vec_ref, bias_ref, ids_ref, second_ref = outs[7:]
        m = SimpleNamespace(**{k: own[v] for k, v in ids.items()})
        sem = SimpleNamespace(**{k: own[v] for k, v in sem_ids.items()})
        pick_refs = lambda some: [own[i] for i in some]
        h, o, y, c = place()
        g = y * 2 + c
        t = h * 4 + g
        side = lambda a: jnp.concatenate([a[0:1], a[1:2]], axis=1).astype(F32)
        for k in range(3):
            m.packed[k : k + 1] = side(src.biases[2 * k : 2 * k + 2])
        m.packed[3:4] = side(src.gains[...])
        m.packed[4:5] = side(src.types[...])
        m.packed[5:7] = src.up_bias[...].astype(F32)
        m.packed[7:8] = side(src.pos_ids[...])
        gather_small = small.run((m.packed,), (m.everyone,), pick_refs(small_ids))
        trades = []

        def trade(ref, dst, s, lanes_of):
            count = len(lanes_of(0))
            for k, p in enumerate(((0, 0, 1, 0), (0, 0, 0, 1), (0, 0, 1, 1))):
                to = (1 - y if p[2] else y) * 2 + (1 - c if p[3] else c)
                for i, lane in enumerate(lanes_of(to)):
                    copy = remote(
                        ref.at[:, pl.ds(pl.multiple_of(lane * 128, 128), 128)],
                        dst.at[g, :, pl.ds(i * 128, 128)],
                        s,
                        k * count + i,
                        peer(*p),
                    )
                    copy.start()
                    trades.append(copy)
            for i, lane in enumerate(lanes_of(g)):
                dst[g, :, i * 128 : (i + 1) * 128] = ref[
                    :, pl.ds(pl.multiple_of(lane * 128, 128), 128)
                ]

        weights = outw.run((src.out_weight,), (outw_ref,), pick_refs(outw_ids))
        qkv_lanes = lambda k: [i * 8 + h * 4 + k for i in range(3)]
        up_lanes = lambda k: [(i * 4 + k) * 2 + h for i in range(4)]
        trade(src.qkv_weight, m.qkv_in, sem.qkv_trade, qkv_lanes)
        next(gather_small)
        yield
        next(weights)
        trade(src.up_weight, up_in, sem.up_trade, up_lanes)
        qkv_line = line_gather_steps(m.qkv_in, lambda z: qkv_ref.at[z], sem.qkv_sem)
        up_first = up_in.at[:, :, pl.ds(0, fh)]
        up_line = line_gather_steps(up_first, lambda z: up_one.at[z], sem.up_sem)

        for _ in gather_small:
            pass

        at, seen = mirrored()
        order = [seen(3), seen(2), seen(1 - at), o]
        b = blk(o, y, c)
        row = lax.broadcasted_iota(jnp.int32, (slots, 1), 0).astype(F32)
        base = (b * slots).astype(F32)
        streams = [pick_refs(i) for i in row_ids]
        core = []
        for i, yy in enumerate((1 - y, y)):
            for j, z in enumerate(order):
                hot = jnp.concatenate(
                    [
                        (m.everyone[blk(z, yy, cc), 7:8] - base == row).astype(F32).astype(BF16)
                        for cc in range(2)
                    ],
                    axis=1,
                )
                rows_of = dot_tn(hot, src.table[...]).astype(BF16)
                m.found[z, yy] = rows_of.reshape(2, seqs, r, d)
                for s in range(seqs):
                    near, csem = streams[s][0], streams[s][7]
                    copy = remote(
                        m.found.at[z, yy, 1 - c, s],
                        near.at[i, j],
                        csem,
                        i * 4 + j,
                        peer(*NEAR_C),
                    )
                    copy.start()
                    core.append(copy)
            if i == 0:
                for copy in trades:
                    copy.wait()
                next(qkv_line)

        lane = lax.broadcasted_iota(jnp.int32, (1, 128), 1)
        for k in range(5):
            for i in range(blks // 2):
                one, two = m.everyone[2 * i, k : k + 1], m.everyone[2 * i + 1, k : k + 1]
                lanes = slice(i * 128, (i + 1) * 128)
                vec_ref[2 * k : 2 * k + 1, lanes] = jnp.where(
                    lane < 64, one, pltpu.roll(two, 64, 1)
                )
                vec_ref[2 * k + 1 : 2 * k + 2, lanes] = jnp.where(
                    lane < 64, pltpu.roll(one, 64, 1), two
                )
        for i in range(blks):
            ids_ref[:, i * 128 : (i + 1) * 128] = (m.everyone[i, 7:8] - base).astype(jnp.int32)
        for i in range(4):
            bias_ref[:, i * 128 : (i + 1) * 128] = m.everyone[i * 4 + g, pl.ds(5 + h, 1)]
        eye = lax.broadcasted_iota(jnp.int32, (128, 128), 0) == lax.broadcasted_iota(
            jnp.int32, (128, 128), 1
        )

        def upright(lanes):
            return jnp.sum(jnp.where(eye, lanes, 0.0), axis=1, keepdims=True)

        def column(k):
            return upright(vec_ref[k : k + 1, pl.ds(pl.multiple_of(t * 128, 128), 128)])

        second_ref[...] = upright(side(src.type_ids[...]))

        def send_pair(s, j):
            z = 2 * s + j
            return place_copy(
                m.projected.at[:, j, :, pl.ds(s * n, n)],
                held.at[:, :, pl.ds(pl.multiple_of(o * n, n), n)],
                sem.send.at[z],
                sem.recv.at[o],
                (h, z * 4 + g),
            )

        def stream(s):
            yield from rows_steps(
                lambda z, yy: m.found.at[z, yy, c, s], *streams[s], m.rows.at[s]
            )
            if s == seqs - 1:
                next(up_line)
            second = second_ref[s * r : (s + 1) * r]
            typed = vec_ref[8:9] * (1.0 - second) + vec_ref[9:10] * second
            value = src.hidden[s].astype(F32) + m.rows[s] + typed
            emb_ref[s] = value
            m.low[s] = value.astype(BF16)
            yield from gather_steps(
                lambda i: m.low.at[s, pl.ds(i * half, half)],
                lambda i, slot: plane_ref.at[s, slot, pl.ds(i * half, half)],
                own[gather_ids[s]],
            )
            if s == 0:
                for _ in qkv_line:
                    pass
            part = lax.dot_general(
                qkv_ref[...].reshape(d, wq),
                plane_ref[s].reshape(n, d),
                (((0,), (1,)), ((), ())),
                preferred_element_type=F32,
            )
            here = slice(s * n, (s + 1) * n)
            third = wq // 3
            m.projected[0, :, :, here] = (part[:third] + column(0)).astype(BF16).reshape(2, he, n)
            m.projected[1, :, :, here] = part[third : 2 * third].astype(BF16).reshape(2, he, n)
            m.projected[2, :, :, here] = (
                (part[2 * third :] + column(1)).astype(BF16).reshape(2, he, n)
            )
            for j in range(2):

                @pl.when(o != 2 * s + j)
                def _():
                    send_pair(s, j).start()

                @pl.when(o == 2 * s + j)
                def _():
                    held[:, :, pl.ds(pl.multiple_of(o * n, n), n)] = m.projected[:, j, :, here]

            yield

        gens = [stream(s) for s in range(seqs)]
        for _ in range(lag):
            next(gens[0])
        turn = 0
        while gens:
            for gen in list(gens):
                try:
                    next(gen)
                except StopIteration:
                    gens.remove(gen)
            if turn in QKV_TURNS:
                next(qkv_line, None)
            if turn in UP_TURNS:
                next(up_line, None)
            turn += 1

        for z in range(4):

            @pl.when(z != o)
            def _():
                ref = held.at[:, :, pl.ds(z * n, n)]
                place_copy(ref, ref, sem.send.at[0], sem.recv.at[z], peer(*NEAR_X)).wait_recv()

        m.keys[...] = held[1].astype(F32).T.astype(BF16)
        mine = pl.ds(pl.multiple_of((o // 2) * n, n), n)

        def back(i, z):
            return remote(
                m.pair_low.at[:, pl.ds(pl.multiple_of(z * n, n), n)],
                attended.at[o % 2, :, mine],
                sem.back_sem,
                i,
                (h, z * 4 + g),
            )

        @pl.loop(0, 4 * (n // cols))
        def _(step):
            i = step // (n // cols)
            z = (o + 1 + i) % 4
            here = pl.ds(pl.multiple_of(z * n + step % (n // cols) * cols, cols), cols)
            q = (held[0, :, here].astype(F32) * scale).astype(BF16)
            s = jnp.dot(m.keys[...], q, preferred_element_type=F32)
            peak = jnp.max(s, axis=0, keepdims=True)
            p = jnp.exp(s - peak)
            total = jnp.sum(p, axis=0, keepdims=True)
            out = jnp.dot(held[2], p.astype(BF16), preferred_element_type=F32) / total
            o_ref[:, here] = out
            m.pair_low[:, here] = out.astype(BF16)
            lse_ref[:, here] = peak + jnp.log(total)

            @pl.when((step % (n // cols) == n // cols - 1) & (i < 3))
            def _():
                back(i, z).start()

        attended[o % 2, :, mine] = m.pair_low[:, pl.ds(pl.multiple_of(o * n, n), n)]
        for i in range(3):
            back(i, (o + 1 + i) % 4).wait_send()
            z = (o + 3 - i) % 4
            landed(attended.at[z % 2, :, pl.ds(pl.multiple_of((z // 2) * n, n), n)], sem.back_sem, i)
        for _ in weights:
            pass
        for _ in up_line:
            pass
        for copy in core:
            copy.wait_send()
        for s in range(seqs):
            for j in range(2):

                @pl.when(o != 2 * s + j)
                def _():
                    send_pair(s, j).wait_send()

    return Part(
        run,
        list(vars(x).values()),
        [
            ((2, he, 2 * n), BF16),
            ((3, he, length), BF16),
            ((he, length), F32),
            ((1, length), F32),
            ((seqs, r, d), F32),
            ((seqs, 8, r, d), BF16),
            ((4, four, e, wq), BF16),
            ((2,) + x.out_weight.shape, BF16),
            ((4, four, e, fh), BF16),
            ((four, e, f), BF16),
            ((10, d), F32),
            ((1, f), F32),
            ((1, blks * seqs * r), jnp.int32),
            ((seqs * r, 1), F32),
        ],
        need,
        ALL,
    )


def finish_kernel(odd, layer, hid, pos, down, up, qkv, out, totals, *outs):
    o_layer, o_hid, o_pos, o_types, o_qkv, o_out, o_up, o_down, o_upb, o_gains, o_bias = outs
    o_layer[...] = layer[...]
    o_hid[...] = hid[...]
    o_pos[...] = pos[...]
    o_qkv[...] = qkv[...].astype(F32)
    o_out[...] = out[...].astype(F32)
    o_up[...] = up[...].astype(F32)
    o_down[...] = down[...].astype(F32)
    t = totals[...]
    mine = jnp.where(odd[0] == 1, t[:, 64:], t[:, :64])
    o_types[...] = mine[6:8]
    o_gains[...] = mine[4:6]
    o_bias[0:1] = mine[8:9]
    o_bias[1:2] = mine[9:10]
    o_bias[2:6] = mine[0:4]
    o_upb[...] = t[16:18]


def finish(odd, layer, hid, pos, down, up, qkv, out, totals, steps=4):
    e = out.shape[0]
    large = [(layer, BF16), (hid, F32), (pos, F32), (qkv, F32), (out, F32), (up, F32), (down, F32)]

    def cut(a):
        return pl.BlockSpec((a.shape[0] // steps, a.shape[1]), lambda i: (i, 0))

    def whole(*shape):
        return pl.BlockSpec(shape, lambda i: (0, 0))

    like = {id(a): jax.ShapeDtypeStruct(a.shape, dtype) for a, dtype in large}
    full = lambda *shape: jax.ShapeDtypeStruct(shape, F32)
    return pl.pallas_call(
        finish_kernel,
        name="finish",
        grid=(steps,),
        out_shape=[like[id(a)] for a in (layer, hid, pos)]
        + [full(2, e)]
        + [like[id(a)] for a in (qkv, out, up, down)]
        + [full(2, 128), full(2, e), full(6, e)],
        in_specs=[pl.BlockSpec(memory_space=pltpu.SMEM)]
        + [cut(a) for a in (layer, hid, pos, down, up, qkv, out)]
        + [whole(24, 128)],
        out_specs=[cut(a) for a in (layer, hid, pos)]
        + [whole(2, e)]
        + [cut(a) for a in (qkv, out, up, down)]
        + [whole(2, 128), whole(2, e), whole(6, e)],
    )(odd, layer, hid, pos, down, up, qkv, out, totals)


def norm_layer(values_in, gain_row, offset_row):
    average = jnp.mean(values_in, axis=-1, keepdims=True)
    centred = values_in - average
    variance = jnp.mean(centred * centred, axis=-1, keepdims=True)
    return centred * lax.rsqrt(variance + 1e-12) * gain_row + offset_row


def gelu_exact(inner_product_sum):
    return jax.nn.gelu(inner_product_sum, approximate=False)


def widest_block(length, limit):
    return max(
        (candidate for candidate in range(1, min(length, limit) + 1) if length % candidate == 0)
    )


def block_scores(query_heads, key_block, score_scale):
    return (
        jnp.einsum("sqhe,skhe->shqk", query_heads, key_block, preferred_element_type=jnp.float32)
        * score_scale
    )


def key_side(query_block, grad_block, lse_block, delta_block, key_heads, value_heads, score_scale):
    scores = block_scores(query_block, key_heads, score_scale)
    weights = jnp.exp(scores - lse_block[..., None])
    more_values = jnp.einsum(
        "shqk,sqhe->shke",
        weights.astype(jnp.bfloat16),
        grad_block,
        preferred_element_type=jnp.float32,
    )
    grad_weights = jnp.einsum(
        "sqhe,skhe->shqk", grad_block, value_heads, preferred_element_type=jnp.float32
    )
    grad_scores = weights * (grad_weights - delta_block[..., None])
    more_keys = jnp.einsum(
        "shqk,sqhe->shke",
        grad_scores.astype(jnp.bfloat16),
        query_block,
        preferred_element_type=jnp.float32,
    )
    return (more_keys, more_values)


def forward_fold(query_heads, score_scale, head_count, head_size):

    def fold_keys(running, portion, offset):
        key_piece, value_piece = portion
        seq_count, length = (key_piece.shape[0], key_piece.shape[1])
        block_size = widest_block(length, 512)

        def one_step(block_index, carried):
            row_peak, row_total, weighted = carried
            row_start = block_index * block_size
            key_block = lax.dynamic_slice_in_dim(key_piece, row_start, block_size, 1).reshape(
                seq_count, block_size, head_count, head_size
            )
            value_block = lax.dynamic_slice_in_dim(value_piece, row_start, block_size, 1).reshape(
                seq_count, block_size, head_count, head_size
            )
            scores = block_scores(query_heads, key_block, score_scale)
            new_peak = jnp.maximum(row_peak, jnp.max(scores, axis=-1))
            shrink = jnp.exp(row_peak - new_peak)
            weights = jnp.exp(scores - new_peak[..., None])
            row_total = row_total * shrink + jnp.sum(weights, axis=-1)
            weighted = weighted * shrink[..., None] + jnp.einsum(
                "shqk,skhe->shqe",
                weights.astype(jnp.bfloat16),
                value_block,
                preferred_element_type=jnp.float32,
            )
            return (new_peak, row_total, weighted)

        return lax.fori_loop(0, length // block_size, one_step, running)

    return fold_keys


def query_fold(query_heads, grad_heads, log_totals, delta_rows, score_scale, head_count, head_size):

    def fold_keys(running, portion, offset):
        key_piece, value_piece = portion
        seq_count, length = (key_piece.shape[0], key_piece.shape[1])
        block_size = widest_block(length, 512)

        def one_step(block_index, weighted):
            row_start = block_index * block_size
            key_block = lax.dynamic_slice_in_dim(key_piece, row_start, block_size, 1).reshape(
                seq_count, block_size, head_count, head_size
            )
            value_block = lax.dynamic_slice_in_dim(value_piece, row_start, block_size, 1).reshape(
                seq_count, block_size, head_count, head_size
            )
            scores = block_scores(query_heads, key_block, score_scale)
            weights = jnp.exp(scores - log_totals[..., None])
            grad_weights = jnp.einsum(
                "sqhe,skhe->shqk", grad_heads, value_block, preferred_element_type=jnp.float32
            )
            grad_scores = weights * (grad_weights - delta_rows[..., None])
            return weighted + jnp.einsum(
                "shqk,skhe->shqe",
                grad_scores.astype(jnp.bfloat16),
                key_block,
                preferred_element_type=jnp.float32,
            )

        return lax.fori_loop(0, length // block_size, one_step, running)

    return fold_keys


def key_fold(key_heads, value_heads, score_scale, head_count, head_size):

    def fold_queries(running, portion, offset):
        query_piece, grad_piece, lse_piece, delta_piece = portion
        seq_count, length = (query_piece.shape[0], query_piece.shape[1])
        block_size = widest_block(length, 512)

        def one_step(block_index, carried):
            grad_keys, grad_values = carried
            row_start = block_index * block_size
            query_block = lax.dynamic_slice_in_dim(query_piece, row_start, block_size, 1).reshape(
                seq_count, block_size, head_count, head_size
            )
            grad_block = lax.dynamic_slice_in_dim(grad_piece, row_start, block_size, 1).reshape(
                seq_count, block_size, head_count, head_size
            )
            lse_block = lax.dynamic_slice_in_dim(lse_piece, row_start, block_size, 1).transpose(
                0, 2, 1
            )
            delta_block = lax.dynamic_slice_in_dim(delta_piece, row_start, block_size, 1).transpose(
                0, 2, 1
            )
            more_keys, more_values = key_side(
                query_block, grad_block, lse_block, delta_block, key_heads, value_heads, score_scale
            )
            return (grad_keys + more_keys, grad_values + more_values)

        return lax.fori_loop(0, length // block_size, one_step, running)

    return fold_queries


def layer_in_blocks(
    hidden,
    pos_ids,
    type_ids,
    cotangent,
    pos_table,
    type_table,
    query_key_value_weight,
    attention_output_weight,
    up_projection_weight,
    down_projection_weight,
    up_projection_bias,
    norm_gains,
    biases,
):
    seq_count, seg_tokens, model_width = hidden.shape
    row_count = seq_count * seg_tokens
    head_count = HEADS // lax.axis_size("head")
    head_size = model_width // HEADS
    local_width = head_count * head_size
    query_rows = lax.axis_size("head") * seg_tokens
    score_scale = 1.0 / math.sqrt(head_size)

    def fetch_weights():
        return (
            lax.all_gather(query_key_value_weight, "blk", axis=0, tiled=True),
            lax.all_gather(attention_output_weight, "blk", axis=0, tiled=True),
            lax.all_gather(up_projection_weight, "blk", axis=0, tiled=True),
            lax.all_gather(down_projection_weight, "blk", axis=0, tiled=True),
            lax.all_gather(up_projection_bias, "blk", axis=0, tiled=True),
            lax.all_gather(norm_gains, "blk", axis=1, tiled=True),
            lax.all_gather(biases, "blk", axis=1, tiled=True),
            lax.all_gather(type_table, "blk", axis=1, tiled=True),
        )

    qkv_full, out_full, up_full, down_full, up_bias_full, gain_full, bias_full, type_full = (
        fetch_weights()
    )
    bias_float = bias_full.astype(jnp.float32)
    gain_float = gain_full.astype(jnp.float32)
    flat_pos = pos_ids.reshape(row_count)
    portion = lax.all_gather(pos_table, "blk", axis=0, tiled=True)
    local_slots = flat_pos
    onehot = (
        local_slots[:, None] == jnp.arange(portion.shape[0], dtype=jnp.int32)[None, :]
    ).astype(jnp.bfloat16)
    positions = jnp.dot(onehot, portion, preferred_element_type=jnp.float32)
    is_second = type_ids.reshape(row_count, 1) == 1
    typed_rows = jnp.where(
        is_second, type_full[1].astype(jnp.float32), type_full[0].astype(jnp.float32)
    )
    embedded_tokens = (
        hidden.reshape(row_count, model_width).astype(jnp.float32) + positions + typed_rows
    )
    embedded_low = embedded_tokens.astype(jnp.bfloat16)
    projected_rows = jnp.dot(embedded_low, qkv_full, preferred_element_type=jnp.float32)
    token_shape = (seq_count, seg_tokens, model_width)
    queries = (
        (projected_rows[:, :model_width] + bias_float[0]).astype(jnp.bfloat16).reshape(token_shape)
    )
    keys_token = (
        projected_rows[:, model_width : 2 * model_width].astype(jnp.bfloat16).reshape(token_shape)
    )
    values_token = (
        (projected_rows[:, 2 * model_width :] + bias_float[1])
        .astype(jnp.bfloat16)
        .reshape(token_shape)
    )
    query_local, key_local, value_local = (
        lax.all_to_all(queries, "head", split_axis=2, concat_axis=1, tiled=True),
        lax.all_to_all(keys_token, "head", split_axis=2, concat_axis=1, tiled=True),
        lax.all_to_all(values_token, "head", split_axis=2, concat_axis=1, tiled=True),
    )
    head_shape = (seq_count, query_rows, head_count, head_size)
    query_heads = query_local.reshape(head_shape)
    key_heads = key_local.reshape(head_shape)
    value_heads = value_local.reshape(head_shape)
    start_peak = jnp.full((seq_count, head_count, query_rows), -jnp.inf, jnp.float32)
    start_total = jnp.zeros((seq_count, head_count, query_rows), jnp.float32)
    zero_heads = jnp.zeros((seq_count, head_count, query_rows, head_size), jnp.float32)
    fold_keys = forward_fold(query_heads, score_scale, head_count, head_size)
    row_peak, row_total, weighted = fold_keys(
        (start_peak, start_total, zero_heads),
        (
            lax.all_gather(key_local, "blk", axis=1, tiled=True),
            lax.all_gather(value_local, "blk", axis=1, tiled=True),
        ),
        jnp.int32(0),
    )
    log_totals = row_peak + jnp.log(row_total)
    attention_result = weighted / row_total[..., None]
    attended_low = (
        attention_result.transpose(0, 2, 1, 3)
        .reshape(seq_count, query_rows, local_width)
        .astype(jnp.bfloat16)
    )
    attended_token = lax.all_to_all(
        attended_low, "head", split_axis=1, concat_axis=2, tiled=True
    ).reshape(row_count, model_width)
    residual_branch = (
        jnp.dot(attended_token, out_full, preferred_element_type=jnp.float32) + bias_float[2]
    )
    first_layer_norm, first_pull = jax.vjp(
        norm_layer, embedded_tokens + residual_branch, gain_float[0], bias_float[3]
    )
    first_low = first_layer_norm.astype(jnp.bfloat16)
    inner_product_sum = jnp.dot(
        first_low, up_full, preferred_element_type=jnp.float32
    ) + up_bias_full.astype(jnp.float32)
    gelu_activations, gelu_pull = jax.vjp(gelu_exact, inner_product_sum)
    activated_low = gelu_activations.astype(jnp.bfloat16)
    second_layer_norm = (
        jnp.dot(activated_low, down_full, preferred_element_type=jnp.float32) + bias_float[4]
    )
    final_norm, final_pull = jax.vjp(
        norm_layer, first_layer_norm + second_layer_norm, gain_float[1], bias_float[5]
    )
    layer_out = final_norm.astype(jnp.bfloat16).reshape(token_shape)
    qkv_full, out_full, up_full, down_full, up_bias_full, gain_full, bias_full, type_full = (
        fetch_weights()
    )
    grad_final, grad_gain_two, grad_shift_two = final_pull(
        cotangent.reshape(row_count, model_width).astype(jnp.float32)
    )
    grad_second = grad_final.astype(jnp.bfloat16)
    grad_down = jnp.einsum(
        "rf,rd->fd", activated_low, grad_second, preferred_element_type=jnp.float32
    )
    grad_bias_second = jnp.sum(grad_second.astype(jnp.float32), axis=0)
    (grad_inner,) = gelu_pull(
        jnp.einsum("rd,fd->rf", grad_second, down_full, preferred_element_type=jnp.float32)
    )
    grad_inner_low = grad_inner.astype(jnp.bfloat16)
    grad_up = jnp.einsum("rd,rf->df", first_low, grad_inner_low, preferred_element_type=jnp.float32)
    grad_up_bias = jnp.sum(grad_inner_low.astype(jnp.float32), axis=0)
    grad_first = grad_final + jnp.einsum(
        "rf,df->rd", grad_inner_low, up_full, preferred_element_type=jnp.float32
    )
    grad_resid, grad_gain_one, grad_shift_one = first_pull(grad_first)
    grad_branch = grad_resid.astype(jnp.bfloat16)
    grad_out = jnp.einsum(
        "re,rd->ed", attended_token, grad_branch, preferred_element_type=jnp.float32
    )
    grad_bias_branch = jnp.sum(grad_branch.astype(jnp.float32), axis=0)
    grad_attended = (
        jnp.einsum("rd,ed->re", grad_branch, out_full, preferred_element_type=jnp.float32)
        .astype(jnp.bfloat16)
        .reshape(token_shape)
    )
    grad_local = lax.all_to_all(grad_attended, "head", split_axis=2, concat_axis=1, tiled=True)
    grad_heads = grad_local.reshape(head_shape)
    delta_rows = jnp.sum(
        grad_heads.astype(jnp.float32).transpose(0, 2, 1, 3) * attention_result, axis=-1
    )
    fold_queries = query_fold(
        query_heads, grad_heads, log_totals, delta_rows, score_scale, head_count, head_size
    )
    grad_query_sum = fold_queries(
        zero_heads,
        (
            lax.all_gather(key_local, "blk", axis=1, tiled=True),
            lax.all_gather(value_local, "blk", axis=1, tiled=True),
        ),
        jnp.int32(0),
    )
    fold_side = key_fold(key_heads, value_heads, score_scale, head_count, head_size)
    grad_key_sum, grad_value_sum = fold_side(
        (zero_heads, zero_heads),
        (
            lax.all_gather(query_local.astype(jnp.float32), "blk", axis=1, tiled=True).astype(
                jnp.bfloat16
            ),
            lax.all_gather(grad_local.astype(jnp.float32), "blk", axis=1, tiled=True).astype(
                jnp.bfloat16
            ),
            lax.all_gather(log_totals.transpose(0, 2, 1), "blk", axis=1, tiled=True),
            lax.all_gather(delta_rows.transpose(0, 2, 1), "blk", axis=1, tiled=True),
        ),
        jnp.int32(0),
    )
    grad_keys_local = (
        (grad_key_sum * score_scale)
        .transpose(0, 2, 1, 3)
        .reshape(seq_count, query_rows, local_width)
        .astype(jnp.bfloat16)
    )
    grad_values_local = (
        grad_value_sum.transpose(0, 2, 1, 3)
        .reshape(seq_count, query_rows, local_width)
        .astype(jnp.bfloat16)
    )
    grad_query_local = (
        (grad_query_sum * score_scale)
        .transpose(0, 2, 1, 3)
        .reshape(seq_count, query_rows, local_width)
        .astype(jnp.bfloat16)
    )
    grad_query_token, grad_key_token, grad_value_token = (
        lax.all_to_all(grad_query_local, "head", split_axis=1, concat_axis=2, tiled=True),
        lax.all_to_all(grad_keys_local, "head", split_axis=1, concat_axis=2, tiled=True),
        lax.all_to_all(grad_values_local, "head", split_axis=1, concat_axis=2, tiled=True),
    )
    grad_qkv = jnp.concatenate(
        [grad_query_token, grad_key_token, grad_value_token], axis=-1
    ).reshape(row_count, 3 * model_width)
    grad_qkv_full = jnp.einsum(
        "rd,rf->df", embedded_low, grad_qkv, preferred_element_type=jnp.float32
    )
    grad_bias_query = jnp.sum(
        grad_query_token.astype(jnp.float32).reshape(row_count, model_width), axis=0
    )
    grad_bias_value = jnp.sum(
        grad_value_token.astype(jnp.float32).reshape(row_count, model_width), axis=0
    )
    grad_embedded = grad_resid + jnp.einsum(
        "rf,df->rd", grad_qkv, qkv_full, preferred_element_type=jnp.float32
    )
    second_mask = is_second.astype(jnp.float32)
    grad_type_one = jnp.sum(grad_embedded * second_mask, axis=0)
    grad_type_zero = jnp.sum(grad_embedded * (1.0 - second_mask), axis=0)
    length = lax.axis_size("blk") * pos_table.shape[0]
    local_slots = flat_pos
    inside = (local_slots >= 0) & (local_slots < length)
    slot_index = jnp.where(inside, local_slots, length)
    buffer = jnp.zeros((length + 1, model_width), jnp.float32).at[slot_index].add(grad_embedded)
    grad_positions = lax.psum_scatter(buffer[:length], "blk", scatter_dimension=0, tiled=True)
    gain_stack = jnp.stack([grad_gain_one, grad_gain_two])
    bias_stack = jnp.stack(
        [
            grad_bias_query,
            grad_bias_value,
            grad_bias_branch,
            grad_shift_one,
            grad_bias_second,
            grad_shift_two,
        ]
    )
    type_stack = jnp.stack([grad_type_zero, grad_type_one])
    (
        shard_qkv,
        shard_out,
        shard_up,
        shard_down,
        shard_up_bias,
        shard_gains,
        shard_biases,
        shard_types,
    ) = (
        lax.psum_scatter(grad_qkv_full, "blk", scatter_dimension=0, tiled=True),
        lax.psum_scatter(grad_out, "blk", scatter_dimension=0, tiled=True),
        lax.psum_scatter(grad_up, "blk", scatter_dimension=0, tiled=True),
        lax.psum_scatter(grad_down, "blk", scatter_dimension=0, tiled=True),
        lax.psum_scatter(grad_up_bias, "blk", scatter_dimension=0, tiled=True),
        lax.psum_scatter(gain_stack, "blk", scatter_dimension=1, tiled=True),
        lax.psum_scatter(bias_stack, "blk", scatter_dimension=1, tiled=True),
        lax.psum_scatter(type_stack, "blk", scatter_dimension=1, tiled=True),
    )
    (
        total_qkv,
        total_out,
        total_up,
        total_down,
        total_up_bias,
        total_gains,
        total_biases,
        total_types,
        total_positions,
    ) = lax.psum(
        (
            shard_qkv,
            shard_out,
            shard_up,
            shard_down,
            shard_up_bias,
            shard_gains,
            shard_biases,
            shard_types,
            grad_positions,
        ),
        "head",
    )
    grad_hidden = grad_embedded.reshape(token_shape)
    return (
        layer_out,
        grad_hidden,
        total_positions,
        total_types,
        total_qkv,
        total_out,
        total_up,
        total_down,
        total_up_bias,
        total_gains,
        total_biases,
    )


BIG = 56 << 20
WHOLE = 67043328
LAG = 1
CHUNKS = 4
CHUNK_LAG = 1
QKV_TURNS = (1, 3, 5)
UP_TURNS = (8, 9, 10)
EARLY = (1, 3)
TURNS = ((1, 3), (3, 5, 8, 11), (10, 14))


def layer_in_planes(
    hidden,
    pos_ids,
    type_ids,
    cotangent,
    pos_table,
    type_table,
    query_key_value_weight,
    attention_output_weight,
    up_projection_weight,
    down_projection_weight,
    up_projection_bias,
    norm_gains,
    biases,
):
    seqs, seg, width = hidden.shape
    b = lax.axis_index("blk")
    rows = seqs * seg
    e = width // HEADS
    scale = 1.0 / math.sqrt(e)
    slots = pos_table.shape[0]
    fcols = down_projection_weight.shape[0] // 2

    token_shape = (seqs, seg, width)
    begin = SimpleNamespace(
        biases=biases,
        gains=norm_gains,
        types=type_table,
        up_bias=up_projection_bias.reshape(2, 2 * e),
        pos_ids=pos_ids,
        type_ids=type_ids,
        qkv_weight=query_key_value_weight,
        out_weight=attention_output_weight,
        up_weight=up_projection_weight,
        table=pos_table,
        hidden=hidden,
    )
    (
        (
            attended,
            held,
            pair_out,
            lse,
            embedded,
            plane_low,
            qkv_own,
            out_own,
            up_one,
            up_cut,
            vectors,
            up_bias,
            pos_all,
            is_second,
        ),
    ) = fused("first_half", 0, [first_half(begin, scale, LAG)], WHOLE)
    parts = SimpleNamespace(
        attended=attended,
        out_own=out_own.reshape(2 * e, width),
        embedded=embedded,
        cotangent=cotangent,
        up_one=up_one,
        up_cut=up_cut,
        down_weight=down_projection_weight,
        up_bias=up_bias,
        vectors=vectors,
        held=held,
        pair_out=pair_out,
        lse=lse,
        qkv_own=qkv_own.reshape(width, 6 * e),
        plane_low=plane_low,
        ids=pos_all,
        second=is_second,
    )
    sizes = (slots, CHUNKS, CHUNK_LAG, scale)
    ((layer_out, grad_hidden, pos, down, up, qkv, out, totals),) = fused(
        "second_half", 4, [second_half(parts, sizes)], WHOLE
    )
    outs = finish(
        (b % 2).reshape(1),
        layer_out.reshape(rows, width),
        grad_hidden.reshape(rows, width),
        pos,
        down.reshape(2 * fcols, width),
        up,
        qkv,
        out,
        totals,
    )
    return (
        outs[0].reshape(token_shape),
        outs[1].reshape(token_shape),
        *outs[2:8],
        outs[8].reshape(4 * e),
        *outs[9:],
    )


def planes_fit(hidden, head_axis, blk_axis):
    seqs, seg, width = hidden.shape
    return head_axis == 2 and blk_axis == HEADS and seqs == 2 and seqs * seg == 2 * width // HEADS


def on_device(hidden, *rest):
    if planes_fit(hidden, lax.axis_size("head"), lax.axis_size("blk")):
        return layer_in_planes(hidden, *rest)
    return layer_in_blocks(hidden, *rest)


def solution(mesh):
    in_specs = (
        P(None, ("head", "blk"), None),
        P(None, ("head", "blk")),
        P(None, ("head", "blk")),
        P(None, ("head", "blk"), None),
        P("blk", None),
        P(None, "blk"),
        P("blk", None),
        P("blk", None),
        P("blk", None),
        P("blk", None),
        P("blk"),
        P(None, "blk"),
        P(None, "blk"),
    )
    out_specs = (
        P(None, ("head", "blk"), None),
        P(None, ("head", "blk"), None),
        P("blk", None),
        P(None, "blk"),
        P("blk", None),
        P("blk", None),
        P("blk", None),
        P("blk", None),
        P("blk"),
        P(None, "blk"),
        P(None, "blk"),
    )
    return jax.shard_map(
        on_device, mesh=mesh, in_specs=in_specs, out_specs=out_specs, check_vma=False
    )
```

```python
import functools
import math
from types import SimpleNamespace

import jax
import jax.numpy as jnp
from jax import lax
from jax.experimental import pallas as pl
from jax.experimental.pallas import tpu as pltpu
from jax.sharding import PartitionSpec as P

HEADS = 16
MESH = pl.DeviceIdType.MESH
F32 = jnp.float32
BF16 = jnp.bfloat16
VSPEC = pl.BlockSpec(memory_space=pltpu.VMEM)


def place():
    h = lax.axis_index("head")
    b = lax.axis_index("blk")
    return h, b // 4, (b // 2) % 2, b % 2


def blk(o, y, c):
    return (o * 2 + y) * 2 + c


def peer(dx, dz, dy, dc):
    h, o, y, c = place()
    flip = lambda v, d: 1 - v if d else v
    return flip(h, dx), blk((o + dz) % 4 if dz else o, flip(y, dy), flip(c, dc))


def remote(src, dst, sems, index, device):
    return pltpu.make_async_remote_copy(
        src_ref=src,
        dst_ref=dst,
        send_sem=sems.at[0, index],
        recv_sem=sems.at[1, index],
        device_id=device,
        device_id_type=MESH,
    )


def landed(ref, sems, index):
    remote(ref, ref, sems, index, peer(1, 0, 0, 0)).wait_recv()


def sems(count):
    return pltpu.SemaphoreType.DMA((2, count))


NEAR_X, NEAR_Y, NEAR_C = (1, 0, 0, 0), (0, 0, 1, 0), (0, 0, 0, 1)
COLUMN = ((0, 1, 0, 0), (0, 2, 0, 0), (0, 3, 0, 0))
PLANE = tuple(
    (dx, 0, dy, dc) for dx in range(2) for dy in range(2) for dc in range(2) if dx or dy or dc
)


class Part:
    def __init__(self, run, ins, outs, scratch, peers):
        self.run, self.ins, self.outs, self.scratch, self.peers = run, ins, outs, scratch, peers
        self.turns = ()

    def on(self, *turns):
        self.turns = turns
        return self


def fused(name, cid, parts, limit=None):
    peers = sorted({p for part in parts for p in part.peers})
    ins = [x for part in parts for x in part.ins]
    outs = [s for part in parts for s in part.outs]
    scratch = [s for part in parts for s in part.scratch]

    def kernel(*refs):
        in_refs, out_refs = refs[: len(ins)], refs[len(ins) : len(ins) + len(outs)]
        own = refs[len(ins) + len(outs) :]
        gens = []
        i = j = k = 0
        for part in parts:
            gens.append(
                part.run(
                    in_refs[i : i + len(part.ins)],
                    out_refs[j : j + len(part.outs)],
                    own[k : k + len(part.scratch)],
                )
            )
            i, j, k = i + len(part.ins), j + len(part.outs), k + len(part.scratch)
        barrier = pltpu.get_barrier_semaphore()
        for p in peers:
            pl.semaphore_signal(barrier, inc=1, device_id=peer(*p), device_id_type=MESH)
        pl.semaphore_wait(barrier, len(peers))
        for gen in gens:
            next(gen)
        for turn, _ in enumerate(gens[0]):
            for part, gen in zip(parts, gens):
                if turn in part.turns:
                    next(gen)
        for gen in gens[1:]:
            for _ in gen:
                pass

    got = pl.pallas_call(
        kernel,
        name=name,
        out_shape=[jax.ShapeDtypeStruct(s, d) for s, d in outs],
        in_specs=[VSPEC] * len(ins),
        out_specs=[VSPEC] * len(outs),
        scratch_shapes=scratch,
        compiler_params=pltpu.CompilerParams(
            collective_id=cid, has_side_effects=True, vmem_limit_bytes=limit
        ),
    )(*ins)
    result = []
    for part in parts:
        result.append(got[: len(part.outs)])
        got = got[len(part.outs) :]
    return result


def exchange(x, peers, out_lead, source, target):
    peers = list(peers)

    def coords(p):
        h, o, y, c = place()
        flip = lambda v, d: 1 - v if d else v
        return flip(h, p[0]), (o + p[1]) % 4 if p[1] else o, flip(y, p[2]), flip(c, p[3])

    def run(ins, outs, own):
        (x_ref,), (out_ref,), (sem,) = ins, outs, own
        me = place()
        copies = []
        for k, p in enumerate(peers):
            copy = remote(
                source(x_ref, coords(p)), target(out_ref, me), sem, k, peer(*p)
            )
            copy.start()
            copies.append(copy)
        yield
        target(out_ref, me)[...] = source(x_ref, me)[...]
        for copy in copies:
            copy.wait()

    return Part(run, [x], [(out_lead, x.dtype)], [sems(len(peers))], peers)


def small_gather(x):
    peers = [
        (0, dz, dy, dc) for dz in range(4) for dy in range(2) for dc in range(2) if dz or dy or dc
    ]
    return exchange(x, peers, (16,) + x.shape, lambda r, d: r, lambda r, s: r.at[blk(*s[1:])])


def place_copy(src, dst, send_sem, recv_sem, device):
    return pltpu.make_async_remote_copy(
        src_ref=src,
        dst_ref=dst,
        send_sem=send_sem,
        recv_sem=recv_sem,
        device_id=device,
        device_id_type=MESH,
    )


BLK = tuple(
    (0, dz, dy, dc) for dz in range(4) for dy in range(2) for dc in range(2) if dz or dy or dc
)


def out_weights(w):
    r, n = w.shape

    def run(ins, outs, own):
        (w_ref,), (out_ref,), (send, recv) = ins, outs, own
        h, o, y, c = place()
        has = o // 2 == h
        serves = (o % 2 == y) & (y == c)

        def each(act):
            for k in range(4):
                device = (h, blk((o + k) % 4, o % 2, y))
                copy = place_copy(w_ref, out_ref.at[c], send.at[k], recv.at[c], device)

                @pl.when(has if k else has & jnp.logical_not(serves))
                def _():
                    act(copy)

        each(lambda copy: copy.start())
        yield

        @pl.when(has & serves)
        def _():
            out_ref[pl.ds(c, 1)] = w_ref[...][None]

        each(lambda copy: copy.wait_send())
        for core in range(2):
            from_self = (o == 2 * h + y) & (y == c) & (c == core)
            ref = out_ref.at[core]

            @pl.when(jnp.logical_not(from_self))
            def _():
                place_copy(ref, ref, send.at[0], recv.at[core], (h, blk(o, y, c))).wait_recv()

    scratch = [pltpu.SemaphoreType.DMA((4,)), pltpu.SemaphoreType.DMA((2,))]
    return Part(run, [w], [((2, r, n), BF16)], scratch, BLK)


def mirrored():
    o = place()[1]
    far = o // 2
    seen = lambda v: v * (1 - 2 * far) + 3 * far
    return seen(o), seen


def gather_steps(src, dst, sem):
    h, o, y, c = place()
    dev_x, dev_y, dev_c = peer(*NEAR_X), peer(*NEAR_Y), peer(*NEAR_C)
    mine = h * 4 + y * 2 + c
    of_x = (1 - h) * 4 + y * 2 + c
    of_y = h * 4 + (1 - y) * 2 + c
    of_d = (1 - h) * 4 + (1 - y) * 2 + c
    flip = 1 - 2 * c
    sent = []

    def go(ref, slot, half, index, device):
        copy = remote(ref, dst(half, slot), sem, index, device)
        copy.start()
        sent.append(copy)

    go(src(0), mine, 0, 0, dev_x)
    go(src(1), mine, 1, 1, dev_y)
    go(src(1), mine, 1, 2, dev_x)
    go(src(0), mine, 0, 3, dev_y)
    go(src(0), mine, 0, 4, dev_c)
    go(src(1), mine, 1, 5, dev_c)
    for half in range(2):
        dst(half, mine)[...] = src(half)[...]

    def relay(slot, half, index, device, onward, to_core):
        landed(dst(half, slot), sem, index)
        if onward is not None:
            go(dst(half, slot), slot, half, onward, device)
        go(dst(half, slot), slot, half, to_core, dev_c)

    yield
    relay(of_x, 0, 0, dev_y, 6, 8)
    relay(of_y, 1, 1, dev_x, 7, 9)
    yield
    relay(of_x, 1, 2, None, None, 10)
    relay(of_y, 0, 3, None, None, 11)
    yield
    relay(of_d, 0, 6, None, None, 12)
    relay(of_d, 1, 7, None, None, 13)
    yield
    for slot, half, index in (
        (mine, 0, 4),
        (mine, 1, 5),
        (of_x, 0, 8),
        (of_y, 1, 9),
        (of_x, 1, 10),
        (of_y, 0, 11),
        (of_d, 0, 12),
        (of_d, 1, 13),
    ):
        landed(dst(half, slot + flip), sem, index)
    for copy in sent:
        copy.wait_send()


def scatter_steps(src, total, near, part, from_x, from_y, diag, sem):
    h, o, y, c = place()
    dev_x, dev_y, dev_c = peer(*NEAR_X), peer(*NEAR_Y), peer(*NEAR_C)
    mine = h * 4 + y * 2 + c
    of_x = (1 - h) * 4 + y * 2 + c
    of_y = h * 4 + (1 - y) * 2 + c
    of_d = (1 - h) * 4 + (1 - y) * 2 + c
    flip = 1 - 2 * c
    order = (of_d, of_x, of_y, mine)
    sent = []

    def go(ref, to, index, device):
        copy = remote(ref, to, sem, index, device)
        copy.start()
        sent.append(copy)

    for k, half in ((0, 0), (0, 1), (1, 0), (2, 1), (1, 1), (2, 0), (3, 0), (3, 1)):
        go(src(half, order[k] + flip), near.at[k, half], 2 * k + half, dev_c)

    def add(k, half):
        landed(near.at[k, half], sem, 2 * k + half)
        return src(half, order[k])[...].astype(F32) + near[k, half].astype(F32)

    yield
    part[0, 0] = add(0, 0).astype(BF16)
    go(part.at[0, 0], diag.at[0], 8, dev_x)
    part[0, 1] = add(0, 1).astype(BF16)
    go(part.at[0, 1], diag.at[1], 9, dev_y)
    part[1, 0] = add(1, 0).astype(BF16)
    go(part.at[1, 0], from_x.at[0], 10, dev_x)
    part[2, 1] = add(2, 1).astype(BF16)
    go(part.at[2, 1], from_y.at[1], 11, dev_y)
    yield
    kept_x = add(1, 1)
    landed(diag.at[1], sem, 9)
    part[1, 1] = (kept_x + diag[1].astype(F32)).astype(BF16)
    go(part.at[1, 1], from_x.at[1], 12, dev_x)
    kept_y = add(2, 0)
    landed(diag.at[0], sem, 8)
    part[2, 0] = (kept_y + diag[0].astype(F32)).astype(BF16)
    go(part.at[2, 0], from_y.at[0], 13, dev_y)
    yield
    own = [add(3, half) for half in range(2)]
    for half, ix, iy in ((0, 10, 13), (1, 12, 11)):
        landed(from_x.at[half], sem, ix)
        landed(from_y.at[half], sem, iy)
        total(half)[...] = own[half] + from_x[half].astype(F32) + from_y[half].astype(F32)
    for copy in sent:
        copy.wait_send()


def scatter_scratch(r, n):
    block = (2, r // 2, n)
    return [
        pltpu.VMEM((4,) + block, BF16),
        pltpu.VMEM((3,) + block, BF16),
        pltpu.VMEM(block, BF16),
        pltpu.VMEM(block, BF16),
        pltpu.VMEM(block, BF16),
        sems(14),
    ]


def norm_parts(r):
    centred = r - jnp.mean(r, axis=-1, keepdims=True)
    scale = lax.rsqrt(jnp.mean(centred * centred, axis=-1, keepdims=True) + 1e-12)
    return centred * scale, scale


def norm_back(xh, scale, dh):
    return (
        dh
        - jnp.mean(dh, axis=-1, keepdims=True)
        - xh * jnp.mean(dh * xh, axis=-1, keepdims=True)
    ) * scale


def dot_nt(a, b):
    return lax.dot_general(a, b, (((1,), (1,)), ((), ())), preferred_element_type=F32)


def dot_tn(a, b):
    return lax.dot_general(a, b, (((0,), (0,)), ((), ())), preferred_element_type=F32)


def blk_gather_steps(src, spot_of, zsem, ysem, csem):
    h, o, y, c = place()
    at, seen = mirrored()
    dev_y, dev_c = peer(*NEAR_Y), peer(*NEAR_C)
    end, inner, other = (h, blk(seen(0), y, c)), (h, blk(seen(1), y, c)), (h, blk(seen(2), y, c))
    sent = []

    def spot(z, yy=y, cc=c):
        return spot_of(z, yy, cc)

    def go(ref, z, yy, sem, index, device):
        copy = remote(ref, spot(z, yy), sem, index, device)
        copy.start()
        sent.append(copy)

    def line(ref, z, index, device):
        return remote(ref, spot(z), zsem, index, device)

    @pl.when(at == 0)
    def _():
        line(src, o, 0, inner).start()

    @pl.when(at == 1)
    def _():
        line(src, o, 1, end).start()
        line(src, o, 2, other).start()

    go(src, o, y, ysem, 0, dev_y)
    go(src, o, y, csem, 0, dev_c)
    spot(o)[...] = src[...]

    def onward(j, z):
        go(spot(z), z, y, ysem, j, dev_y)
        go(spot(z), z, y, csem, j, dev_c)

    first = seen(1 - at)
    order = (o, first, seen(2), seen(3))

    def from_y(j):
        landed(spot(order[j], 1 - y), ysem, j)
        go(spot(order[j], 1 - y), order[j], 1 - y, csem, 4 + j, dev_c)

    yield

    @pl.when(at == 0)
    def _():
        landed(spot(seen(1)), zsem, 1)

    @pl.when(at == 1)
    def _():
        landed(spot(seen(0)), zsem, 0)
        line(spot(seen(0)), seen(0), 3, other).start()

    onward(1, first)

    @pl.when(at == 1)
    def _():
        landed(spot(seen(2)), zsem, 2)
        line(spot(seen(2)), seen(2), 4, end).start()

    yield
    from_y(0)

    @pl.when(at == 0)
    def _():
        landed(spot(seen(2)), zsem, 4)

    onward(2, seen(2))

    @pl.when(at == 1)
    def _():
        landed(spot(seen(3)), zsem, 3)
        line(spot(seen(3)), seen(3), 5, end).start()

    yield
    from_y(1)

    @pl.when(at == 0)
    def _():
        landed(spot(seen(3)), zsem, 5)

    onward(3, seen(3))
    yield
    from_y(2)
    yield
    from_y(3)
    yield
    for j, z in enumerate(order):
        landed(spot(z, y, 1 - c), csem, j)
        landed(spot(z, 1 - y, 1 - c), csem, 4 + j)

    @pl.when(at == 0)
    def _():
        line(src, o, 0, inner).wait_send()

    @pl.when(at == 1)
    def _():
        line(src, o, 1, end).wait_send()
        line(src, o, 2, other).wait_send()
        line(spot(seen(0)), seen(0), 3, other).wait_send()
        line(spot(seen(2)), seen(2), 4, end).wait_send()
        line(spot(seen(3)), seen(3), 5, end).wait_send()

    for copy in sent:
        copy.wait_send()


ALL = tuple(
    (dx, dz, dy, dc)
    for dx in range(2)
    for dz in range(4)
    for dy in range(2)
    for dc in range(2)
    if dx or dz or dy or dc
)


def line_gather_steps(src, spot, sem):
    h, o, y, c = place()
    at, seen = mirrored()
    end, inner, other = (h, blk(seen(0), y, c)), (h, blk(seen(1), y, c)), (h, blk(seen(2), y, c))

    def line(ref, z, index, device):
        return remote(ref, spot(z), sem, index, device)

    @pl.when(at == 0)
    def _():
        line(src, o, 0, inner).start()

    @pl.when(at == 1)
    def _():
        line(src, o, 2, other).start()
        line(src, o, 1, end).start()

    spot(o)[...] = src[...]
    for k, (z, to, device) in enumerate(((0, 3, other), (2, 4, end), (3, 5, end))):
        yield

        @pl.when(at == 1)
        def _():
            landed(spot(seen(z)), sem, (0, 2, 3)[k])
            line(spot(seen(z)), seen(z), to, device).start()

    yield

    @pl.when(at == 0)
    def _():
        for z, index in ((1, 1), (2, 4), (3, 5)):
            landed(spot(seen(z)), sem, index)
        line(src, o, 0, inner).wait_send()

    @pl.when(at == 1)
    def _():
        line(src, o, 1, end).wait_send()
        line(src, o, 2, other).wait_send()
        for z, to, device in ((0, 3, other), (2, 4, end), (3, 5, end)):
            line(spot(seen(z)), seen(z), to, device).wait_send()


def line_sum_steps(term_of, out, terms, ends, mids, last, sem):
    h, o, y, c = place()
    at, seen = mirrored()
    end, inner, other = (h, blk(seen(0), y, c)), (h, blk(seen(1), y, c)), (h, blk(seen(2), y, c))
    order = [seen(3), seen(2), seen(1 - at)]
    plus = lambda a, b: a[...].astype(F32) + b[...].astype(F32)

    @pl.when(at == 0)
    def _():
        for j in range(3):
            remote(term_of(order[j]), ends.at[j], sem, j, inner).start()

    for j in range(2):
        yield

        @pl.when(at == 1)
        def _():
            landed(ends.at[j], sem, j)
            terms[j] = plus(term_of(order[j]), ends.at[j]).astype(BF16)
            remote(terms.at[j], mids.at[j], sem, 3 + j, other).start()

    yield

    @pl.when(at == 1)
    def _():
        landed(mids.at[0], sem, 3)
        terms[2] = plus(term_of(order[2]), mids.at[0]).astype(BF16)
        remote(terms.at[2], last, sem, 5, end).start()

    yield

    @pl.when(at == 1)
    def _():
        landed(ends.at[2], sem, 2)
        landed(mids.at[1], sem, 4)
        out[...] = (plus(term_of(o), ends.at[2]) + mids[1].astype(F32)).astype(BF16)
        for j in range(2):
            remote(terms.at[j], mids.at[j], sem, 3 + j, other).wait_send()
        remote(terms.at[2], last, sem, 5, end).wait_send()

    @pl.when(at == 0)
    def _():
        landed(last, sem, 5)
        out[...] = plus(term_of(o), last).astype(BF16)
        for j in range(3):
            remote(term_of(order[j]), ends.at[j], sem, j, inner).wait_send()


def line_sum_scratch(block):
    return [
        pltpu.VMEM((3,) + block, BF16),
        pltpu.VMEM((3,) + block, BF16),
        pltpu.VMEM((2,) + block, BF16),
        pltpu.VMEM(block, BF16),
        sems(6),
    ]


def spread_steps(rows_of, out, spots, sem):
    h, o, y, c = place()
    t = h * 4 + y * 2 + c
    columns = [
        out.at[:, pl.ds(pl.multiple_of(lane * 128, 128), 128)] for lane in spots(t)
    ]
    pieces = len(columns)
    copies = []
    for k, p in enumerate(PLANE):
        to = (1 - y if p[2] else y) * 2 + (1 - c if p[3] else c)
        for i in range(pieces):
            src = rows_of(to).at[:, pl.ds(i * 128, 128)]
            copy = remote(src, columns[i], sem, k * pieces + i, peer(*p))
            copy.start()
            copies.append(copy)
    for i in range(pieces):
        columns[i][...] = rows_of(y * 2 + c)[:, i * 128 : (i + 1) * 128]
    yield
    for copy in copies:
        copy.wait()


def second_half(x, consts):
    names = list(vars(x))
    seqs, r, d = x.embedded.shape
    planes, four, e, fh = x.up_one.shape
    f = 2 * fh
    fcols = x.down_weight.shape[0] // 2
    half_d = d // 2
    rows, q_rows = 8 * r, 4 * r
    three, he, length = x.held.shape
    n = length // 4
    slots, chunks, chunk_lag, scale = consts
    own_rows, w, blks = seqs * r, d // chunks, 16
    key_rows = 256
    width_qkv = 3 * 2 * he

    need = []

    def scratch(shape, dtype):
        need.append(pltpu.VMEM(shape, dtype))
        return len(need) - 1

    def many(specs):
        start = len(need)
        need.extend(specs)
        return list(range(start, len(need)))

    plane = (seqs, 8, r, d)
    shapes = dict(
        partial=(plane, BF16),
        up_two=(x.up_one.shape, BF16),
        down_all=((planes, fcols, d), BF16),
        first_g=(plane, BF16),
        grad_g=(plane, BF16),
        branch_g=(plane, BF16),
        act=((seqs * rows, f), BF16),
        slope=((seqs * rows, f), F32),
        inner_grad=((seqs * rows, f), BF16),
        first=((seqs, r, d), F32),
        xh_one=((seqs, r, d), F32),
        scale_one=((seqs, r, 1), F32),
        grad_two=((seqs, r, d), F32),
        low=((seqs, r, d), BF16),
        total=((seqs, r, d), F32),
        resid=((seqs, r, d), F32),
        down_part=((planes, fcols, d), BF16),
        up_part=((planes, 4 * e, f), BF16),
        up_total=((4 * e, f), BF16),
        out_part=((2, he, d), BF16),
        out_held=((4, he, d), BF16),
        out_acc=((he, d), F32),
        sums=((16, d), F32),
        up_sums=((1, f), F32),
        up_spots=((32, 128), F32),
        go=((2, he, 2 * n), BF16),
        gs=((he, length), BF16),
        qs=((he, length), BF16),
        q_rows=((length, he), BF16),
        g_rows=((length, he), BF16),
        dq=((he, length), F32),
        delta=((1, length), F32),
        pair_low=((three, he, length), BF16),
        dqkv=((three, 2, he, 2 * n), BF16),
        qkv_part=((planes, 4 * e, width_qkv), BF16),
        qkv_total=((4 * e, width_qkv), BF16),
        own=((chunks, own_rows, w), BF16),
        gathered=((chunks, blks, own_rows, w), BF16),
        pick=((slots, blks * own_rows), BF16),
        pos_low=((chunks, slots, w), BF16),
        pos_held=((chunks, slots, w), BF16),
        pack=((blks, 24, 128), F32),
        packs=((31, 24, 128), F32),
    )
    ids = {name: scratch(*spec) for name, spec in shapes.items()}
    counts = dict(
        up_sem=6,
        down_sem=6,
        ksem=3,
        qsem=3,
        down_pair=1,
        up_spread=28,
        qkv_spread=21,
        out_pair=1,
        pair_sem=chunks,
        pack_sem=31,
    )
    sem_ids = {k: many([sems(v)])[0] for k, v in counts.items()}
    for k, v in dict(go_send=4, go_recv=4, out_send=2, out_recv=4).items():
        sem_ids[k] = many([pltpu.SemaphoreType.DMA((v,))])[0]
    stream_ids = [
        ([many(scatter_scratch(2 * r, d)) for _ in range(3)], [many([sems(14)])[0] for _ in range(3)])
    ]
    chunk_ids = [
        (many(scatter_scratch(2 * r, w)), many([sems(6), sems(4), sems(8)])) for _ in range(chunks)
    ]
    down_line = many(line_sum_scratch((fcols, d)))
    up_line = many(line_sum_scratch((4 * e, f)))
    qkv_line = many(line_sum_scratch((4 * e, width_qkv)))

    def run(ins, outs, own):
        src = SimpleNamespace(**dict(zip(names, ins)))
        out_ref, grad_ref, pos_ref, got_down, got_up, got_qkv, got_out, totals = outs
        m = SimpleNamespace(**{k: own[v] for k, v in ids.items()})
        sem = SimpleNamespace(**{k: own[v] for k, v in sem_ids.items()})
        pick_refs = lambda some: [own[i] for i in some]
        h, o, y, c = place()
        g = y * 2 + c
        t = h * 4 + g
        tail = []

        up_more = src.up_cut.at[:, :, pl.ds(fh, fh)]
        down_rows = pl.ds(pl.multiple_of(h * fcols, fcols), fcols)
        down_more = src.down_weight.at[down_rows]
        up_line_in = line_gather_steps(up_more, lambda z: m.up_two.at[z], sem.up_sem)
        down_line_in = line_gather_steps(down_more, lambda z: m.down_all.at[z], sem.down_sem)
        next(up_line_in)
        next(down_line_in)
        for ref in (m.sums, m.up_sums, m.up_spots, m.dq):
            ref[...] = jnp.zeros_like(ref)
        yield

        ups = [lambda k=k: src.up_one[...].reshape(d, fh) if k == 0 else m.up_two[...].reshape(d, fh) for k in range(2)]
        downs = [
            lambda k=k: m.down_all[:, :, k * half_d : (k + 1) * half_d].reshape(f, half_d)
            for k in range(2)
        ]
        vec = lambda k: src.vectors[k + 2 : k + 3]
        partial, low, total = m.partial, m.low, m.total

        both = range(seqs)

        def piece(ref):
            return lambda i, slot: ref.at[i, slot]

        def plain(ref):
            return lambda i: ref.at[i]

        def quarter(ref, s, q):
            return ref[s, 4 * q : 4 * q + 4].reshape(q_rows, d)

        def note(k, value):
            m.sums[k : k + 1] += jnp.sum(value, axis=0, keepdims=True)

        def step(*some):
            for gen in some:
                next(gen, None)

        def down_sums():
            yield from line_sum_steps(
                lambda z: m.down_part.at[z], got_down.at[h], *pick_refs(down_line)
            )
            copy = remote(got_down.at[h], got_down.at[h], sem.down_pair, 0, peer(*NEAR_X))
            copy.start()
            yield
            copy.wait_send()
            landed(got_down.at[1 - h], sem.down_pair, 0)

        def up_sums():
            yield from line_sum_steps(lambda z: m.up_part.at[z], m.up_total, *pick_refs(up_line))
            yield from spread_steps(
                lambda k: m.up_total.at[pl.ds(k * e, e)],
                got_up,
                lambda k: [(i * 4 + k % 4) * 2 + k // 4 for i in range(4)],
                sem.up_spread,
            )

        def qkv_sums():
            yield from line_sum_steps(
                lambda z: m.qkv_part.at[z], m.qkv_total, *pick_refs(qkv_line)
            )
            yield from spread_steps(
                lambda k: m.qkv_total.at[pl.ds(k * e, e)],
                got_qkv,
                lambda k: [i * 8 + k for i in range(3)],
                sem.qkv_spread,
            )

        def out_sums():
            has = o // 2 == h
            held, acc, send, recv = m.out_held, m.out_acc, sem.out_send, sem.out_recv

            def each(act):
                for j in range(2):
                    device = (h, blk(2 * h + y, c, j))
                    copy = place_copy(m.out_part.at[j], held.at[o], send.at[j], recv.at[o], device)

                    @pl.when(jnp.logical_not((o == 2 * h + y) & (y == c) & (c == j)))
                    def _():
                        act(copy)

            each(lambda copy: copy.start())
            yield
            acc[...] = jnp.zeros_like(acc)
            for z in range(4):
                mine = (z == o) & (o % 2 == y) & (y == c)

                @pl.when(has & mine)
                def _():
                    acc[...] += m.out_part[c].astype(F32)

                @pl.when(has & jnp.logical_not(mine))
                def _():
                    ref = held.at[z]
                    place_copy(ref, ref, send.at[0], recv.at[z], (h, blk(o, y, c))).wait_recv()
                    acc[...] += held[z].astype(F32)

            pair = remote(got_out, got_out, sem.out_pair, 0, peer(*NEAR_X))

            @pl.when(has)
            def _():
                got_out[...] = acc[...].astype(BF16)
                pair.start()

            yield
            each(lambda copy: copy.wait_send())

            @pl.when(has)
            def _():
                pair.wait_send()

            @pl.when(jnp.logical_not(has))
            def _():
                landed(got_out, sem.out_pair, 0)

        def go_copy(s, j):
            z = 2 * s + j
            return place_copy(
                m.go.at[j, :, pl.ds(s * n, n)],
                m.gs.at[:, pl.ds(pl.multiple_of(o * n, n), n)],
                sem.go_send.at[z],
                sem.go_recv.at[o],
                (h, z * 4 + g),
            )

        def stream():
            scatters = [pick_refs(i) for i in stream_ids[0][0]]
            gathers = pick_refs(stream_ids[0][1])
            at = lambda s, q: pl.ds(s * rows + q * q_rows, q_rows)
            for s in both:
                branch = dot_tn(
                    src.attended[:, :, s * n : (s + 1) * n].reshape(2 * he, n), src.out_own[...]
                )
                partial[s] = branch.astype(BF16).reshape(8, r, d)
            for k, _ in enumerate(scatter_steps(piece(partial), plain(total), *scatters[0])):
                if k > 0:
                    step(up_line_in)
                yield
            for s in both:
                xh, scale_r = norm_parts(src.embedded[s] + (total[s] + vec(0)))
                m.xh_one[s] = xh
                m.scale_one[s] = scale_r
                value = xh * vec(4) + vec(1)
                m.first[s] = value
                low[s] = value.astype(BF16)
            step(up_line_in, down_line_in)
            for k, _ in enumerate(gather_steps(plain(low), piece(m.first_g), gathers[0])):
                if k in (1, 3):
                    step(down_line_in)
                yield
            for _ in up_line_in:
                pass
            for s in both:
                for q in range(2):
                    rows_in = quarter(m.first_g, s, q)
                    for k in range(2):
                        cols = slice(k * fh, (k + 1) * fh)
                        inner = jnp.dot(rows_in, ups[k](), preferred_element_type=F32)
                        inner = inner + src.up_bias[:, cols]
                        phi = 0.5 + 0.5 * lax.erf(inner * (0.5**0.5))
                        m.act[at(s, q), cols] = (inner * phi).astype(BF16)
                        bell = jnp.exp(inner * inner * -0.5) * (1.0 / math.sqrt(2.0 * math.pi))
                        m.slope[at(s, q), cols] = phi + inner * bell
            for _ in down_line_in:
                pass
            for s in both:
                for k in range(2):
                    part = jnp.dot(
                        m.act[s * rows : (s + 1) * rows], downs[k](), preferred_element_type=F32
                    )
                    partial[s, :, :, k * half_d : (k + 1) * half_d] = part.astype(BF16).reshape(
                        8, r, half_d
                    )
            yield from scatter_steps(piece(partial), plain(total), *scatters[1])
            for s in both:
                xh, scale_r = norm_parts(m.first[s] + (total[s] + vec(2)))
                out_ref[s] = (xh * vec(5) + vec(3)).astype(BF16)
                cot = src.cotangent[s].astype(F32)
                note(5, cot * xh)
                note(3, cot)
                grad = norm_back(xh, scale_r, cot * vec(5))
                m.grad_two[s] = grad
                low[s] = grad.astype(BF16)
                note(2, low[s].astype(F32))
            yield from gather_steps(plain(low), piece(m.grad_g), gathers[1])
            for s in both:
                for q in range(2):
                    rows_in = quarter(m.grad_g, s, q)
                    back = dot_nt(rows_in[:, :half_d], downs[0]()) + dot_nt(
                        rows_in[:, half_d:], downs[1]()
                    )
                    back = (back * m.slope[at(s, q)]).astype(BF16)
                    m.inner_grad[at(s, q)] = back
                    m.up_sums[...] += jnp.sum(back.astype(F32), axis=0, keepdims=True)
                    part = dot_nt(back[:, :fh], ups[0]()) + dot_nt(back[:, fh:], ups[1]())
                    partial[s, 4 * q : 4 * q + 4] = part.astype(BF16).reshape(4, r, d)
            last = scatter_steps(piece(partial), plain(total), *scatters[2])
            next(last)

            @pl.loop(0, planes)
            def _(z):
                cols = pl.ds(pl.multiple_of(z * fcols, fcols), fcols)
                all_grads = m.grad_g[...].reshape(seqs * rows, d)
                m.down_part[z] = dot_tn(m.act[:, cols], all_grads).astype(BF16)

            step(down)
            next(last)

            @pl.loop(0, planes)
            def _(z):
                cols = pl.ds(pl.multiple_of(z * 4 * e, 4 * e), 4 * e)
                all_first = m.first_g[:, :, :, cols].reshape(seqs * rows, 4 * e)
                m.up_part[z] = dot_tn(all_first, m.inner_grad[...]).astype(BF16)

            yield from last
            for s in both:
                grad = m.grad_two[s] + total[s]
                note(4, grad * m.xh_one[s])
                note(1, grad)
                grad = norm_back(m.xh_one[s], m.scale_one[s], grad * vec(4))
                m.resid[s] = grad
                low[s] = grad.astype(BF16)
                note(0, low[s].astype(F32))
            for k, _ in enumerate(gather_steps(plain(low), piece(m.branch_g), gathers[2])):
                yield
                if k in EARLY:
                    step(down)
            for s in both:
                go = dot_nt(src.out_own[...], m.branch_g[s].reshape(rows, d))
                m.go[:, :, s * n : (s + 1) * n] = go.astype(BF16).reshape(2, he, n)
                for j in range(2):

                    @pl.when(o != 2 * s + j)
                    def _():
                        go_copy(s, j).start()

                    @pl.when(o == 2 * s + j)
                    def _():
                        m.gs[:, pl.ds(pl.multiple_of(o * n, n), n)] = m.go[
                            j, :, s * n : (s + 1) * n
                        ]

        down, up, out, qkv = down_sums(), up_sums(), out_sums(), qkv_sums()
        for _ in stream():
            pass
        step(up)
        grad_out = jnp.dot(
            src.attended[...].reshape(2 * he, 2 * n),
            m.branch_g[...].reshape(seqs * rows, d),
            preferred_element_type=F32,
        )
        m.out_part[...] = grad_out.astype(BF16).reshape(2, he, d)
        held = src.held
        gs, qs, q_t, g_t, dq, delta, pair_low = (
            m.gs, m.qs, m.q_rows, m.g_rows, m.dq, m.delta, m.pair_low
        )
        q32 = held[0].astype(F32) * scale
        qs[...] = q32.astype(BF16)
        q_t[...] = q32.T.astype(BF16)

        @pl.loop(0, slots // 64)
        def _(k):
            row = lax.broadcasted_iota(jnp.int32, (64, 1), 0) + k * 64
            some = pl.ds(pl.multiple_of(k * 64, 64), 64)
            m.pick[some] = (src.ids[...] == row).astype(F32).astype(BF16)

        for z in range(4):

            @pl.when(z != o)
            def _():
                ref = gs.at[:, pl.ds(z * n, n)]
                place_copy(
                    ref, ref, sem.go_send.at[0], sem.go_recv.at[z], peer(*NEAR_X)
                ).wait_recv()

        g32 = gs[...].astype(F32)
        g_t[...] = g32.T.astype(BF16)
        delta[...] = jnp.sum(g32 * src.pair_out[...], axis=0, keepdims=True)
        mine = pl.ds(pl.multiple_of((o // 2) * n, n), n)
        dqkv = m.dqkv

        def back(part, which, i, z):
            return remote(
                pair_low.at[part, :, pl.ds(pl.multiple_of(z * n, n), n)],
                dqkv.at[part, o % 2, :, mine],
                which,
                i,
                (h, z * 4 + g),
            )

        late = pl.ds(1, 2)
        for i in range(4):
            z = (o + 1 + i) % 4

            @pl.loop(0, n // key_rows)
            def _(step):
                at = pl.ds(pl.multiple_of(z * n + step * key_rows, key_rows), key_rows)
                k_cols = held[1, :, at]
                k_rows = k_cols.astype(F32).T.astype(BF16)
                v_rows = held[2, :, at].astype(F32).T.astype(BF16)
                s = jnp.dot(k_rows, qs[...], preferred_element_type=F32)
                p = jnp.exp(s - src.lse[...])
                dv = jnp.dot(p.astype(BF16), g_t[...], preferred_element_type=F32)
                dp = jnp.dot(v_rows, gs[...], preferred_element_type=F32)
                ds = (p * (dp - delta[...])).astype(BF16)
                dk = jnp.dot(ds, q_t[...], preferred_element_type=F32)
                dq[...] += jnp.dot(k_cols, ds, preferred_element_type=F32)
                pair_low[1, :, at] = dk.T.astype(BF16)
                pair_low[2, :, at] = dv.T.astype(BF16)

            if i < 3:
                back(late, sem.ksem, i, z).start()
            if i == 0:
                step(*[down] * (3 - len(EARLY)))
            if i == 2:
                step(up)
        pair_low[0] = (dq[...] * scale).astype(BF16)
        for i in range(3):
            back(pl.ds(0, 1), sem.qsem, i, (o + 1 + i) % 4).start()
        dqkv[:, o % 2, :, mine] = pair_low[:, :, pl.ds(pl.multiple_of(o * n, n), n)]
        step(down, up)
        for i in range(3):
            z = (o + 3 - i) % 4
            there = pl.ds(pl.multiple_of((z // 2) * n, n), n)
            landed(dqkv.at[late, z % 2, :, there], sem.ksem, i)
            landed(dqkv.at[pl.ds(0, 1), z % 2, :, there], sem.qsem, i)

        all_dqkv = lambda: dqkv[...].reshape(width_qkv, 2 * n)

        def back_chunk(q):
            part = lax.dot_general(
                all_dqkv(),
                src.qkv_own[q * w : (q + 1) * w],
                (((0,), (1,)), ((), ())),
                preferred_element_type=F32,
            )
            partial[:, :, :, q * w : (q + 1) * w] = part.astype(BF16).reshape(seqs, 8, r, w)

        def chunk(q):
            cols = pl.ds(q * w, w)
            scatter, (zsem, ysem, csem) = pick_refs(chunk_ids[q][0]), pick_refs(chunk_ids[q][1])
            back_chunk(q)
            yield from scatter_steps(
                lambda i, slot: partial.at[i, slot, :, cols],
                lambda i: grad_ref.at[i, :, cols],
                *scatter,
            )
            grad = grad_ref[:, :, cols] + m.resid[:, :, cols]
            grad_ref[:, :, cols] = grad
            grad = grad.reshape(own_rows, w)
            m.own[q] = grad.astype(BF16)
            second = src.second[...]
            m.sums[6:7, cols] = jnp.sum(grad * (1.0 - second), axis=0, keepdims=True)
            m.sums[7:8, cols] = jnp.sum(grad * second, axis=0, keepdims=True)
            yield from blk_gather_steps(
                m.own.at[q],
                lambda z, yy, cc: m.gathered.at[q, blk(z, yy, cc)],
                zsem,
                ysem,
                csem,
            )

            @pl.loop(0, slots // 128)
            def _(k):
                some = pl.ds(pl.multiple_of(k * 128, 128), 128)
                found = jnp.dot(
                    m.pick[some],
                    m.gathered[q].reshape(blks * own_rows, w),
                    preferred_element_type=F32,
                )
                pos_ref[some, cols] = found
                m.pos_low[q, some] = found.astype(BF16)

            copy = remote(
                m.pos_low.at[q], m.pos_held.at[q], sem.pair_sem, q, peer(*NEAR_X)
            )
            copy.start()
            pairs.append(copy)
            yield

        pairs = []
        active, waiting = [], [chunk(q) for q in range(chunks)]
        turn = 0
        while active or waiting:
            if waiting and turn % chunk_lag == 0:
                active.append(waiting.pop(0))
            for gen in list(active):
                try:
                    next(gen)
                except StopIteration:
                    active.remove(gen)
            if turn == 0:
                @pl.loop(0, planes)
                def _(z):
                    cols = pl.ds(pl.multiple_of(z * 4 * e, 4 * e), 4 * e)
                    part = lax.dot_general(
                        src.plane_low[:, :, :, cols].reshape(seqs * rows, 4 * e),
                        all_dqkv(),
                        (((0,), (1,)), ((), ())),
                        preferred_element_type=F32,
                    )
                    m.qkv_part[z] = part.astype(BF16)

                step(qkv)
                ones = jnp.ones((8, 2 * n), BF16)
                heads = dot_nt(ones, all_dqkv())
                own_lanes = pl.ds(pl.multiple_of(t * 128, 128), 128)
                m.sums[8:9, own_lanes] = heads[0:1, 0:128]
                m.sums[9:10, own_lanes] = heads[0:1, 256:384]
                for i in range(4):
                    m.up_spots[pl.ds((i * 4 + g) * 2 + h, 1)] = m.up_sums[
                        :, i * 128 : (i + 1) * 128
                    ]
            for when, gen in zip(TURNS, (up, qkv, out)):
                if turn in when:
                    step(gen)
            turn += 1
        for b in range(blks):
            m.pack[b, 0:16] = m.sums[:, b // 2 * 128 : (b // 2 + 1) * 128]
            m.pack[b, 16:18] = m.up_spots[2 * b : 2 * b + 2]
            m.pack[b, 18:24] = jnp.zeros((6, 128), F32)
        copies = []
        for k, p in enumerate(ALL):
            to = peer(*p)
            copy = remote(m.pack.at[to[1]], m.packs.at[k], sem.pack_sem, k, to)
            copy.start()
            copies.append(copy)
        for gen in (down, up, out, qkv):
            for _ in gen:
                pass
        for q, copy in enumerate(pairs):
            copy.wait()
            cols = pl.ds(q * w, w)
            pos_ref[:, cols] = pos_ref[:, cols] + m.pos_held[q].astype(F32)
        for copy in copies:
            copy.wait()
        totals[...] = m.pack[blk(o, y, c)] + jnp.sum(m.packs[...], axis=0)
        for i in range(3):
            back(late, sem.ksem, i, (o + 1 + i) % 4).wait_send()
            back(pl.ds(0, 1), sem.qsem, i, (o + 1 + i) % 4).wait_send()
        for s in range(seqs):
            for j in range(2):

                @pl.when(o != 2 * s + j)
                def _():
                    go_copy(s, j).wait_send()

    return Part(
        run,
        list(vars(x).values()),
        [
            ((seqs, r, d), BF16),
            ((seqs, r, d), F32),
            ((slots, d), F32),
            ((2, fcols, d), BF16),
            ((e, 8 * f), BF16),
            ((e, 3 * d), BF16),
            ((he, d), BF16),
            ((24, 128), F32),
        ],
        need,
        ALL,
    )


def rows_steps(own_of, near, part, from_y, term, ends, mids, last, csem, ysem, zsem, out):
    h, o, y, c = place()
    at, seen = mirrored()
    dev_y = peer(*NEAR_Y)
    order = [seen(3), seen(2), seen(1 - at), o]
    end, inner, other = (h, blk(seen(0), y, c)), (h, blk(seen(1), y, c)), (h, blk(seen(2), y, c))
    sent = []
    for j, z in enumerate(order):
        landed(near.at[0, j], csem, j)
        part[j] = own_of(z, 1 - y)[...] + near[0, j]
        copy = remote(part.at[j], from_y.at[j], ysem, j, dev_y)
        copy.start()
        sent.append(copy)
    for j, z in enumerate(order):
        yield
        landed(near.at[1, j], csem, 4 + j)
        landed(from_y.at[j], ysem, j)
        term[j] = own_of(z, y)[...] + near[1, j] + from_y[j]
        if j < 3:

            @pl.when(at == 0)
            def _():
                remote(term.at[j], ends.at[j], zsem, j, inner).start()

        if j < 2:

            @pl.when(at == 1)
            def _():
                landed(ends.at[j], zsem, j)
                term[j] += ends[j]
                remote(term.at[j], mids.at[j], zsem, 3 + j, other).start()

    yield

    @pl.when(at == 1)
    def _():
        landed(mids.at[0], zsem, 3)
        term[2] += mids[0]
        remote(term.at[2], last, zsem, 5, end).start()

    yield

    @pl.when(at == 1)
    def _():
        landed(ends.at[2], zsem, 2)
        landed(mids.at[1], zsem, 4)
        out[...] = (term[3] + ends[2] + mids[1]).astype(F32)
        for j in range(2):
            remote(term.at[j], mids.at[j], zsem, 3 + j, other).wait_send()
        remote(term.at[2], last, zsem, 5, end).wait_send()

    @pl.when(at == 0)
    def _():
        landed(last, zsem, 5)
        out[...] = (term[3] + last[...]).astype(F32)
        for j in range(3):
            remote(term.at[j], ends.at[j], zsem, j, inner).wait_send()

    for copy in sent:
        copy.wait_send()


def first_half(x, scale, lag):
    names = list(vars(x))
    seqs, r, d = x.hidden.shape
    slots = x.table.shape[0]
    e = x.qkv_weight.shape[0]
    four, wq, f = 4, x.qkv_weight.shape[1] // 8, x.up_weight.shape[1] // 8
    he = wq // 6
    n = 8 * r
    length = 4 * n
    half, fh = r // 2, f // 2
    blks = 16
    cols = 512
    small = small_gather(jax.ShapeDtypeStruct((8, 128), F32))
    outw = out_weights(x.out_weight)
    need = []

    def many(specs):
        start = len(need)
        need.extend(specs)
        return list(range(start, len(need)))

    block = (r, d)
    shapes = dict(
        packed=((8, 128), F32),
        everyone=((blks, 8, 128), F32),
        found=((4, 2, 2, seqs, r, d), BF16),
        rows=((seqs, r, d), F32),
        low=((seqs, r, d), BF16),
        qkv_in=((four, e, wq), BF16),
        projected=((3, 2, he, 2 * n), BF16),
        keys=((length, he), BF16),
        pair_low=((he, length), BF16),
    )
    ids = {k: many([pltpu.VMEM(*v)])[0] for k, v in shapes.items()}
    counts = dict(qkv_sem=6, up_sem=6, back_sem=3, qkv_trade=9, up_trade=12)
    sem_ids = {k: many([sems(v)])[0] for k, v in counts.items()}
    for k in ("send", "recv"):
        sem_ids[k] = many([pltpu.SemaphoreType.DMA((4,))])[0]
    small_ids, outw_ids = many(small.scratch), many(outw.scratch)
    row_ids = [
        many(
            [
                pltpu.VMEM((2, 4) + block, BF16),
                pltpu.VMEM((4,) + block, BF16),
                pltpu.VMEM((4,) + block, BF16),
                pltpu.VMEM((4,) + block, BF16),
                pltpu.VMEM((3,) + block, BF16),
                pltpu.VMEM((2,) + block, BF16),
                pltpu.VMEM(block, BF16),
                sems(8),
                sems(4),
                sems(6),
            ]
        )
        for _ in range(seqs)
    ]
    gather_ids = [many([sems(14)])[0] for _ in range(seqs)]

    def run(ins, outs, own):
        src = SimpleNamespace(**dict(zip(names, ins)))
        attended, held, o_ref, lse_ref, emb_ref, plane_ref, qkv_ref = outs[:7]
        outw_ref, up_one, up_in, vec_ref, bias_ref, ids_ref, second_ref = outs[7:]
        m = SimpleNamespace(**{k: own[v] for k, v in ids.items()})
        sem = SimpleNamespace(**{k: own[v] for k, v in sem_ids.items()})
        pick_refs = lambda some: [own[i] for i in some]
        h, o, y, c = place()
        g = y * 2 + c
        t = h * 4 + g
        side = lambda a: jnp.concatenate([a[0:1], a[1:2]], axis=1).astype(F32)
        for k in range(3):
            m.packed[k : k + 1] = side(src.biases[2 * k : 2 * k + 2])
        m.packed[3:4] = side(src.gains[...])
        m.packed[4:5] = side(src.types[...])
        m.packed[5:7] = src.up_bias[...].astype(F32)
        m.packed[7:8] = side(src.pos_ids[...])
        gather_small = small.run((m.packed,), (m.everyone,), pick_refs(small_ids))
        trades = []

        def trade(ref, dst, s, lanes_of):
            count = len(lanes_of(0))
            for k, p in enumerate(((0, 0, 1, 0), (0, 0, 0, 1), (0, 0, 1, 1))):
                to = (1 - y if p[2] else y) * 2 + (1 - c if p[3] else c)
                for i, lane in enumerate(lanes_of(to)):
                    copy = remote(
                        ref.at[:, pl.ds(pl.multiple_of(lane * 128, 128), 128)],
                        dst.at[g, :, pl.ds(i * 128, 128)],
                        s,
                        k * count + i,
                        peer(*p),
                    )
                    copy.start()
                    trades.append(copy)
            for i, lane in enumerate(lanes_of(g)):
                dst[g, :, i * 128 : (i + 1) * 128] = ref[
                    :, pl.ds(pl.multiple_of(lane * 128, 128), 128)
                ]

        weights = outw.run((src.out_weight,), (outw_ref,), pick_refs(outw_ids))
        qkv_lanes = lambda k: [i * 8 + h * 4 + k for i in range(3)]
        up_lanes = lambda k: [(i * 4 + k) * 2 + h for i in range(4)]
        trade(src.qkv_weight, m.qkv_in, sem.qkv_trade, qkv_lanes)
        next(gather_small)
        yield
        next(weights)
        trade(src.up_weight, up_in, sem.up_trade, up_lanes)
        qkv_line = line_gather_steps(m.qkv_in, lambda z: qkv_ref.at[z], sem.qkv_sem)
        up_first = up_in.at[:, :, pl.ds(0, fh)]
        up_line = line_gather_steps(up_first, lambda z: up_one.at[z], sem.up_sem)

        for _ in gather_small:
            pass

        at, seen = mirrored()
        order = [seen(3), seen(2), seen(1 - at), o]
        b = blk(o, y, c)
        row = lax.broadcasted_iota(jnp.int32, (slots, 1), 0).astype(F32)
        base = (b * slots).astype(F32)
        streams = [pick_refs(i) for i in row_ids]
        core = []
        for i, yy in enumerate((1 - y, y)):
            for j, z in enumerate(order):
                hot = jnp.concatenate(
                    [
                        (m.everyone[blk(z, yy, cc), 7:8] - base == row).astype(F32).astype(BF16)
                        for cc in range(2)
                    ],
                    axis=1,
                )
                rows_of = dot_tn(hot, src.table[...]).astype(BF16)
                m.found[z, yy] = rows_of.reshape(2, seqs, r, d)
                for s in range(seqs):
                    near, csem = streams[s][0], streams[s][7]
                    copy = remote(
                        m.found.at[z, yy, 1 - c, s],
                        near.at[i, j],
                        csem,
                        i * 4 + j,
                        peer(*NEAR_C),
                    )
                    copy.start()
                    core.append(copy)
            if i == 0:
                for copy in trades:
                    copy.wait()
                next(qkv_line)

        lane = lax.broadcasted_iota(jnp.int32, (1, 128), 1)
        for k in range(5):
            for i in range(blks // 2):
                one, two = m.everyone[2 * i, k : k + 1], m.everyone[2 * i + 1, k : k + 1]
                lanes = slice(i * 128, (i + 1) * 128)
                vec_ref[2 * k : 2 * k + 1, lanes] = jnp.where(
                    lane < 64, one, pltpu.roll(two, 64, 1)
                )
                vec_ref[2 * k + 1 : 2 * k + 2, lanes] = jnp.where(
                    lane < 64, pltpu.roll(one, 64, 1), two
                )
        for i in range(blks):
            ids_ref[:, i * 128 : (i + 1) * 128] = (m.everyone[i, 7:8] - base).astype(jnp.int32)
        for i in range(4):
            bias_ref[:, i * 128 : (i + 1) * 128] = m.everyone[i * 4 + g, pl.ds(5 + h, 1)]
        eye = lax.broadcasted_iota(jnp.int32, (128, 128), 0) == lax.broadcasted_iota(
            jnp.int32, (128, 128), 1
        )

        def upright(lanes):
            return jnp.sum(jnp.where(eye, lanes, 0.0), axis=1, keepdims=True)

        def column(k):
            return upright(vec_ref[k : k + 1, pl.ds(pl.multiple_of(t * 128, 128), 128)])

        second_ref[...] = upright(side(src.type_ids[...]))

        def send_pair(s, j):
            z = 2 * s + j
            return place_copy(
                m.projected.at[:, j, :, pl.ds(s * n, n)],
                held.at[:, :, pl.ds(pl.multiple_of(o * n, n), n)],
                sem.send.at[z],
                sem.recv.at[o],
                (h, z * 4 + g),
            )

        def stream(s):
            yield from rows_steps(
                lambda z, yy: m.found.at[z, yy, c, s], *streams[s], m.rows.at[s]
            )
            if s == seqs - 1:
                next(up_line)
            second = second_ref[s * r : (s + 1) * r]
            typed = vec_ref[8:9] * (1.0 - second) + vec_ref[9:10] * second
            value = src.hidden[s].astype(F32) + m.rows[s] + typed
            emb_ref[s] = value
            m.low[s] = value.astype(BF16)
            yield from gather_steps(
                lambda i: m.low.at[s, pl.ds(i * half, half)],
                lambda i, slot: plane_ref.at[s, slot, pl.ds(i * half, half)],
                own[gather_ids[s]],
            )
            if s == 0:
                for _ in qkv_line:
                    pass
            part = lax.dot_general(
                qkv_ref[...].reshape(d, wq),
                plane_ref[s].reshape(n, d),
                (((0,), (1,)), ((), ())),
                preferred_element_type=F32,
            )
            here = slice(s * n, (s + 1) * n)
            third = wq // 3
            m.projected[0, :, :, here] = (part[:third] + column(0)).astype(BF16).reshape(2, he, n)
            m.projected[1, :, :, here] = part[third : 2 * third].astype(BF16).reshape(2, he, n)
            m.projected[2, :, :, here] = (
                (part[2 * third :] + column(1)).astype(BF16).reshape(2, he, n)
            )
            for j in range(2):

                @pl.when(o != 2 * s + j)
                def _():
                    send_pair(s, j).start()

                @pl.when(o == 2 * s + j)
                def _():
                    held[:, :, pl.ds(pl.multiple_of(o * n, n), n)] = m.projected[:, j, :, here]

            yield

        gens = [stream(s) for s in range(seqs)]
        for _ in range(lag):
            next(gens[0])
        turn = 0
        while gens:
            for gen in list(gens):
                try:
                    next(gen)
                except StopIteration:
                    gens.remove(gen)
            if turn in QKV_TURNS:
                next(qkv_line, None)
            if turn in UP_TURNS:
                next(up_line, None)
            turn += 1

        for z in range(4):

            @pl.when(z != o)
            def _():
                ref = held.at[:, :, pl.ds(z * n, n)]
                place_copy(ref, ref, sem.send.at[0], sem.recv.at[z], peer(*NEAR_X)).wait_recv()

        m.keys[...] = held[1].astype(F32).T.astype(BF16)
        mine = pl.ds(pl.multiple_of((o // 2) * n, n), n)

        def back(i, z):
            return remote(
                m.pair_low.at[:, pl.ds(pl.multiple_of(z * n, n), n)],
                attended.at[o % 2, :, mine],
                sem.back_sem,
                i,
                (h, z * 4 + g),
            )

        @pl.loop(0, 4 * (n // cols))
        def _(step):
            i = step // (n // cols)
            z = (o + 1 + i) % 4
            here = pl.ds(pl.multiple_of(z * n + step % (n // cols) * cols, cols), cols)
            q = (held[0, :, here].astype(F32) * scale).astype(BF16)
            s = jnp.dot(m.keys[...], q, preferred_element_type=F32)
            peak = jnp.max(s, axis=0, keepdims=True)
            p = jnp.exp(s - peak)
            total = jnp.sum(p, axis=0, keepdims=True)
            out = jnp.dot(held[2], p.astype(BF16), preferred_element_type=F32) / total
            o_ref[:, here] = out
            m.pair_low[:, here] = out.astype(BF16)
            lse_ref[:, here] = peak + jnp.log(total)

            @pl.when((step % (n // cols) == n // cols - 1) & (i < 3))
            def _():
                back(i, z).start()

        attended[o % 2, :, mine] = m.pair_low[:, pl.ds(pl.multiple_of(o * n, n), n)]
        for i in range(3):
            back(i, (o + 1 + i) % 4).wait_send()
            z = (o + 3 - i) % 4
            landed(attended.at[z % 2, :, pl.ds(pl.multiple_of((z // 2) * n, n), n)], sem.back_sem, i)
        for _ in weights:
            pass
        for _ in up_line:
            pass
        for copy in core:
            copy.wait_send()
        for s in range(seqs):
            for j in range(2):

                @pl.when(o != 2 * s + j)
                def _():
                    send_pair(s, j).wait_send()

    return Part(
        run,
        list(vars(x).values()),
        [
            ((2, he, 2 * n), BF16),
            ((3, he, length), BF16),
            ((he, length), F32),
            ((1, length), F32),
            ((seqs, r, d), F32),
            ((seqs, 8, r, d), BF16),
            ((4, four, e, wq), BF16),
            ((2,) + x.out_weight.shape, BF16),
            ((4, four, e, fh), BF16),
            ((four, e, f), BF16),
            ((10, d), F32),
            ((1, f), F32),
            ((1, blks * seqs * r), jnp.int32),
            ((seqs * r, 1), F32),
        ],
        need,
        ALL,
    )


def finish_kernel(odd, layer, hid, pos, down, up, qkv, out, totals, *outs):
    o_layer, o_hid, o_pos, o_types, o_qkv, o_out, o_up, o_down, o_upb, o_gains, o_bias = outs
    o_layer[...] = layer[...]
    o_hid[...] = hid[...]
    o_pos[...] = pos[...]
    o_qkv[...] = qkv[...].astype(F32)
    o_out[...] = out[...].astype(F32)
    o_up[...] = up[...].astype(F32)
    o_down[...] = down[...].astype(F32)
    t = totals[...]
    mine = jnp.where(odd[0] == 1, t[:, 64:], t[:, :64])
    o_types[...] = mine[6:8]
    o_gains[...] = mine[4:6]
    o_bias[0:1] = mine[8:9]
    o_bias[1:2] = mine[9:10]
    o_bias[2:6] = mine[0:4]
    o_upb[...] = t[16:18]


def finish(odd, layer, hid, pos, down, up, qkv, out, totals, steps=4):
    e = out.shape[0]
    large = [(layer, BF16), (hid, F32), (pos, F32), (qkv, F32), (out, F32), (up, F32), (down, F32)]

    def cut(a):
        return pl.BlockSpec((a.shape[0] // steps, a.shape[1]), lambda i: (i, 0))

    def whole(*shape):
        return pl.BlockSpec(shape, lambda i: (0, 0))

    like = {id(a): jax.ShapeDtypeStruct(a.shape, dtype) for a, dtype in large}
    full = lambda *shape: jax.ShapeDtypeStruct(shape, F32)
    return pl.pallas_call(
        finish_kernel,
        name="finish",
        grid=(steps,),
        out_shape=[like[id(a)] for a in (layer, hid, pos)]
        + [full(2, e)]
        + [like[id(a)] for a in (qkv, out, up, down)]
        + [full(2, 128), full(2, e), full(6, e)],
        in_specs=[pl.BlockSpec(memory_space=pltpu.SMEM)]
        + [cut(a) for a in (layer, hid, pos, down, up, qkv, out)]
        + [whole(24, 128)],
        out_specs=[cut(a) for a in (layer, hid, pos)]
        + [whole(2, e)]
        + [cut(a) for a in (qkv, out, up, down)]
        + [whole(2, 128), whole(2, e), whole(6, e)],
    )(odd, layer, hid, pos, down, up, qkv, out, totals)


def norm_layer(values_in, gain_row, offset_row):
    average = jnp.mean(values_in, axis=-1, keepdims=True)
    centred = values_in - average
    variance = jnp.mean(centred * centred, axis=-1, keepdims=True)
    return centred * lax.rsqrt(variance + 1e-12) * gain_row + offset_row


def gelu_exact(inner_product_sum):
    return jax.nn.gelu(inner_product_sum, approximate=False)


def widest_block(length, limit):
    return max(
        (candidate for candidate in range(1, min(length, limit) + 1) if length % candidate == 0)
    )


def block_scores(query_heads, key_block, score_scale):
    return (
        jnp.einsum("sqhe,skhe->shqk", query_heads, key_block, preferred_element_type=jnp.float32)
        * score_scale
    )


def key_side(query_block, grad_block, lse_block, delta_block, key_heads, value_heads, score_scale):
    scores = block_scores(query_block, key_heads, score_scale)
    weights = jnp.exp(scores - lse_block[..., None])
    more_values = jnp.einsum(
        "shqk,sqhe->shke",
        weights.astype(jnp.bfloat16),
        grad_block,
        preferred_element_type=jnp.float32,
    )
    grad_weights = jnp.einsum(
        "sqhe,skhe->shqk", grad_block, value_heads, preferred_element_type=jnp.float32
    )
    grad_scores = weights * (grad_weights - delta_block[..., None])
    more_keys = jnp.einsum(
        "shqk,sqhe->shke",
        grad_scores.astype(jnp.bfloat16),
        query_block,
        preferred_element_type=jnp.float32,
    )
    return (more_keys, more_values)


def forward_fold(query_heads, score_scale, head_count, head_size):

    def fold_keys(running, portion, offset):
        key_piece, value_piece = portion
        seq_count, length = (key_piece.shape[0], key_piece.shape[1])
        block_size = widest_block(length, 512)

        def one_step(block_index, carried):
            row_peak, row_total, weighted = carried
            row_start = block_index * block_size
            key_block = lax.dynamic_slice_in_dim(key_piece, row_start, block_size, 1).reshape(
                seq_count, block_size, head_count, head_size
            )
            value_block = lax.dynamic_slice_in_dim(value_piece, row_start, block_size, 1).reshape(
                seq_count, block_size, head_count, head_size
            )
            scores = block_scores(query_heads, key_block, score_scale)
            new_peak = jnp.maximum(row_peak, jnp.max(scores, axis=-1))
            shrink = jnp.exp(row_peak - new_peak)
            weights = jnp.exp(scores - new_peak[..., None])
            row_total = row_total * shrink + jnp.sum(weights, axis=-1)
            weighted = weighted * shrink[..., None] + jnp.einsum(
                "shqk,skhe->shqe",
                weights.astype(jnp.bfloat16),
                value_block,
                preferred_element_type=jnp.float32,
            )
            return (new_peak, row_total, weighted)

        return lax.fori_loop(0, length // block_size, one_step, running)

    return fold_keys


def query_fold(query_heads, grad_heads, log_totals, delta_rows, score_scale, head_count, head_size):

    def fold_keys(running, portion, offset):
        key_piece, value_piece = portion
        seq_count, length = (key_piece.shape[0], key_piece.shape[1])
        block_size = widest_block(length, 512)

        def one_step(block_index, weighted):
            row_start = block_index * block_size
            key_block = lax.dynamic_slice_in_dim(key_piece, row_start, block_size, 1).reshape(
                seq_count, block_size, head_count, head_size
            )
            value_block = lax.dynamic_slice_in_dim(value_piece, row_start, block_size, 1).reshape(
                seq_count, block_size, head_count, head_size
            )
            scores = block_scores(query_heads, key_block, score_scale)
            weights = jnp.exp(scores - log_totals[..., None])
            grad_weights = jnp.einsum(
                "sqhe,skhe->shqk", grad_heads, value_block, preferred_element_type=jnp.float32
            )
            grad_scores = weights * (grad_weights - delta_rows[..., None])
            return weighted + jnp.einsum(
                "shqk,skhe->shqe",
                grad_scores.astype(jnp.bfloat16),
                key_block,
                preferred_element_type=jnp.float32,
            )

        return lax.fori_loop(0, length // block_size, one_step, running)

    return fold_keys


def key_fold(key_heads, value_heads, score_scale, head_count, head_size):

    def fold_queries(running, portion, offset):
        query_piece, grad_piece, lse_piece, delta_piece = portion
        seq_count, length = (query_piece.shape[0], query_piece.shape[1])
        block_size = widest_block(length, 512)

        def one_step(block_index, carried):
            grad_keys, grad_values = carried
            row_start = block_index * block_size
            query_block = lax.dynamic_slice_in_dim(query_piece, row_start, block_size, 1).reshape(
                seq_count, block_size, head_count, head_size
            )
            grad_block = lax.dynamic_slice_in_dim(grad_piece, row_start, block_size, 1).reshape(
                seq_count, block_size, head_count, head_size
            )
            lse_block = lax.dynamic_slice_in_dim(lse_piece, row_start, block_size, 1).transpose(
                0, 2, 1
            )
            delta_block = lax.dynamic_slice_in_dim(delta_piece, row_start, block_size, 1).transpose(
                0, 2, 1
            )
            more_keys, more_values = key_side(
                query_block, grad_block, lse_block, delta_block, key_heads, value_heads, score_scale
            )
            return (grad_keys + more_keys, grad_values + more_values)

        return lax.fori_loop(0, length // block_size, one_step, running)

    return fold_queries


def layer_in_blocks(
    hidden,
    pos_ids,
    type_ids,
    cotangent,
    pos_table,
    type_table,
    query_key_value_weight,
    attention_output_weight,
    up_projection_weight,
    down_projection_weight,
    up_projection_bias,
    norm_gains,
    biases,
):
    seq_count, seg_tokens, model_width = hidden.shape
    row_count = seq_count * seg_tokens
    head_count = HEADS // lax.axis_size("head")
    head_size = model_width // HEADS
    local_width = head_count * head_size
    query_rows = lax.axis_size("head") * seg_tokens
    score_scale = 1.0 / math.sqrt(head_size)

    def fetch_weights():
        return (
            lax.all_gather(query_key_value_weight, "blk", axis=0, tiled=True),
            lax.all_gather(attention_output_weight, "blk", axis=0, tiled=True),
            lax.all_gather(up_projection_weight, "blk", axis=0, tiled=True),
            lax.all_gather(down_projection_weight, "blk", axis=0, tiled=True),
            lax.all_gather(up_projection_bias, "blk", axis=0, tiled=True),
            lax.all_gather(norm_gains, "blk", axis=1, tiled=True),
            lax.all_gather(biases, "blk", axis=1, tiled=True),
            lax.all_gather(type_table, "blk", axis=1, tiled=True),
        )

    qkv_full, out_full, up_full, down_full, up_bias_full, gain_full, bias_full, type_full = (
        fetch_weights()
    )
    bias_float = bias_full.astype(jnp.float32)
    gain_float = gain_full.astype(jnp.float32)
    flat_pos = pos_ids.reshape(row_count)
    portion = lax.all_gather(pos_table, "blk", axis=0, tiled=True)
    local_slots = flat_pos
    onehot = (
        local_slots[:, None] == jnp.arange(portion.shape[0], dtype=jnp.int32)[None, :]
    ).astype(jnp.bfloat16)
    positions = jnp.dot(onehot, portion, preferred_element_type=jnp.float32)
    is_second = type_ids.reshape(row_count, 1) == 1
    typed_rows = jnp.where(
        is_second, type_full[1].astype(jnp.float32), type_full[0].astype(jnp.float32)
    )
    embedded_tokens = (
        hidden.reshape(row_count, model_width).astype(jnp.float32) + positions + typed_rows
    )
    embedded_low = embedded_tokens.astype(jnp.bfloat16)
    projected_rows = jnp.dot(embedded_low, qkv_full, preferred_element_type=jnp.float32)
    token_shape = (seq_count, seg_tokens, model_width)
    queries = (
        (projected_rows[:, :model_width] + bias_float[0]).astype(jnp.bfloat16).reshape(token_shape)
    )
    keys_token = (
        projected_rows[:, model_width : 2 * model_width].astype(jnp.bfloat16).reshape(token_shape)
    )
    values_token = (
        (projected_rows[:, 2 * model_width :] + bias_float[1])
        .astype(jnp.bfloat16)
        .reshape(token_shape)
    )
    query_local, key_local, value_local = (
        lax.all_to_all(queries, "head", split_axis=2, concat_axis=1, tiled=True),
        lax.all_to_all(keys_token, "head", split_axis=2, concat_axis=1, tiled=True),
        lax.all_to_all(values_token, "head", split_axis=2, concat_axis=1, tiled=True),
    )
    head_shape = (seq_count, query_rows, head_count, head_size)
    query_heads = query_local.reshape(head_shape)
    key_heads = key_local.reshape(head_shape)
    value_heads = value_local.reshape(head_shape)
    start_peak = jnp.full((seq_count, head_count, query_rows), -jnp.inf, jnp.float32)
    start_total = jnp.zeros((seq_count, head_count, query_rows), jnp.float32)
    zero_heads = jnp.zeros((seq_count, head_count, query_rows, head_size), jnp.float32)
    fold_keys = forward_fold(query_heads, score_scale, head_count, head_size)
    row_peak, row_total, weighted = fold_keys(
        (start_peak, start_total, zero_heads),
        (
            lax.all_gather(key_local, "blk", axis=1, tiled=True),
            lax.all_gather(value_local, "blk", axis=1, tiled=True),
        ),
        jnp.int32(0),
    )
    log_totals = row_peak + jnp.log(row_total)
    attention_result = weighted / row_total[..., None]
    attended_low = (
        attention_result.transpose(0, 2, 1, 3)
        .reshape(seq_count, query_rows, local_width)
        .astype(jnp.bfloat16)
    )
    attended_token = lax.all_to_all(
        attended_low, "head", split_axis=1, concat_axis=2, tiled=True
    ).reshape(row_count, model_width)
    residual_branch = (
        jnp.dot(attended_token, out_full, preferred_element_type=jnp.float32) + bias_float[2]
    )
    first_layer_norm, first_pull = jax.vjp(
        norm_layer, embedded_tokens + residual_branch, gain_float[0], bias_float[3]
    )
    first_low = first_layer_norm.astype(jnp.bfloat16)
    inner_product_sum = jnp.dot(
        first_low, up_full, preferred_element_type=jnp.float32
    ) + up_bias_full.astype(jnp.float32)
    gelu_activations, gelu_pull = jax.vjp(gelu_exact, inner_product_sum)
    activated_low = gelu_activations.astype(jnp.bfloat16)
    second_layer_norm = (
        jnp.dot(activated_low, down_full, preferred_element_type=jnp.float32) + bias_float[4]
    )
    final_norm, final_pull = jax.vjp(
        norm_layer, first_layer_norm + second_layer_norm, gain_float[1], bias_float[5]
    )
    layer_out = final_norm.astype(jnp.bfloat16).reshape(token_shape)
    qkv_full, out_full, up_full, down_full, up_bias_full, gain_full, bias_full, type_full = (
        fetch_weights()
    )
    grad_final, grad_gain_two, grad_shift_two = final_pull(
        cotangent.reshape(row_count, model_width).astype(jnp.float32)
    )
    grad_second = grad_final.astype(jnp.bfloat16)
    grad_down = jnp.einsum(
        "rf,rd->fd", activated_low, grad_second, preferred_element_type=jnp.float32
    )
    grad_bias_second = jnp.sum(grad_second.astype(jnp.float32), axis=0)
    (grad_inner,) = gelu_pull(
        jnp.einsum("rd,fd->rf", grad_second, down_full, preferred_element_type=jnp.float32)
    )
    grad_inner_low = grad_inner.astype(jnp.bfloat16)
    grad_up = jnp.einsum("rd,rf->df", first_low, grad_inner_low, preferred_element_type=jnp.float32)
    grad_up_bias = jnp.sum(grad_inner_low.astype(jnp.float32), axis=0)
    grad_first = grad_final + jnp.einsum(
        "rf,df->rd", grad_inner_low, up_full, preferred_element_type=jnp.float32
    )
    grad_resid, grad_gain_one, grad_shift_one = first_pull(grad_first)
    grad_branch = grad_resid.astype(jnp.bfloat16)
    grad_out = jnp.einsum(
        "re,rd->ed", attended_token, grad_branch, preferred_element_type=jnp.float32
    )
    grad_bias_branch = jnp.sum(grad_branch.astype(jnp.float32), axis=0)
    grad_attended = (
        jnp.einsum("rd,ed->re", grad_branch, out_full, preferred_element_type=jnp.float32)
        .astype(jnp.bfloat16)
        .reshape(token_shape)
    )
    grad_local = lax.all_to_all(grad_attended, "head", split_axis=2, concat_axis=1, tiled=True)
    grad_heads = grad_local.reshape(head_shape)
    delta_rows = jnp.sum(
        grad_heads.astype(jnp.float32).transpose(0, 2, 1, 3) * attention_result, axis=-1
    )
    fold_queries = query_fold(
        query_heads, grad_heads, log_totals, delta_rows, score_scale, head_count, head_size
    )
    grad_query_sum = fold_queries(
        zero_heads,
        (
            lax.all_gather(key_local, "blk", axis=1, tiled=True),
            lax.all_gather(value_local, "blk", axis=1, tiled=True),
        ),
        jnp.int32(0),
    )
    fold_side = key_fold(key_heads, value_heads, score_scale, head_count, head_size)
    grad_key_sum, grad_value_sum = fold_side(
        (zero_heads, zero_heads),
        (
            lax.all_gather(query_local.astype(jnp.float32), "blk", axis=1, tiled=True).astype(
                jnp.bfloat16
            ),
            lax.all_gather(grad_local.astype(jnp.float32), "blk", axis=1, tiled=True).astype(
                jnp.bfloat16
            ),
            lax.all_gather(log_totals.transpose(0, 2, 1), "blk", axis=1, tiled=True),
            lax.all_gather(delta_rows.transpose(0, 2, 1), "blk", axis=1, tiled=True),
        ),
        jnp.int32(0),
    )
    grad_keys_local = (
        (grad_key_sum * score_scale)
        .transpose(0, 2, 1, 3)
        .reshape(seq_count, query_rows, local_width)
        .astype(jnp.bfloat16)
    )
    grad_values_local = (
        grad_value_sum.transpose(0, 2, 1, 3)
        .reshape(seq_count, query_rows, local_width)
        .astype(jnp.bfloat16)
    )
    grad_query_local = (
        (grad_query_sum * score_scale)
        .transpose(0, 2, 1, 3)
        .reshape(seq_count, query_rows, local_width)
        .astype(jnp.bfloat16)
    )
    grad_query_token, grad_key_token, grad_value_token = (
        lax.all_to_all(grad_query_local, "head", split_axis=1, concat_axis=2, tiled=True),
        lax.all_to_all(grad_keys_local, "head", split_axis=1, concat_axis=2, tiled=True),
        lax.all_to_all(grad_values_local, "head", split_axis=1, concat_axis=2, tiled=True),
    )
    grad_qkv = jnp.concatenate(
        [grad_query_token, grad_key_token, grad_value_token], axis=-1
    ).reshape(row_count, 3 * model_width)
    grad_qkv_full = jnp.einsum(
        "rd,rf->df", embedded_low, grad_qkv, preferred_element_type=jnp.float32
    )
    grad_bias_query = jnp.sum(
        grad_query_token.astype(jnp.float32).reshape(row_count, model_width), axis=0
    )
    grad_bias_value = jnp.sum(
        grad_value_token.astype(jnp.float32).reshape(row_count, model_width), axis=0
    )
    grad_embedded = grad_resid + jnp.einsum(
        "rf,df->rd", grad_qkv, qkv_full, preferred_element_type=jnp.float32
    )
    second_mask = is_second.astype(jnp.float32)
    grad_type_one = jnp.sum(grad_embedded * second_mask, axis=0)
    grad_type_zero = jnp.sum(grad_embedded * (1.0 - second_mask), axis=0)
    length = lax.axis_size("blk") * pos_table.shape[0]
    local_slots = flat_pos
    inside = (local_slots >= 0) & (local_slots < length)
    slot_index = jnp.where(inside, local_slots, length)
    buffer = jnp.zeros((length + 1, model_width), jnp.float32).at[slot_index].add(grad_embedded)
    grad_positions = lax.psum_scatter(buffer[:length], "blk", scatter_dimension=0, tiled=True)
    gain_stack = jnp.stack([grad_gain_one, grad_gain_two])
    bias_stack = jnp.stack(
        [
            grad_bias_query,
            grad_bias_value,
            grad_bias_branch,
            grad_shift_one,
            grad_bias_second,
            grad_shift_two,
        ]
    )
    type_stack = jnp.stack([grad_type_zero, grad_type_one])
    (
        shard_qkv,
        shard_out,
        shard_up,
        shard_down,
        shard_up_bias,
        shard_gains,
        shard_biases,
        shard_types,
    ) = (
        lax.psum_scatter(grad_qkv_full, "blk", scatter_dimension=0, tiled=True),
        lax.psum_scatter(grad_out, "blk", scatter_dimension=0, tiled=True),
        lax.psum_scatter(grad_up, "blk", scatter_dimension=0, tiled=True),
        lax.psum_scatter(grad_down, "blk", scatter_dimension=0, tiled=True),
        lax.psum_scatter(grad_up_bias, "blk", scatter_dimension=0, tiled=True),
        lax.psum_scatter(gain_stack, "blk", scatter_dimension=1, tiled=True),
        lax.psum_scatter(bias_stack, "blk", scatter_dimension=1, tiled=True),
        lax.psum_scatter(type_stack, "blk", scatter_dimension=1, tiled=True),
    )
    (
        total_qkv,
        total_out,
        total_up,
        total_down,
        total_up_bias,
        total_gains,
        total_biases,
        total_types,
        total_positions,
    ) = lax.psum(
        (
            shard_qkv,
            shard_out,
            shard_up,
            shard_down,
            shard_up_bias,
            shard_gains,
            shard_biases,
            shard_types,
            grad_positions,
        ),
        "head",
    )
    grad_hidden = grad_embedded.reshape(token_shape)
    return (
        layer_out,
        grad_hidden,
        total_positions,
        total_types,
        total_qkv,
        total_out,
        total_up,
        total_down,
        total_up_bias,
        total_gains,
        total_biases,
    )


BIG = 56 << 20
WHOLE = 67043328
LAG = 1
CHUNKS = 4
CHUNK_LAG = 1
QKV_TURNS = (1, 3, 5)
UP_TURNS = (8, 9, 10)
EARLY = (1, 3)
TURNS = ((1, 3), (3, 5, 8, 11), (10, 14))


def layer_in_planes(
    hidden,
    pos_ids,
    type_ids,
    cotangent,
    pos_table,
    type_table,
    query_key_value_weight,
    attention_output_weight,
    up_projection_weight,
    down_projection_weight,
    up_projection_bias,
    norm_gains,
    biases,
):
    seqs, seg, width = hidden.shape
    b = lax.axis_index("blk")
    rows = seqs * seg
    e = width // HEADS
    scale = 1.0 / math.sqrt(e)
    slots = pos_table.shape[0]
    fcols = down_projection_weight.shape[0] // 2

    token_shape = (seqs, seg, width)
    begin = SimpleNamespace(
        biases=biases,
        gains=norm_gains,
        types=type_table,
        up_bias=up_projection_bias.reshape(2, 2 * e),
        pos_ids=pos_ids,
        type_ids=type_ids,
        qkv_weight=query_key_value_weight,
        out_weight=attention_output_weight,
        up_weight=up_projection_weight,
        table=pos_table,
        hidden=hidden,
    )
    (
        (
            attended,
            held,
            pair_out,
            lse,
            embedded,
            plane_low,
            qkv_own,
            out_own,
            up_one,
            up_cut,
            vectors,
            up_bias,
            pos_all,
            is_second,
        ),
    ) = fused("first_half", 0, [first_half(begin, scale, LAG)], WHOLE)
    parts = SimpleNamespace(
        attended=attended,
        out_own=out_own.reshape(2 * e, width),
        embedded=embedded,
        cotangent=cotangent,
        up_one=up_one,
        up_cut=up_cut,
        down_weight=down_projection_weight,
        up_bias=up_bias,
        vectors=vectors,
        held=held,
        pair_out=pair_out,
        lse=lse,
        qkv_own=qkv_own.reshape(width, 6 * e),
        plane_low=plane_low,
        ids=pos_all,
        second=is_second,
    )
    sizes = (slots, CHUNKS, CHUNK_LAG, scale)
    ((layer_out, grad_hidden, pos, down, up, qkv, out, totals),) = fused(
        "second_half", 4, [second_half(parts, sizes)], WHOLE
    )
    outs = finish(
        (b % 2).reshape(1),
        layer_out.reshape(rows, width),
        grad_hidden.reshape(rows, width),
        pos,
        down.reshape(2 * fcols, width),
        up,
        qkv,
        out,
        totals,
    )
    return (
        outs[0].reshape(token_shape),
        outs[1].reshape(token_shape),
        *outs[2:8],
        outs[8].reshape(4 * e),
        *outs[9:],
    )


def planes_fit(hidden, head_axis, blk_axis):
    seqs, seg, width = hidden.shape
    return head_axis == 2 and blk_axis == HEADS and seqs == 2 and seqs * seg == 2 * width // HEADS


def on_device(hidden, *rest):
    if planes_fit(hidden, lax.axis_size("head"), lax.axis_size("blk")):
        return layer_in_planes(hidden, *rest)
    return layer_in_blocks(hidden, *rest)


def solution(mesh):
    in_specs = (
        P(None, ("head", "blk"), None),
        P(None, ("head", "blk")),
        P(None, ("head", "blk")),
        P(None, ("head", "blk"), None),
        P("blk", None),
        P(None, "blk"),
        P("blk", None),
        P("blk", None),
        P("blk", None),
        P("blk", None),
        P("blk"),
        P(None, "blk"),
        P(None, "blk"),
    )
    out_specs = (
        P(None, ("head", "blk"), None),
        P(None, ("head", "blk"), None),
        P("blk", None),
        P(None, "blk"),
        P("blk", None),
        P("blk", None),
        P("blk", None),
        P("blk", None),
        P("blk"),
        P(None, "blk"),
        P(None, "blk"),
    )
    return jax.shard_map(
        on_device, mesh=mesh, in_specs=in_specs, out_specs=out_specs, check_vma=False
    )
```
